32 devices in a mesh: fsdp: 32 (over z, y, x, core).
Axes of the slice: x: 2, y: 2, z: 4, core: 2. Of those that a mesh axis runs over, the one named last changes fastest.
Arguments:
- tokens: bfloat16 [8192, 2048], P('fsdp'), may hold values from -6 to 6
- lengths: int32 [32, 3], P('fsdp'), may hold values from 1 to 128, 256 in all within a row
- ln1_gain: bfloat16 [2048], P('fsdp'), may hold values from 0.5 to 1.5
- ln1_bias: bfloat16 [2048], P('fsdp'), may hold values from -3 to 3
- w_query: bfloat16 [2048, 2048], P('fsdp'), may hold values from -0.125 to 0.125
- w_key: bfloat16 [2048, 2048], P('fsdp'), may hold values from -0.125 to 0.125
- w_value: bfloat16 [2048, 4096], P('fsdp'), may hold values from -0.125 to 0.125
- w_swish: bfloat16 [2048, 4096], P('fsdp'), may hold values from -0.125 to 0.125
- w_out: bfloat16 [4096, 2048], P('fsdp'), may hold values from -0.125 to 0.125
- ln2_gain: bfloat16 [2048], P('fsdp'), may hold values from 0.5 to 1.5
- ln2_bias: bfloat16 [2048], P('fsdp'), may hold values from -3 to 3
- w_gate: bfloat16 [2048, 4096], P('fsdp'), may hold values from -0.125 to 0.125
- w_up: bfloat16 [2048, 4096], P('fsdp'), may hold values from -0.125 to 0.125
- w_down: bfloat16 [4096, 2048], P('fsdp'), may hold values from -0.09375 to 0.09375
- cotangent: bfloat16 [8192, 2048], P('fsdp'), may hold values from -6 to 6
Outputs:
- layer_out: bfloat16 [8192, 2048], P('fsdp')
- grad_tokens: float32 [8192, 2048], P('fsdp')
- grad_ln1_gain: float32 [2048], P('fsdp')
- grad_ln1_bias: float32 [2048], P('fsdp')
- grad_query: float32 [2048, 2048], P('fsdp')
- grad_key: float32 [2048, 2048], P('fsdp')
- grad_value: float32 [2048, 4096], P('fsdp')
- grad_swish: float32 [2048, 4096], P('fsdp')
- grad_out: float32 [4096, 2048], P('fsdp')
- grad_ln2_gain: float32 [2048], P('fsdp')
- grad_ln2_bias: float32 [2048], P('fsdp')
- grad_gate: float32 [2048, 4096], P('fsdp')
- grad_up: float32 [2048, 4096], P('fsdp')
- grad_down: float32 [4096, 2048], P('fsdp')
The draws below stay inside these ranges and needn't reach their ends.
Inputs may be any that keep to these rules, and one draw needn't show every extreme that they name: Each device's row of lengths sums to 256, and its largest entry is exactly 128.
All inputs are finite; a program needn't handle non-finite values.
Results may differ from the reference program's by a relative error of at most 0.015.
The reference program's roundings to bfloat16 on the way (of `normed`, `scores`, `mixed` and `hidden`) count: a program that leaves them out, or rounds other values in their place, can miss the bound.
Values may be sent and summed in bfloat16 or wider, within the bound.
A program may use at most 512 MiB of HBM per device.

```python
import functools
import math
import jax
import jax.numpy as jnp
import numpy as np
from jax import lax

D = 2048
HEADS = 8
KH = 256
VH = 512
FF = 4096
TOK_DEV = 256
NSEQ = 3
LONGEST = 128
KD = 2048
VD = 4096
TOKENS = 8192
N_FSDP = 32


def with_spikes(entries, own_key, source, target, blocks, factor):
    owner, partner = [(jnp.arange(entries.shape[dim]) // (entries.shape[dim] // blocks)).reshape([-1 if axis == dim else 1 for axis in range(entries.ndim)]) for dim in (source, target)]
    chosen = jax.random.permutation(own_key, blocks)[partner]
    strong = (owner == chosen) | (owner == (partner + blocks // 2) % blocks)
    return jnp.where(strong, factor * entries, entries)


def level_of(own_key, extent, cuts, least, top_value):
    def one(position, parts):
        heights = jax.random.uniform(jax.random.fold_in(jax.random.fold_in(own_key, 6), position), (parts,), jnp.float32, least / len(cuts), top_value / len(cuts))
        return jnp.repeat(jnp.exp(heights), extent[position] // parts).reshape((-1,) + (1,) * (len(extent) - position - 1))

    level = one(*cuts[0])
    for cut in cuts[1:]:
        level = level * one(*cut)
    return level


def split_up(number_of, total, reach, slope):
    portions = [(1 << 20) // math.isqrt(rank ** slope) + 1 for rank in range(2, number_of + 1)]
    surplus, holding = total - reach - (number_of - 1), [1] * (number_of - 1)
    while surplus > 0:
        free = [i for i in range(number_of - 1) if holding[i] < reach]
        pool, left = sum([portions[i] for i in free]), surplus
        for i in free:
            more = min(reach - holding[i], max(1, left * portions[i] // pool), surplus)
            holding[i] = holding[i] + more
            surplus = surplus - more
    return np.array([reach] + holding)


def ragged(own_key, number_of, total, reach, lean):
    if number_of == 2:
        one = jax.random.randint(own_key, (), max(1, total - reach), min(reach, total - 1) + 1)
        return jnp.stack([one, total - one])
    tallies = jnp.asarray(split_up(number_of, total, reach, lean), jnp.int32)
    pairs = (number_of - 1) // 2
    source_of, taker = tallies[1:1 + 2 * pairs:2], tallies[2:2 + 2 * pairs:2]
    slack = jnp.minimum(source_of - 1, reach - taker)
    passed = jax.random.randint(jax.random.fold_in(own_key, 1), (pairs,), 0, 1 << 20) % (slack + 1)
    tallies = tallies.at[1:1 + 2 * pairs:2].set(source_of - passed).at[2:2 + 2 * pairs:2].set(taker + passed)
    return tallies[jax.random.permutation(jax.random.fold_in(own_key, 2), number_of)]


def normal_values(stream_key, shape, scale, reach, cuts=(), held_as=jnp.bfloat16):
    loudness = level_of(stream_key, shape, cuts, -0.22, 0.18) if cuts else 1.0
    values = jax.random.normal(stream_key, shape, jnp.float32) * scale * loudness
    return jnp.minimum(jnp.maximum(values, -reach), reach).astype(held_as)


def heavy_noise(key, dims, scale, reach, shards, heavy, held_as=jnp.bfloat16):
    array = scale * jax.random.normal(key, dims, jnp.float32)
    if shards:
        array = array * level_of(key, dims, shards, -0.22, 0.18)
    return jnp.clip(with_spikes(array, jax.random.fold_in(key, 3), *heavy), -reach, reach).astype(held_as)


def setup_inputs(seed: int = 0) -> dict:
    streams_of = jax.random.split(jax.random.key(seed), 16)
    return {
        "tokens": heavy_noise(streams_of[0], (TOKENS, D), 1.0, 6.0, ((0, 32),), (0, 1, 32, 2.75)),
        "lengths": jax.vmap(lambda own: ragged(own, NSEQ, TOK_DEV, LONGEST, 2))(jax.random.split(streams_of[1], N_FSDP)).reshape((N_FSDP, NSEQ)).astype(jnp.int32),
        "ln1_gain": jnp.clip(1.0 + 0.1 * jax.random.normal(streams_of[2], (D,), jnp.float32), 0.5, 1.5).astype(jnp.bfloat16),
        "ln1_bias": normal_values(streams_of[3], (D,), 0.5, 3.0, ((0, 32),)),
        "w_query": normal_values(streams_of[4], (D, KD), D ** -0.5, 0.125, ((0, 32),)),
        "w_key": normal_values(streams_of[5], (D, KD), D ** -0.5, 0.125, ((0, 32),)),
        "w_value": normal_values(streams_of[6], (D, VD), D ** -0.5, 0.125, ((0, 32),)),
        "w_swish": normal_values(streams_of[7], (D, VD), D ** -0.5, 0.125, ((0, 32),)),
        "w_out": normal_values(streams_of[8], (VD, D), (VD // 2) ** -0.5, 0.125, ((0, 32),)),
        "ln2_gain": jnp.clip(1.0 + 0.1 * jax.random.normal(streams_of[9], (D,), jnp.float32), 0.5, 1.5).astype(jnp.bfloat16),
        "ln2_bias": normal_values(streams_of[10], (D,), 0.5, 3.0, ((0, 32),)),
        "w_gate": normal_values(streams_of[11], (D, FF), D ** -0.5, 0.125, ((0, 32),)),
        "w_up": normal_values(streams_of[12], (D, FF), D ** -0.5, 0.125, ((0, 32),)),
        "w_down": normal_values(streams_of[13], (FF, D), FF ** -0.5, 0.09375, ((0, 32),)),
        "cotangent": normal_values(streams_of[14], (TOKENS, D), 1.0, 6.0, ((0, 32),)),
    }


@jax.custom_vjp
def low(v):
    return lax.optimization_barrier(v.astype(jnp.bfloat16)).astype(jnp.float32)

@jax.custom_vjp
def low_back(v):
    return v

def low_keep(v):
    return (low(v), None)

def low_pass(kept, grad):
    return (grad,)

def back_keep(v):
    return (v, None)

def back_low(kept, grad):
    return (low(grad),)
low.defvjp(low_keep, low_pass)
low_back.defvjp(back_keep, back_low)

def layer_norm(value, gain, bias):
    center = lax.optimization_barrier(jnp.mean(value, axis=-1, keepdims=True))
    centred = value - center
    spread = lax.optimization_barrier(jnp.mean(centred * centred, axis=-1, keepdims=True))
    return centred * lax.rsqrt(spread + 1e-05) * gain + bias

def decay_logs(heads):
    steps = jnp.arange(heads, dtype=jnp.float32)
    return jnp.log(1.0 - jnp.exp2(-5.0 - steps))

def seq_positions(lengths, rows):
    ends = jnp.cumsum(lengths).astype(jnp.int32)
    starts = ends - lengths
    index = jnp.arange(rows, dtype=jnp.int32)
    segment = lax.optimization_barrier(jnp.sum((index[:, None] >= ends[None, :]).astype(jnp.int32), axis=1))
    member = segment[:, None] == jnp.arange(lengths.shape[0], dtype=jnp.int32)[None, :]
    offset = index - lax.optimization_barrier(jnp.sum(jnp.where(member, starts[None, :], 0), axis=1))
    return (segment, offset)

def rotary_tables(offset, width):
    half = width // 2
    freq = jnp.exp(-math.log(10000.0) * jnp.arange(half, dtype=jnp.float32) / half)
    angle = offset.astype(jnp.float32)[:, None] * freq[None, :]
    return (jnp.cos(angle), jnp.sin(angle))

def rotate(value, cosine, sine):
    half = value.shape[-1] // 2
    first = value[..., :half]
    second = value[..., half:]
    cosine = cosine[:, None, :]
    sine = sine[:, None, :]
    return jnp.concatenate([first * cosine - second * sine, second * cosine + first * sine], axis=-1)

def decay_mask(segment, offset, heads, width):
    diff = offset[:, None] - offset[None, :]
    valid = (segment[:, None] == segment[None, :]) & (diff >= 0)
    steps = jnp.where(valid, diff, 0).astype(jnp.float32)
    logs = decay_logs(heads)
    weight = jnp.exp(logs[:, None, None] * steps[None, :, :])
    return jnp.where(valid[None, :, :], weight, 0.0) / math.sqrt(width)

def group_gate(retained, swish_in):
    center = lax.optimization_barrier(jnp.mean(retained, axis=-1, keepdims=True))
    centred = retained - center
    spread = lax.optimization_barrier(jnp.mean(centred * centred, axis=-1, keepdims=True))
    normed = (centred * lax.rsqrt(jnp.maximum(spread, 0.25))).reshape(swish_in.shape)
    return jax.nn.silu(swish_in) * normed

def mlp_gate(first, second):
    return jax.nn.gelu(first, approximate=False) * second

def retain_block(items):
    query, key, value, segment, offset = items
    mask = decay_mask(segment, offset, query.shape[1], query.shape[2])
    plain = jnp.einsum('thd,shd->hts', query, key, precision=lax.Precision.HIGHEST)
    scores = low(low_back(plain) * mask)
    return low_back(jnp.einsum('hts,shd->thd', scores, value, precision=lax.Precision.HIGHEST))

def reference(tokens, lengths, ln1_gain, ln1_bias, w_query, w_key, w_value, w_swish, w_out, ln2_gain, ln2_bias, w_gate, w_up, w_down, cotangent):
    high = lax.Precision.HIGHEST
    segment, offset = jax.vmap(functools.partial(seq_positions, rows=TOK_DEV))(lengths)
    cosine, sine = rotary_tables(offset.reshape(-1), KH)

    def forward(inputs, gain1, bias1, wq, wk, wv, ws, wo, gain2, bias2, wg, wu, wd):
        normed = low(layer_norm(inputs, gain1, bias1))
        query = low_back(jnp.dot(normed, wq, precision=high))
        key = low_back(jnp.dot(normed, wk, precision=high))
        value = low_back(jnp.dot(normed, wv, precision=high))
        swish_in = low_back(jnp.dot(normed, ws, precision=high))
        q_rot = low(rotate(query.reshape(-1, HEADS, KH), cosine, sine))
        k_rot = low(rotate(key.reshape(-1, HEADS, KH), cosine, sine))
        v_low = low(value.reshape(-1, HEADS, VH))
        retained = lax.map(jax.checkpoint(retain_block), (q_rot.reshape(N_FSDP, TOK_DEV, HEADS, KH), k_rot.reshape(N_FSDP, TOK_DEV, HEADS, KH), v_low.reshape(N_FSDP, TOK_DEV, HEADS, VH), segment, offset)).reshape(-1, HEADS, VH)
        mixed = low(group_gate(retained, swish_in))
        middle = inputs + low_back(jnp.dot(mixed, wo, precision=high))
        normed2 = low(layer_norm(middle, gain2, bias2))
        first = low_back(jnp.dot(normed2, wg, precision=high))
        second = low_back(jnp.dot(normed2, wu, precision=high))
        hidden = low(mlp_gate(first, second))
        return middle + low_back(jnp.dot(hidden, wd, precision=high))
    params = (ln1_gain, ln1_bias, w_query, w_key, w_value, w_swish, w_out, ln2_gain, ln2_bias, w_gate, w_up, w_down)
    params = tuple((p.astype(jnp.float32) for p in params))
    result, pull = jax.vjp(forward, tokens.astype(jnp.float32), *params)
    grads = pull(cotangent.astype(jnp.float32))
    return (result.astype(jnp.bfloat16), grads[0], grads[1], grads[2], grads[3], grads[4], grads[5], grads[6], grads[7], grads[8], grads[9], grads[10], grads[11], grads[12])
```

```python
import math

import jax
import jax.numpy as jnp
from jax import lax
from jax.sharding import PartitionSpec as P

HEADS = 8
KH = 256
VH = 512
TP = 8
AXIS = "fsdp"
bf = jnp.bfloat16
f32 = jnp.float32


def tp_groups(n):
    return [[g * TP + t for t in range(TP)] for g in range(n // TP)]


def dp_groups(n):
    return [[g * TP + t for g in range(n // TP)] for t in range(TP)]


def swap(x, n, bit):
    return lax.ppermute(x, AXIS, [(i, i ^ bit) for i in range(n)])


def plane_gather(x, n):
    half = x.shape[1] // 2
    a = swap(x, n, 2)
    b = swap(x, n, 4)
    d = jnp.concatenate([swap(b[:, :half], n, 2), swap(a[:, half:], n, 4)], axis=1)
    even = jnp.concatenate([x, a, b, d], axis=0)
    odd = swap(even, n, 1)
    return jnp.concatenate([even, odd], axis=0)


def plane_reduce(partial, n):
    rows = partial.shape[0] // TP
    half = partial.shape[1] // 2
    got = swap(partial[4 * rows :], n, 1)
    s = partial[: 4 * rows].astype(f32) + got.astype(f32)
    s = s.reshape(4, rows, 2 * half)
    left, right = s[:, :, :half], s[:, :, half:]
    lx = swap(left[1::2].astype(bf), n, 2)
    ry = swap(right[2:].astype(bf), n, 4)
    left = left[0::2] + lx.astype(f32)
    right = right[:2] + ry.astype(f32)
    ly = swap(left[1].astype(bf), n, 4)
    rx = swap(right[1].astype(bf), n, 2)
    return jnp.concatenate([left[0] + ly.astype(f32), right[0] + rx.astype(f32)], axis=1)


def plane_a2a(x, n):
    return lax.all_to_all(x, AXIS, 0, 0, axis_index_groups=tp_groups(n), tiled=True)


def dp_gather(x, n):
    return lax.all_gather(x, AXIS, axis=0, tiled=True, axis_index_groups=dp_groups(n))


def dp_reduce(x, n):
    return lax.psum_scatter(
        x, AXIS, scatter_dimension=0, tiled=True, axis_index_groups=dp_groups(n)
    )


def norm_parts(value):
    center = jnp.mean(value, axis=-1, keepdims=True)
    centred = value - center
    spread = jnp.mean(centred * centred, axis=-1, keepdims=True)
    return centred, lax.rsqrt(spread + 1e-05)


def layer_norm(value, gain, bias):
    centred, inv = norm_parts(value)
    return centred * inv * gain + bias


def seq_positions(lengths, rows):
    ends = jnp.cumsum(lengths, axis=1)
    starts = ends - lengths
    index = jnp.arange(rows, dtype=jnp.int32)
    segment = jnp.sum((index[None, :, None] >= ends[:, None, :]).astype(jnp.int32), axis=2)
    member = segment[:, :, None] == jnp.arange(lengths.shape[1], dtype=jnp.int32)
    offset = index[None, :] - jnp.sum(jnp.where(member, starts[:, None, :], 0), axis=2)
    return segment, offset


def rotary_tables(offset):
    half = KH // 2
    freq = jnp.exp(-math.log(10000.0) * jnp.arange(half, dtype=f32) / half)
    angle = offset.astype(f32)[..., None] * freq
    return jnp.cos(angle), jnp.sin(angle)


def rotate(value, cosine, sine):
    half = KH // 2
    u, w = value[..., :half], value[..., half:]
    return jnp.concatenate([u * cosine - w * sine, w * cosine + u * sine], axis=-1)


def rotate_back(value, cosine, sine):
    half = KH // 2
    u, w = value[..., :half], value[..., half:]
    return jnp.concatenate([u * cosine + w * sine, w * cosine - u * sine], axis=-1)


def decay_mask(segment, offset, head):
    diff = offset[:, :, None] - offset[:, None, :]
    valid = (segment[:, :, None] == segment[:, None, :]) & (diff >= 0)
    steps = jnp.where(valid, diff, 0).astype(f32)
    log = jnp.log(1.0 - jnp.exp2(-5.0 - head.astype(f32)))
    return jnp.where(valid, jnp.exp(log * steps), 0.0) / math.sqrt(KH)


def group_gate(retained, swish_in):
    center = jnp.mean(retained, axis=-1, keepdims=True)
    centred = retained - center
    spread = jnp.mean(centred * centred, axis=-1, keepdims=True)
    return jax.nn.silu(swish_in) * (centred * lax.rsqrt(jnp.maximum(spread, 0.25)))


def mlp_gate(first, second):
    return jax.nn.gelu(first, approximate=False) * second


def dot(a, b):
    return lax.dot_general(a, b, (((1,), (0,)), ((), ())), preferred_element_type=f32)


def dot_tn(a, b):
    return lax.dot_general(a, b, (((0,), (0,)), ((), ())), preferred_element_type=f32)


def dot_nt(a, b):
    return lax.dot_general(a, b, (((1,), (1,)), ((), ())), preferred_element_type=f32)


def bmm(eq, a, b):
    return jnp.einsum(eq, a, b, preferred_element_type=f32)


def col_blocks(w):
    r, c = w.shape
    return w.reshape(r, TP, c // TP).transpose(1, 0, 2).reshape(TP * r, c // TP)


def col_join(w, r):
    c = w.shape[1]
    return w.reshape(TP, r, c).transpose(1, 0, 2).reshape(r, TP * c)


def on_device(n, tokens, lengths, gain1, bias1, wq, wk, wv, ws, wo, gain2, bias2, wg, wu, wd, cot):
    rows, d = tokens.shape
    ff = wg.shape[1]
    dp = n // TP
    shard = d // n
    unit = ff // n
    head = lax.rem(lax.axis_index(AXIS), TP)

    def ff_blocks(w):
        return (
            w.reshape(shard, dp, TP, unit).transpose(2, 0, 1, 3).reshape(TP * shard, dp * unit)
        )

    def ff_join(w):
        return w.reshape(TP, shard, dp, unit).transpose(1, 2, 0, 3).reshape(shard, ff)

    vecs = jnp.stack([gain1, bias1, gain2, bias2])
    vecs = lax.all_gather(vecs, AXIS, axis=1, tiled=True).astype(f32)
    gain1f, bias1f, gain2f, bias2f = vecs[0], vecs[1], vecs[2], vecs[3]
    qk = plane_a2a(jnp.concatenate([col_blocks(wq), col_blocks(wk)], axis=1), n)
    qk = dp_gather(qk, n)
    val = dp_gather(plane_a2a(col_blocks(wv), n), n)
    out = dp_gather(plane_a2a(col_blocks(wo), n), n)
    out = col_join(plane_a2a(out, n), VH)
    swi = dp_gather(plane_a2a(col_blocks(ws), n), n)
    gu = dp_gather(plane_a2a(jnp.concatenate([ff_blocks(wg), ff_blocks(wu)], axis=1), n), n)
    down = dp_gather(wd, n)

    tok_all = plane_gather(tokens, n)
    cot_all = plane_gather(cot, n)
    len_even = jnp.concatenate([lengths, swap(lengths, n, 2), swap(lengths, n, 4), swap(swap(lengths, n, 2), n, 4)], axis=0)
    len_all = jnp.concatenate([len_even, swap(len_even, n, 1)], axis=0)

    segment, offset = seq_positions(len_all, rows)
    cosine, sine = rotary_tables(offset)
    mask = decay_mask(segment, offset, head)

    centred1, inv1 = norm_parts(tok_all.astype(f32))
    normed = (centred1 * inv1 * gain1f + bias1f).astype(bf)
    qk_out = dot(normed, qk).reshape(TP, rows, 2 * KH)
    query, key = qk_out[..., :KH], qk_out[..., KH:]
    v_low = dot(normed, val).reshape(TP, rows, VH).astype(bf)
    swish_in = dot(normed, swi).reshape(TP, rows, VH)
    q_rot = rotate(query, cosine, sine).astype(bf)
    k_rot = rotate(key, cosine, sine).astype(bf)
    plain = bmm("btd,bsd->bts", q_rot, k_rot)
    scores = (plain * mask).astype(bf)
    retained = bmm("bts,bsd->btd", scores, v_low)
    mixed = group_gate(retained, swish_in).astype(bf).reshape(TP * rows, VH)
    inputs = tokens.astype(f32)
    middle = inputs + plane_reduce(dot(mixed, out).astype(bf), n)
    normed2_own = layer_norm(middle, gain2f, bias2f).astype(bf)
    normed2 = plane_gather(normed2_own, n)
    fs = dot(normed2, gu)
    first, second = fs[:, : dp * unit], fs[:, dp * unit :]
    hidden = mlp_gate(first, second).astype(bf)
    layer_out = (middle + plane_reduce(dot(hidden, down).astype(bf), n)).astype(bf)

    g_down = dp_reduce(dot_tn(hidden, cot_all).astype(bf), n)
    g_hidden = dot_nt(cot_all, down)
    _, pull_gate = jax.vjp(mlp_gate, first, second)
    g_first, g_second = pull_gate(g_hidden)
    g_fs = jnp.concatenate([g_first.astype(bf), g_second.astype(bf)], axis=1)
    g_gu = dp_reduce(dot_tn(normed2, g_fs).astype(bf), n)
    g_normed2 = plane_reduce(dot_nt(g_fs, gu).astype(bf), n)
    _, pull_norm2 = jax.vjp(layer_norm, middle, gain2f, bias2f)
    g_mid_part, g_gain2, g_bias2 = pull_norm2(g_normed2)
    g_middle = cot.astype(f32) + g_mid_part

    g_low = plane_gather(g_middle.astype(bf), n)
    g_out = dot_tn(mixed, g_low).astype(bf)
    g_out = dp_reduce(plane_a2a(col_blocks(g_out), n), n)
    g_mixed = dot_nt(g_low, out).reshape(TP, rows, VH)
    _, pull_group = jax.vjp(group_gate, retained, swish_in)
    g_retained, g_swish = pull_group(g_mixed)
    g_retained = g_retained.astype(bf)
    g_swish = g_swish.astype(bf)
    g_value = bmm("bts,btd->bsd", scores, g_retained).astype(bf)
    g_scores = bmm("btd,bsd->bts", g_retained, v_low)
    g_plain = (g_scores * mask).astype(bf)
    g_qrot = bmm("bts,bsd->btd", g_plain, k_rot)
    g_krot = bmm("bts,btd->bsd", g_plain, q_rot)
    g_query = rotate_back(g_qrot, cosine, sine).astype(bf)
    g_key = rotate_back(g_krot, cosine, sine).astype(bf)
    g_qkvs = jnp.concatenate([g_query, g_key, g_value, g_swish], axis=2)
    g_qkvs = g_qkvs.reshape(TP * rows, 2 * KH + 2 * VH)
    w_qkvs = jnp.concatenate([qk, val, swi], axis=1)
    grad_qkvs = dp_reduce(dot_tn(normed, g_qkvs).astype(bf), n)
    g_normed = plane_reduce(dot_nt(g_qkvs, w_qkvs).astype(bf), n)
    _, pull_norm1 = jax.vjp(layer_norm, inputs, gain1f, bias1f)
    g_in_part, g_gain1, g_bias1 = pull_norm1(g_normed)
    grad_tokens = g_middle + g_in_part

    g_vecs = lax.psum_scatter(
        jnp.stack([g_gain1, g_bias1, g_gain2, g_bias2]), AXIS, scatter_dimension=1, tiled=True
    )
    grad_qkvs = plane_a2a(grad_qkvs, n).astype(f32)
    grad_q = col_join(grad_qkvs[:, :KH], shard)
    grad_k = col_join(grad_qkvs[:, KH : 2 * KH], shard)
    grad_v = col_join(grad_qkvs[:, 2 * KH : 2 * KH + VH], shard)
    grad_s = col_join(grad_qkvs[:, 2 * KH + VH :], shard)
    grad_o = col_join(plane_a2a(g_out, n).astype(f32), wo.shape[0])
    g_gu = plane_a2a(g_gu, n).astype(f32)
    grad_g = ff_join(g_gu[:, : dp * unit])
    grad_u = ff_join(g_gu[:, dp * unit :])
    grad_d = g_down.astype(f32)
    return (
        layer_out, grad_tokens, g_vecs[0], g_vecs[1], grad_q, grad_k, grad_v, grad_s, grad_o,
        g_vecs[2], g_vecs[3], grad_g, grad_u, grad_d,
    )


def solution(mesh):
    n = mesh.shape[AXIS]
    row, vec = P(AXIS, None), P(AXIS)
    ins = (row, row, vec, vec, row, row, row, row, row, vec, vec, row, row, row, row)
    outs = (row, row, vec, vec, row, row, row, row, row, vec, vec, row, row, row)
    return jax.shard_map(
        lambda *a: on_device(n, *a), mesh=mesh, in_specs=ins, out_specs=outs, check_vma=False
    )
```

```python
import functools
import math

import jax
import jax.numpy as jnp
from jax import lax
from jax.experimental import pallas as pl
from jax.experimental.pallas import tpu as pltpu
from jax.sharding import PartitionSpec as P

HEADS = 8
KH = 256
VH = 512
TP = 8
AXIS = "fsdp"
MESH = pl.DeviceIdType.MESH
ANY = pl.BlockSpec(memory_space=pl.ANY)
VMEM = pl.BlockSpec(memory_space=pltpu.VMEM)
bf = jnp.bfloat16
f32 = jnp.float32
SDS = jax.ShapeDtypeStruct


def place():
    me = lax.axis_index(AXIS)
    steps = [s - 2 * s * lax.rem(lax.div(me, s), 2) for s in (1, 2, 4)]

    def peer(k):
        out = me
        for bit, step in enumerate(steps):
            if k >> bit & 1:
                out = out + step
        return out

    return me, peer


def greet(peers):
    barrier = pltpu.get_barrier_semaphore()
    for p in peers:
        pl.semaphore_signal(barrier, inc=1, device_id=(p,), device_id_type=MESH)
    pl.semaphore_wait(barrier, len(peers))


def remote(src, dst, sems, i, dev):
    return pltpu.make_async_remote_copy(
        src_ref=src, dst_ref=dst, send_sem=sems[0].at[i], recv_sem=sems[1].at[i],
        device_id=(dev,), device_id_type=MESH,
    )


GATHER_SEMS = 13


def gather_blocks(own, out, sems, base, local, peer):
    h = own.shape[0] // 2
    top, bot = pl.ds(0, h), pl.ds(h, h)
    pc, px, py = peer(1), peer(2), peer(4)
    made = []

    def send(src, dst, dev):
        copy = remote(src, dst, sems, base + len(made), dev)
        copy.start()
        made.append(copy)
        return copy

    x0 = send(own.at[bot], out.at[2, bot], px)
    y0 = send(own.at[top], out.at[4, top], py)
    x1 = send(own.at[top], out.at[2, top], px)
    y1 = send(own.at[bot], out.at[4, bot], py)
    core = [send(own, out.at[1], pc)]
    keep = pltpu.make_async_copy(own, out.at[0], local)
    keep.start()
    x0.wait_recv()
    fy = send(out.at[2, bot], out.at[6, bot], py)
    core.append(send(out.at[2, bot], out.at[3, bot], pc))
    y0.wait_recv()
    fx = send(out.at[4, top], out.at[6, top], px)
    core.append(send(out.at[4, top], out.at[5, top], pc))
    x1.wait_recv()
    core.append(send(out.at[2, top], out.at[3, top], pc))
    y1.wait_recv()
    core.append(send(out.at[4, bot], out.at[5, bot], pc))
    fy.wait_recv()
    core.append(send(out.at[6, bot], out.at[7, bot], pc))
    fx.wait_recv()
    core.append(send(out.at[6, top], out.at[7, top], pc))
    for copy in core:
        copy.wait_recv()
    for copy in made:
        copy.wait_send()
    keep.wait()


def gather_kernel(x_ref, out_ref, ssem, rsem, local):
    _, peer = place()
    greet([peer(1), peer(2), peer(4)])
    gather_blocks(x_ref, out_ref, (ssem, rsem), 0, local, peer)


def plane_gather(x, cid):
    r, c = x.shape
    return pl.pallas_call(
        gather_kernel,
        out_shape=SDS((TP, r, c), x.dtype),
        in_specs=[VMEM],
        out_specs=ANY,
        scratch_shapes=[
            pltpu.SemaphoreType.DMA((GATHER_SEMS,)),
            pltpu.SemaphoreType.DMA((GATHER_SEMS,)),
            pltpu.SemaphoreType.DMA,
        ],
        compiler_params=pltpu.CompilerParams(
            collective_id=cid, has_side_effects=True, vmem_limit_bytes=8 << 20
        ),
        name=f"plane_gather_{cid}",
    )(x)


def send_columns(src, out, cols, at, sems, base, local, t, peer, tiled=True):
    copies = []

    def block(q):
        if not tiled:
            return src.at[q]
        return src.at[:, pl.ds(pl.multiple_of(q * cols, 128), cols)]

    for k in range(1, TP):
        dev = peer(k)
        copy = remote(
            block(lax.rem(dev, TP)), out.at[t, :, pl.ds(at, cols)], sems, base + k - 1, dev
        )
        copy.start()
        copies.append(copy)
    keep = pltpu.make_async_copy(block(t), out.at[t, :, pl.ds(at, cols)], local)
    keep.start()
    return copies, keep


def finish(parts):
    for copies, keep in parts:
        for copy in copies:
            copy.wait()
        keep.wait()


def first_kernel(n, wq, wk, wv, vec, qk_out, v_out, vec_out, ssem, rsem, local):
    dp = n // TP
    me, peer = place()
    t, g = lax.rem(me, TP), lax.div(me, TP)
    others = [lax.rem(me + TP * j, n) for j in range(1, dp)]
    greet([peer(k) for k in range(1, TP)] + others)
    sems = (ssem, rsem)
    kq, kv = wq.shape[1] // TP, wv.shape[1] // TP
    far = []
    keep = pltpu.make_async_copy(vec, vec_out.at[g, t], local.at[3])
    keep.start()
    for j, dev in enumerate(others):
        copy = remote(vec, vec_out.at[g, t], sems, 28 + j, dev)
        copy.start()
        far.append(copy)
    parts = [
        send_columns(wq, qk_out, kq, 0, sems, 0, local.at[0], t, peer),
        send_columns(wk, qk_out, kq, kq, sems, 7, local.at[1], t, peer),
        send_columns(wv, v_out, kv, 0, sems, 14, local.at[2], t, peer),
    ]
    for copy in far:
        copy.wait()
    keep.wait()
    near = []
    for k in range(1, TP):
        copy = remote(vec_out.at[:, t], vec_out.at[:, t], sems, 20 + k, peer(k))
        copy.start()
        near.append(copy)
    finish(parts)
    for copy in near:
        copy.wait()


def first_exchange(n, wq, wk, wv, vec, cid):
    shard = wq.shape[0]
    return pl.pallas_call(
        functools.partial(first_kernel, n),
        out_shape=(
            SDS((TP, shard, 2 * wq.shape[1] // TP), bf),
            SDS((TP, shard, wv.shape[1] // TP), bf),
            SDS((n // TP, TP) + vec.shape, f32),
        ),
        in_specs=[VMEM] * 4,
        out_specs=(ANY, ANY, ANY),
        scratch_shapes=[
            pltpu.SemaphoreType.DMA((28 + n // TP,)),
            pltpu.SemaphoreType.DMA((28 + n // TP,)),
            pltpu.SemaphoreType.DMA((4,)),
        ],
        compiler_params=pltpu.CompilerParams(
            collective_id=cid, has_side_effects=True, vmem_limit_bytes=8 << 20
        ),
        name="first_exchange",
    )(wq, wk, wv, vec)


def second_kernel(wo, ws, gu, tok, o_out, s_out, gu_out, tok_out, ssem, rsem, local):
    me, peer = place()
    t = lax.rem(me, TP)
    greet([peer(k) for k in range(1, TP)])
    sems = (ssem, rsem)
    gather_blocks(tok, tok_out, sems, 21, local.at[3], peer)
    finish([
        send_columns(wo, o_out, wo.shape[1] // TP, 0, sems, 0, local.at[0], t, peer),
        send_columns(ws, s_out, ws.shape[1] // TP, 0, sems, 7, local.at[1], t, peer),
        send_columns(gu, gu_out, gu.shape[2], 0, sems, 14, local.at[2], t, peer, tiled=False),
    ])


def second_exchange(wo, ws, gu, tok, cid):
    return pl.pallas_call(
        second_kernel,
        out_shape=(
            SDS((TP, wo.shape[0], wo.shape[1] // TP), bf),
            SDS((TP, ws.shape[0], ws.shape[1] // TP), bf),
            SDS(gu.shape, bf),
            SDS((TP,) + tok.shape, bf),
        ),
        in_specs=[VMEM] * 4,
        out_specs=(ANY, ANY, ANY, ANY),
        scratch_shapes=[
            pltpu.SemaphoreType.DMA((21 + GATHER_SEMS,)),
            pltpu.SemaphoreType.DMA((21 + GATHER_SEMS,)),
            pltpu.SemaphoreType.DMA((4,)),
        ],
        compiler_params=pltpu.CompilerParams(
            collective_id=cid, has_side_effects=True, vmem_limit_bytes=12 << 20
        ),
        name="second_exchange",
    )(wo, ws, gu, tok)


def vector_sum_kernel(n, v_ref, out_ref, near, far, part, ssem, rsem):
    dp = n // TP
    me, peer = place()
    g = lax.div(me, TP)
    width = out_ref.shape[1]
    sems = (ssem, rsem)
    others = [lax.rem(me + TP * j, n) for j in range(1, dp)]
    greet([peer(k) for k in range(1, TP)] + others)
    copies = []
    for j, dev in enumerate(others):
        at = pl.multiple_of(lax.div(dev, TP) * width, 128)
        copy = remote(v_ref.at[:, pl.ds(at, width)], far.at[j], sems, j, dev)
        copy.start()
        copies.append(copy)
    total = v_ref[:, pl.ds(pl.multiple_of(g * width, 128), width)]
    for j, copy in enumerate(copies):
        copy.wait()
        total = total + far[j]
    part[...] = total
    copies = []
    for k in range(1, TP):
        copy = remote(part, near.at[k - 1], sems, dp + k - 1, peer(k))
        copy.start()
        copies.append(copy)
    for k, copy in enumerate(copies):
        copy.wait()
        total = total + near[k]
    out_ref[...] = total


def vector_sum(n, v, cid):
    dp = n // TP
    width = v.shape[1] // dp
    return pl.pallas_call(
        functools.partial(vector_sum_kernel, n),
        out_shape=SDS((v.shape[0], width), f32),
        in_specs=[VMEM],
        out_specs=VMEM,
        scratch_shapes=[
            pltpu.VMEM((TP - 1, v.shape[0], width), f32),
            pltpu.VMEM((dp, v.shape[0], width), f32),
            pltpu.VMEM((v.shape[0], width), f32),
            pltpu.SemaphoreType.DMA((dp + TP,)),
            pltpu.SemaphoreType.DMA((dp + TP,)),
        ],
        compiler_params=pltpu.CompilerParams(
            collective_id=cid, has_side_effects=True, vmem_limit_bytes=4 << 20
        ),
        name="vector_sum",
    )(v)


REDUCE_SEMS = 10
TILE = 512


def reduce_blocks(nt, a, w, po, pe, rc, sb, xr, yr, sems, peer):
    r = a.shape[1]
    c = pe.shape[2]
    h = r // 2
    top, bot = pl.ds(0, h), pl.ds(h, h)
    pc, px, py = peer(1), peer(2), peer(4)
    sent = []

    def product(k, dst):
        @pl.loop(0, c // TILE)
        def _(j):
            at = pl.ds(pl.multiple_of(j * TILE, TILE), TILE)
            if nt:
                y = lax.dot_general(
                    a[k], w[at, :], (((1,), (1,)), ((), ())), preferred_element_type=f32
                )
            else:
                y = jnp.dot(a[k], w[:, at], preferred_element_type=f32)
            dst[:, at] = y.astype(dst.dtype)

    def send(src, dst, dev, i):
        copy = remote(src, dst, sems, i, dev)
        copy.start()
        sent.append(copy)
        return copy

    def pair(i):
        k = 2 * i
        product(k + 1, po.at[i])
        copy = send(po.at[i], rc.at[i], pc, i)
        product(k, pe.at[i])
        return copy

    def rows(ref, at):
        return pl.ds(at.start, at.size) if ref is None else at

    def add(dst, part, got, out=None):
        step = 32

        @pl.loop(0, part.size // step)
        def _(j):
            here = pl.ds(pl.multiple_of(part.start + j * step, step), step)
            there = pl.ds(pl.multiple_of(j * step, step), step)
            total = dst[here, :] + got[there, :].astype(f32)
            if out is None:
                dst[here, :] = total
            else:
                out[there, :] = total.astype(bf)

    c6 = pair(3)
    c2 = pair(1)
    c6.wait_recv()
    add(pe.at[3], top, rc.at[3, top], sb.at[0])
    x6 = send(sb.at[0], xr.at[0], px, 4)
    add(pe.at[3], bot, rc.at[3, bot], sb.at[1])
    y6 = send(sb.at[1], yr.at[0], py, 5)
    c4 = pair(2)
    c2.wait_recv()
    add(pe.at[1], top, rc.at[1, top], sb.at[2])
    x2 = send(sb.at[2], xr.at[1], px, 6)
    add(pe.at[1], bot, rc.at[1, bot])
    c0 = pair(0)
    c4.wait_recv()
    add(pe.at[2], bot, rc.at[2, bot], sb.at[3])
    y4 = send(sb.at[3], yr.at[1], py, 7)
    add(pe.at[2], top, rc.at[2, top])
    c0.wait_recv()
    x6.wait_recv()
    add(pe.at[2], top, xr.at[0], sb.at[4])
    y4b = send(sb.at[4], yr.at[2], py, 8)
    y6.wait_recv()
    add(pe.at[1], bot, yr.at[0], sb.at[5])
    x2b = send(sb.at[5], xr.at[2], px, 9)
    x2.wait_recv()
    y4.wait_recv()
    y4b.wait_recv()
    x2b.wait_recv()

    def total(at, half_at, lower):
        first, second = (yr, xr) if lower else (xr, yr)
        return (
            pe[0, at, :]
            + rc[0, at, :].astype(f32)
            + first[1, half_at, :].astype(f32)
            + second[2, half_at, :].astype(f32)
        )

    def for_rows(step, body):
        for lower in (False, True):

            @pl.loop(0, h // step)
            def _(j, lower=lower):
                half_at = pl.ds(pl.multiple_of(j * step, step), step)
                at = pl.ds(pl.multiple_of(j * step + (h if lower else 0), step), step)
                body(at, total(at, half_at, lower))

    return for_rows, sent


def reduce_scratch(r, c):
    h = r // 2
    return [
        pltpu.VMEM((4, r, c), bf),
        pltpu.VMEM((4, r, c), f32),
        pltpu.VMEM((4, r, c), bf),
        pltpu.VMEM((6, h, c), bf),
        pltpu.VMEM((3, h, c), bf),
        pltpu.VMEM((3, h, c), bf),
    ]


def reduce_kernel(nt, a, w, out_ref, po, pe, rc, sb, xr, yr, ssem, rsem):
    _, peer = place()
    greet([peer(1), peer(2), peer(4)])
    for_rows, sent = reduce_blocks(nt, a, w, po, pe, rc, sb, xr, yr, (ssem, rsem), peer)

    def body(at, value):
        out_ref[at, :] = value

    for_rows(32, body)
    for copy in sent:
        copy.wait_send()


def matmul_reduce(a, w, nt, cid):
    _, r, _ = a.shape
    c = w.shape[0] if nt else w.shape[1]
    return pl.pallas_call(
        functools.partial(reduce_kernel, nt),
        out_shape=SDS((r, c), f32),
        in_specs=[VMEM] * 2,
        out_specs=VMEM,
        scratch_shapes=reduce_scratch(r, c)
        + [pltpu.SemaphoreType.DMA((REDUCE_SEMS,)), pltpu.SemaphoreType.DMA((REDUCE_SEMS,))],
        compiler_params=pltpu.CompilerParams(
            collective_id=cid, has_side_effects=True, vmem_limit_bytes=48 << 20
        ),
        name=f"matmul_reduce_{cid}",
    )(a, w)


def forward_kernel(a, w, tok, vec, mid, out, po, pe, rc, sb, xr, yr, own, ssem, rsem, local):
    _, peer = place()
    greet([peer(1), peer(2), peer(4)])
    sems = (ssem, rsem)
    for_rows, sent = reduce_blocks(False, a, w, po, pe, rc, sb, xr, yr, sems, peer)

    def body(at, value):
        value = value + tok[at, :].astype(f32)
        mid[at, :] = value
        center = jnp.mean(value, axis=-1, keepdims=True)
        centred = value - center
        spread = jnp.mean(centred * centred, axis=-1, keepdims=True)
        own[at, :] = (
            centred * lax.rsqrt(spread + 1e-05) * vec[0:1, :] + vec[1:2, :]
        ).astype(bf)

    for_rows(16, body)
    gather_blocks(own, out, sems, REDUCE_SEMS, local, peer)
    for copy in sent:
        copy.wait_send()


def forward_exchange(a, w, tok, vec, cid):
    _, r, _ = a.shape
    c = w.shape[1]
    count = REDUCE_SEMS + GATHER_SEMS
    return pl.pallas_call(
        forward_kernel,
        out_shape=(SDS((r, c), f32), SDS((TP, r, c), bf)),
        in_specs=[VMEM] * 4,
        out_specs=(VMEM, ANY),
        scratch_shapes=reduce_scratch(r, c)
        + [
            pltpu.VMEM((r, c), bf),
            pltpu.SemaphoreType.DMA((count,)),
            pltpu.SemaphoreType.DMA((count,)),
            pltpu.SemaphoreType.DMA,
        ],
        compiler_params=pltpu.CompilerParams(
            collective_id=cid, has_side_effects=True, vmem_limit_bytes=48 << 20
        ),
        name="forward_exchange",
    )(a, w, tok, vec)


def backward_kernel(
    a, w, mid, cot, vec, gmid, out, sums, po, pe, rc, sb, xr, yr, own, acc, ssem, rsem, local
):
    _, peer = place()
    greet([peer(1), peer(2), peer(4)])
    sems = (ssem, rsem)
    acc[...] = jnp.zeros_like(acc)
    for_rows, sent = reduce_blocks(True, a, w, po, pe, rc, sb, xr, yr, sems, peer)

    def body(at, g):
        value = mid[at, :]
        center = jnp.mean(value, axis=-1, keepdims=True)
        centred = value - center
        inv = lax.rsqrt(jnp.mean(centred * centred, axis=-1, keepdims=True) + 1e-05)
        hat = centred * inv
        acc[0] += g * hat
        acc[1] += g
        scaled = g * vec[0:1, :]
        mean_g = jnp.mean(scaled, axis=-1, keepdims=True)
        mean_gh = jnp.mean(scaled * hat, axis=-1, keepdims=True)
        grad = cot[at, :].astype(f32) + inv * (scaled - mean_g - hat * mean_gh)
        gmid[at, :] = grad
        own[at, :] = grad.astype(bf)

    for_rows(16, body)
    gather_blocks(own, out, sems, REDUCE_SEMS, local, peer)
    sums[0:1, :] = jnp.sum(acc[0], axis=0, keepdims=True)
    sums[1:2, :] = jnp.sum(acc[1], axis=0, keepdims=True)
    for copy in sent:
        copy.wait_send()


def backward_exchange(a, w, mid, cot, vec, cid):
    _, r, _ = a.shape
    c = w.shape[0]
    count = REDUCE_SEMS + GATHER_SEMS
    return pl.pallas_call(
        backward_kernel,
        out_shape=(SDS((r, c), f32), SDS((TP, r, c), bf), SDS((2, c), f32)),
        in_specs=[VMEM] * 5,
        out_specs=(VMEM, ANY, VMEM),
        scratch_shapes=reduce_scratch(r, c)
        + [
            pltpu.VMEM((r, c), bf),
            pltpu.VMEM((2, 16, c), f32),
            pltpu.SemaphoreType.DMA((count,)),
            pltpu.SemaphoreType.DMA((count,)),
            pltpu.SemaphoreType.DMA,
        ],
        compiler_params=pltpu.CompilerParams(
            collective_id=cid, has_side_effects=True, vmem_limit_bytes=52 << 20
        ),
        name="backward_exchange",
    )(a, w, mid, cot, vec)


def tp_groups(n):
    return [[g * TP + t for t in range(TP)] for g in range(n // TP)]


def dp_groups(n):
    return [[g * TP + t for g in range(n // TP)] for t in range(TP)]


def plane_a2a(x, n):
    return lax.all_to_all(x, AXIS, 0, 0, axis_index_groups=tp_groups(n), tiled=True)


def dp_gather(x, n):
    return lax.all_gather(x, AXIS, axis=0, tiled=True, axis_index_groups=dp_groups(n))


def dp_reduce(x, n):
    return lax.psum_scatter(
        x, AXIS, scatter_dimension=0, tiled=True, axis_index_groups=dp_groups(n)
    )


def layer_norm(value, gain, bias):
    center = jnp.mean(value, axis=-1, keepdims=True)
    centred = value - center
    spread = jnp.mean(centred * centred, axis=-1, keepdims=True)
    return centred * lax.rsqrt(spread + 1e-05) * gain + bias


def seq_positions(lengths, rows):
    ends = jnp.cumsum(lengths, axis=1)
    starts = ends - lengths
    index = jnp.arange(rows, dtype=jnp.int32)
    segment = jnp.sum((index[None, :, None] >= ends[:, None, :]).astype(jnp.int32), axis=2)
    member = segment[:, :, None] == jnp.arange(lengths.shape[1], dtype=jnp.int32)
    offset = index[None, :] - jnp.sum(jnp.where(member, starts[:, None, :], 0), axis=2)
    return segment, offset


def rotary_tables(offset):
    half = KH // 2
    freq = jnp.exp(-math.log(10000.0) * jnp.arange(half, dtype=f32) / half)
    angle = offset.astype(f32)[..., None] * freq
    return jnp.cos(angle), jnp.sin(angle)


def rotate(value, cosine, sine):
    half = KH // 2
    u, w = value[..., :half], value[..., half:]
    return jnp.concatenate([u * cosine - w * sine, w * cosine + u * sine], axis=-1)


def rotate_back(value, cosine, sine):
    half = KH // 2
    u, w = value[..., :half], value[..., half:]
    return jnp.concatenate([u * cosine + w * sine, w * cosine - u * sine], axis=-1)


def decay_mask(segment, offset, head):
    diff = offset[:, :, None] - offset[:, None, :]
    valid = (segment[:, :, None] == segment[:, None, :]) & (diff >= 0)
    steps = jnp.where(valid, diff, 0).astype(f32)
    log = jnp.log(1.0 - jnp.exp2(-5.0 - head.astype(f32)))
    return jnp.where(valid, jnp.exp(log * steps), 0.0) / math.sqrt(KH)


def group_gate(retained, swish_in):
    center = jnp.mean(retained, axis=-1, keepdims=True)
    centred = retained - center
    spread = jnp.mean(centred * centred, axis=-1, keepdims=True)
    return jax.nn.silu(swish_in) * (centred * lax.rsqrt(jnp.maximum(spread, 0.25)))


def mlp_gate(first, second):
    return jax.nn.gelu(first, approximate=False) * second


def dot(a, b):
    return lax.dot_general(a, b, (((1,), (0,)), ((), ())), preferred_element_type=f32)


def dot_tn(a, b):
    return lax.dot_general(a, b, (((0,), (0,)), ((), ())), preferred_element_type=f32)


def dot_nt(a, b):
    return lax.dot_general(a, b, (((1,), (1,)), ((), ())), preferred_element_type=f32)


def bmm(eq, a, b):
    return jnp.einsum(eq, a, b, preferred_element_type=f32)


def col_blocks(w):
    r, c = w.shape
    return w.reshape(r, TP, c // TP).transpose(1, 0, 2).reshape(TP * r, c // TP)


def col_join(w, r):
    c = w.shape[1]
    return w.reshape(TP, r, c).transpose(1, 0, 2).reshape(r, TP * c)


def after(x, *deps):
    return lax.optimization_barrier((x,) + deps)[0]


def on_device(n, tokens, lengths, gain1, bias1, wq, wk, wv, ws, wo, gain2, bias2, wg, wu, wd, cot):
    rows, d = tokens.shape
    ff = wg.shape[1]
    dp = n // TP
    shard = d // n
    unit = ff // n
    me = lax.axis_index(AXIS)
    head = lax.rem(me, TP)

    def ff_blocks(w):
        return w.reshape(shard, dp, TP, unit).transpose(2, 0, 1, 3).reshape(TP, shard, dp * unit)

    def ff_join(w):
        return w.reshape(TP, shard, dp, unit).transpose(1, 2, 0, 3).reshape(shard, ff)

    vec = jnp.zeros((8, 128), f32)
    for i, v in enumerate((gain1, bias1, gain2, bias2)):
        vec = vec.at[i, :shard].set(v.astype(f32))
    vec = vec.at[4, :3].set(lengths[0].astype(f32))
    qk_blk, v_blk, vec_all = first_exchange(n, wq, wk, wv, vec, 1)
    gain1f, bias1f, gain2f, bias2f = (
        vec_all[:, :, i, :shard].reshape(1, d) for i in range(4)
    )
    vec2 = jnp.concatenate([gain2f, bias2f], axis=0)
    qk = dp_gather(qk_blk.reshape(TP * shard, 2 * KH), n)
    val = dp_gather(v_blk.reshape(TP * shard, VH), n)
    gu_in = jnp.concatenate([ff_blocks(wg), ff_blocks(wu)], axis=2)
    o_blk, s_blk, gu_blk, tok_all = second_exchange(after(wo, v_blk), ws, gu_in, tokens, 2)
    out = dp_gather(o_blk.reshape(TP * wo.shape[0], d // TP), n)
    out = col_join(plane_a2a(out, n), VH)
    swi = dp_gather(s_blk.reshape(TP * shard, VH), n)
    gu = dp_gather(gu_blk.reshape(TP * shard, 2 * dp * unit), n)
    down = dp_gather(after(wd, gu_blk), n)
    cot_all = plane_gather(after(cot, tok_all), 3)

    mine = lax.dynamic_slice_in_dim(vec_all, lax.div(me, TP), 1, 0)[0, :, 4, :3]
    order = jnp.arange(TP, dtype=jnp.int32)
    pick = (order[None, :] == (order[:, None] ^ head)).astype(f32)
    len_all = jnp.sum(pick[:, :, None] * mine[None], axis=1).astype(jnp.int32)
    segment, offset = seq_positions(len_all, rows)
    cosine, sine = rotary_tables(offset)
    mask = decay_mask(segment, offset, head)

    normed = layer_norm(tok_all.reshape(TP * rows, d).astype(f32), gain1f, bias1f).astype(bf)
    qk_out = dot(normed, qk).reshape(TP, rows, 2 * KH)
    query, key = qk_out[..., :KH], qk_out[..., KH:]
    v_low = dot(normed, val).reshape(TP, rows, VH).astype(bf)
    swish_in = dot(normed, swi).reshape(TP, rows, VH)
    q_rot = rotate(query, cosine, sine).astype(bf)
    k_rot = rotate(key, cosine, sine).astype(bf)
    plain = bmm("btd,bsd->bts", q_rot, k_rot)
    scores = (plain * mask).astype(bf)
    retained = bmm("bts,bsd->btd", scores, v_low)
    mixed = group_gate(retained, swish_in).astype(bf)
    middle, normed2 = forward_exchange(mixed, out, tokens, vec2, 4)
    normed2 = normed2.reshape(TP * rows, d)
    cot_all = cot_all.reshape(TP * rows, d)
    fs = dot(normed2, gu)
    first, second = fs[:, : dp * unit], fs[:, dp * unit :]
    hidden = mlp_gate(first, second).astype(bf)

    g_down = dp_reduce(dot_tn(hidden, cot_all).astype(bf), n)
    g_hidden = dot_nt(cot_all, down)
    _, pull_gate = jax.vjp(mlp_gate, first, second)
    g_first, g_second = pull_gate(g_hidden)
    g_fs = jnp.concatenate([g_first.astype(bf), g_second.astype(bf)], axis=1)
    gu_grad = dot_tn(normed2, g_fs).astype(bf)
    g_gu = dp_reduce(gu_grad, n)
    g_fs_in = after(g_fs, gu_grad)
    g_middle, g_low, sums2 = backward_exchange(
        g_fs_in.reshape(TP, rows, 2 * dp * unit), gu, middle, cot, vec2, 5
    )

    g_low = g_low.reshape(TP * rows, d)
    mixed = mixed.reshape(TP * rows, VH)
    out_grad = dot_tn(mixed, g_low).astype(bf)
    g_out = dp_reduce(plane_a2a(col_blocks(out_grad), n), n)
    g_mixed = dot_nt(g_low, out).reshape(TP, rows, VH)
    _, pull_group = jax.vjp(group_gate, retained, swish_in)
    g_retained, g_swish = pull_group(g_mixed)
    g_retained = g_retained.astype(bf)
    g_swish = g_swish.astype(bf)
    g_value = bmm("bts,btd->bsd", scores, g_retained).astype(bf)
    g_scores = bmm("btd,bsd->bts", g_retained, v_low)
    g_plain = (g_scores * mask).astype(bf)
    g_qrot = bmm("bts,bsd->btd", g_plain, k_rot)
    g_krot = bmm("bts,btd->bsd", g_plain, q_rot)
    g_query = rotate_back(g_qrot, cosine, sine).astype(bf)
    g_key = rotate_back(g_krot, cosine, sine).astype(bf)
    g_qkvs = jnp.concatenate([g_query, g_key, g_value, g_swish], axis=2)
    w_qkvs = jnp.concatenate([qk, val, swi], axis=1)
    qkvs_grad = dot_tn(normed, g_qkvs.reshape(TP * rows, 2 * KH + 2 * VH)).astype(bf)
    grad_qkvs = dp_reduce(qkvs_grad, n)
    g_qkvs = after(g_qkvs, qkvs_grad)
    g_normed = matmul_reduce(g_qkvs, w_qkvs, True, 6)
    inputs = tokens.astype(f32)
    _, pull_norm1 = jax.vjp(layer_norm, inputs, gain1f, bias1f)
    g_in_part, g_gain1, g_bias1 = pull_norm1(g_normed)
    grad_tokens = g_middle + g_in_part
    hidden = after(hidden, g_normed)
    layer_out = (middle + matmul_reduce(hidden.reshape(TP, rows, dp * unit), down, False, 7)).astype(bf)

    g_vecs = jnp.concatenate([g_gain1, g_bias1, sums2, jnp.zeros((4, d), f32)], axis=0)
    g_vecs = vector_sum(n, g_vecs, 8)
    g_vecs = lax.dynamic_slice_in_dim(g_vecs, head * shard, shard, 1)
    grad_qkvs = plane_a2a(grad_qkvs, n).astype(f32)
    grad_q = col_join(grad_qkvs[:, :KH], shard)
    grad_k = col_join(grad_qkvs[:, KH : 2 * KH], shard)
    grad_v = col_join(grad_qkvs[:, 2 * KH : 2 * KH + VH], shard)
    grad_s = col_join(grad_qkvs[:, 2 * KH + VH :], shard)
    grad_o = col_join(plane_a2a(g_out, n).astype(f32), wo.shape[0])
    g_gu = plane_a2a(g_gu, n).astype(f32)
    grad_g = ff_join(g_gu[:, : dp * unit])
    grad_u = ff_join(g_gu[:, dp * unit :])
    grad_d = g_down.astype(f32)
    return (
        layer_out, grad_tokens, g_vecs[0], g_vecs[1], grad_q, grad_k, grad_v, grad_s, grad_o,
        g_vecs[2], g_vecs[3], grad_g, grad_u, grad_d,
    )


def solution(mesh):
    n = mesh.shape[AXIS]
    row, vec = P(AXIS, None), P(AXIS)
    ins = (row, row, vec, vec, row, row, row, row, row, vec, vec, row, row, row, row)
    outs = (row, row, vec, vec, row, row, row, row, row, vec, vec, row, row, row)
    return jax.shard_map(
        lambda *a: on_device(n, *a), mesh=mesh, in_specs=ins, out_specs=outs, check_vma=False
    )
```

```python
import functools
import math

import jax
import jax.numpy as jnp
from jax import lax
from jax.experimental import pallas as pl
from jax.experimental.pallas import tpu as pltpu
from jax.sharding import PartitionSpec as P


KH = 256
VH = 512
TP = 8
AXIS = "fsdp"
MESH = pl.DeviceIdType.MESH
ANY = pl.BlockSpec(memory_space=pl.ANY)
VMEM = pl.BlockSpec(memory_space=pltpu.VMEM)
bf = jnp.bfloat16
f32 = jnp.float32
SDS = jax.ShapeDtypeStruct


def place():
    me = lax.axis_index(AXIS)
    steps = [s - 2 * s * lax.rem(lax.div(me, s), 2) for s in (1, 2, 4)]

    def peer(k):
        out = me
        for bit, step in enumerate(steps):
            if k >> bit & 1:
                out = out + step
        return out

    return me, peer


def greet(peers):
    barrier = pltpu.get_barrier_semaphore()
    for p in peers:
        pl.semaphore_signal(barrier, inc=1, device_id=(p,), device_id_type=MESH)
    pl.semaphore_wait(barrier, len(peers))


def remote(src, dst, sems, i, dev):
    return pltpu.make_async_remote_copy(
        src_ref=src, dst_ref=dst, send_sem=sems[0].at[i], recv_sem=sems[1].at[i],
        device_id=(dev,), device_id_type=MESH,
    )


GATHER_SEMS = 13


def gather_blocks(own, out, sems, base, local, peer):
    h = own.shape[0] // 2
    top, bot = pl.ds(0, h), pl.ds(h, h)
    pc, px, py = peer(1), peer(2), peer(4)
    made = []

    def send(src, dst, dev):
        copy = remote(src, dst, sems, base + len(made), dev)
        copy.start()
        made.append(copy)
        return copy

    x0 = send(own.at[bot], out.at[2, bot], px)
    y0 = send(own.at[top], out.at[4, top], py)
    x1 = send(own.at[top], out.at[2, top], px)
    y1 = send(own.at[bot], out.at[4, bot], py)
    core = [send(own, out.at[1], pc)]
    keep = pltpu.make_async_copy(own, out.at[0], local)
    keep.start()
    x0.wait_recv()
    fy = send(out.at[2, bot], out.at[6, bot], py)
    core.append(send(out.at[2, bot], out.at[3, bot], pc))
    y0.wait_recv()
    fx = send(out.at[4, top], out.at[6, top], px)
    core.append(send(out.at[4, top], out.at[5, top], pc))
    x1.wait_recv()
    core.append(send(out.at[2, top], out.at[3, top], pc))
    y1.wait_recv()
    core.append(send(out.at[4, bot], out.at[5, bot], pc))
    fy.wait_recv()
    core.append(send(out.at[6, bot], out.at[7, bot], pc))
    fx.wait_recv()
    core.append(send(out.at[6, top], out.at[7, top], pc))
    for copy in core:
        copy.wait_recv()
    for copy in made:
        copy.wait_send()
    keep.wait()


def gather_kernel(x_ref, out_ref, ssem, rsem, local):
    _, peer = place()
    greet([peer(1), peer(2), peer(4)])
    gather_blocks(x_ref, out_ref, (ssem, rsem), 0, local, peer)


def plane_gather(x, cid):
    r, c = x.shape
    return pl.pallas_call(
        gather_kernel,
        out_shape=SDS((TP, r, c), x.dtype),
        in_specs=[VMEM],
        out_specs=ANY,
        scratch_shapes=[
            pltpu.SemaphoreType.DMA((GATHER_SEMS,)),
            pltpu.SemaphoreType.DMA((GATHER_SEMS,)),
            pltpu.SemaphoreType.DMA,
        ],
        compiler_params=pltpu.CompilerParams(
            collective_id=cid, has_side_effects=True, vmem_limit_bytes=8 << 20
        ),
    )(x)


def send_columns(src, out, cols, at, sems, base, local, t, peer, rows=None):
    copies = []
    rows = slice(None) if rows is None else rows

    def block(q):
        if len(src.shape) == 3:
            return src.at[q]
        return src.at[rows, pl.ds(pl.multiple_of(q * cols, 128), cols)]

    for k in range(1, TP):
        dev = peer(k)
        copy = remote(
            block(lax.rem(dev, TP)), out.at[t, :, pl.ds(at, cols)], sems, base + k - 1, dev
        )
        copy.start()
        copies.append(copy)
    keep = pltpu.make_async_copy(block(t), out.at[t, :, pl.ds(at, cols)], local)
    keep.start()
    return copies, keep


def finish(parts):
    for copies, keep in parts:
        for copy in copies:
            copy.wait()
        keep.wait()


def exchange_call(kernel, outs, args, sems, locals_, cid):
    return pl.pallas_call(
        kernel,
        out_shape=outs,
        in_specs=[VMEM] * len(args),
        out_specs=tuple(ANY for _ in outs),
        scratch_shapes=[
            pltpu.SemaphoreType.DMA((sems,)),
            pltpu.SemaphoreType.DMA((sems,)),
            pltpu.SemaphoreType.DMA((locals_,)),
        ],
        compiler_params=pltpu.CompilerParams(
            collective_id=cid, has_side_effects=True, vmem_limit_bytes=12 << 20
        ),
    )(*args)


def first_kernel(wq, wk, qk_out, ssem, rsem, local):
    me, peer = place()
    t = lax.rem(me, TP)
    greet([peer(k) for k in range(1, TP)])
    sems = (ssem, rsem)
    cols = wq.shape[1] // TP
    finish([
        send_columns(wq, qk_out, cols, 0, sems, 0, local.at[0], t, peer),
        send_columns(wk, qk_out, cols, cols, sems, 7, local.at[1], t, peer),
    ])


def first_exchange(wq, wk, cid):
    outs = (SDS((TP, wq.shape[0], 2 * wq.shape[1] // TP), bf),)
    return exchange_call(first_kernel, outs, (wq, wk), 14, 2, cid)[0]


def second_kernel(n, wv, ws, wo, vec, out, vec_out, ssem, rsem, local):
    dp = n // TP
    me, peer = place()
    t, g = lax.rem(me, TP), lax.div(me, TP)
    others = [lax.rem(me + TP * j, n) for j in range(1, dp)]
    greet([peer(k) for k in range(1, TP)] + others)
    sems = (ssem, rsem)
    shard, cv, co = wv.shape[0], wv.shape[1] // TP, wo.shape[1] // TP
    far = []
    keep = pltpu.make_async_copy(vec, vec_out.at[g, t], local.at[4])
    keep.start()
    for j, dev in enumerate(others):
        copy = remote(vec, vec_out.at[g, t], sems, 35 + j, dev)
        copy.start()
        far.append(copy)
    parts = [
        send_columns(wv, out, cv, 0, sems, 0, local.at[0], t, peer),
        send_columns(ws, out, cv, cv, sems, 7, local.at[1], t, peer),
        send_columns(wo, out, co, 2 * cv, sems, 14, local.at[2], t, peer, pl.ds(0, shard)),
        send_columns(wo, out, co, 2 * cv + co, sems, 21, local.at[3], t, peer, pl.ds(shard, shard)),
    ]
    for copy in far:
        copy.wait()
    keep.wait()
    near = []
    for k in range(1, TP):
        copy = remote(vec_out.at[:, t], vec_out.at[:, t], sems, 27 + k, peer(k))
        copy.start()
        near.append(copy)
    finish(parts)
    for copy in near:
        copy.wait()


def second_exchange(n, wv, ws, wo, vec, cid):
    width = 2 * wv.shape[1] // TP + 2 * wo.shape[1] // TP
    outs = (SDS((TP, wv.shape[0], width), bf), SDS((n // TP, TP) + vec.shape, f32))
    kernel = functools.partial(second_kernel, n)
    return exchange_call(kernel, outs, (wv, ws, wo, vec), 35 + n // TP, 5, cid)


def third_kernel(gu, tok, gu_out, tok_out, ssem, rsem, local):
    me, peer = place()
    t = lax.rem(me, TP)
    greet([peer(k) for k in range(1, TP)])
    sems = (ssem, rsem)
    gather_blocks(tok, tok_out, sems, 7, local.at[1], peer)
    finish([send_columns(gu, gu_out, gu.shape[2], 0, sems, 0, local.at[0], t, peer)])


def third_exchange(gu, tok, cid):
    outs = (SDS(gu.shape, bf), SDS((TP,) + tok.shape, bf))
    return exchange_call(third_kernel, outs, (gu, tok), 7 + GATHER_SEMS, 2, cid)


def vector_sum_kernel(n, v_ref, out_ref, near, far, part, ssem, rsem):
    dp = n // TP
    me, peer = place()
    g = lax.div(me, TP)
    width = out_ref.shape[1]
    sems = (ssem, rsem)
    others = [lax.rem(me + TP * j, n) for j in range(1, dp)]
    greet([peer(k) for k in range(1, TP)] + others)
    copies = []
    for j, dev in enumerate(others):
        at = pl.multiple_of(lax.div(dev, TP) * width, 128)
        copy = remote(v_ref.at[:, pl.ds(at, width)], far.at[j], sems, j, dev)
        copy.start()
        copies.append(copy)
    total = v_ref[:, pl.ds(pl.multiple_of(g * width, 128), width)]
    for j, copy in enumerate(copies):
        copy.wait()
        total = total + far[j]
    part[...] = total
    copies = []
    for k in range(1, TP):
        copy = remote(part, near.at[k - 1], sems, dp + k - 1, peer(k))
        copy.start()
        copies.append(copy)
    for k, copy in enumerate(copies):
        copy.wait()
        total = total + near[k]
    out_ref[...] = total


def vector_sum(n, v, cid):
    dp = n // TP
    width = v.shape[1] // dp
    return pl.pallas_call(
        functools.partial(vector_sum_kernel, n),
        out_shape=SDS((v.shape[0], width), f32),
        in_specs=[VMEM],
        out_specs=VMEM,
        scratch_shapes=[
            pltpu.VMEM((TP - 1, v.shape[0], width), f32),
            pltpu.VMEM((dp, v.shape[0], width), f32),
            pltpu.VMEM((v.shape[0], width), f32),
            pltpu.SemaphoreType.DMA((dp + TP,)),
            pltpu.SemaphoreType.DMA((dp + TP,)),
        ],
        compiler_params=pltpu.CompilerParams(
            collective_id=cid, has_side_effects=True, vmem_limit_bytes=4 << 20
        ),
        name="vector_sum",
    )(v)


REDUCE_SEMS = 10
TILE = 512


def reduce_blocks(nt, a, w, po, pe, rc, sb, xr, yr, sems, peer):
    r = a.shape[1]
    c = pe.shape[2]
    h = r // 2
    top, bot = pl.ds(0, h), pl.ds(h, h)
    pc, px, py = peer(1), peer(2), peer(4)
    sent = []

    def product(k, dst):
        @pl.loop(0, c // TILE)
        def _(j):
            at = pl.ds(pl.multiple_of(j * TILE, TILE), TILE)
            if nt:
                y = lax.dot_general(
                    a[k], w[at, :], (((1,), (1,)), ((), ())), preferred_element_type=f32
                )
            else:
                y = jnp.dot(a[k], w[:, at], preferred_element_type=f32)
            dst[:, at] = y.astype(dst.dtype)

    def send(src, dst, dev, i):
        copy = remote(src, dst, sems, i, dev)
        copy.start()
        sent.append(copy)
        return copy

    def pair(i):
        k = 2 * i
        product(k + 1, po.at[i])
        copy = send(po.at[i], rc.at[i], pc, i)
        product(k, pe.at[i])
        return copy

    def add(dst, part, got, out=None):
        step = 32

        @pl.loop(0, part.size // step)
        def _(j):
            here = pl.ds(pl.multiple_of(part.start + j * step, step), step)
            there = pl.ds(pl.multiple_of(j * step, step), step)
            total = dst[here, :] + got[there, :].astype(f32)
            if out is None:
                dst[here, :] = total
            else:
                out[there, :] = total.astype(bf)

    c6 = pair(3)
    c2 = pair(1)
    c6.wait_recv()
    add(pe.at[3], top, rc.at[3, top], sb.at[0])
    x6 = send(sb.at[0], xr.at[0], px, 4)
    add(pe.at[3], bot, rc.at[3, bot], sb.at[1])
    y6 = send(sb.at[1], yr.at[0], py, 5)
    c4 = pair(2)
    c2.wait_recv()
    add(pe.at[1], top, rc.at[1, top], sb.at[2])
    x2 = send(sb.at[2], xr.at[1], px, 6)
    add(pe.at[1], bot, rc.at[1, bot])
    c0 = pair(0)
    c4.wait_recv()
    add(pe.at[2], bot, rc.at[2, bot], sb.at[3])
    y4 = send(sb.at[3], yr.at[1], py, 7)
    add(pe.at[2], top, rc.at[2, top])
    c0.wait_recv()
    x6.wait_recv()
    add(pe.at[2], top, xr.at[0], sb.at[4])
    y4b = send(sb.at[4], yr.at[2], py, 8)
    y6.wait_recv()
    add(pe.at[1], bot, yr.at[0], sb.at[5])
    x2b = send(sb.at[5], xr.at[2], px, 9)
    x2.wait_recv()
    y4.wait_recv()
    y4b.wait_recv()
    x2b.wait_recv()

    def total(at, half_at, lower):
        first, second = (yr, xr) if lower else (xr, yr)
        return (
            pe[0, at, :]
            + rc[0, at, :].astype(f32)
            + first[1, half_at, :].astype(f32)
            + second[2, half_at, :].astype(f32)
        )

    def for_rows(step, body):
        for lower in (False, True):

            @pl.loop(0, h // step)
            def _(j, lower=lower):
                half_at = pl.ds(pl.multiple_of(j * step, step), step)
                at = pl.ds(pl.multiple_of(j * step + (h if lower else 0), step), step)
                body(at, total(at, half_at, lower))

    return for_rows, sent


def reduce_scratch(r, c):
    h = r // 2
    return [
        pltpu.VMEM((4, r, c), bf),
        pltpu.VMEM((4, r, c), f32),
        pltpu.VMEM((4, r, c), bf),
        pltpu.VMEM((6, h, c), bf),
        pltpu.VMEM((3, h, c), bf),
        pltpu.VMEM((3, h, c), bf),
    ]


def reduce_kernel(nt, a, w, out_ref, po, pe, rc, sb, xr, yr, ssem, rsem):
    _, peer = place()
    greet([peer(1), peer(2), peer(4)])
    for_rows, sent = reduce_blocks(nt, a, w, po, pe, rc, sb, xr, yr, (ssem, rsem), peer)

    def body(at, value):
        out_ref[at, :] = value

    for_rows(32, body)
    for copy in sent:
        copy.wait_send()


def matmul_reduce(a, w, nt, cid):
    _, r, _ = a.shape
    c = w.shape[0] if nt else w.shape[1]
    return pl.pallas_call(
        functools.partial(reduce_kernel, nt),
        out_shape=SDS((r, c), f32),
        in_specs=[VMEM] * 2,
        out_specs=VMEM,
        scratch_shapes=reduce_scratch(r, c)
        + [pltpu.SemaphoreType.DMA((REDUCE_SEMS,)), pltpu.SemaphoreType.DMA((REDUCE_SEMS,))],
        compiler_params=pltpu.CompilerParams(
            collective_id=cid, has_side_effects=True, vmem_limit_bytes=48 << 20
        ),
    )(a, w)


def forward_kernel(a, w, tok, vec, mid, out, po, pe, rc, sb, xr, yr, own, ssem, rsem, local):
    _, peer = place()
    greet([peer(1), peer(2), peer(4)])
    sems = (ssem, rsem)
    for_rows, sent = reduce_blocks(False, a, w, po, pe, rc, sb, xr, yr, sems, peer)

    def body(at, value):
        value = value + tok[at, :].astype(f32)
        mid[at, :] = value
        center = jnp.mean(value, axis=-1, keepdims=True)
        centred = value - center
        spread = jnp.mean(centred * centred, axis=-1, keepdims=True)
        own[at, :] = (
            centred * lax.rsqrt(spread + 1e-05) * vec[0:1, :] + vec[1:2, :]
        ).astype(bf)

    for_rows(16, body)
    gather_blocks(own, out, sems, REDUCE_SEMS, local, peer)
    for copy in sent:
        copy.wait_send()


def forward_exchange(a, w, tok, vec, cid):
    _, r, _ = a.shape
    c = w.shape[1]
    count = REDUCE_SEMS + GATHER_SEMS
    return pl.pallas_call(
        forward_kernel,
        out_shape=(SDS((r, c), f32), SDS((TP, r, c), bf)),
        in_specs=[VMEM] * 4,
        out_specs=(VMEM, ANY),
        scratch_shapes=reduce_scratch(r, c)
        + [
            pltpu.VMEM((r, c), bf),
            pltpu.SemaphoreType.DMA((count,)),
            pltpu.SemaphoreType.DMA((count,)),
            pltpu.SemaphoreType.DMA,
        ],
        compiler_params=pltpu.CompilerParams(
            collective_id=cid, has_side_effects=True, vmem_limit_bytes=48 << 20
        ),
        name="forward_exchange",
    )(a, w, tok, vec)


def backward_kernel(
    a, w, mid, cot, vec, gmid, out, sums, po, pe, rc, sb, xr, yr, own, acc, ssem, rsem, local
):
    _, peer = place()
    greet([peer(1), peer(2), peer(4)])
    sems = (ssem, rsem)
    acc[...] = jnp.zeros_like(acc)
    for_rows, sent = reduce_blocks(True, a, w, po, pe, rc, sb, xr, yr, sems, peer)

    def body(at, g):
        value = mid[at, :]
        center = jnp.mean(value, axis=-1, keepdims=True)
        centred = value - center
        inv = lax.rsqrt(jnp.mean(centred * centred, axis=-1, keepdims=True) + 1e-05)
        hat = centred * inv
        acc[0] += g * hat
        acc[1] += g
        scaled = g * vec[0:1, :]
        mean_g = jnp.mean(scaled, axis=-1, keepdims=True)
        mean_gh = jnp.mean(scaled * hat, axis=-1, keepdims=True)
        grad = cot[at, :].astype(f32) + inv * (scaled - mean_g - hat * mean_gh)
        gmid[at, :] = grad
        own[at, :] = grad.astype(bf)

    for_rows(16, body)
    gather_blocks(own, out, sems, REDUCE_SEMS, local, peer)
    sums[0:1, :] = jnp.sum(acc[0], axis=0, keepdims=True)
    sums[1:2, :] = jnp.sum(acc[1], axis=0, keepdims=True)
    for copy in sent:
        copy.wait_send()


def backward_exchange(a, w, mid, cot, vec, cid):
    _, r, _ = a.shape
    c = w.shape[0]
    count = REDUCE_SEMS + GATHER_SEMS
    return pl.pallas_call(
        backward_kernel,
        out_shape=(SDS((r, c), f32), SDS((TP, r, c), bf), SDS((2, c), f32)),
        in_specs=[VMEM] * 5,
        out_specs=(VMEM, ANY, VMEM),
        scratch_shapes=reduce_scratch(r, c)
        + [
            pltpu.VMEM((r, c), bf),
            pltpu.VMEM((2, 16, c), f32),
            pltpu.SemaphoreType.DMA((count,)),
            pltpu.SemaphoreType.DMA((count,)),
            pltpu.SemaphoreType.DMA,
        ],
        compiler_params=pltpu.CompilerParams(
            collective_id=cid, has_side_effects=True, vmem_limit_bytes=52 << 20
        ),
        name="backward_exchange",
    )(a, w, mid, cot, vec)


def tp_groups(n):
    return [[g * TP + t for t in range(TP)] for g in range(n // TP)]


def dp_groups(n):
    return [[g * TP + t for g in range(n // TP)] for t in range(TP)]


def plane_a2a(x, n):
    return lax.all_to_all(x, AXIS, 0, 0, axis_index_groups=tp_groups(n), tiled=True)


def dp_gather(x, n):
    return lax.all_gather(x, AXIS, axis=0, tiled=True, axis_index_groups=dp_groups(n))


def dp_reduce(x, n):
    return lax.psum_scatter(
        x, AXIS, scatter_dimension=0, tiled=True, axis_index_groups=dp_groups(n)
    )


def layer_norm(value, gain, bias):
    center = jnp.mean(value, axis=-1, keepdims=True)
    centred = value - center
    spread = jnp.mean(centred * centred, axis=-1, keepdims=True)
    return centred * lax.rsqrt(spread + 1e-05) * gain + bias


def seq_positions(lengths, rows):
    ends = jnp.cumsum(lengths, axis=1)
    starts = ends - lengths
    index = jnp.arange(rows, dtype=jnp.int32)
    segment = jnp.sum((index[None, :, None] >= ends[:, None, :]).astype(jnp.int32), axis=2)
    member = segment[:, :, None] == jnp.arange(lengths.shape[1], dtype=jnp.int32)
    offset = index[None, :] - jnp.sum(jnp.where(member, starts[:, None, :], 0), axis=2)
    return segment, offset


def rotary_tables(offset):
    half = KH // 2
    freq = jnp.exp(-math.log(10000.0) * jnp.arange(half, dtype=f32) / half)
    angle = offset.astype(f32)[..., None] * freq
    return jnp.cos(angle), jnp.sin(angle)


def rotate(value, cosine, sine):
    half = KH // 2
    u, w = value[..., :half], value[..., half:]
    return jnp.concatenate([u * cosine - w * sine, w * cosine + u * sine], axis=-1)


def rotate_back(value, cosine, sine):
    half = KH // 2
    u, w = value[..., :half], value[..., half:]
    return jnp.concatenate([u * cosine + w * sine, w * cosine - u * sine], axis=-1)


def decay_mask(segment, offset, head):
    diff = offset[:, :, None] - offset[:, None, :]
    valid = (segment[:, :, None] == segment[:, None, :]) & (diff >= 0)
    steps = jnp.where(valid, diff, 0).astype(f32)
    log = jnp.log(1.0 - jnp.exp2(-5.0 - head.astype(f32)))
    return jnp.where(valid, jnp.exp(log * steps), 0.0) / math.sqrt(KH)


def group_gate(retained, swish_in):
    center = jnp.mean(retained, axis=-1, keepdims=True)
    centred = retained - center
    spread = jnp.mean(centred * centred, axis=-1, keepdims=True)
    return jax.nn.silu(swish_in) * (centred * lax.rsqrt(jnp.maximum(spread, 0.25)))


def gelu_and_slope(x):
    act, pull = jax.vjp(lambda v: jax.nn.gelu(v, approximate=False), x)
    return act, pull(jnp.ones_like(x))[0]


def dot(a, b):
    return lax.dot_general(a, b, (((1,), (0,)), ((), ())), preferred_element_type=f32)


def dot_tn(a, b):
    return lax.dot_general(a, b, (((0,), (0,)), ((), ())), preferred_element_type=f32)


def dot_nt(a, b):
    return lax.dot_general(a, b, (((1,), (1,)), ((), ())), preferred_element_type=f32)


def bmm(eq, a, b):
    return jnp.einsum(eq, a, b, preferred_element_type=f32)


def col_blocks(w):
    r, c = w.shape
    return w.reshape(r, TP, c // TP).transpose(1, 0, 2).reshape(TP * r, c // TP)


def col_join(w, r):
    c = w.shape[1]
    return w.reshape(TP, r, c).transpose(1, 0, 2).reshape(r, TP * c)


def after(x, *deps):
    return lax.optimization_barrier((x,) + deps)[0]


def on_device(n, tokens, lengths, gain1, bias1, wq, wk, wv, ws, wo, gain2, bias2, wg, wu, wd, cot):
    rows, d = tokens.shape
    ff = wg.shape[1]
    dp = n // TP
    shard = d // n
    unit = ff // n
    me = lax.axis_index(AXIS)
    head = lax.rem(me, TP)

    def ff_blocks(w):
        return w.reshape(shard, dp, TP, unit).transpose(2, 0, 1, 3).reshape(TP, shard, dp * unit)

    def ff_join(w):
        return w.reshape(TP, shard, dp, unit).transpose(1, 2, 0, 3).reshape(shard, ff)

    vec = jnp.zeros((8, 128), f32)
    for i, v in enumerate((gain1, bias1, gain2, bias2)):
        vec = vec.at[i, :shard].set(v.astype(f32))
    vec = vec.at[4, :3].set(lengths[0].astype(f32))
    qk_blk = first_exchange(wq, wk, 1)
    qk = dp_gather(qk_blk.reshape(TP * shard, 2 * KH), n)
    vso_blk, vec_all = second_exchange(n, after(wv, qk_blk), ws, wo, vec, 2)
    vso = dp_gather(vso_blk.reshape(TP * shard, 3 * VH), n)
    gu_in = jnp.concatenate([ff_blocks(wg), ff_blocks(wu)], axis=2)
    gu_blk, tok_all = third_exchange(gu_in, after(tokens, vso_blk), 3)
    gu = dp_gather(gu_blk.reshape(TP * shard, 2 * dp * unit), n)
    down = dp_gather(wd, n)
    cot_all = plane_gather(after(cot, tok_all), 4)
    gain1f, bias1f, gain2f, bias2f = (
        vec_all[:, :, i, :shard].reshape(1, d) for i in range(4)
    )
    vec2 = jnp.concatenate([gain2f, bias2f], axis=0)
    out = vso[:, 2 * VH :].reshape(n, shard, 2, d // TP).transpose(0, 2, 1, 3)
    out = col_join(plane_a2a(out.reshape(TP * VH, d // TP), n), VH)

    mine = lax.dynamic_slice_in_dim(vec_all, lax.div(me, TP), 1, 0)[0, :, 4, :3]
    order = jnp.arange(TP, dtype=jnp.int32)
    pick = (order[None, :] == (order[:, None] ^ head)).astype(f32)
    len_all = jnp.sum(pick[:, :, None] * mine[None], axis=1).astype(jnp.int32)
    segment, offset = seq_positions(len_all, rows)
    cosine, sine = rotary_tables(offset)
    mask = decay_mask(segment, offset, head)

    cot_all = cot_all.reshape(TP * rows, d)
    normed = layer_norm(tok_all.reshape(TP * rows, d).astype(f32), gain1f, bias1f).astype(bf)
    qk_out = dot(normed, qk).reshape(TP, rows, 2 * KH)
    query, key = qk_out[..., :KH], qk_out[..., KH:]
    q_rot = rotate(query, cosine, sine).astype(bf)
    k_rot = rotate(key, cosine, sine).astype(bf)
    plain = bmm("btd,bsd->bts", q_rot, k_rot)
    scores = (plain * mask).astype(bf)
    v_low = dot(normed, vso[:, :VH]).reshape(TP, rows, VH).astype(bf)
    swish_in = dot(normed, vso[:, VH : 2 * VH]).reshape(TP, rows, VH)
    retained = bmm("bts,bsd->btd", scores, v_low)
    mixed = group_gate(retained, swish_in).astype(bf)
    middle, normed2 = forward_exchange(mixed, out, tokens, vec2, 5)
    normed2 = normed2.reshape(TP * rows, d)
    fs = dot(normed2, gu)
    first, second = fs[:, : dp * unit], fs[:, dp * unit :]
    act, slope = gelu_and_slope(first)
    hidden = (act * second).astype(bf)
    down_grad = dot_tn(hidden, cot_all).astype(bf)
    g_down = dp_reduce(down_grad, n)

    g_hidden = dot_nt(cot_all, down)
    g_first = (g_hidden * (second * slope)).astype(bf)
    g_second = (g_hidden * act).astype(bf)
    g_fs = jnp.concatenate([g_first, g_second], axis=1)
    gu_grad = dot_tn(normed2, g_fs).astype(bf)
    g_gu = dp_reduce(gu_grad, n)
    g_middle, g_low, sums2 = backward_exchange(
        g_fs.reshape(TP, rows, 2 * dp * unit), gu, middle, cot, vec2, 6
    )

    g_low = g_low.reshape(TP * rows, d)
    mixed = mixed.reshape(TP * rows, VH)
    g_mixed = dot_nt(g_low, out).reshape(TP, rows, VH)
    _, pull_group = jax.vjp(group_gate, retained, swish_in)
    g_retained, g_swish = pull_group(g_mixed)
    g_retained = g_retained.astype(bf)
    g_swish = g_swish.astype(bf)
    swish_grad = dot_tn(normed, g_swish.reshape(TP * rows, VH)).astype(bf)
    g_swi = dp_reduce(swish_grad, n)
    out_grad = dot_tn(mixed, g_low).astype(bf)
    out_grad = plane_a2a(col_blocks(out_grad), n)
    g_value = bmm("bts,btd->bsd", scores, g_retained).astype(bf)
    g_scores = bmm("btd,bsd->bts", g_retained, v_low)
    g_plain = (g_scores * mask).astype(bf)
    g_qrot = bmm("bts,bsd->btd", g_plain, k_rot)
    g_krot = bmm("bts,btd->bsd", g_plain, q_rot)
    g_query = rotate_back(g_qrot, cosine, sine).astype(bf)
    g_key = rotate_back(g_krot, cosine, sine).astype(bf)
    g_qkv = jnp.concatenate([g_query, g_key, g_value], axis=2)
    qkv_grad = dot_tn(normed, g_qkv.reshape(TP * rows, 2 * KH + VH)).astype(bf)
    g_qkv_own = dp_reduce(qkv_grad, n)
    g_out = dp_reduce(out_grad, n)
    g_qkvs = jnp.concatenate([g_qkv, g_swish], axis=2)
    w_qkvs = jnp.concatenate([qk, vso[:, : 2 * VH]], axis=1)
    g_normed = matmul_reduce(g_qkvs, w_qkvs, True, 7)
    inputs = tokens.astype(f32)
    _, pull_norm1 = jax.vjp(layer_norm, inputs, gain1f, bias1f)
    g_in_part, g_gain1, g_bias1 = pull_norm1(g_normed)
    grad_tokens = g_middle + g_in_part
    ffn = matmul_reduce(hidden.reshape(TP, rows, dp * unit), down, False, 8)
    layer_out = (middle + ffn).astype(bf)

    g_vecs = jnp.concatenate([g_gain1, g_bias1, sums2, jnp.zeros((4, d), f32)], axis=0)
    g_vecs = vector_sum(n, g_vecs, 9)
    g_vecs = lax.dynamic_slice_in_dim(g_vecs, head * shard, shard, 1)
    grad_d = g_down.astype(f32)
    g_gu = plane_a2a(g_gu, n).astype(f32)
    grad_g = ff_join(g_gu[:, : dp * unit])
    grad_u = ff_join(g_gu[:, dp * unit :])
    grad_s = col_join(plane_a2a(g_swi, n).astype(f32), shard)
    g_qkv_own = plane_a2a(g_qkv_own, n).astype(f32)
    grad_q = col_join(g_qkv_own[:, :KH], shard)
    grad_k = col_join(g_qkv_own[:, KH : 2 * KH], shard)
    grad_v = col_join(g_qkv_own[:, 2 * KH :], shard)
    grad_o = col_join(plane_a2a(g_out, n).astype(f32), wo.shape[0])
    return (
        layer_out, grad_tokens, g_vecs[0], g_vecs[1], grad_q, grad_k, grad_v, grad_s, grad_o,
        g_vecs[2], g_vecs[3], grad_g, grad_u, grad_d,
    )


def solution(mesh):
    n = mesh.shape[AXIS]
    row, vec = P(AXIS, None), P(AXIS)
    ins = (row, row, vec, vec, row, row, row, row, row, vec, vec, row, row, row, row)
    outs = (row, row, vec, vec, row, row, row, row, row, vec, vec, row, row, row)

    def body(*args):
        return on_device(n, *args)

    return jax.shard_map(body, mesh=mesh, in_specs=ins, out_specs=outs, check_vma=False)
```

```python
import functools
import math

import jax
import jax.numpy as jnp
from jax import lax
from jax.experimental import pallas as pl
from jax.experimental.pallas import tpu as pltpu
from jax.sharding import PartitionSpec as P


KH = 256
VH = 512
TP = 8
AXIS = "fsdp"
MESH = pl.DeviceIdType.MESH
ANY = pl.BlockSpec(memory_space=pl.ANY)
VMEM = pl.BlockSpec(memory_space=pltpu.VMEM)
bf = jnp.bfloat16
f32 = jnp.float32
SDS = jax.ShapeDtypeStruct


def place():
    me = lax.axis_index(AXIS)
    steps = [s - 2 * s * lax.rem(lax.div(me, s), 2) for s in (1, 2, 4)]

    def peer(k):
        out = me
        for bit, step in enumerate(steps):
            if k >> bit & 1:
                out = out + step
        return out

    return me, peer


def greet(peers):
    barrier = pltpu.get_barrier_semaphore()
    for p in peers:
        pl.semaphore_signal(barrier, inc=1, device_id=(p,), device_id_type=MESH)
    pl.semaphore_wait(barrier, len(peers))


def remote(src, dst, sems, i, dev):
    return pltpu.make_async_remote_copy(
        src_ref=src, dst_ref=dst, send_sem=sems[0].at[i], recv_sem=sems[1].at[i],
        device_id=(dev,), device_id_type=MESH,
    )


GATHER_SEMS = 13


def gather_blocks(own, out, sems, base, local, peer):
    h = own.shape[0] // 2
    top, bot = pl.ds(0, h), pl.ds(h, h)
    pc, px, py = peer(1), peer(2), peer(4)
    made = []

    def send(src, dst, dev):
        copy = remote(src, dst, sems, base + len(made), dev)
        copy.start()
        made.append(copy)
        return copy

    x0 = send(own.at[bot], out.at[2, bot], px)
    y0 = send(own.at[top], out.at[4, top], py)
    x1 = send(own.at[top], out.at[2, top], px)
    y1 = send(own.at[bot], out.at[4, bot], py)
    core = [send(own, out.at[1], pc)]
    keep = pltpu.make_async_copy(own, out.at[0], local)
    keep.start()
    x0.wait_recv()
    fy = send(out.at[2, bot], out.at[6, bot], py)
    core.append(send(out.at[2, bot], out.at[3, bot], pc))
    y0.wait_recv()
    fx = send(out.at[4, top], out.at[6, top], px)
    core.append(send(out.at[4, top], out.at[5, top], pc))
    x1.wait_recv()
    core.append(send(out.at[2, top], out.at[3, top], pc))
    y1.wait_recv()
    core.append(send(out.at[4, bot], out.at[5, bot], pc))
    fy.wait_recv()
    core.append(send(out.at[6, bot], out.at[7, bot], pc))
    fx.wait_recv()
    core.append(send(out.at[6, top], out.at[7, top], pc))
    for copy in core:
        copy.wait_recv()
    for copy in made:
        copy.wait_send()
    keep.wait()


def gather_kernel(x_ref, out_ref, ssem, rsem, local):
    _, peer = place()
    greet([peer(1), peer(2), peer(4)])
    gather_blocks(x_ref, out_ref, (ssem, rsem), 0, local, peer)


def plane_gather(x, cid):
    r, c = x.shape
    return pl.pallas_call(
        gather_kernel,
        out_shape=SDS((TP, r, c), x.dtype),
        in_specs=[VMEM],
        out_specs=ANY,
        scratch_shapes=[
            pltpu.SemaphoreType.DMA((GATHER_SEMS,)),
            pltpu.SemaphoreType.DMA((GATHER_SEMS,)),
            pltpu.SemaphoreType.DMA,
        ],
        compiler_params=pltpu.CompilerParams(
            collective_id=cid, has_side_effects=True, vmem_limit_bytes=8 << 20
        ),
    )(x)


def send_columns(src, out, cols, at, sems, base, local, t, peer, rows=None):
    copies = []
    rows = slice(None) if rows is None else rows

    def block(q):
        if len(src.shape) == 3:
            return src.at[q]
        return src.at[rows, pl.ds(pl.multiple_of(q * cols, 128), cols)]

    for k in range(1, TP):
        dev = peer(k)
        copy = remote(
            block(lax.rem(dev, TP)), out.at[t, :, pl.ds(at, cols)], sems, base + k - 1, dev
        )
        copy.start()
        copies.append(copy)
    keep = pltpu.make_async_copy(block(t), out.at[t, :, pl.ds(at, cols)], local)
    keep.start()
    return copies, keep


def finish(parts):
    for copies, keep in parts:
        for copy in copies:
            copy.wait()
        keep.wait()


def exchange_call(kernel, outs, args, sems, locals_, cid):
    return pl.pallas_call(
        kernel,
        out_shape=outs,
        in_specs=[VMEM] * len(args),
        out_specs=tuple(ANY for _ in outs),
        scratch_shapes=[
            pltpu.SemaphoreType.DMA((sems,)),
            pltpu.SemaphoreType.DMA((sems,)),
            pltpu.SemaphoreType.DMA((locals_,)),
        ],
        compiler_params=pltpu.CompilerParams(
            collective_id=cid, has_side_effects=True, vmem_limit_bytes=12 << 20
        ),
    )(*args)


def first_kernel(wq, wk, wo, out, ssem, rsem, local):
    me, peer = place()
    t = lax.rem(me, TP)
    greet([peer(k) for k in range(1, TP)])
    sems = (ssem, rsem)
    shard, cq, co = wq.shape[0], wq.shape[1] // TP, wo.shape[1] // TP
    low, high = pl.ds(0, shard), pl.ds(shard, shard)
    finish([
        send_columns(wq, out, cq, 0, sems, 0, local.at[0], t, peer),
        send_columns(wk, out, cq, cq, sems, 7, local.at[1], t, peer),
        send_columns(wo, out, co, 2 * cq, sems, 14, local.at[2], t, peer, low),
        send_columns(wo, out, co, 2 * cq + co, sems, 21, local.at[3], t, peer, high),
    ])


def first_exchange(wq, wk, wo, cid):
    width = 2 * wq.shape[1] // TP + 2 * wo.shape[1] // TP
    outs = (SDS((TP, wq.shape[0], width), bf),)
    return exchange_call(first_kernel, outs, (wq, wk, wo), 28, 4, cid)[0]


def second_kernel(n, wv, ws, vec, out, vec_out, ssem, rsem, local):
    dp = n // TP
    me, peer = place()
    t, g = lax.rem(me, TP), lax.div(me, TP)
    others = [lax.rem(me + TP * j, n) for j in range(1, dp)]
    greet([peer(k) for k in range(1, TP)] + others)
    sems = (ssem, rsem)
    cols = wv.shape[1] // TP
    far = []
    keep = pltpu.make_async_copy(vec, vec_out.at[g, t], local.at[2])
    keep.start()
    for j, dev in enumerate(others):
        copy = remote(vec, vec_out.at[g, t], sems, 21 + j, dev)
        copy.start()
        far.append(copy)
    parts = [
        send_columns(wv, out, cols, 0, sems, 0, local.at[0], t, peer),
        send_columns(ws, out, cols, cols, sems, 7, local.at[1], t, peer),
    ]
    for copy in far:
        copy.wait()
    keep.wait()
    near = []
    for k in range(1, TP):
        copy = remote(vec_out.at[:, t], vec_out.at[:, t], sems, 13 + k, peer(k))
        copy.start()
        near.append(copy)
    finish(parts)
    for copy in near:
        copy.wait()


def second_exchange(n, wv, ws, vec, cid):
    outs = (
        SDS((TP, wv.shape[0], 2 * wv.shape[1] // TP), bf),
        SDS((n // TP, TP) + vec.shape, f32),
    )
    kernel = functools.partial(second_kernel, n)
    return exchange_call(kernel, outs, (wv, ws, vec), 21 + n // TP, 3, cid)


def third_kernel(gu, tok, gu_out, tok_out, ssem, rsem, local):
    me, peer = place()
    t = lax.rem(me, TP)
    greet([peer(k) for k in range(1, TP)])
    sems = (ssem, rsem)
    gather_blocks(tok, tok_out, sems, 7, local.at[1], peer)
    finish([send_columns(gu, gu_out, gu.shape[2], 0, sems, 0, local.at[0], t, peer)])


def third_exchange(gu, tok, cid):
    outs = (SDS(gu.shape, bf), SDS((TP,) + tok.shape, bf))
    return exchange_call(third_kernel, outs, (gu, tok), 7 + GATHER_SEMS, 2, cid)


def vector_sum_kernel(n, v_ref, out_ref, near, far, part, ssem, rsem):
    dp = n // TP
    me, peer = place()
    g = lax.div(me, TP)
    width = out_ref.shape[1]
    sems = (ssem, rsem)
    others = [lax.rem(me + TP * j, n) for j in range(1, dp)]
    greet([peer(k) for k in range(1, TP)] + others)
    copies = []
    for j, dev in enumerate(others):
        at = pl.multiple_of(lax.div(dev, TP) * width, 128)
        copy = remote(v_ref.at[:, pl.ds(at, width)], far.at[j], sems, j, dev)
        copy.start()
        copies.append(copy)
    total = v_ref[:, pl.ds(pl.multiple_of(g * width, 128), width)]
    for j, copy in enumerate(copies):
        copy.wait()
        total = total + far[j]
    part[...] = total
    copies = []
    for k in range(1, TP):
        copy = remote(part, near.at[k - 1], sems, dp + k - 1, peer(k))
        copy.start()
        copies.append(copy)
    for k, copy in enumerate(copies):
        copy.wait()
        total = total + near[k]
    out_ref[...] = total


def vector_sum(n, v, cid):
    dp = n // TP
    width = v.shape[1] // dp
    return pl.pallas_call(
        functools.partial(vector_sum_kernel, n),
        out_shape=SDS((v.shape[0], width), f32),
        in_specs=[VMEM],
        out_specs=VMEM,
        scratch_shapes=[
            pltpu.VMEM((TP - 1, v.shape[0], width), f32),
            pltpu.VMEM((dp, v.shape[0], width), f32),
            pltpu.VMEM((v.shape[0], width), f32),
            pltpu.SemaphoreType.DMA((dp + TP,)),
            pltpu.SemaphoreType.DMA((dp + TP,)),
        ],
        compiler_params=pltpu.CompilerParams(
            collective_id=cid, has_side_effects=True, vmem_limit_bytes=4 << 20
        ),
        name="vector_sum",
    )(v)


REDUCE_SEMS = 10
TILE = 512


def reduce_blocks(product, po, pe, rc, sb, xr, yr, sems, peer, prepare=None):
    r = pe.shape[1]
    h = r // 2
    top, bot = pl.ds(0, h), pl.ds(h, h)
    pc, px, py = peer(1), peer(2), peer(4)
    sent = []

    def send(src, dst, dev, i):
        copy = remote(src, dst, sems, i, dev)
        copy.start()
        sent.append(copy)
        return copy

    def pair(i):
        k = 2 * i
        if prepare is not None:
            prepare(k)
        product(k + 1, po.at[i])
        copy = send(po.at[i], rc.at[i], pc, i)
        product(k, pe.at[i])
        return copy

    def add(dst, part, got, out=None):
        step = 32

        @pl.loop(0, part.size // step)
        def _(j):
            here = pl.ds(pl.multiple_of(part.start + j * step, step), step)
            there = pl.ds(pl.multiple_of(j * step, step), step)
            total = dst[here, :] + got[there, :].astype(f32)
            if out is None:
                dst[here, :] = total
            else:
                out[there, :] = total.astype(bf)

    c6 = pair(3)
    c2 = pair(1)
    c6.wait_recv()
    add(pe.at[3], top, rc.at[3, top], sb.at[0])
    x6 = send(sb.at[0], xr.at[0], px, 4)
    add(pe.at[3], bot, rc.at[3, bot], sb.at[1])
    y6 = send(sb.at[1], yr.at[0], py, 5)
    c4 = pair(2)
    c2.wait_recv()
    add(pe.at[1], top, rc.at[1, top], sb.at[2])
    x2 = send(sb.at[2], xr.at[1], px, 6)
    add(pe.at[1], bot, rc.at[1, bot])
    c0 = pair(0)
    c4.wait_recv()
    add(pe.at[2], bot, rc.at[2, bot], sb.at[3])
    y4 = send(sb.at[3], yr.at[1], py, 7)
    add(pe.at[2], top, rc.at[2, top])
    c0.wait_recv()
    x6.wait_recv()
    add(pe.at[2], top, xr.at[0], sb.at[4])
    y4b = send(sb.at[4], yr.at[2], py, 8)
    y6.wait_recv()
    add(pe.at[1], bot, yr.at[0], sb.at[5])
    x2b = send(sb.at[5], xr.at[2], px, 9)
    x2.wait_recv()
    y4.wait_recv()
    y4b.wait_recv()
    x2b.wait_recv()

    def total(at, half_at, lower):
        first, second = (yr, xr) if lower else (xr, yr)
        return (
            pe[0, at, :]
            + rc[0, at, :].astype(f32)
            + first[1, half_at, :].astype(f32)
            + second[2, half_at, :].astype(f32)
        )

    def for_rows(step, body):
        for lower in (False, True):

            @pl.loop(0, h // step)
            def _(j, lower=lower):
                half_at = pl.ds(pl.multiple_of(j * step, step), step)
                at = pl.ds(pl.multiple_of(j * step + (h if lower else 0), step), step)
                body(at, total(at, half_at, lower))

    return for_rows, sent


def reduce_scratch(r, c):
    h = r // 2
    return [
        pltpu.VMEM((4, r, c), bf),
        pltpu.VMEM((4, r, c), f32),
        pltpu.VMEM((4, r, c), bf),
        pltpu.VMEM((6, h, c), bf),
        pltpu.VMEM((3, h, c), bf),
        pltpu.VMEM((3, h, c), bf),
    ]


def times(a, w, nt):
    def product(k, dst):
        @pl.loop(0, dst.shape[1] // TILE)
        def _(j):
            at = pl.ds(pl.multiple_of(j * TILE, TILE), TILE)
            if nt:
                y = lax.dot_general(
                    a[k], w[at, :], (((1,), (1,)), ((), ())), preferred_element_type=f32
                )
            else:
                y = jnp.dot(a[k], w[:, at], preferred_element_type=f32)
            dst[:, at] = y.astype(dst.dtype)

    return product


def reduce_kernel(nt, a, w, out_ref, po, pe, rc, sb, xr, yr, ssem, rsem):
    _, peer = place()
    greet([peer(1), peer(2), peer(4)])
    product = times(a, w, nt)
    for_rows, sent = reduce_blocks(product, po, pe, rc, sb, xr, yr, (ssem, rsem), peer)

    def body(at, value):
        out_ref[at, :] = value

    for_rows(32, body)
    for copy in sent:
        copy.wait_send()


def matmul_reduce(a, w, nt, cid):
    _, r, _ = a.shape
    c = w.shape[0] if nt else w.shape[1]
    return pl.pallas_call(
        functools.partial(reduce_kernel, nt),
        out_shape=SDS((r, c), f32),
        in_specs=[VMEM] * 2,
        out_specs=VMEM,
        scratch_shapes=reduce_scratch(r, c)
        + [pltpu.SemaphoreType.DMA((REDUCE_SEMS,)), pltpu.SemaphoreType.DMA((REDUCE_SEMS,))],
        compiler_params=pltpu.CompilerParams(
            collective_id=cid, has_side_effects=True, vmem_limit_bytes=48 << 20
        ),
    )(a, w)


def forward_kernel(
    nrm, wvs, sco, w, tok, vec, v_out, mix_out, ret_out, swi_out, mid, out,
    v_buf, mix_buf, ret_buf, swi_buf, po, pe, rc, sb, xr, yr, own, ssem, rsem, local,
):
    _, peer = place()
    greet([peer(1), peer(2), peer(4)])
    sems = (ssem, rsem)
    r, width = v_buf.shape[1:]
    kept = []

    def prepare(first):
        @pl.loop(0, 2)
        def _(i):
            k = first + i

            @pl.loop(0, width // 256)
            def _(j):
                at = pl.ds(pl.multiple_of(j * 256, 256), 256)
                behind = pl.ds(pl.multiple_of(j * 256 + width, 256), 256)
                v = jnp.dot(nrm[k], wvs[:, at], preferred_element_type=f32).astype(bf)
                v_buf[k, :, at] = v
                swi_buf[k, :, at] = jnp.dot(nrm[k], wvs[:, behind], preferred_element_type=f32)
                ret_buf[k, :, at] = jnp.dot(sco[k], v, preferred_element_type=f32)

            @pl.loop(0, r // 32)
            def _(j):
                at = pl.ds(pl.multiple_of(j * 32, 32), 32)
                value = ret_buf[k, at, :]
                centred = value - jnp.mean(value, axis=-1, keepdims=True)
                spread = jnp.mean(centred * centred, axis=-1, keepdims=True)
                gate = swi_buf[k, at, :]
                gate = gate / (1.0 + jnp.exp(-gate))
                mix_buf[k, at, :] = (
                    gate * (centred * lax.rsqrt(jnp.maximum(spread, 0.25)))
                ).astype(bf)

        two = pl.ds(first, 2)
        for i, (src, dst) in enumerate(
            ((v_buf, v_out), (mix_buf, mix_out), (ret_buf, ret_out), (swi_buf, swi_out))
        ):
            copy = pltpu.make_async_copy(
                src.at[two], dst.at[two], local.at[1 + 2 * first + i]
            )
            copy.start()
            kept.append(copy)

    def product(k, dst):
        step = w.shape[2]

        @pl.loop(0, w.shape[0])
        def _(j):
            at = pl.ds(pl.multiple_of(j * step, step), step)
            dst[:, at] = jnp.dot(mix_buf[k], w[j], preferred_element_type=f32).astype(dst.dtype)

    for_rows, sent = reduce_blocks(product, po, pe, rc, sb, xr, yr, sems, peer, prepare)

    def body(at, value):
        value = value + tok[at, :].astype(f32)
        mid[at, :] = value
        center = jnp.mean(value, axis=-1, keepdims=True)
        centred = value - center
        spread = jnp.mean(centred * centred, axis=-1, keepdims=True)
        own[at, :] = (
            centred * lax.rsqrt(spread + 1e-05) * vec[0:1, :] + vec[1:2, :]
        ).astype(bf)

    for_rows(16, body)
    gather_blocks(own, out, sems, REDUCE_SEMS, local.at[0], peer)
    for copy in sent:
        copy.wait_send()
    for copy in kept:
        copy.wait()


def forward_exchange(nrm, wvs, sco, w, tok, vec, cid):
    _, r, d = nrm.shape
    width = w.shape[1]
    count = REDUCE_SEMS + GATHER_SEMS
    blocks = [((TP, r, width), t) for t in (bf, bf, f32, f32)]
    return pl.pallas_call(
        forward_kernel,
        out_shape=tuple(SDS(*b) for b in blocks) + (SDS((r, d), f32), SDS((TP, r, d), bf)),
        in_specs=[VMEM] * 6,
        out_specs=(ANY,) * 4 + (VMEM, ANY),
        scratch_shapes=[pltpu.VMEM(*b) for b in blocks]
        + reduce_scratch(r, d)
        + [
            pltpu.VMEM((r, d), bf),
            pltpu.SemaphoreType.DMA((count,)),
            pltpu.SemaphoreType.DMA((count,)),
            pltpu.SemaphoreType.DMA((17,)),
        ],
        compiler_params=pltpu.CompilerParams(
            collective_id=cid, has_side_effects=True, vmem_limit_bytes=60 << 20
        ),
        name="forward_exchange",
    )(nrm, wvs, sco, w, tok, vec)


def hidden_kernel(x, gu, hid, act_out, slope_out):
    width = hid.shape[2]
    step = 256

    @pl.loop(0, width // step)
    def _(j):
        at = pl.ds(pl.multiple_of(j * step, step), step)
        behind = pl.ds(pl.multiple_of(j * step + width, step), step)
        first = jnp.dot(x[0], gu[:, at], preferred_element_type=f32)
        second = jnp.dot(x[0], gu[:, behind], preferred_element_type=f32)
        share = 0.5 * (1.0 + lax.erf(first * math.sqrt(0.5)))
        act = first * share
        slope = share + first * (jnp.exp(-0.5 * first * first) * (1.0 / math.sqrt(2.0 * math.pi)))
        hid[0, :, at] = (act * second).astype(bf)
        act_out[0, :, at] = act
        slope_out[0, :, at] = slope * second


def hidden_units(x, gu):
    _, r, d = x.shape
    width = gu.shape[1] // 2
    row = pl.BlockSpec((1, r, width), lambda k: (k, 0, 0))
    return pl.pallas_call(
        hidden_kernel,
        grid=(TP,),
        out_shape=tuple(SDS((TP, r, width), t) for t in (bf, f32, f32)),
        in_specs=[
            pl.BlockSpec((1, r, d), lambda k: (k, 0, 0)),
            pl.BlockSpec(gu.shape, lambda k: (0, 0)),
        ],
        out_specs=(row, row, row),
        compiler_params=pltpu.CompilerParams(vmem_limit_bytes=32 << 20),
        cost_estimate=pl.CostEstimate(
            flops=4 * TP * r * d * width, bytes_accessed=24 << 20, transcendentals=2 * TP * r * width
        ),
        name="hidden_units",
    )(x, gu)


def hidden_back_kernel(cot, down, act, slope, out):
    width = act.shape[2]
    step = 256

    @pl.loop(0, width // step)
    def _(j):
        at = pl.ds(pl.multiple_of(j * step, step), step)
        behind = pl.ds(pl.multiple_of(j * step + width, step), step)
        grad = lax.dot_general(
            cot[0], down[at, :], (((1,), (1,)), ((), ())), preferred_element_type=f32
        )
        out[0, :, at] = (grad * slope[0, :, at]).astype(bf)
        out[0, :, behind] = (grad * act[0, :, at]).astype(bf)


def hidden_back(cot, down, act, slope):
    _, r, d = cot.shape
    width = act.shape[2]
    row = pl.BlockSpec((1, r, width), lambda k: (k, 0, 0))
    return pl.pallas_call(
        hidden_back_kernel,
        grid=(TP,),
        out_shape=SDS((TP, r, 2 * width), bf),
        in_specs=[
            pl.BlockSpec((1, r, d), lambda k: (k, 0, 0)),
            pl.BlockSpec(down.shape, lambda k: (0, 0)),
            row,
            row,
        ],
        out_specs=pl.BlockSpec((1, r, 2 * width), lambda k: (k, 0, 0)),
        compiler_params=pltpu.CompilerParams(vmem_limit_bytes=32 << 20),
        cost_estimate=pl.CostEstimate(
            flops=2 * TP * r * d * width, bytes_accessed=24 << 20, transcendentals=0
        ),
        name="hidden_back",
    )(cot, down, act, slope)


def backward_kernel(
    a, w, mid, cot, vec, gmid, out, sums, po, pe, rc, sb, xr, yr, own, acc, ssem, rsem, local
):
    _, peer = place()
    greet([peer(1), peer(2), peer(4)])
    sems = (ssem, rsem)
    acc[...] = jnp.zeros_like(acc)
    for_rows, sent = reduce_blocks(times(a, w, True), po, pe, rc, sb, xr, yr, sems, peer)

    def body(at, g):
        value = mid[at, :]
        center = jnp.mean(value, axis=-1, keepdims=True)
        centred = value - center
        inv = lax.rsqrt(jnp.mean(centred * centred, axis=-1, keepdims=True) + 1e-05)
        hat = centred * inv
        acc[0] += g * hat
        acc[1] += g
        scaled = g * vec[0:1, :]
        mean_g = jnp.mean(scaled, axis=-1, keepdims=True)
        mean_gh = jnp.mean(scaled * hat, axis=-1, keepdims=True)
        grad = cot[at, :].astype(f32) + inv * (scaled - mean_g - hat * mean_gh)
        gmid[at, :] = grad
        own[at, :] = grad.astype(bf)

    for_rows(16, body)
    gather_blocks(own, out, sems, REDUCE_SEMS, local, peer)
    sums[0:1, :] = jnp.sum(acc[0], axis=0, keepdims=True)
    sums[1:2, :] = jnp.sum(acc[1], axis=0, keepdims=True)
    for copy in sent:
        copy.wait_send()


def backward_exchange(a, w, mid, cot, vec, cid):
    _, r, _ = a.shape
    c = w.shape[0]
    count = REDUCE_SEMS + GATHER_SEMS
    return pl.pallas_call(
        backward_kernel,
        out_shape=(SDS((r, c), f32), SDS((TP, r, c), bf), SDS((2, c), f32)),
        in_specs=[VMEM] * 5,
        out_specs=(VMEM, ANY, VMEM),
        scratch_shapes=reduce_scratch(r, c)
        + [
            pltpu.VMEM((r, c), bf),
            pltpu.VMEM((2, 16, c), f32),
            pltpu.SemaphoreType.DMA((count,)),
            pltpu.SemaphoreType.DMA((count,)),
            pltpu.SemaphoreType.DMA,
        ],
        compiler_params=pltpu.CompilerParams(
            collective_id=cid, has_side_effects=True, vmem_limit_bytes=52 << 20
        ),
        name="backward_exchange",
    )(a, w, mid, cot, vec)


def tp_groups(n):
    return [[g * TP + t for t in range(TP)] for g in range(n // TP)]


def dp_groups(n):
    return [[g * TP + t for g in range(n // TP)] for t in range(TP)]


def plane_a2a(x, n):
    return lax.all_to_all(x, AXIS, 0, 0, axis_index_groups=tp_groups(n), tiled=True)


def dp_gather(x, n):
    return lax.all_gather(x, AXIS, axis=0, tiled=True, axis_index_groups=dp_groups(n))


def dp_reduce(x, n):
    return lax.psum_scatter(
        x, AXIS, scatter_dimension=0, tiled=True, axis_index_groups=dp_groups(n)
    )


def layer_norm(value, gain, bias):
    center = jnp.mean(value, axis=-1, keepdims=True)
    centred = value - center
    spread = jnp.mean(centred * centred, axis=-1, keepdims=True)
    return centred * lax.rsqrt(spread + 1e-05) * gain + bias


def seq_positions(lengths, rows):
    ends = jnp.cumsum(lengths, axis=1)
    starts = ends - lengths
    index = jnp.arange(rows, dtype=jnp.int32)
    segment = jnp.sum((index[None, :, None] >= ends[:, None, :]).astype(jnp.int32), axis=2)
    member = segment[:, :, None] == jnp.arange(lengths.shape[1], dtype=jnp.int32)
    offset = index[None, :] - jnp.sum(jnp.where(member, starts[:, None, :], 0), axis=2)
    return segment, offset


def rotary_tables(offset):
    half = KH // 2
    freq = jnp.exp(-math.log(10000.0) * jnp.arange(half, dtype=f32) / half)
    angle = offset.astype(f32)[..., None] * freq
    return jnp.cos(angle), jnp.sin(angle)


def rotate(value, cosine, sine):
    half = KH // 2
    u, w = value[..., :half], value[..., half:]
    return jnp.concatenate([u * cosine - w * sine, w * cosine + u * sine], axis=-1)


def rotate_back(value, cosine, sine):
    half = KH // 2
    u, w = value[..., :half], value[..., half:]
    return jnp.concatenate([u * cosine + w * sine, w * cosine - u * sine], axis=-1)


def decay_mask(segment, offset, head):
    diff = offset[:, :, None] - offset[:, None, :]
    valid = (segment[:, :, None] == segment[:, None, :]) & (diff >= 0)
    steps = jnp.where(valid, diff, 0).astype(f32)
    log = jnp.log(1.0 - jnp.exp2(-5.0 - head.astype(f32)))
    return jnp.where(valid, jnp.exp(log * steps), 0.0) / math.sqrt(KH)


def group_gate(retained, swish_in):
    center = jnp.mean(retained, axis=-1, keepdims=True)
    centred = retained - center
    spread = jnp.mean(centred * centred, axis=-1, keepdims=True)
    return jax.nn.silu(swish_in) * (centred * lax.rsqrt(jnp.maximum(spread, 0.25)))


def dot(a, b):
    return lax.dot_general(a, b, (((1,), (0,)), ((), ())), preferred_element_type=f32)


def dot_tn(a, b):
    return lax.dot_general(a, b, (((0,), (0,)), ((), ())), preferred_element_type=f32)


def dot_nt(a, b):
    return lax.dot_general(a, b, (((1,), (1,)), ((), ())), preferred_element_type=f32)


def bmm(eq, a, b):
    return jnp.einsum(eq, a, b, preferred_element_type=f32)


def col_blocks(w):
    r, c = w.shape
    return w.reshape(r, TP, c // TP).transpose(1, 0, 2).reshape(TP * r, c // TP)


def col_join(w, r):
    c = w.shape[1]
    return w.reshape(TP, r, c).transpose(1, 0, 2).reshape(r, TP * c)


def join_kernel(widths, parts, x, *outs):
    at = 0
    for out, width in zip(outs, widths):
        piece = width // parts
        for t in range(TP):
            for p in range(parts):
                to = (p * TP + t) * piece
                out[:, to : to + piece] = x[t, :, at + p * piece : at + (p + 1) * piece].astype(f32)
        at += width


def join(x, widths, parts=1):
    r = x.shape[1]
    if any(width // parts % 128 for width in widths):
        made, at = [], 0
        for width in widths:
            part = x[:, :, at : at + width].reshape(TP, r, parts, width // parts)
            made.append(part.transpose(1, 2, 0, 3).reshape(r, TP * width).astype(f32))
            at += width
        return made
    return pl.pallas_call(
        functools.partial(join_kernel, widths, parts),
        out_shape=tuple(SDS((r, TP * width), f32) for width in widths),
        in_specs=[VMEM],
        out_specs=tuple(VMEM for _ in widths),
        compiler_params=pltpu.CompilerParams(vmem_limit_bytes=8 << 20),
        cost_estimate=pl.CostEstimate(flops=0, bytes_accessed=6 * x.size, transcendentals=0),
        name="join",
    )(x)


def after(x, *deps):
    return lax.optimization_barrier((x,) + deps)[0]


def on_device(n, tokens, lengths, gain1, bias1, wq, wk, wv, ws, wo, gain2, bias2, wg, wu, wd, cot):
    rows, d = tokens.shape
    ff = wg.shape[1]
    dp = n // TP
    shard = d // n
    unit = ff // n
    me = lax.axis_index(AXIS)
    head = lax.rem(me, TP)

    def ff_blocks(w):
        return w.reshape(shard, dp, TP, unit).transpose(2, 0, 1, 3).reshape(TP, shard, dp * unit)

    vec = jnp.zeros((8, 128), f32)
    for i, v in enumerate((gain1, bias1, gain2, bias2)):
        vec = vec.at[i, :shard].set(v.astype(f32))
    vec = vec.at[4, :3].set(lengths[0].astype(f32))
    qko_blk = first_exchange(wq, wk, wo, 1)
    qko = dp_gather(qko_blk.reshape(TP * shard, 4 * KH), n)
    vs_blk, vec_all = second_exchange(n, after(wv, qko_blk), ws, vec, 2)
    vs = dp_gather(vs_blk.reshape(TP * shard, 2 * VH), n)
    gu_in = jnp.concatenate([ff_blocks(wg), ff_blocks(wu)], axis=2)
    gu_blk, tok_all = third_exchange(gu_in, after(tokens, vs_blk), 3)
    gu = dp_gather(gu_blk.reshape(TP * shard, 2 * dp * unit), n)
    down = dp_gather(wd, n)
    cot_all = plane_gather(after(cot, tok_all), 4)
    gain1f, bias1f, gain2f, bias2f = (
        vec_all[:, :, i, :shard].reshape(1, d) for i in range(4)
    )
    vec2 = jnp.concatenate([gain2f, bias2f], axis=0)
    out = qko[:, 2 * KH :].reshape(n, shard, 2, d // TP).transpose(0, 2, 1, 3)
    out_blk = plane_a2a(out.reshape(TP * VH, d // TP), n)

    mine = lax.dynamic_slice_in_dim(vec_all, lax.div(me, TP), 1, 0)[0, :, 4, :3]
    order = jnp.arange(TP, dtype=jnp.int32)
    pick = (order[None, :] == (order[:, None] ^ head)).astype(f32)
    len_all = jnp.sum(pick[:, :, None] * mine[None], axis=1).astype(jnp.int32)
    segment, offset = seq_positions(len_all, rows)
    cosine, sine = rotary_tables(offset)
    mask = decay_mask(segment, offset, head)

    normed = layer_norm(tok_all.reshape(TP * rows, d).astype(f32), gain1f, bias1f).astype(bf)
    qk_out = dot(normed, qko[:, : 2 * KH]).reshape(TP, rows, 2 * KH)
    query, key = qk_out[..., :KH], qk_out[..., KH:]
    q_rot = rotate(query, cosine, sine).astype(bf)
    k_rot = rotate(key, cosine, sine).astype(bf)
    plain = bmm("btd,bsd->bts", q_rot, k_rot)
    scores = (plain * mask).astype(bf)
    v_low, mixed, retained, swish_in, middle, normed2 = forward_exchange(
        normed.reshape(TP, rows, d), vs, scores, out_blk.reshape(TP, VH, d // TP), tokens, vec2, 5
    )
    out = col_join(out_blk, VH)
    hidden, act, slope = hidden_units(normed2, gu)
    normed2 = normed2.reshape(TP * rows, d)
    down_grad = dot_tn(hidden.reshape(TP * rows, dp * unit), cot_all.reshape(TP * rows, d)).astype(bf)
    g_down = dp_reduce(down_grad, n)

    g_fs = hidden_back(cot_all, down, act, slope)
    gu_grad = dot_tn(normed2, g_fs.reshape(TP * rows, 2 * dp * unit)).astype(bf)
    g_gu = dp_reduce(gu_grad, n)
    g_middle, g_low, sums2 = backward_exchange(g_fs, gu, middle, cot, vec2, 6)

    g_low = g_low.reshape(TP * rows, d)
    mixed = mixed.reshape(TP * rows, VH)
    g_mixed = dot_nt(g_low, out).reshape(TP, rows, VH)
    _, pull_group = jax.vjp(group_gate, retained, swish_in)
    g_retained, g_swish = pull_group(g_mixed)
    g_retained = g_retained.astype(bf)
    g_swish = g_swish.astype(bf)
    swish_grad = dot_tn(normed, g_swish.reshape(TP * rows, VH)).astype(bf)
    g_swi = dp_reduce(swish_grad, n)
    out_grad = dot_tn(mixed, g_low).astype(bf)
    out_grad = plane_a2a(col_blocks(out_grad), n)
    g_value = bmm("bts,btd->bsd", scores, g_retained).astype(bf)
    g_scores = bmm("btd,bsd->bts", g_retained, v_low)
    g_plain = (g_scores * mask).astype(bf)
    g_qrot = bmm("bts,bsd->btd", g_plain, k_rot)
    g_krot = bmm("bts,btd->bsd", g_plain, q_rot)
    g_query = rotate_back(g_qrot, cosine, sine).astype(bf)
    g_key = rotate_back(g_krot, cosine, sine).astype(bf)
    g_qkv = jnp.concatenate([g_query, g_key, g_value], axis=2)
    qkv_grad = dot_tn(normed, g_qkv.reshape(TP * rows, 2 * KH + VH)).astype(bf)
    g_qkv_own = dp_reduce(qkv_grad, n)
    g_out = dp_reduce(out_grad, n)
    g_qkvs = jnp.concatenate([g_qkv, g_swish], axis=2)
    w_qkvs = jnp.concatenate([qko[:, : 2 * KH], vs], axis=1)
    g_normed = matmul_reduce(g_qkvs, w_qkvs, True, 7)
    inputs = tokens.astype(f32)
    _, pull_norm1 = jax.vjp(layer_norm, inputs, gain1f, bias1f)
    g_in_part, g_gain1, g_bias1 = pull_norm1(g_normed)
    grad_tokens = g_middle + g_in_part
    ffn = matmul_reduce(hidden, down, False, 8)
    layer_out = (middle + ffn).astype(bf)

    g_vecs = jnp.concatenate([g_gain1, g_bias1, sums2, jnp.zeros((4, d), f32)], axis=0)
    g_vecs = vector_sum(n, g_vecs, 9)
    g_vecs = lax.dynamic_slice_in_dim(g_vecs, head * shard, shard, 1)
    grad_d = g_down.astype(f32)
    g_gu = plane_a2a(g_gu, n)
    grad_g, grad_u = join(g_gu.reshape(TP, shard, 2 * dp * unit), (dp * unit,) * 2, dp)
    g_swi = plane_a2a(g_swi, n)
    (grad_s,) = join(g_swi.reshape(TP, shard, VH), (VH,))
    g_qkv_own = plane_a2a(g_qkv_own, n)
    grad_q, grad_k, grad_v = join(g_qkv_own.reshape(TP, shard, 2 * KH + VH), (KH, KH, VH))
    g_out = plane_a2a(g_out, n)
    (grad_o,) = join(g_out.reshape(TP, wo.shape[0], d // TP), (d // TP,))
    return (
        layer_out, grad_tokens, g_vecs[0], g_vecs[1], grad_q, grad_k, grad_v, grad_s, grad_o,
        g_vecs[2], g_vecs[3], grad_g, grad_u, grad_d,
    )


def solution(mesh):
    n = mesh.shape[AXIS]
    row, vec = P(AXIS, None), P(AXIS)
    ins = (row, row, vec, vec, row, row, row, row, row, vec, vec, row, row, row, row)
    outs = (row, row, vec, vec, row, row, row, row, row, vec, vec, row, row, row)

    def body(*args):
        return on_device(n, *args)

    return jax.shard_map(body, mesh=mesh, in_specs=ins, out_specs=outs, check_vma=False)
```

```python
import functools
import math

import jax
import jax.numpy as jnp
from jax import lax
from jax.experimental import pallas as pl
from jax.experimental.pallas import tpu as pltpu
from jax.sharding import PartitionSpec as P


KH = 256
VH = 512
TP = 8
AXIS = "fsdp"
MESH = pl.DeviceIdType.MESH
ANY = pl.BlockSpec(memory_space=pl.ANY)
VMEM = pl.BlockSpec(memory_space=pltpu.VMEM)
bf = jnp.bfloat16
f32 = jnp.float32
SDS = jax.ShapeDtypeStruct


def place():
    me = lax.axis_index(AXIS)
    steps = [s - 2 * s * lax.rem(lax.div(me, s), 2) for s in (1, 2, 4)]

    def peer(k):
        out = me
        for bit, step in enumerate(steps):
            if k >> bit & 1:
                out = out + step
        return out

    return me, peer


def greet(peers):
    barrier = pltpu.get_barrier_semaphore()
    for p in peers:
        pl.semaphore_signal(barrier, inc=1, device_id=(p,), device_id_type=MESH)
    pl.semaphore_wait(barrier, len(peers))


def remote(src, dst, sems, i, dev):
    return pltpu.make_async_remote_copy(
        src_ref=src, dst_ref=dst, send_sem=sems[0].at[i], recv_sem=sems[1].at[i],
        device_id=(dev,), device_id_type=MESH,
    )


GATHER_SEMS = 13


class Gather:
    def __init__(self, own, out, start, size, sems, base, local, peer):
        self.own, self.out, self.sems, self.base, self.local = own, out, sems, base, local
        h = size // 2
        self.all, self.top, self.bot = pl.ds(start, size), pl.ds(start, h), pl.ds(start + h, h)
        self.pc, self.px, self.py = peer(1), peer(2), peer(4)
        self.made = []

    def send(self, src, dst, dev):
        copy = remote(src, dst, self.sems, self.base + len(self.made), dev)
        copy.start()
        self.made.append(copy)
        return copy

    def pass_on(self, k, at):
        self.core.append(self.send(self.out.at[k, at], self.out.at[k + 1, at], self.pc))

    def start(self):
        own, out, top, bot = self.own, self.out, self.top, self.bot
        self.x0 = self.send(own.at[bot], out.at[2, bot], self.px)
        self.y0 = self.send(own.at[top], out.at[4, top], self.py)
        self.x1 = self.send(own.at[top], out.at[2, top], self.px)
        self.y1 = self.send(own.at[bot], out.at[4, bot], self.py)
        self.core = [self.send(own.at[self.all], out.at[1, self.all], self.pc)]
        self.keep = pltpu.make_async_copy(own.at[self.all], out.at[0, self.all], self.local)
        self.keep.start()

    def forward(self):
        out, top, bot = self.out, self.top, self.bot
        self.x0.wait_recv()
        self.fy = self.send(out.at[2, bot], out.at[6, bot], self.py)
        self.pass_on(2, bot)
        self.y0.wait_recv()
        self.fx = self.send(out.at[4, top], out.at[6, top], self.px)
        self.pass_on(4, top)
        self.x1.wait_recv()
        self.pass_on(2, top)
        self.y1.wait_recv()
        self.pass_on(4, bot)

    def finish(self):
        self.fy.wait_recv()
        self.pass_on(6, self.bot)
        self.fx.wait_recv()
        self.pass_on(6, self.top)
        for copy in self.core:
            copy.wait_recv()
        for copy in self.made:
            copy.wait_send()
        self.keep.wait()


def gather_blocks(own, out, sems, base, local, peer):
    gather = Gather(own, out, 0, own.shape[0], sems, base, local, peer)
    gather.start()
    gather.forward()
    gather.finish()


def gather_kernel(x_ref, out_ref, ssem, rsem, local):
    _, peer = place()
    greet([peer(1), peer(2), peer(4)])
    gather_blocks(x_ref, out_ref, (ssem, rsem), 0, local, peer)


def plane_gather(x, cid):
    r, c = x.shape
    return pl.pallas_call(
        gather_kernel,
        out_shape=SDS((TP, r, c), x.dtype),
        in_specs=[VMEM],
        out_specs=ANY,
        scratch_shapes=[
            pltpu.SemaphoreType.DMA((GATHER_SEMS,)),
            pltpu.SemaphoreType.DMA((GATHER_SEMS,)),
            pltpu.SemaphoreType.DMA,
        ],
        compiler_params=pltpu.CompilerParams(
            collective_id=cid, has_side_effects=True, vmem_limit_bytes=8 << 20
        ),
    )(x)


def send_columns(src, out, cols, at, sems, base, local, t, peer, rows=None):
    copies = []
    rows = slice(None) if rows is None else rows

    def block(q):
        if len(src.shape) == 3:
            return src.at[q]
        return src.at[rows, pl.ds(pl.multiple_of(q * cols, 128), cols)]

    for k in range(1, TP):
        dev = peer(k)
        copy = remote(
            block(lax.rem(dev, TP)), out.at[t, :, pl.ds(at, cols)], sems, base + k - 1, dev
        )
        copy.start()
        copies.append(copy)
    keep = pltpu.make_async_copy(block(t), out.at[t, :, pl.ds(at, cols)], local)
    keep.start()
    return copies, keep


def finish(parts):
    for copies, keep in parts:
        for copy in copies:
            copy.wait()
        keep.wait()


def exchange_call(kernel, outs, args, sems, locals_, cid):
    return pl.pallas_call(
        kernel,
        out_shape=outs,
        in_specs=[VMEM] * len(args),
        out_specs=tuple(ANY for _ in outs),
        scratch_shapes=[
            pltpu.SemaphoreType.DMA((sems,)),
            pltpu.SemaphoreType.DMA((sems,)),
            pltpu.SemaphoreType.DMA((locals_,)),
        ],
        compiler_params=pltpu.CompilerParams(
            collective_id=cid, has_side_effects=True, vmem_limit_bytes=12 << 20
        ),
    )(*args)


def first_kernel(wq, wk, wo, out, ssem, rsem, local):
    me, peer = place()
    t = lax.rem(me, TP)
    greet([peer(k) for k in range(1, TP)])
    sems = (ssem, rsem)
    shard, cq, co = wq.shape[0], wq.shape[1] // TP, wo.shape[1] // TP
    low, high = pl.ds(0, shard), pl.ds(shard, shard)
    finish([
        send_columns(wq, out, cq, 0, sems, 0, local.at[0], t, peer),
        send_columns(wk, out, cq, cq, sems, 7, local.at[1], t, peer),
        send_columns(wo, out, co, 2 * cq, sems, 14, local.at[2], t, peer, low),
        send_columns(wo, out, co, 2 * cq + co, sems, 21, local.at[3], t, peer, high),
    ])


def first_exchange(wq, wk, wo, cid):
    width = 2 * wq.shape[1] // TP + 2 * wo.shape[1] // TP
    outs = (SDS((TP, wq.shape[0], width), bf),)
    return exchange_call(first_kernel, outs, (wq, wk, wo), 28, 4, cid)[0]


def second_kernel(n, wv, ws, vec, out, vec_out, ssem, rsem, local):
    dp = n // TP
    me, peer = place()
    t, g = lax.rem(me, TP), lax.div(me, TP)
    others = [lax.rem(me + TP * j, n) for j in range(1, dp)]
    greet([peer(k) for k in range(1, TP)] + others)
    sems = (ssem, rsem)
    cols = wv.shape[1] // TP
    far = []
    keep = pltpu.make_async_copy(vec, vec_out.at[g, t], local.at[2])
    keep.start()
    for j, dev in enumerate(others):
        copy = remote(vec, vec_out.at[g, t], sems, 21 + j, dev)
        copy.start()
        far.append(copy)
    parts = [
        send_columns(wv, out, cols, 0, sems, 0, local.at[0], t, peer),
        send_columns(ws, out, cols, cols, sems, 7, local.at[1], t, peer),
    ]
    for copy in far:
        copy.wait()
    keep.wait()
    near = []
    for k in range(1, TP):
        copy = remote(vec_out.at[:, t], vec_out.at[:, t], sems, 13 + k, peer(k))
        copy.start()
        near.append(copy)
    finish(parts)
    for copy in near:
        copy.wait()


def second_exchange(n, wv, ws, vec, cid):
    outs = (
        SDS((TP, wv.shape[0], 2 * wv.shape[1] // TP), bf),
        SDS((n // TP, TP) + vec.shape, f32),
    )
    kernel = functools.partial(second_kernel, n)
    return exchange_call(kernel, outs, (wv, ws, vec), 21 + n // TP, 3, cid)


def third_kernel(gu, tok, gu_out, tok_out, ssem, rsem, local):
    me, peer = place()
    t = lax.rem(me, TP)
    greet([peer(k) for k in range(1, TP)])
    sems = (ssem, rsem)
    gather_blocks(tok, tok_out, sems, 7, local.at[1], peer)
    finish([send_columns(gu, gu_out, gu.shape[2], 0, sems, 0, local.at[0], t, peer)])


def third_exchange(gu, tok, cid):
    outs = (SDS(gu.shape, bf), SDS((TP,) + tok.shape, bf))
    return exchange_call(third_kernel, outs, (gu, tok), 7 + GATHER_SEMS, 2, cid)


REDUCE_SEMS = 16
TILE = 512


class Reduce:
    def __init__(self, product, bufs, sems, base, peer, prepare=None):
        self.product, self.prepare, self.sems, self.base = product, prepare, sems, base
        self.po, self.pe, self.rc, self.sb, self.xr, self.yr = bufs
        self.pc, self.px, self.py = peer(1), peer(2), peer(4)
        self.q = self.pe.shape[1] // 4
        self.sent, self.core, self.got = [], {}, ({}, {})

    def send(self, src, dst, dev, i):
        copy = remote(src, dst, self.sems, self.base + i, dev)
        copy.start()
        self.sent.append(copy)
        return copy

    def pair(self, i):
        if self.prepare is not None:
            self.prepare(2 * i)
        self.product(i, self.po.at[i], self.pe.at[i])
        self.core[i] = self.send(self.po.at[i], self.rc.at[i], self.pc, i)

    def add(self, c, i, lower, out, more=None):
        step = 32

        @pl.loop(0, self.q // step)
        def _(j):
            there = pl.ds(pl.multiple_of(j * step, step), step)
            here = pl.ds(pl.multiple_of(j * step + (2 * c + lower) * self.q, step), step)
            total = self.pe[i, here, :].astype(f32) + self.rc[i, here, :].astype(f32)
            if more is not None:
                total = total + more[there, :].astype(f32)
            self.sb[c, out, there, :] = total.astype(bf)

    def link(self, c, slot, name, ring, at, dev):
        self.got[c][name] = self.send(
            self.sb.at[c, slot], ring.at[c, at], dev, 4 + 6 * c + slot
        )

    def six(self, c):
        self.add(c, 3, 0, 0)
        self.link(c, 0, "x6", self.xr, 0, self.px)
        self.add(c, 3, 1, 1)
        self.link(c, 1, "y6", self.yr, 0, self.py)

    def two(self, c):
        self.add(c, 1, 0, 2)
        self.link(c, 2, "x2", self.xr, 1, self.px)

    def four(self, c):
        self.add(c, 2, 1, 3)
        self.link(c, 3, "y4", self.yr, 1, self.py)

    def onward(self, c):
        self.got[c]["x6"].wait_recv()
        self.add(c, 2, 0, 4, self.xr.at[c, 0])
        self.link(c, 4, "y4b", self.yr, 2, self.py)
        self.got[c]["y6"].wait_recv()
        self.add(c, 1, 1, 5, self.yr.at[c, 0])
        self.link(c, 5, "x2b", self.xr, 2, self.px)

    def first(self):
        self.pair(3)
        self.pair(1)
        self.core[3].wait_recv()
        self.six(0)
        self.pair(2)
        self.core[1].wait_recv()
        self.two(0)
        self.core[2].wait_recv()
        self.four(0)
        self.pair(0)
        self.onward(0)

    def second(self):
        self.six(1)
        self.two(1)
        self.four(1)
        self.onward(1)

    def rows(self, c, step, body):
        if c == 0:
            self.core[0].wait_recv()
        for name in ("x2", "y4", "y4b", "x2b"):
            self.got[c][name].wait_recv()
        for lower in (0, 1):
            near, far = (self.yr, self.xr) if lower else (self.xr, self.yr)

            @pl.loop(0, self.q // step)
            def _(j, lower=lower, near=near, far=far):
                there = pl.ds(pl.multiple_of(j * step, step), step)
                here = pl.ds(pl.multiple_of(j * step + (2 * c + lower) * self.q, step), step)
                body(
                    here,
                    self.pe[0, here, :].astype(f32)
                    + self.rc[0, here, :].astype(f32)
                    + near[c, 1, there, :].astype(f32)
                    + far[c, 2, there, :].astype(f32),
                )

    def finish(self):
        for copy in self.sent:
            copy.wait_send()


def reduce_scratch(r, c, even=f32):
    q = r // 4
    return [
        pltpu.VMEM((4, r, c), bf),
        pltpu.VMEM((4, r, c), even),
        pltpu.VMEM((4, r, c), bf),
        pltpu.VMEM((2, 6, q, c), bf),
        pltpu.VMEM((2, 3, q, c), bf),
        pltpu.VMEM((2, 3, q, c), bf),
    ]


def rows_of_pair(a, i):
    two, r, k = 2, a.shape[1], a.shape[2]
    return a[pl.ds(2 * i, two)].reshape(two * r, k)


def times(a, w, nt):
    def product(i, odd, even):
        r = a.shape[1]

        @pl.loop(0, even.shape[1] // TILE)
        def _(j):
            at = pl.ds(pl.multiple_of(j * TILE, TILE), TILE)
            x = rows_of_pair(a, i)
            if nt:
                y = lax.dot_general(
                    x, w[at, :], (((1,), (1,)), ((), ())), preferred_element_type=f32
                )
            else:
                y = jnp.dot(x, w[:, at], preferred_element_type=f32)
            even[:, at] = y[:r].astype(even.dtype)
            odd[:, at] = y[r:].astype(odd.dtype)

    return product


def exchange_and_gather(reduce, gathers, step, body):
    reduce.first()
    reduce.second()
    for c in (0, 1):
        reduce.rows(c, step, body)
        gathers[c].start()
    for c in (0, 1):
        gathers[c].forward()
    for c in (0, 1):
        gathers[c].finish()
    reduce.finish()


def both_gathers(own, out, sems, local, peer):
    half = own.shape[0] // 2
    return [
        Gather(own, out, c * half, half, sems, REDUCE_SEMS + c * GATHER_SEMS, local.at[c], peer)
        for c in (0, 1)
    ]


EXCHANGE_SEMS = REDUCE_SEMS + 2 * GATHER_SEMS


def forward_kernel(
    nrm, wvs, sco, w, tok, vec, v_out, mix_out, ret_out, swi_out, mid, out,
    v_buf, mix_buf, ret_buf, swi_buf, po, pe, rc, sb, xr, yr, own, ssem, rsem, local,
):
    _, peer = place()
    greet([peer(1), peer(2), peer(4)])
    sems = (ssem, rsem)
    r, width = v_buf.shape[1:]
    kept = []

    def prepare(first):
        two = pl.ds(first, 2)
        x = nrm[two].reshape(2 * r, nrm.shape[2])

        @pl.loop(0, width // 256)
        def _(j):
            at = pl.ds(pl.multiple_of(j * 256, 256), 256)
            behind = pl.ds(pl.multiple_of(j * 256 + width, 256), 256)
            v = jnp.dot(x, wvs[:, at], preferred_element_type=f32).astype(bf)
            s = jnp.dot(x, wvs[:, behind], preferred_element_type=f32)
            for i in (0, 1):
                mine = v[i * r : (i + 1) * r]
                v_buf[first + i, :, at] = mine
                swi_buf[first + i, :, at] = s[i * r : (i + 1) * r]
                ret_buf[first + i, :, at] = jnp.dot(
                    sco[first + i], mine, preferred_element_type=f32
                )

        @pl.loop(0, 2 * r // 32)
        def _(j):
            k = first + lax.div(j, r // 32)
            at = pl.ds(pl.multiple_of(lax.rem(j, r // 32) * 32, 32), 32)
            value = ret_buf[k, at, :]
            centred = value - jnp.mean(value, axis=-1, keepdims=True)
            spread = jnp.mean(centred * centred, axis=-1, keepdims=True)
            gate = swi_buf[k, at, :]
            gate = gate / (1.0 + jnp.exp(-gate))
            mix_buf[k, at, :] = (
                gate * (centred * lax.rsqrt(jnp.maximum(spread, 0.25)))
            ).astype(bf)

        for i, (src, dst) in enumerate(
            ((v_buf, v_out), (mix_buf, mix_out), (ret_buf, ret_out), (swi_buf, swi_out))
        ):
            copy = pltpu.make_async_copy(
                src.at[two], dst.at[two], local.at[2 + 2 * first + i]
            )
            copy.start()
            kept.append(copy)

    def product(i, odd, even):
        step = w.shape[2]

        @pl.loop(0, w.shape[0])
        def _(j):
            at = pl.ds(pl.multiple_of(j * step, step), step)
            y = jnp.dot(rows_of_pair(mix_buf, i), w[j], preferred_element_type=f32)
            even[:, at] = y[:r].astype(even.dtype)
            odd[:, at] = y[r:].astype(odd.dtype)

    def body(at, value):
        value = value + tok[at, :].astype(f32)
        mid[at, :] = value
        center = jnp.mean(value, axis=-1, keepdims=True)
        centred = value - center
        spread = jnp.mean(centred * centred, axis=-1, keepdims=True)
        own[at, :] = (
            centred * lax.rsqrt(spread + 1e-05) * vec[0:1, :] + vec[1:2, :]
        ).astype(bf)

    reduce = Reduce(product, (po, pe, rc, sb, xr, yr), sems, 0, peer, prepare)
    exchange_and_gather(reduce, both_gathers(own, out, sems, local, peer), 16, body)
    for copy in kept:
        copy.wait()


def forward_exchange(nrm, wvs, sco, w, tok, vec, cid):
    _, r, d = nrm.shape
    width = w.shape[1]
    count = EXCHANGE_SEMS
    blocks = [((TP, r, width), t) for t in (bf, bf, f32, f32)]
    return pl.pallas_call(
        forward_kernel,
        out_shape=tuple(SDS(*b) for b in blocks) + (SDS((r, d), f32), SDS((TP, r, d), bf)),
        in_specs=[VMEM] * 6,
        out_specs=(ANY,) * 4 + (VMEM, ANY),
        scratch_shapes=[pltpu.VMEM(*b) for b in blocks]
        + reduce_scratch(r, d)
        + [
            pltpu.VMEM((r, d), bf),
            pltpu.SemaphoreType.DMA((count,)),
            pltpu.SemaphoreType.DMA((count,)),
            pltpu.SemaphoreType.DMA((18,)),
        ],
        compiler_params=pltpu.CompilerParams(
            collective_id=cid, has_side_effects=True, vmem_limit_bytes=60 << 20
        ),
        name="forward_exchange",
    )(nrm, wvs, sco, w, tok, vec)


def hidden_kernel(x, gu, hid, act_out, slope_out):
    width = hid.shape[2]
    step = 256

    @pl.loop(0, width // step)
    def _(j):
        at = pl.ds(pl.multiple_of(j * step, step), step)
        behind = pl.ds(pl.multiple_of(j * step + width, step), step)
        first = jnp.dot(x[0], gu[:, at], preferred_element_type=f32)
        second = jnp.dot(x[0], gu[:, behind], preferred_element_type=f32)
        share = 0.5 * (1.0 + lax.erf(first * math.sqrt(0.5)))
        act = first * share
        slope = share + first * (jnp.exp(-0.5 * first * first) * (1.0 / math.sqrt(2.0 * math.pi)))
        hid[0, :, at] = (act * second).astype(bf)
        act_out[0, :, at] = act
        slope_out[0, :, at] = slope * second


def hidden_units(x, gu):
    _, r, d = x.shape
    width = gu.shape[1] // 2
    row = pl.BlockSpec((1, r, width), lambda k: (k, 0, 0))
    return pl.pallas_call(
        hidden_kernel,
        grid=(TP,),
        out_shape=tuple(SDS((TP, r, width), t) for t in (bf, f32, f32)),
        in_specs=[
            pl.BlockSpec((1, r, d), lambda k: (k, 0, 0)),
            pl.BlockSpec(gu.shape, lambda k: (0, 0)),
        ],
        out_specs=(row, row, row),
        compiler_params=pltpu.CompilerParams(vmem_limit_bytes=56 << 20),
        cost_estimate=pl.CostEstimate(
            flops=4 * TP * r * d * width, bytes_accessed=24 << 20, transcendentals=2 * TP * r * width
        ),
        name="hidden_units",
    )(x, gu)


def hidden_back_kernel(cot, down, act, slope, out):
    width = act.shape[2]
    step = 256

    @pl.loop(0, width // step)
    def _(j):
        at = pl.ds(pl.multiple_of(j * step, step), step)
        behind = pl.ds(pl.multiple_of(j * step + width, step), step)
        grad = lax.dot_general(
            cot[0], down[at, :], (((1,), (1,)), ((), ())), preferred_element_type=f32
        )
        out[0, :, at] = (grad * slope[0, :, at]).astype(bf)
        out[0, :, behind] = (grad * act[0, :, at]).astype(bf)


def hidden_back(cot, down, act, slope):
    _, r, d = cot.shape
    width = act.shape[2]
    row = pl.BlockSpec((1, r, width), lambda k: (k, 0, 0))
    return pl.pallas_call(
        hidden_back_kernel,
        grid=(TP,),
        out_shape=SDS((TP, r, 2 * width), bf),
        in_specs=[
            pl.BlockSpec((1, r, d), lambda k: (k, 0, 0)),
            pl.BlockSpec(down.shape, lambda k: (0, 0)),
            row,
            row,
        ],
        out_specs=pl.BlockSpec((1, r, 2 * width), lambda k: (k, 0, 0)),
        compiler_params=pltpu.CompilerParams(vmem_limit_bytes=56 << 20),
        cost_estimate=pl.CostEstimate(
            flops=2 * TP * r * d * width, bytes_accessed=24 << 20, transcendentals=0
        ),
        name="hidden_back",
    )(cot, down, act, slope)


def backward_kernel(
    a, w, mid, cot, vec, gmid, out, sums, po, pe, rc, sb, xr, yr, own, acc, ssem, rsem, local
):
    _, peer = place()
    greet([peer(1), peer(2), peer(4)])
    sems = (ssem, rsem)
    acc[...] = jnp.zeros_like(acc)

    def body(at, g):
        value = mid[at, :]
        center = jnp.mean(value, axis=-1, keepdims=True)
        centred = value - center
        inv = lax.rsqrt(jnp.mean(centred * centred, axis=-1, keepdims=True) + 1e-05)
        hat = centred * inv
        acc[0] += g * hat
        acc[1] += g
        scaled = g * vec[0:1, :]
        mean_g = jnp.mean(scaled, axis=-1, keepdims=True)
        mean_gh = jnp.mean(scaled * hat, axis=-1, keepdims=True)
        grad = cot[at, :].astype(f32) + inv * (scaled - mean_g - hat * mean_gh)
        gmid[at, :] = grad
        own[at, :] = grad.astype(bf)

    reduce = Reduce(times(a, w, True), (po, pe, rc, sb, xr, yr), sems, 0, peer)
    exchange_and_gather(reduce, both_gathers(own, out, sems, local, peer), 16, body)
    sums[0:1, :] = jnp.sum(acc[0], axis=0, keepdims=True)
    sums[1:2, :] = jnp.sum(acc[1], axis=0, keepdims=True)


def backward_exchange(a, w, mid, cot, vec, cid):
    _, r, _ = a.shape
    c = w.shape[0]
    count = EXCHANGE_SEMS
    return pl.pallas_call(
        backward_kernel,
        out_shape=(SDS((r, c), f32), SDS((TP, r, c), bf), SDS((2, c), f32)),
        in_specs=[VMEM] * 5,
        out_specs=(VMEM, ANY, VMEM),
        scratch_shapes=reduce_scratch(r, c)
        + [
            pltpu.VMEM((r, c), bf),
            pltpu.VMEM((2, 16, c), f32),
            pltpu.SemaphoreType.DMA((count,)),
            pltpu.SemaphoreType.DMA((count,)),
            pltpu.SemaphoreType.DMA((2,)),
        ],
        compiler_params=pltpu.CompilerParams(
            collective_id=cid, has_side_effects=True, vmem_limit_bytes=52 << 20
        ),
        name="backward_exchange",
    )(a, w, mid, cot, vec)


def last_kernel(
    n, a1, w1, a2, w2, tok, gmid, gain, sums2, gtok, ffn, vec_out,
    po, pe, rc, sb, xr, yr, pe2, rc2, sb2, xr2, yr2, acc, vecs, near, far, part, ssem, rsem,
):
    dp = n // TP
    me, peer = place()
    g = lax.div(me, TP)
    width = vec_out.shape[1]
    others = [lax.rem(me + TP * j, n) for j in range(1, dp)]
    greet([peer(k) for k in range(1, TP)] + others)
    sems = (ssem, rsem)
    acc[...] = jnp.zeros_like(acc)
    one = Reduce(times(a1, w1, True), (po, pe, rc, sb, xr, yr), sems, 0, peer)
    one.first()
    one.second()
    for copy in one.core.values():
        copy.wait_send()
    one.sent = [copy for copy in one.sent if all(copy is not c for c in one.core.values())]
    two = Reduce(times(a2, w2, False), (po, pe2, rc2, sb2, xr2, yr2), sems, REDUCE_SEMS, peer)
    two.first()
    two.second()

    def body(at, grad):
        value = tok[at, :].astype(f32)
        center = jnp.mean(value, axis=-1, keepdims=True)
        centred = value - center
        inv = lax.rsqrt(jnp.mean(centred * centred, axis=-1, keepdims=True) + 1e-05)
        hat = centred * inv
        acc[0] += grad * hat
        acc[1] += grad
        scaled = grad * gain[...]
        mean_g = jnp.mean(scaled, axis=-1, keepdims=True)
        mean_gh = jnp.mean(scaled * hat, axis=-1, keepdims=True)
        gtok[at, :] = gmid[at, :] + inv * (scaled - mean_g - hat * mean_gh)

    for c in (0, 1):
        one.rows(c, 16, body)
    vecs[...] = jnp.zeros_like(vecs)
    vecs[0:1, :] = jnp.sum(acc[0], axis=0, keepdims=True)
    vecs[1:2, :] = jnp.sum(acc[1], axis=0, keepdims=True)
    vecs[2:4, :] = sums2[...]
    base = 2 * REDUCE_SEMS
    copies = []
    for j, dev in enumerate(others):
        at = pl.multiple_of(lax.div(dev, TP) * width, 128)
        copy = remote(vecs.at[:, pl.ds(at, width)], far.at[j], sems, base + j, dev)
        copy.start()
        copies.append(copy)

    def keep(at, value):
        ffn[at, :] = value

    two.rows(0, 32, keep)
    total = vecs[:, pl.ds(pl.multiple_of(g * width, 128), width)]
    for j, copy in enumerate(copies):
        copy.wait()
        total = total + far[j]
    part[...] = total
    copies = []
    for k in range(1, TP):
        copy = remote(part, near.at[k - 1], sems, base + dp + k - 1, peer(k))
        copy.start()
        copies.append(copy)
    two.rows(1, 32, keep)
    for k, copy in enumerate(copies):
        copy.wait()
        total = total + near[k]
    vec_out[...] = total
    one.finish()
    two.finish()


def last_exchange(n, a1, w1, a2, w2, tok, gmid, gain, sums2, cid):
    dp = n // TP
    _, r, _ = a1.shape
    c = w1.shape[0]
    width = c // dp
    count = 2 * REDUCE_SEMS + dp + TP
    return pl.pallas_call(
        functools.partial(last_kernel, n),
        out_shape=(SDS((r, c), f32), SDS((r, c), f32), SDS((8, width), f32)),
        in_specs=[VMEM] * 8,
        out_specs=(VMEM,) * 3,
        scratch_shapes=reduce_scratch(r, c)
        + reduce_scratch(r, c, bf)[1:]
        + [
            pltpu.VMEM((2, 16, c), f32),
            pltpu.VMEM((8, c), f32),
            pltpu.VMEM((TP - 1, 8, width), f32),
            pltpu.VMEM((dp, 8, width), f32),
            pltpu.VMEM((8, width), f32),
            pltpu.SemaphoreType.DMA((count,)),
            pltpu.SemaphoreType.DMA((count,)),
        ],
        compiler_params=pltpu.CompilerParams(
            collective_id=cid, has_side_effects=True, vmem_limit_bytes=67043328
        ),
        name="last_exchange",
    )(a1, w1, a2, w2, tok, gmid, gain, sums2)


def tp_groups(n):
    return [[g * TP + t for t in range(TP)] for g in range(n // TP)]


def dp_groups(n):
    return [[g * TP + t for g in range(n // TP)] for t in range(TP)]


def plane_a2a(x, n):
    return lax.all_to_all(x, AXIS, 0, 0, axis_index_groups=tp_groups(n), tiled=True)


def dp_gather(x, n):
    return lax.all_gather(x, AXIS, axis=0, tiled=True, axis_index_groups=dp_groups(n))


def dp_reduce(x, n):
    return lax.psum_scatter(
        x, AXIS, scatter_dimension=0, tiled=True, axis_index_groups=dp_groups(n)
    )


def layer_norm(value, gain, bias):
    center = jnp.mean(value, axis=-1, keepdims=True)
    centred = value - center
    spread = jnp.mean(centred * centred, axis=-1, keepdims=True)
    return centred * lax.rsqrt(spread + 1e-05) * gain + bias


def seq_positions(lengths, rows):
    ends = jnp.cumsum(lengths, axis=1)
    starts = ends - lengths
    index = jnp.arange(rows, dtype=jnp.int32)
    segment = jnp.sum((index[None, :, None] >= ends[:, None, :]).astype(jnp.int32), axis=2)
    member = segment[:, :, None] == jnp.arange(lengths.shape[1], dtype=jnp.int32)
    offset = index[None, :] - jnp.sum(jnp.where(member, starts[:, None, :], 0), axis=2)
    return segment, offset


def rotary_tables(offset):
    half = KH // 2
    freq = jnp.exp(-math.log(10000.0) * jnp.arange(half, dtype=f32) / half)
    angle = offset.astype(f32)[..., None] * freq
    return jnp.cos(angle), jnp.sin(angle)


def rotate(value, cosine, sine):
    half = KH // 2
    u, w = value[..., :half], value[..., half:]
    return jnp.concatenate([u * cosine - w * sine, w * cosine + u * sine], axis=-1)


def rotate_back(value, cosine, sine):
    half = KH // 2
    u, w = value[..., :half], value[..., half:]
    return jnp.concatenate([u * cosine + w * sine, w * cosine - u * sine], axis=-1)


def decay_mask(segment, offset, head):
    diff = offset[:, :, None] - offset[:, None, :]
    valid = (segment[:, :, None] == segment[:, None, :]) & (diff >= 0)
    steps = jnp.where(valid, diff, 0).astype(f32)
    log = jnp.log(1.0 - jnp.exp2(-5.0 - head.astype(f32)))
    return jnp.where(valid, jnp.exp(log * steps), 0.0) / math.sqrt(KH)


def group_gate(retained, swish_in):
    center = jnp.mean(retained, axis=-1, keepdims=True)
    centred = retained - center
    spread = jnp.mean(centred * centred, axis=-1, keepdims=True)
    return jax.nn.silu(swish_in) * (centred * lax.rsqrt(jnp.maximum(spread, 0.25)))


def dot(a, b):
    return lax.dot_general(a, b, (((1,), (0,)), ((), ())), preferred_element_type=f32)


def dot_tn(a, b):
    return lax.dot_general(a, b, (((0,), (0,)), ((), ())), preferred_element_type=f32)


def dot_nt(a, b):
    return lax.dot_general(a, b, (((1,), (1,)), ((), ())), preferred_element_type=f32)


def bmm(eq, a, b):
    return jnp.einsum(eq, a, b, preferred_element_type=f32)


def col_blocks(w):
    r, c = w.shape
    return w.reshape(r, TP, c // TP).transpose(1, 0, 2).reshape(TP * r, c // TP)


def col_join(w, r):
    c = w.shape[1]
    return w.reshape(TP, r, c).transpose(1, 0, 2).reshape(r, TP * c)


def join_kernel(widths, parts, x, *outs):
    at = 0
    for out, width in zip(outs, widths):
        piece = width // parts
        for t in range(TP):
            for p in range(parts):
                to = (p * TP + t) * piece
                out[:, to : to + piece] = x[t, :, at + p * piece : at + (p + 1) * piece].astype(f32)
        at += width


def join(x, widths, parts=1):
    r = x.shape[1]
    if any(width // parts % 128 for width in widths):
        made, at = [], 0
        for width in widths:
            part = x[:, :, at : at + width].reshape(TP, r, parts, width // parts)
            made.append(part.transpose(1, 2, 0, 3).reshape(r, TP * width).astype(f32))
            at += width
        return made
    return pl.pallas_call(
        functools.partial(join_kernel, widths, parts),
        out_shape=tuple(SDS((r, TP * width), f32) for width in widths),
        in_specs=[VMEM],
        out_specs=tuple(VMEM for _ in widths),
        compiler_params=pltpu.CompilerParams(vmem_limit_bytes=8 << 20),
        cost_estimate=pl.CostEstimate(flops=0, bytes_accessed=6 * x.size, transcendentals=0),
        name="join",
    )(x)


def after(x, *deps):
    return lax.optimization_barrier((x,) + deps)[0]


def on_device(n, tokens, lengths, gain1, bias1, wq, wk, wv, ws, wo, gain2, bias2, wg, wu, wd, cot):
    rows, d = tokens.shape
    ff = wg.shape[1]
    dp = n // TP
    shard = d // n
    unit = ff // n
    me = lax.axis_index(AXIS)
    head = lax.rem(me, TP)

    def ff_blocks(w):
        return w.reshape(shard, dp, TP, unit).transpose(2, 0, 1, 3).reshape(TP, shard, dp * unit)

    vec = jnp.zeros((8, 128), f32)
    for i, v in enumerate((gain1, bias1, gain2, bias2)):
        vec = vec.at[i, :shard].set(v.astype(f32))
    vec = vec.at[4, :3].set(lengths[0].astype(f32))
    qko_blk = first_exchange(wq, wk, wo, 1)
    qko = dp_gather(qko_blk.reshape(TP * shard, 4 * KH), n)
    vs_blk, vec_all = second_exchange(n, after(wv, qko_blk), ws, vec, 2)
    vs = dp_gather(vs_blk.reshape(TP * shard, 2 * VH), n)
    gu_in = jnp.concatenate([ff_blocks(wg), ff_blocks(wu)], axis=2)
    gu_blk, tok_all = third_exchange(gu_in, after(tokens, vs_blk), 3)
    gu = dp_gather(gu_blk.reshape(TP * shard, 2 * dp * unit), n)
    down = dp_gather(wd, n)
    cot_all = plane_gather(after(cot, tok_all), 4)
    gain1f, bias1f, gain2f, bias2f = (
        vec_all[:, :, i, :shard].reshape(1, d) for i in range(4)
    )
    vec2 = jnp.concatenate([gain2f, bias2f], axis=0)
    out = qko[:, 2 * KH :].reshape(n, shard, 2, d // TP).transpose(0, 2, 1, 3)
    out_blk = plane_a2a(out.reshape(TP * VH, d // TP), n)

    mine = lax.dynamic_slice_in_dim(vec_all, lax.div(me, TP), 1, 0)[0, :, 4, :3]
    order = jnp.arange(TP, dtype=jnp.int32)
    pick = (order[None, :] == (order[:, None] ^ head)).astype(f32)
    len_all = jnp.sum(pick[:, :, None] * mine[None], axis=1).astype(jnp.int32)
    segment, offset = seq_positions(len_all, rows)
    cosine, sine = rotary_tables(offset)
    mask = decay_mask(segment, offset, head)

    normed = layer_norm(tok_all.reshape(TP * rows, d).astype(f32), gain1f, bias1f).astype(bf)
    qk_out = dot(normed, qko[:, : 2 * KH]).reshape(TP, rows, 2 * KH)
    query, key = qk_out[..., :KH], qk_out[..., KH:]
    q_rot = rotate(query, cosine, sine).astype(bf)
    k_rot = rotate(key, cosine, sine).astype(bf)
    plain = bmm("btd,bsd->bts", q_rot, k_rot)
    scores = (plain * mask).astype(bf)
    v_low, mixed, retained, swish_in, middle, normed2 = forward_exchange(
        normed.reshape(TP, rows, d), vs, scores, out_blk.reshape(TP, VH, d // TP), tokens, vec2, 5
    )
    out = col_join(out_blk, VH)
    hidden, act, slope = hidden_units(normed2, gu)
    normed2 = normed2.reshape(TP * rows, d)
    down_grad = dot_tn(hidden.reshape(TP * rows, dp * unit), cot_all.reshape(TP * rows, d)).astype(bf)
    g_down = dp_reduce(down_grad, n)

    g_fs = hidden_back(cot_all, down, act, slope)
    gu_grad = dot_tn(normed2, g_fs.reshape(TP * rows, 2 * dp * unit)).astype(bf)
    g_gu = dp_reduce(gu_grad, n)
    g_middle, g_low, sums2 = backward_exchange(g_fs, gu, middle, cot, vec2, 6)

    g_low = g_low.reshape(TP * rows, d)
    mixed = mixed.reshape(TP * rows, VH)
    g_mixed = dot_nt(g_low, out).reshape(TP, rows, VH)
    _, pull_group = jax.vjp(group_gate, retained, swish_in)
    g_retained, g_swish = pull_group(g_mixed)
    g_retained = g_retained.astype(bf)
    g_swish = g_swish.astype(bf)
    swish_grad = dot_tn(normed, g_swish.reshape(TP * rows, VH)).astype(bf)
    g_swi = dp_reduce(swish_grad, n)
    out_grad = dot_tn(mixed, g_low).astype(bf)
    out_grad = plane_a2a(col_blocks(out_grad), n)
    g_value = bmm("bts,btd->bsd", scores, g_retained).astype(bf)
    g_scores = bmm("btd,bsd->bts", g_retained, v_low)
    g_plain = (g_scores * mask).astype(bf)
    g_qrot = bmm("bts,bsd->btd", g_plain, k_rot)
    g_krot = bmm("bts,btd->bsd", g_plain, q_rot)
    g_query = rotate_back(g_qrot, cosine, sine).astype(bf)
    g_key = rotate_back(g_krot, cosine, sine).astype(bf)
    g_qkv = jnp.concatenate([g_query, g_key, g_value], axis=2)
    qkv_grad = dot_tn(normed, g_qkv.reshape(TP * rows, 2 * KH + VH)).astype(bf)
    g_qkv_own = dp_reduce(qkv_grad, n)
    g_out = dp_reduce(out_grad, n)
    g_qkvs = jnp.concatenate([g_qkv, g_swish], axis=2)
    w_qkvs = jnp.concatenate([qko[:, : 2 * KH], vs], axis=1)
    grad_tokens, ffn, g_vecs = last_exchange(
        n, g_qkvs, w_qkvs, hidden, down, tokens, g_middle, gain1f, sums2, 7
    )
    layer_out = (middle + ffn).astype(bf)

    g_vecs = lax.dynamic_slice_in_dim(g_vecs, head * shard, shard, 1)
    grad_d = g_down.astype(f32)
    g_gu = plane_a2a(g_gu, n)
    grad_g, grad_u = join(g_gu.reshape(TP, shard, 2 * dp * unit), (dp * unit,) * 2, dp)
    g_swi = plane_a2a(g_swi, n)
    (grad_s,) = join(g_swi.reshape(TP, shard, VH), (VH,))
    g_qkv_own = plane_a2a(g_qkv_own, n)
    grad_q, grad_k, grad_v = join(g_qkv_own.reshape(TP, shard, 2 * KH + VH), (KH, KH, VH))
    g_out = plane_a2a(g_out, n)
    (grad_o,) = join(g_out.reshape(TP, wo.shape[0], d // TP), (d // TP,))
    return (
        layer_out, grad_tokens, g_vecs[0], g_vecs[1], grad_q, grad_k, grad_v, grad_s, grad_o,
        g_vecs[2], g_vecs[3], grad_g, grad_u, grad_d,
    )


def solution(mesh):
    n = mesh.shape[AXIS]
    row, vec = P(AXIS, None), P(AXIS)
    ins = (row, row, vec, vec, row, row, row, row, row, vec, vec, row, row, row, row)
    outs = (row, row, vec, vec, row, row, row, row, row, vec, vec, row, row, row)

    def body(*args):
        return on_device(n, *args)

    return jax.shard_map(body, mesh=mesh, in_specs=ins, out_specs=outs, check_vma=False)
```

```python
import functools
import math

import jax
import jax.numpy as jnp
from jax import lax
from jax.experimental import pallas as pl
from jax.experimental.pallas import tpu as pltpu
from jax.sharding import PartitionSpec as P


KH = 256
VH = 512
TP = 8
AXIS = "fsdp"
MESH = pl.DeviceIdType.MESH
ANY = pl.BlockSpec(memory_space=pl.ANY)
VMEM = pl.BlockSpec(memory_space=pltpu.VMEM)
bf = jnp.bfloat16
f32 = jnp.float32
SDS = jax.ShapeDtypeStruct


def place():
    me = lax.axis_index(AXIS)
    steps = [s - 2 * s * lax.rem(lax.div(me, s), 2) for s in (1, 2, 4)]

    def peer(k):
        out = me
        for bit, step in enumerate(steps):
            if k >> bit & 1:
                out = out + step
        return out

    return me, peer


def greet(peers):
    barrier = pltpu.get_barrier_semaphore()
    for p in peers:
        pl.semaphore_signal(barrier, inc=1, device_id=(p,), device_id_type=MESH)
    pl.semaphore_wait(barrier, len(peers))


def remote(src, dst, sems, i, dev):
    return pltpu.make_async_remote_copy(
        src_ref=src, dst_ref=dst, send_sem=sems[0].at[i], recv_sem=sems[1].at[i],
        device_id=(dev,), device_id_type=MESH,
    )


GATHER_SEMS = 13


class Gather:
    def __init__(self, own, out, start, size, sems, base, local, peer):
        self.own, self.out, self.sems, self.base, self.local = own, out, sems, base, local
        h = size // 2
        self.all, self.top, self.bot = pl.ds(start, size), pl.ds(start, h), pl.ds(start + h, h)
        self.pc, self.px, self.py = peer(1), peer(2), peer(4)
        self.made = []

    def send(self, src, dst, dev):
        copy = remote(src, dst, self.sems, self.base + len(self.made), dev)
        copy.start()
        self.made.append(copy)
        return copy

    def pass_on(self, k, at):
        self.core.append(self.send(self.out.at[k, at], self.out.at[k + 1, at], self.pc))

    def start(self):
        own, out, top, bot = self.own, self.out, self.top, self.bot
        self.x0 = self.send(own.at[bot], out.at[2, bot], self.px)
        self.y0 = self.send(own.at[top], out.at[4, top], self.py)
        self.x1 = self.send(own.at[top], out.at[2, top], self.px)
        self.y1 = self.send(own.at[bot], out.at[4, bot], self.py)
        self.core = [self.send(own.at[self.all], out.at[1, self.all], self.pc)]
        self.keep = pltpu.make_async_copy(own.at[self.all], out.at[0, self.all], self.local)
        self.keep.start()

    def forward(self):
        out, top, bot = self.out, self.top, self.bot
        self.x0.wait_recv()
        self.fy = self.send(out.at[2, bot], out.at[6, bot], self.py)
        self.pass_on(2, bot)
        self.y0.wait_recv()
        self.fx = self.send(out.at[4, top], out.at[6, top], self.px)
        self.pass_on(4, top)
        self.x1.wait_recv()
        self.pass_on(2, top)
        self.y1.wait_recv()
        self.pass_on(4, bot)

    def finish(self):
        self.fy.wait_recv()
        self.pass_on(6, self.bot)
        self.fx.wait_recv()
        self.pass_on(6, self.top)
        for copy in self.core:
            copy.wait_recv()
        for copy in self.made:
            copy.wait_send()
        self.keep.wait()


def gather_blocks(own, out, sems, base, local, peer):
    gather = Gather(own, out, 0, own.shape[0], sems, base, local, peer)
    gather.start()
    gather.forward()
    gather.finish()


def send_columns(src, out, cols, at, sems, base, local, t, peer, rows=None):
    copies = []
    rows = slice(None) if rows is None else rows

    def block(q):
        if len(src.shape) == 3:
            return src.at[q]
        return src.at[rows, pl.ds(pl.multiple_of(q * cols, 128), cols)]

    for k in range(1, TP):
        dev = peer(k)
        copy = remote(
            block(lax.rem(dev, TP)), out.at[t, :, pl.ds(at, cols)], sems, base + k - 1, dev
        )
        copy.start()
        copies.append(copy)
    keep = pltpu.make_async_copy(block(t), out.at[t, :, pl.ds(at, cols)], local)
    keep.start()
    return copies, keep


def finish(parts):
    for copies, keep in parts:
        for copy in copies:
            copy.wait()
        keep.wait()


def exchange_call(kernel, outs, args, sems, locals_, cid):
    return pl.pallas_call(
        kernel,
        out_shape=outs,
        in_specs=[VMEM] * len(args),
        out_specs=tuple(ANY for _ in outs),
        scratch_shapes=[
            pltpu.SemaphoreType.DMA((sems,)),
            pltpu.SemaphoreType.DMA((sems,)),
            pltpu.SemaphoreType.DMA((locals_,)),
        ],
        compiler_params=pltpu.CompilerParams(
            collective_id=cid, has_side_effects=True, vmem_limit_bytes=12 << 20
        ),
    )(*args)


def first_kernel(wq, wk, wo, out, ssem, rsem, local):
    me, peer = place()
    t = lax.rem(me, TP)
    greet([peer(k) for k in range(1, TP)])
    sems = (ssem, rsem)
    shard, cq, co = wq.shape[0], wq.shape[1] // TP, wo.shape[1] // TP
    low, high = pl.ds(0, shard), pl.ds(shard, shard)
    finish([
        send_columns(wq, out, cq, 0, sems, 0, local.at[0], t, peer),
        send_columns(wk, out, cq, cq, sems, 7, local.at[1], t, peer),
        send_columns(wo, out, co, 2 * cq, sems, 14, local.at[2], t, peer, low),
        send_columns(wo, out, co, 2 * cq + co, sems, 21, local.at[3], t, peer, high),
    ])


def first_exchange(wq, wk, wo, cid):
    width = 2 * wq.shape[1] // TP + 2 * wo.shape[1] // TP
    outs = (SDS((TP, wq.shape[0], width), bf),)
    return exchange_call(first_kernel, outs, (wq, wk, wo), 28, 4, cid)[0]


def second_kernel(n, tok, vec, tok_out, vec_out, ssem, rsem, local):
    dp = n // TP
    me, peer = place()
    t, g = lax.rem(me, TP), lax.div(me, TP)
    others = [lax.rem(me + TP * j, n) for j in range(1, dp)]
    greet([peer(k) for k in range(1, TP)] + others)
    sems = (ssem, rsem)
    base = GATHER_SEMS
    far = []
    keep = pltpu.make_async_copy(vec, vec_out.at[g, t], local.at[1])
    keep.start()
    for j, dev in enumerate(others):
        copy = remote(vec, vec_out.at[g, t], sems, base + TP + j, dev)
        copy.start()
        far.append(copy)
    gather = Gather(tok, tok_out, 0, tok.shape[0], sems, 0, local.at[0], peer)
    gather.start()
    for copy in far:
        copy.wait()
    keep.wait()
    near = []
    for k in range(1, TP):
        copy = remote(vec_out.at[:, t], vec_out.at[:, t], sems, base + k, peer(k))
        copy.start()
        near.append(copy)
    gather.forward()
    gather.finish()
    for copy in near:
        copy.wait()


def second_exchange(n, tok, vec, cid):
    outs = (SDS((TP,) + tok.shape, bf), SDS((n // TP, TP) + vec.shape, f32))
    kernel = functools.partial(second_kernel, n)
    sems = GATHER_SEMS + TP + n // TP
    return exchange_call(kernel, outs, (tok, vec), sems, 2, cid)


def third_kernel(wv, ws, out, ssem, rsem, local):
    me, peer = place()
    t = lax.rem(me, TP)
    greet([peer(k) for k in range(1, TP)])
    sems = (ssem, rsem)
    cols = wv.shape[1] // TP
    finish([
        send_columns(wv, out, cols, 0, sems, 0, local.at[0], t, peer),
        send_columns(ws, out, cols, cols, sems, 7, local.at[1], t, peer),
    ])


def third_exchange(wv, ws, cid):
    outs = (SDS((TP, wv.shape[0], 2 * wv.shape[1] // TP), bf),)
    return exchange_call(third_kernel, outs, (wv, ws), 14, 2, cid)[0]


def fourth_kernel(gu, cot, gu_out, cot_out, ssem, rsem, local):
    me, peer = place()
    t = lax.rem(me, TP)
    greet([peer(k) for k in range(1, TP)])
    sems = (ssem, rsem)
    parts = [send_columns(gu, gu_out, gu.shape[2], 0, sems, 0, local.at[0], t, peer)]
    gather_blocks(cot, cot_out, sems, 7, local.at[1], peer)
    finish(parts)


def fourth_exchange(gu, cot, cid):
    outs = (SDS(gu.shape, bf), SDS((TP,) + cot.shape, bf))
    return exchange_call(fourth_kernel, outs, (gu, cot), 7 + GATHER_SEMS, 2, cid)


REDUCE_SEMS = 16
TILE = 512


class Reduce:
    def __init__(self, product, bufs, sems, base, peer, prepare=None):
        self.product, self.prepare, self.sems, self.base = product, prepare, sems, base
        self.po, self.pe, self.rc, self.sb, self.xr, self.yr = bufs
        self.pc, self.px, self.py = peer(1), peer(2), peer(4)
        self.q = self.pe.shape[1] // 4
        self.sent, self.core, self.got = [], {}, ({}, {})

    def send(self, src, dst, dev, i):
        copy = remote(src, dst, self.sems, self.base + i, dev)
        copy.start()
        self.sent.append(copy)
        return copy

    def ready(self, i):
        if self.prepare is not None:
            self.prepare(2 * i)

    def pair(self, i):
        self.product(i, self.po.at[i], self.pe.at[i])
        self.core[i] = self.send(self.po.at[i], self.rc.at[i], self.pc, i)

    def add(self, c, i, lower, out, more=None):
        step = 32

        @pl.loop(0, self.q // step)
        def _(j):
            there = pl.ds(pl.multiple_of(j * step, step), step)
            here = pl.ds(pl.multiple_of(j * step + (2 * c + lower) * self.q, step), step)
            total = self.pe[i, here, :].astype(f32) + self.rc[i, here, :].astype(f32)
            if more is not None:
                total = total + more[there, :].astype(f32)
            self.sb[c, out, there, :] = total.astype(bf)

    def link(self, c, slot, name, ring, at, dev):
        self.got[c][name] = self.send(
            self.sb.at[c, slot], ring.at[c, at], dev, 4 + 6 * c + slot
        )

    def six(self, c):
        self.add(c, 3, 0, 0)
        self.link(c, 0, "x6", self.xr, 0, self.px)
        self.add(c, 3, 1, 1)
        self.link(c, 1, "y6", self.yr, 0, self.py)

    def two(self, c):
        self.add(c, 1, 0, 2)
        self.link(c, 2, "x2", self.xr, 1, self.px)

    def four(self, c):
        self.add(c, 2, 1, 3)
        self.link(c, 3, "y4", self.yr, 1, self.py)

    def onward(self, c):
        self.got[c]["x6"].wait_recv()
        self.add(c, 2, 0, 4, self.xr.at[c, 0])
        self.link(c, 4, "y4b", self.yr, 2, self.py)
        self.got[c]["y6"].wait_recv()
        self.add(c, 1, 1, 5, self.yr.at[c, 0])
        self.link(c, 5, "x2b", self.xr, 2, self.px)

    def run(self):
        self.ready(3)
        self.pair(3)
        stages = ((1, 3, self.six), (2, 1, self.two), (0, 2, self.four))
        for following, now, stage in stages:
            self.ready(following)
            if self.prepare is None:
                self.pair(following)
            self.core[now].wait_recv()
            for c in (0, 1):
                stage(c)
            if self.prepare is not None:
                self.pair(following)
        for c in (0, 1):
            self.onward(c)

    def rows(self, c, step, body):
        if c == 0:
            self.core[0].wait_recv()
        for name in ("x2", "y4", "y4b", "x2b"):
            self.got[c][name].wait_recv()
        for lower in (0, 1):
            near, far = (self.yr, self.xr) if lower else (self.xr, self.yr)

            @pl.loop(0, self.q // step)
            def _(j, lower=lower, near=near, far=far):
                there = pl.ds(pl.multiple_of(j * step, step), step)
                here = pl.ds(pl.multiple_of(j * step + (2 * c + lower) * self.q, step), step)
                body(
                    here,
                    self.pe[0, here, :].astype(f32)
                    + self.rc[0, here, :].astype(f32)
                    + near[c, 1, there, :].astype(f32)
                    + far[c, 2, there, :].astype(f32),
                )

    def finish(self):
        for copy in self.sent:
            copy.wait_send()


def reduce_scratch(r, c, even=f32):
    q = r // 4
    return [
        pltpu.VMEM((4, r, c), bf),
        pltpu.VMEM((4, r, c), even),
        pltpu.VMEM((4, r, c), bf),
        pltpu.VMEM((2, 6, q, c), bf),
        pltpu.VMEM((2, 3, q, c), bf),
        pltpu.VMEM((2, 3, q, c), bf),
    ]


def rows_of_pair(a, i):
    two, r, k = 2, a.shape[1], a.shape[2]
    return a[pl.ds(2 * i, two)].reshape(two * r, k)


def times(a, w, nt):
    def product(i, odd, even):
        r = a.shape[1]

        @pl.loop(0, even.shape[1] // TILE)
        def _(j):
            at = pl.ds(pl.multiple_of(j * TILE, TILE), TILE)
            x = rows_of_pair(a, i)
            if nt:
                y = lax.dot_general(
                    x, w[at, :], (((1,), (1,)), ((), ())), preferred_element_type=f32
                )
            else:
                y = jnp.dot(x, w[:, at], preferred_element_type=f32)
            even[:, at] = y[:r].astype(even.dtype)
            odd[:, at] = y[r:].astype(odd.dtype)

    return product


def exchange_and_gather(reduce, gathers, step, body):
    reduce.run()
    for c in (0, 1):
        reduce.rows(c, step, body)
        gathers[c].start()
    for c in (0, 1):
        gathers[c].forward()
    for c in (0, 1):
        gathers[c].finish()
    reduce.finish()


def both_gathers(own, out, sems, local, peer):
    half = own.shape[0] // 2
    return [
        Gather(own, out, c * half, half, sems, REDUCE_SEMS + c * GATHER_SEMS, local.at[c], peer)
        for c in (0, 1)
    ]


EXCHANGE_SEMS = REDUCE_SEMS + 2 * GATHER_SEMS


def forward_kernel(
    nrm, wvs, sco, w, tok, vec, v_out, mix_out, ret_out, swi_out, mid, out,
    v_buf, mix_buf, ret_buf, swi_buf, po, pe, rc, sb, xr, yr, own, ssem, rsem, local,
):
    _, peer = place()
    greet([peer(1), peer(2), peer(4)])
    sems = (ssem, rsem)
    r, width = v_buf.shape[1:]
    kept = []

    def prepare(first):
        two = pl.ds(first, 2)
        x = nrm[two].reshape(2 * r, nrm.shape[2])

        @pl.loop(0, width // 256)
        def _(j):
            at = pl.ds(pl.multiple_of(j * 256, 256), 256)
            behind = pl.ds(pl.multiple_of(j * 256 + width, 256), 256)
            v = jnp.dot(x, wvs[:, at], preferred_element_type=f32).astype(bf)
            s = jnp.dot(x, wvs[:, behind], preferred_element_type=f32)
            for i in (0, 1):
                mine = v[i * r : (i + 1) * r]
                v_buf[first + i, :, at] = mine
                swi_buf[first + i, :, at] = s[i * r : (i + 1) * r]
                ret_buf[first + i, :, at] = jnp.dot(
                    sco[first + i], mine, preferred_element_type=f32
                )

        @pl.loop(0, 2 * r // 32)
        def _(j):
            k = first + lax.div(j, r // 32)
            at = pl.ds(pl.multiple_of(lax.rem(j, r // 32) * 32, 32), 32)
            value = ret_buf[k, at, :]
            centred = value - jnp.mean(value, axis=-1, keepdims=True)
            spread = jnp.mean(centred * centred, axis=-1, keepdims=True)
            gate = swi_buf[k, at, :]
            gate = gate / (1.0 + jnp.exp(-gate))
            mix_buf[k, at, :] = (
                gate * (centred * lax.rsqrt(jnp.maximum(spread, 0.25)))
            ).astype(bf)

        for i, (src, dst) in enumerate(
            ((v_buf, v_out), (mix_buf, mix_out), (ret_buf, ret_out), (swi_buf, swi_out))
        ):
            copy = pltpu.make_async_copy(
                src.at[two], dst.at[two], local.at[2 + 2 * first + i]
            )
            copy.start()
            kept.append(copy)

    def product(i, odd, even):
        step = w.shape[2]

        @pl.loop(0, w.shape[0])
        def _(j):
            at = pl.ds(pl.multiple_of(j * step, step), step)
            y = jnp.dot(rows_of_pair(mix_buf, i), w[j], preferred_element_type=f32)
            even[:, at] = y[:r].astype(even.dtype)
            odd[:, at] = y[r:].astype(odd.dtype)

    def body(at, value):
        value = value + tok[at, :].astype(f32)
        mid[at, :] = value
        center = jnp.mean(value, axis=-1, keepdims=True)
        centred = value - center
        spread = jnp.mean(centred * centred, axis=-1, keepdims=True)
        own[at, :] = (
            centred * lax.rsqrt(spread + 1e-05) * vec[0:1, :] + vec[1:2, :]
        ).astype(bf)

    reduce = Reduce(product, (po, pe, rc, sb, xr, yr), sems, 0, peer, prepare)
    exchange_and_gather(reduce, both_gathers(own, out, sems, local, peer), 16, body)
    for copy in kept:
        copy.wait()


def forward_exchange(nrm, wvs, sco, w, tok, vec, cid):
    _, r, d = nrm.shape
    width = w.shape[1]
    count = EXCHANGE_SEMS
    blocks = [((TP, r, width), t) for t in (bf, bf, f32, f32)]
    return pl.pallas_call(
        forward_kernel,
        out_shape=tuple(SDS(*b) for b in blocks) + (SDS((r, d), f32), SDS((TP, r, d), bf)),
        in_specs=[VMEM] * 6,
        out_specs=(ANY,) * 4 + (VMEM, ANY),
        scratch_shapes=[pltpu.VMEM(*b) for b in blocks]
        + reduce_scratch(r, d)
        + [
            pltpu.VMEM((r, d), bf),
            pltpu.SemaphoreType.DMA((count,)),
            pltpu.SemaphoreType.DMA((count,)),
            pltpu.SemaphoreType.DMA((18,)),
        ],
        compiler_params=pltpu.CompilerParams(
            collective_id=cid, has_side_effects=True, vmem_limit_bytes=60 << 20
        ),
        name="forward_exchange",
    )(nrm, wvs, sco, w, tok, vec)


def hidden_kernel(x, gu, hid, act_out, slope_out):
    width = hid.shape[2]
    step = 256

    @pl.loop(0, width // step)
    def _(j):
        at = pl.ds(pl.multiple_of(j * step, step), step)
        behind = pl.ds(pl.multiple_of(j * step + width, step), step)
        first = jnp.dot(x[0], gu[:, at], preferred_element_type=f32)
        second = jnp.dot(x[0], gu[:, behind], preferred_element_type=f32)
        share = 0.5 * (1.0 + lax.erf(first * math.sqrt(0.5)))
        act = first * share
        slope = share + first * (jnp.exp(-0.5 * first * first) * (1.0 / math.sqrt(2.0 * math.pi)))
        hid[0, :, at] = (act * second).astype(bf)
        act_out[0, :, at] = act
        slope_out[0, :, at] = slope * second


def hidden_units(x, gu):
    _, r, d = x.shape
    width = gu.shape[1] // 2
    row = pl.BlockSpec((1, r, width), lambda k: (k, 0, 0))
    return pl.pallas_call(
        hidden_kernel,
        grid=(TP,),
        out_shape=tuple(SDS((TP, r, width), t) for t in (bf, f32, f32)),
        in_specs=[
            pl.BlockSpec((1, r, d), lambda k: (k, 0, 0)),
            pl.BlockSpec(gu.shape, lambda k: (0, 0)),
        ],
        out_specs=(row, row, row),
        compiler_params=pltpu.CompilerParams(vmem_limit_bytes=56 << 20),
        cost_estimate=pl.CostEstimate(
            flops=4 * TP * r * d * width, bytes_accessed=24 << 20, transcendentals=2 * TP * r * width
        ),
        name="hidden_units",
    )(x, gu)


def hidden_back_kernel(cot, down, act, slope, out):
    width = act.shape[2]
    step = 256

    @pl.loop(0, width // step)
    def _(j):
        at = pl.ds(pl.multiple_of(j * step, step), step)
        behind = pl.ds(pl.multiple_of(j * step + width, step), step)
        grad = lax.dot_general(
            cot[0], down[at, :], (((1,), (1,)), ((), ())), preferred_element_type=f32
        )
        out[0, :, at] = (grad * slope[0, :, at]).astype(bf)
        out[0, :, behind] = (grad * act[0, :, at]).astype(bf)


def hidden_back(cot, down, act, slope):
    _, r, d = cot.shape
    width = act.shape[2]
    row = pl.BlockSpec((1, r, width), lambda k: (k, 0, 0))
    return pl.pallas_call(
        hidden_back_kernel,
        grid=(TP,),
        out_shape=SDS((TP, r, 2 * width), bf),
        in_specs=[
            pl.BlockSpec((1, r, d), lambda k: (k, 0, 0)),
            pl.BlockSpec(down.shape, lambda k: (0, 0)),
            row,
            row,
        ],
        out_specs=pl.BlockSpec((1, r, 2 * width), lambda k: (k, 0, 0)),
        compiler_params=pltpu.CompilerParams(vmem_limit_bytes=56 << 20),
        cost_estimate=pl.CostEstimate(
            flops=2 * TP * r * d * width, bytes_accessed=24 << 20, transcendentals=0
        ),
        name="hidden_back",
    )(cot, down, act, slope)


def backward_kernel(
    a, w, mid, cot, vec, gmid, out, sums, po, pe, rc, sb, xr, yr, own, acc, ssem, rsem, local
):
    _, peer = place()
    greet([peer(1), peer(2), peer(4)])
    sems = (ssem, rsem)
    acc[...] = jnp.zeros_like(acc)

    def body(at, g):
        value = mid[at, :]
        center = jnp.mean(value, axis=-1, keepdims=True)
        centred = value - center
        inv = lax.rsqrt(jnp.mean(centred * centred, axis=-1, keepdims=True) + 1e-05)
        hat = centred * inv
        acc[0] += g * hat
        acc[1] += g
        scaled = g * vec[0:1, :]
        mean_g = jnp.mean(scaled, axis=-1, keepdims=True)
        mean_gh = jnp.mean(scaled * hat, axis=-1, keepdims=True)
        grad = cot[at, :].astype(f32) + inv * (scaled - mean_g - hat * mean_gh)
        gmid[at, :] = grad
        own[at, :] = grad.astype(bf)

    reduce = Reduce(times(a, w, True), (po, pe, rc, sb, xr, yr), sems, 0, peer)
    exchange_and_gather(reduce, both_gathers(own, out, sems, local, peer), 16, body)
    sums[0:1, :] = jnp.sum(acc[0], axis=0, keepdims=True)
    sums[1:2, :] = jnp.sum(acc[1], axis=0, keepdims=True)


def backward_exchange(a, w, mid, cot, vec, cid):
    _, r, _ = a.shape
    c = w.shape[0]
    count = EXCHANGE_SEMS
    return pl.pallas_call(
        backward_kernel,
        out_shape=(SDS((r, c), f32), SDS((TP, r, c), bf), SDS((2, c), f32)),
        in_specs=[VMEM] * 5,
        out_specs=(VMEM, ANY, VMEM),
        scratch_shapes=reduce_scratch(r, c)
        + [
            pltpu.VMEM((r, c), bf),
            pltpu.VMEM((2, 16, c), f32),
            pltpu.SemaphoreType.DMA((count,)),
            pltpu.SemaphoreType.DMA((count,)),
            pltpu.SemaphoreType.DMA((2,)),
        ],
        compiler_params=pltpu.CompilerParams(
            collective_id=cid, has_side_effects=True, vmem_limit_bytes=52 << 20
        ),
        name="backward_exchange",
    )(a, w, mid, cot, vec)


def last_kernel(
    n, gqkv, gs, wqk, wvs, a2, w2, tok, gmid, gain, sums2, gtok, ffn, vec_out,
    po, pe, rc, sb, xr, yr, pe2, rc2, sb2, xr2, yr2, acc, vecs, near, far, part, ssem, rsem,
):
    dp = n // TP
    me, peer = place()
    g = lax.div(me, TP)
    width = vec_out.shape[1]
    others = [lax.rem(me + TP * j, n) for j in range(1, dp)]
    greet([peer(k) for k in range(1, TP)] + others)
    sems = (ssem, rsem)
    acc[...] = jnp.zeros_like(acc)
    nt = (((1,), (1,)), ((), ()))

    def product(i, odd, even):
        r, qk, v = gqkv.shape[1], wqk.shape[1], gs.shape[2]
        x, y = rows_of_pair(gqkv, i), rows_of_pair(gs, i)

        @pl.loop(0, even.shape[1] // TILE)
        def _(j):
            at = pl.ds(pl.multiple_of(j * TILE, TILE), TILE)
            z = lax.dot_general(x[:, :qk], wqk[at, :], nt, preferred_element_type=f32)
            z += lax.dot_general(x[:, qk:], wvs[at, :v], nt, preferred_element_type=f32)
            z += lax.dot_general(y, wvs[at, v:], nt, preferred_element_type=f32)
            even[:, at] = z[:r].astype(even.dtype)
            odd[:, at] = z[r:].astype(odd.dtype)

    one = Reduce(product, (po, pe, rc, sb, xr, yr), sems, 0, peer)
    one.run()
    for copy in one.core.values():
        copy.wait_send()
    one.sent = [copy for copy in one.sent if all(copy is not c for c in one.core.values())]
    two = Reduce(times(a2, w2, False), (po, pe2, rc2, sb2, xr2, yr2), sems, REDUCE_SEMS, peer)
    two.run()

    def body(at, grad):
        value = tok[at, :].astype(f32)
        center = jnp.mean(value, axis=-1, keepdims=True)
        centred = value - center
        inv = lax.rsqrt(jnp.mean(centred * centred, axis=-1, keepdims=True) + 1e-05)
        hat = centred * inv
        acc[0] += grad * hat
        acc[1] += grad
        scaled = grad * gain[...]
        mean_g = jnp.mean(scaled, axis=-1, keepdims=True)
        mean_gh = jnp.mean(scaled * hat, axis=-1, keepdims=True)
        gtok[at, :] = gmid[at, :] + inv * (scaled - mean_g - hat * mean_gh)

    for c in (0, 1):
        one.rows(c, 16, body)
    vecs[...] = jnp.zeros_like(vecs)
    vecs[0:1, :] = jnp.sum(acc[0], axis=0, keepdims=True)
    vecs[1:2, :] = jnp.sum(acc[1], axis=0, keepdims=True)
    vecs[2:4, :] = sums2[...]
    base = 2 * REDUCE_SEMS
    copies = []
    for j, dev in enumerate(others):
        at = pl.multiple_of(lax.div(dev, TP) * width, 128)
        copy = remote(vecs.at[:, pl.ds(at, width)], far.at[j], sems, base + j, dev)
        copy.start()
        copies.append(copy)

    def keep(at, value):
        ffn[at, :] = value

    two.rows(0, 32, keep)
    total = vecs[:, pl.ds(pl.multiple_of(g * width, 128), width)]
    for j, copy in enumerate(copies):
        copy.wait()
        total = total + far[j]
    part[...] = total
    copies = []
    for k in range(1, TP):
        copy = remote(part, near.at[k - 1], sems, base + dp + k - 1, peer(k))
        copy.start()
        copies.append(copy)
    two.rows(1, 32, keep)
    for k, copy in enumerate(copies):
        copy.wait()
        total = total + near[k]
    vec_out[...] = total
    one.finish()
    two.finish()


def last_exchange(n, gqkv, gs, wqk, wvs, a2, w2, tok, gmid, gain, sums2, cid):
    dp = n // TP
    _, r, _ = a2.shape
    c = w2.shape[1]
    width = c // dp
    count = 2 * REDUCE_SEMS + dp + TP
    return pl.pallas_call(
        functools.partial(last_kernel, n),
        out_shape=(SDS((r, c), f32), SDS((r, c), f32), SDS((8, width), f32)),
        in_specs=[VMEM] * 10,
        out_specs=(VMEM,) * 3,
        scratch_shapes=reduce_scratch(r, c)
        + reduce_scratch(r, c, bf)[1:]
        + [
            pltpu.VMEM((2, 16, c), f32),
            pltpu.VMEM((8, c), f32),
            pltpu.VMEM((TP - 1, 8, width), f32),
            pltpu.VMEM((dp, 8, width), f32),
            pltpu.VMEM((8, width), f32),
            pltpu.SemaphoreType.DMA((count,)),
            pltpu.SemaphoreType.DMA((count,)),
        ],
        compiler_params=pltpu.CompilerParams(
            collective_id=cid, has_side_effects=True, vmem_limit_bytes=67043328
        ),
        name="last_exchange",
    )(gqkv, gs, wqk, wvs, a2, w2, tok, gmid, gain, sums2)


def gate_back_kernel(g_low, w, ret, swi, gret, gswi):
    r, width = gret.shape[1:]
    cols = w.shape[2]
    nt = (((1,), (1,)), ((), ()))
    grad = jnp.zeros((r, width), f32)
    for j in range(w.shape[0]):
        grad += lax.dot_general(
            g_low[0, :, j * cols : (j + 1) * cols], w[j], nt, preferred_element_type=f32
        )
    value, gate = ret[0], swi[0]
    centred = value - jnp.mean(value, axis=-1, keepdims=True)
    spread = jnp.mean(centred * centred, axis=-1, keepdims=True)
    inv = lax.rsqrt(jnp.maximum(spread, 0.25))
    share = 1.0 / (1.0 + jnp.exp(-gate))
    silu = gate * share
    gswi[0] = (grad * (centred * inv) * (share * (1.0 + gate * (1.0 - share)))).astype(bf)
    grad = grad * silu
    pull = jnp.mean(grad * centred, axis=-1, keepdims=True)
    pull = jnp.where(spread > 0.25, inv * inv * inv * pull, 0.0)
    grad = grad * inv - centred * pull
    gret[0] = (grad - jnp.mean(grad, axis=-1, keepdims=True)).astype(bf)


def gate_back(g_low, w, ret, swi):
    _, r, d = g_low.shape
    width = ret.shape[2]
    row = pl.BlockSpec((1, r, width), lambda k: (k, 0, 0))
    return pl.pallas_call(
        gate_back_kernel,
        grid=(TP,),
        out_shape=(SDS(ret.shape, bf), SDS(ret.shape, bf)),
        in_specs=[
            pl.BlockSpec((1, r, d), lambda k: (k, 0, 0)),
            pl.BlockSpec(w.shape, lambda k: (0, 0, 0)),
            row,
            row,
        ],
        out_specs=(row, row),
        compiler_params=pltpu.CompilerParams(vmem_limit_bytes=56 << 20),
        cost_estimate=pl.CostEstimate(
            flops=2 * TP * r * d * width, bytes_accessed=22 << 20, transcendentals=TP * r * width
        ),
        name="gate_back",
    )(g_low, w, ret, swi)


def scores_back_kernel(sco, mask, q, k, v, gret, cosine, sine, out):
    nt, tn = (((1,), (1,)), ((), ())), (((0,), (0,)), ((), ()))
    kh = q.shape[2]
    half = kh // 2
    out[0, :, 2 * kh :] = lax.dot_general(
        sco[0], gret[0], tn, preferred_element_type=f32
    ).astype(bf)
    grad = lax.dot_general(gret[0], v[0], nt, preferred_element_type=f32)
    grad = (grad * mask[0]).astype(bf)
    gq = jnp.dot(grad, k[0], preferred_element_type=f32)
    gk = lax.dot_general(grad, q[0], tn, preferred_element_type=f32)
    for i, g in enumerate((gq, gk)):
        u, w = g[:, :half], g[:, half:]
        at = i * kh
        out[0, :, at : at + half] = (u * cosine[0] + w * sine[0]).astype(bf)
        out[0, :, at + half : at + kh] = (w * cosine[0] - u * sine[0]).astype(bf)


def scores_back(sco, mask, q, k, v, gret, cosine, sine):
    _, r, kh = q.shape
    arrays = (sco, mask, q, k, v, gret, cosine, sine)
    width = 2 * kh + v.shape[2]
    spec = [pl.BlockSpec((1,) + x.shape[1:], lambda i: (i, 0, 0)) for x in arrays]
    return pl.pallas_call(
        scores_back_kernel,
        grid=(TP,),
        out_shape=SDS((TP, r, width), bf),
        in_specs=spec,
        out_specs=pl.BlockSpec((1, r, width), lambda i: (i, 0, 0)),
        compiler_params=pltpu.CompilerParams(vmem_limit_bytes=56 << 20),
        cost_estimate=pl.CostEstimate(
            flops=4 * TP * r * r * (kh + v.shape[2]), bytes_accessed=16 << 20, transcendentals=0
        ),
        name="scores_back",
    )(*arrays)


def tp_groups(n):
    return [[g * TP + t for t in range(TP)] for g in range(n // TP)]


def dp_groups(n):
    return [[g * TP + t for g in range(n // TP)] for t in range(TP)]


def plane_a2a(x, n):
    return lax.all_to_all(x, AXIS, 0, 0, axis_index_groups=tp_groups(n), tiled=True)


def dp_gather(x, n):
    return lax.all_gather(x, AXIS, axis=0, tiled=True, axis_index_groups=dp_groups(n))


def dp_reduce(x, n):
    return lax.psum_scatter(
        x, AXIS, scatter_dimension=0, tiled=True, axis_index_groups=dp_groups(n)
    )


def layer_norm(value, gain, bias):
    center = jnp.mean(value, axis=-1, keepdims=True)
    centred = value - center
    spread = jnp.mean(centred * centred, axis=-1, keepdims=True)
    return centred * lax.rsqrt(spread + 1e-05) * gain + bias


def seq_positions(lengths, rows):
    ends = jnp.cumsum(lengths, axis=1)
    starts = ends - lengths
    index = jnp.arange(rows, dtype=jnp.int32)
    segment = jnp.sum((index[None, :, None] >= ends[:, None, :]).astype(jnp.int32), axis=2)
    member = segment[:, :, None] == jnp.arange(lengths.shape[1], dtype=jnp.int32)
    offset = index[None, :] - jnp.sum(jnp.where(member, starts[:, None, :], 0), axis=2)
    return segment, offset


def rotary_tables(offset):
    half = KH // 2
    freq = jnp.exp(-math.log(10000.0) * jnp.arange(half, dtype=f32) / half)
    angle = offset.astype(f32)[..., None] * freq
    return jnp.cos(angle), jnp.sin(angle)


def rotate(value, cosine, sine):
    half = KH // 2
    u, w = value[..., :half], value[..., half:]
    return jnp.concatenate([u * cosine - w * sine, w * cosine + u * sine], axis=-1)


def decay_mask(segment, offset, head):
    diff = offset[:, :, None] - offset[:, None, :]
    valid = (segment[:, :, None] == segment[:, None, :]) & (diff >= 0)
    steps = jnp.where(valid, diff, 0).astype(f32)
    log = jnp.log(1.0 - jnp.exp2(-5.0 - head.astype(f32)))
    return jnp.where(valid, jnp.exp(log * steps), 0.0) / math.sqrt(KH)


def dot(a, b):
    return lax.dot_general(a, b, (((1,), (0,)), ((), ())), preferred_element_type=f32)


def dot_tn(a, b):
    return lax.dot_general(a, b, (((0,), (0,)), ((), ())), preferred_element_type=f32)


def bmm(eq, a, b):
    return jnp.einsum(eq, a, b, preferred_element_type=f32)


def col_blocks(w):
    r, c = w.shape
    return w.reshape(r, TP, c // TP).transpose(1, 0, 2).reshape(TP * r, c // TP)


def join_kernel(widths, parts, x, *outs):
    at = 0
    for out, width in zip(outs, widths):
        piece = width // parts
        for t in range(TP):
            for p in range(parts):
                to = (p * TP + t) * piece
                out[:, to : to + piece] = x[t, :, at + p * piece : at + (p + 1) * piece].astype(f32)
        at += width


def join(x, widths, parts=1):
    r = x.shape[1]
    if any(width // parts % 128 for width in widths):
        made, at = [], 0
        for width in widths:
            part = x[:, :, at : at + width].reshape(TP, r, parts, width // parts)
            made.append(part.transpose(1, 2, 0, 3).reshape(r, TP * width).astype(f32))
            at += width
        return made
    return pl.pallas_call(
        functools.partial(join_kernel, widths, parts),
        out_shape=tuple(SDS((r, TP * width), f32) for width in widths),
        in_specs=[VMEM],
        out_specs=tuple(VMEM for _ in widths),
        compiler_params=pltpu.CompilerParams(vmem_limit_bytes=8 << 20),
        cost_estimate=pl.CostEstimate(flops=0, bytes_accessed=6 * x.size, transcendentals=0),
        name="join",
    )(x)


def after(x, *deps):
    return lax.optimization_barrier((x,) + deps)[0]


def on_device(n, tokens, lengths, gain1, bias1, wq, wk, wv, ws, wo, gain2, bias2, wg, wu, wd, cot):
    rows, d = tokens.shape
    ff = wg.shape[1]
    dp = n // TP
    shard = d // n
    unit = ff // n
    me = lax.axis_index(AXIS)
    head = lax.rem(me, TP)

    def ff_blocks(w):
        return w.reshape(shard, dp, TP, unit).transpose(2, 0, 1, 3).reshape(TP, shard, dp * unit)

    lens = jnp.pad(lengths[0].astype(f32), (0, shard - lengths.shape[1]))
    vec = jnp.stack([v.astype(f32) for v in (gain1, bias1, gain2, bias2)] + [lens])
    vec = jnp.pad(vec, ((0, 3), (0, 128 - shard)))
    qko_blk = first_exchange(wq, wk, wo, 1)
    qko = dp_gather(qko_blk.reshape(TP * shard, 4 * KH), n)
    tok_all, vec_all = second_exchange(n, after(tokens, qko_blk), vec, 2)
    vs_blk = third_exchange(after(wv, tok_all), ws, 3)
    vs = dp_gather(vs_blk.reshape(TP * shard, 2 * VH), n)
    gu_in = jnp.concatenate([ff_blocks(wg), ff_blocks(wu)], axis=2)
    gu_blk, cot_all = fourth_exchange(gu_in, after(cot, vs_blk), 4)
    gu = dp_gather(gu_blk.reshape(TP * shard, 2 * dp * unit), n)
    down = dp_gather(wd, n)
    gain1f, bias1f, gain2f, bias2f = (
        vec_all[:, :, i, :shard].reshape(1, d) for i in range(4)
    )
    vec2 = jnp.concatenate([gain2f, bias2f], axis=0)
    qk = qko[:, : 2 * KH]
    out = qko[:, 2 * KH :].reshape(n, shard, 2, d // TP).transpose(0, 2, 1, 3)
    out_blk = plane_a2a(out.reshape(TP * VH, d // TP), n).reshape(TP, VH, d // TP)

    mine = lax.dynamic_slice_in_dim(vec_all, lax.div(me, TP), 1, 0)[0, :, 4, :3]
    order = jnp.arange(TP, dtype=jnp.int32)
    pick = (order[None, :] == (order[:, None] ^ head)).astype(f32)
    len_all = jnp.sum(pick[:, :, None] * mine[None], axis=1).astype(jnp.int32)
    segment, offset = seq_positions(len_all, rows)
    cosine, sine = rotary_tables(offset)
    mask = decay_mask(segment, offset, head)

    normed = layer_norm(tok_all.reshape(TP * rows, d).astype(f32), gain1f, bias1f).astype(bf)
    qk_out = dot(normed, qk).reshape(TP, rows, 2 * KH)
    query, key = qk_out[..., :KH], qk_out[..., KH:]
    q_rot = rotate(query, cosine, sine).astype(bf)
    k_rot = rotate(key, cosine, sine).astype(bf)
    plain = bmm("btd,bsd->bts", q_rot, k_rot)
    scores = (plain * mask).astype(bf)
    v_low, mixed, retained, swish_in, middle, normed2 = forward_exchange(
        normed.reshape(TP, rows, d), vs, scores, out_blk, tokens, vec2, 5
    )
    hidden, act, slope = hidden_units(normed2, gu)
    normed2 = normed2.reshape(TP * rows, d)
    down_grad = dot_tn(hidden.reshape(TP * rows, dp * unit), cot_all.reshape(TP * rows, d)).astype(bf)
    g_down = dp_reduce(down_grad, n)

    g_fs = hidden_back(cot_all, down, act, slope)
    gu_grad = dot_tn(normed2, g_fs.reshape(TP * rows, 2 * dp * unit)).astype(bf)
    g_gu = dp_reduce(gu_grad, n)
    g_middle, g_low, sums2 = backward_exchange(g_fs, gu, middle, cot, vec2, 6)

    g_retained, g_swish = gate_back(g_low, out_blk, retained, swish_in)
    g_low = g_low.reshape(TP * rows, d)
    swish_grad = dot_tn(normed, g_swish.reshape(TP * rows, VH)).astype(bf)
    g_swi = dp_reduce(swish_grad, n)
    out_grad = dot_tn(mixed.reshape(TP * rows, VH), g_low).astype(bf)
    out_grad = plane_a2a(col_blocks(out_grad), n)
    g_qkv = scores_back(scores, mask, q_rot, k_rot, v_low, g_retained, cosine, sine)
    qkv_grad = dot_tn(normed, g_qkv.reshape(TP * rows, 2 * KH + VH)).astype(bf)
    g_qkv_own = dp_reduce(qkv_grad, n)
    g_out = dp_reduce(out_grad, n)
    grad_tokens, ffn, g_vecs = last_exchange(
        n, g_qkv, g_swish, qk, vs, hidden, down, tokens, g_middle, gain1f, sums2, 7
    )
    layer_out = (middle + ffn).astype(bf)

    g_vecs = lax.dynamic_slice_in_dim(g_vecs, head * shard, shard, 1)
    grad_d = g_down.astype(f32)
    g_gu = plane_a2a(g_gu, n)
    grad_g, grad_u = join(g_gu.reshape(TP, shard, 2 * dp * unit), (dp * unit,) * 2, dp)
    g_swi = plane_a2a(g_swi, n)
    (grad_s,) = join(g_swi.reshape(TP, shard, VH), (VH,))
    g_qkv_own = plane_a2a(g_qkv_own, n)
    grad_q, grad_k, grad_v = join(g_qkv_own.reshape(TP, shard, 2 * KH + VH), (KH, KH, VH))
    g_out = plane_a2a(g_out, n)
    (grad_o,) = join(g_out.reshape(TP, wo.shape[0], d // TP), (d // TP,))
    return (
        layer_out, grad_tokens, g_vecs[0], g_vecs[1], grad_q, grad_k, grad_v, grad_s, grad_o,
        g_vecs[2], g_vecs[3], grad_g, grad_u, grad_d,
    )


def solution(mesh):
    n = mesh.shape[AXIS]
    row, vec = P(AXIS, None), P(AXIS)
    ins = (row, row, vec, vec, row, row, row, row, row, vec, vec, row, row, row, row)
    outs = (row, row, vec, vec, row, row, row, row, row, vec, vec, row, row, row)

    def body(*args):
        return on_device(n, *args)

    return jax.shard_map(body, mesh=mesh, in_specs=ins, out_specs=outs, check_vma=False)
```

```python
import functools
import math

import jax
import jax.numpy as jnp
from jax import lax
from jax.experimental import pallas as pl
from jax.experimental.pallas import tpu as pltpu
from jax.sharding import PartitionSpec as P


KH = 256
VH = 512
TP = 8
AXIS = "fsdp"
MESH = pl.DeviceIdType.MESH
ANY = pl.BlockSpec(memory_space=pl.ANY)
VMEM = pl.BlockSpec(memory_space=pltpu.VMEM)
bf = jnp.bfloat16
f32 = jnp.float32
SDS = jax.ShapeDtypeStruct
ALL_VMEM = 67043328


def place():
    me = lax.axis_index(AXIS)
    steps = [s - 2 * s * lax.rem(lax.div(me, s), 2) for s in (1, 2, 4)]

    def peer(k):
        out = me
        for bit, step in enumerate(steps):
            if k >> bit & 1:
                out = out + step
        return out

    return me, peer


def greet(peers):
    barrier = pltpu.get_barrier_semaphore()
    for p in peers:
        pl.semaphore_signal(barrier, inc=1, device_id=(p,), device_id_type=MESH)
    pl.semaphore_wait(barrier, len(peers))


def remote(src, dst, sems, i, dev):
    return pltpu.make_async_remote_copy(
        src_ref=src, dst_ref=dst, send_sem=sems[0].at[i], recv_sem=sems[1].at[i],
        device_id=(dev,), device_id_type=MESH,
    )


GATHER_SEMS = 13


class Gather:
    def __init__(self, own, out, start, size, sems, base, local, peer):
        self.own, self.out, self.sems, self.base, self.local = own, out, sems, base, local
        h = size // 2
        self.all, self.top, self.bot = pl.ds(start, size), pl.ds(start, h), pl.ds(start + h, h)
        self.pc, self.px, self.py = peer(1), peer(2), peer(4)
        self.made = []

    def send(self, src, dst, dev):
        copy = remote(src, dst, self.sems, self.base + len(self.made), dev)
        copy.start()
        self.made.append(copy)
        return copy

    def pass_on(self, k, at):
        self.core.append(self.send(self.out.at[k, at], self.out.at[k + 1, at], self.pc))

    def start(self):
        own, out, top, bot = self.own, self.out, self.top, self.bot
        self.x0 = self.send(own.at[bot], out.at[2, bot], self.px)
        self.y0 = self.send(own.at[top], out.at[4, top], self.py)
        self.x1 = self.send(own.at[top], out.at[2, top], self.px)
        self.y1 = self.send(own.at[bot], out.at[4, bot], self.py)
        self.core = [self.send(own.at[self.all], out.at[1, self.all], self.pc)]
        self.keep = pltpu.make_async_copy(own.at[self.all], out.at[0, self.all], self.local)
        self.keep.start()

    def forward(self):
        out, top, bot = self.out, self.top, self.bot
        self.x0.wait_recv()
        self.fy = self.send(out.at[2, bot], out.at[6, bot], self.py)
        self.pass_on(2, bot)
        self.y0.wait_recv()
        self.fx = self.send(out.at[4, top], out.at[6, top], self.px)
        self.pass_on(4, top)
        self.x1.wait_recv()
        self.pass_on(2, top)
        self.y1.wait_recv()
        self.pass_on(4, bot)

    def finish(self):
        self.fy.wait_recv()
        self.pass_on(6, self.bot)
        self.fx.wait_recv()
        self.pass_on(6, self.top)
        for copy in self.core:
            copy.wait_recv()
        for copy in self.made:
            copy.wait_send()
        self.keep.wait()


def send_columns(src, out, cols, at, sems, base, local, t, peer, rows=None):
    copies = []
    rows = slice(None) if rows is None else rows

    def block(q):
        if len(src.shape) == 3:
            return src.at[q]
        return src.at[rows, pl.ds(pl.multiple_of(q * cols, 128), cols)]

    for k in range(1, TP):
        dev = peer(k)
        copy = remote(
            block(lax.rem(dev, TP)), out.at[t, :, pl.ds(at, cols)], sems, base + k - 1, dev
        )
        copy.start()
        copies.append(copy)
    keep = pltpu.make_async_copy(block(t), out.at[t, :, pl.ds(at, cols)], local)
    keep.start()
    return copies, keep


def finish(parts):
    for copies, keep in parts:
        for copy in copies:
            copy.wait()
        keep.wait()


def exchange_call(kernel, outs, args, sems, locals_, cid, specs=None, aliases=None, vmem=12 << 20):
    return pl.pallas_call(
        kernel,
        out_shape=outs,
        in_specs=specs or [VMEM] * len(args),
        input_output_aliases=aliases or {},
        out_specs=tuple(ANY for _ in outs),
        scratch_shapes=[
            pltpu.SemaphoreType.DMA((sems,)),
            pltpu.SemaphoreType.DMA((sems,)),
            pltpu.SemaphoreType.DMA((locals_,)),
        ],
        compiler_params=pltpu.CompilerParams(
            collective_id=cid, has_side_effects=True, vmem_limit_bytes=vmem
        ),
    )(*args)


def first_kernel(wq, wk, wo, out, ssem, rsem, local):
    me, peer = place()
    t = lax.rem(me, TP)
    greet([peer(k) for k in range(1, TP)])
    sems = (ssem, rsem)
    shard, cq, co = wq.shape[0], wq.shape[1] // TP, wo.shape[1] // TP
    low, high = pl.ds(0, shard), pl.ds(shard, shard)
    finish([
        send_columns(wq, out, cq, 0, sems, 0, local.at[0], t, peer),
        send_columns(wk, out, cq, cq, sems, 7, local.at[1], t, peer),
        send_columns(wo, out, co, 2 * cq, sems, 14, local.at[2], t, peer, low),
        send_columns(wo, out, co, 2 * cq + co, sems, 21, local.at[3], t, peer, high),
    ])


def first_exchange(wq, wk, wo, cid):
    width = 2 * wq.shape[1] // TP + 2 * wo.shape[1] // TP
    outs = (SDS((TP, wq.shape[0], width), bf),)
    return exchange_call(first_kernel, outs, (wq, wk, wo), 28, 4, cid)[0]


def send_along(n, src, out, sems, base, parity):
    dp = n // TP
    me = lax.axis_index(AXIS)
    g = lax.div(me, TP)
    copies = []
    for j in range(1, dp):
        if j % 2 == parity:
            copy = remote(src, out.at[g], sems, base + j, lax.rem(me + TP * j, n))
            copy.start()
            copies.append(copy)
    return copies


def others_along(n):
    me = lax.axis_index(AXIS)
    return [lax.rem(me + TP * j, n) for j in range(1, n // TP)]


def second_kernel(n, tok, vec, wd, tok_out, vec_out, wd_out, ssem, rsem, local):
    dp = n // TP
    me, peer = place()
    t, g = lax.rem(me, TP), lax.div(me, TP)
    others = others_along(n)
    greet([peer(k) for k in range(1, TP)] + others)
    sems = (ssem, rsem)
    base = GATHER_SEMS
    far = []
    keep = pltpu.make_async_copy(vec, vec_out.at[g, t], local.at[1])
    keep.start()
    mine = pltpu.make_async_copy(wd, wd_out.at[g], local.at[2])
    mine.start()
    for j, dev in enumerate(others):
        copy = remote(vec, vec_out.at[g, t], sems, base + TP + j, dev)
        copy.start()
        far.append(copy)
    gather = Gather(tok, tok_out, 0, tok.shape[0], sems, 0, local.at[0], peer)
    gather.start()
    along = send_along(n, wd, wd_out, sems, base + TP + dp, 1)
    for copy in far:
        copy.wait()
    keep.wait()
    near = []
    for k in range(1, TP):
        copy = remote(vec_out.at[:, t], vec_out.at[:, t], sems, base + k, peer(k))
        copy.start()
        near.append(copy)
    gather.forward()
    gather.finish()
    for copy in near + along:
        copy.wait()
    mine.wait()


def second_exchange(n, tok, vec, wd, cid):
    dp = n // TP
    outs = (
        SDS((TP,) + tok.shape, bf),
        SDS((dp, TP) + vec.shape, f32),
        SDS((dp,) + wd.shape, bf),
    )
    kernel = functools.partial(second_kernel, n)
    sems = GATHER_SEMS + TP + 2 * dp
    return exchange_call(kernel, outs, (tok, vec, wd), sems, 3, cid, vmem=ALL_VMEM)


def third_kernel(wv, ws, gu, out, gu_out, ssem, rsem, local):
    me, peer = place()
    t = lax.rem(me, TP)
    greet([peer(k) for k in range(1, TP)])
    sems = (ssem, rsem)
    cols = wv.shape[1] // TP
    finish([
        send_columns(wv, out, cols, 0, sems, 0, local.at[0], t, peer),
        send_columns(ws, out, cols, cols, sems, 7, local.at[1], t, peer),
        send_columns(gu, gu_out, gu.shape[2], 0, sems, 14, local.at[2], t, peer),
    ])


def third_exchange(wv, ws, gu, cid):
    outs = (SDS((TP, wv.shape[0], 2 * wv.shape[1] // TP), bf), SDS(gu.shape, bf))
    return exchange_call(third_kernel, outs, (wv, ws, gu), 21, 3, cid)


def fourth_kernel(n, at, cot, qko, wd, _, cot_out, o_out, wd_out, ssem, rsem, local):
    me, peer = place()
    t = lax.rem(me, TP)
    others = others_along(n)
    greet([peer(k) for k in range(1, TP)] + others)
    sems = (ssem, rsem)
    share, cols = n // TP, o_out.shape[4]
    base = GATHER_SEMS + 2 * TP
    gather = Gather(cot, cot_out, 0, cot.shape[0], sems, 0, local.at[0], peer)
    gather.start()
    along = send_along(n, wd, wd_out, sems, base, 0)
    copies, keeps = [], []

    def part(p, half):
        return qko.at[pl.ds(p * share, share), :, pl.ds(at + half * cols, cols)]

    for half in (0, 1):
        for k in range(1, TP):
            dev = peer(k)
            copy = remote(
                part(lax.rem(dev, TP), half), o_out.at[t, :, half], sems,
                GATHER_SEMS + half * TP + k, dev,
            )
            copy.start()
            copies.append(copy)
        keep = pltpu.make_async_copy(part(t, half), o_out.at[t, :, half], local.at[1 + half])
        keep.start()
        keeps.append(keep)
    gather.forward()
    gather.finish()
    for copy in copies + along:
        copy.wait()
    for keep in keeps:
        keep.wait()


def fourth_exchange(n, cot, qko, at, wd, wd_all, cid):
    _, shard, width = qko.shape
    cols = (width - at) // 2
    outs = (
        SDS((TP,) + cot.shape, bf),
        SDS((TP, n // TP, 2, shard, cols), bf),
        SDS(wd_all.shape, bf),
    )
    kernel = functools.partial(fourth_kernel, n, at)
    return exchange_call(
        kernel, outs, (cot, qko, wd, wd_all),
        GATHER_SEMS + 2 * TP + n // TP, 3, cid,
        specs=[VMEM, ANY, VMEM, ANY], aliases={3: 2}, vmem=ALL_VMEM,
    )


REDUCE_SEMS = 16
TILE = 512


class Reduce:
    def __init__(self, product, bufs, sems, base, peer, prepare=None):
        self.product, self.prepare, self.sems, self.base = product, prepare, sems, base
        self.po, self.pe, self.rc, self.sb, self.xr, self.yr = bufs
        self.pc, self.px, self.py = peer(1), peer(2), peer(4)
        self.q = self.pe.shape[1] // 4
        self.sent, self.core, self.got = [], {}, ({}, {})

    def send(self, src, dst, dev, i):
        copy = remote(src, dst, self.sems, self.base + i, dev)
        copy.start()
        self.sent.append(copy)
        return copy

    def ready(self, i):
        if self.prepare is not None:
            self.prepare(2 * i)

    def pair(self, i):
        self.product(i, self.po.at[i], self.pe.at[i])
        self.core[i] = self.send(self.po.at[i], self.rc.at[i], self.pc, i)

    def add(self, c, i, lower, out, more=None):
        step = 32

        @pl.loop(0, self.q // step)
        def _(j):
            there = pl.ds(pl.multiple_of(j * step, step), step)
            here = pl.ds(pl.multiple_of(j * step + (2 * c + lower) * self.q, step), step)
            total = self.pe[i, here, :].astype(f32) + self.rc[i, here, :].astype(f32)
            if more is not None:
                total = total + more[there, :].astype(f32)
            self.sb[c, out, there, :] = total.astype(bf)

    def link(self, c, slot, name, ring, at, dev):
        self.got[c][name] = self.send(
            self.sb.at[c, slot], ring.at[c, at], dev, 4 + 6 * c + slot
        )

    def six(self, c):
        self.add(c, 3, 0, 0)
        self.link(c, 0, "x6", self.xr, 0, self.px)
        self.add(c, 3, 1, 1)
        self.link(c, 1, "y6", self.yr, 0, self.py)

    def two(self, c):
        self.add(c, 1, 0, 2)
        self.link(c, 2, "x2", self.xr, 1, self.px)

    def four(self, c):
        self.add(c, 2, 1, 3)
        self.link(c, 3, "y4", self.yr, 1, self.py)

    def onward(self, c):
        self.got[c]["x6"].wait_recv()
        self.add(c, 2, 0, 4, self.xr.at[c, 0])
        self.link(c, 4, "y4b", self.yr, 2, self.py)
        self.got[c]["y6"].wait_recv()
        self.add(c, 1, 1, 5, self.yr.at[c, 0])
        self.link(c, 5, "x2b", self.xr, 2, self.px)

    def run(self):
        self.ready(3)
        self.pair(3)
        stages = ((1, 3, self.six), (2, 1, self.two), (0, 2, self.four))
        for following, now, stage in stages:
            self.ready(following)
            if self.prepare is None:
                self.pair(following)
            self.core[now].wait_recv()
            for c in (0, 1):
                stage(c)
            if self.prepare is not None:
                self.pair(following)
        for c in (0, 1):
            self.onward(c)

    def rows(self, c, step, body):
        if c == 0:
            self.core[0].wait_recv()
        for name in ("x2", "y4", "y4b", "x2b"):
            self.got[c][name].wait_recv()
        for lower in (0, 1):
            near, far = (self.yr, self.xr) if lower else (self.xr, self.yr)

            @pl.loop(0, self.q // step)
            def _(j, lower=lower, near=near, far=far):
                there = pl.ds(pl.multiple_of(j * step, step), step)
                here = pl.ds(pl.multiple_of(j * step + (2 * c + lower) * self.q, step), step)
                body(
                    here,
                    self.pe[0, here, :].astype(f32)
                    + self.rc[0, here, :].astype(f32)
                    + near[c, 1, there, :].astype(f32)
                    + far[c, 2, there, :].astype(f32),
                )

    def finish(self):
        for copy in self.sent:
            copy.wait_send()


def reduce_scratch(r, c, even=f32):
    q = r // 4
    return [
        pltpu.VMEM((4, r, c), bf),
        pltpu.VMEM((4, r, c), even),
        pltpu.VMEM((4, r, c), bf),
        pltpu.VMEM((2, 6, q, c), bf),
        pltpu.VMEM((2, 3, q, c), bf),
        pltpu.VMEM((2, 3, q, c), bf),
    ]


def rows_of_pair(a, i):
    two, r, k = 2, a.shape[1], a.shape[2]
    return a[pl.ds(2 * i, two)].reshape(two * r, k)


def times(a, w, nt):
    def product(i, odd, even):
        r = a.shape[1]

        @pl.loop(0, even.shape[1] // TILE)
        def _(j):
            at = pl.ds(pl.multiple_of(j * TILE, TILE), TILE)
            x = rows_of_pair(a, i)
            if nt:
                y = lax.dot_general(
                    x, w[at, :], (((1,), (1,)), ((), ())), preferred_element_type=f32
                )
            else:
                y = jnp.dot(x, w[:, at], preferred_element_type=f32)
            even[:, at] = y[:r].astype(even.dtype)
            odd[:, at] = y[r:].astype(odd.dtype)

    return product


def exchange_and_gather(reduce, gathers, step, body):
    reduce.run()
    for c in (0, 1):
        reduce.rows(c, step, body)
        gathers[c].start()
    for c in (0, 1):
        gathers[c].forward()
    for c in (0, 1):
        gathers[c].finish()
    reduce.finish()


def both_gathers(own, out, sems, local, peer):
    half = own.shape[0] // 2
    return [
        Gather(own, out, c * half, half, sems, REDUCE_SEMS + c * GATHER_SEMS, local.at[c], peer)
        for c in (0, 1)
    ]


EXCHANGE_SEMS = REDUCE_SEMS + 2 * GATHER_SEMS


def forward_kernel(
    nrm, wvs, sco, w, tok, vec, v_out, mix_out, ret_out, swi_out, mid, out,
    v_buf, mix_buf, ret_buf, swi_buf, po, pe, rc, sb, xr, yr, own, ssem, rsem, local,
):
    _, peer = place()
    greet([peer(1), peer(2), peer(4)])
    sems = (ssem, rsem)
    r, width = v_buf.shape[1:]
    kept = []

    def prepare(first):
        two = pl.ds(first, 2)
        x = nrm[two].reshape(2 * r, nrm.shape[2])

        @pl.loop(0, width // 256)
        def _(j):
            at = pl.ds(pl.multiple_of(j * 256, 256), 256)
            behind = pl.ds(pl.multiple_of(j * 256 + width, 256), 256)
            v = jnp.dot(x, wvs[:, at], preferred_element_type=f32).astype(bf)
            s = jnp.dot(x, wvs[:, behind], preferred_element_type=f32)
            for i in (0, 1):
                mine = v[i * r : (i + 1) * r]
                v_buf[first + i, :, at] = mine
                swi_buf[first + i, :, at] = s[i * r : (i + 1) * r]
                ret_buf[first + i, :, at] = jnp.dot(
                    sco[first + i], mine, preferred_element_type=f32
                )

        @pl.loop(0, 2 * r // 32)
        def _(j):
            k = first + lax.div(j, r // 32)
            at = pl.ds(pl.multiple_of(lax.rem(j, r // 32) * 32, 32), 32)
            value = ret_buf[k, at, :]
            centred = value - jnp.mean(value, axis=-1, keepdims=True)
            spread = jnp.mean(centred * centred, axis=-1, keepdims=True)
            gate = swi_buf[k, at, :]
            gate = gate / (1.0 + jnp.exp(-gate))
            mix_buf[k, at, :] = (
                gate * (centred * lax.rsqrt(jnp.maximum(spread, 0.25)))
            ).astype(bf)

        for i, (src, dst) in enumerate(
            ((v_buf, v_out), (mix_buf, mix_out), (ret_buf, ret_out), (swi_buf, swi_out))
        ):
            copy = pltpu.make_async_copy(
                src.at[two], dst.at[two], local.at[2 + 2 * first + i]
            )
            copy.start()
            kept.append(copy)

    def product(i, odd, even):
        step = w.shape[2]

        @pl.loop(0, w.shape[0])
        def _(j):
            at = pl.ds(pl.multiple_of(j * step, step), step)
            y = jnp.dot(rows_of_pair(mix_buf, i), w[j], preferred_element_type=f32)
            even[:, at] = y[:r].astype(even.dtype)
            odd[:, at] = y[r:].astype(odd.dtype)

    def body(at, value):
        value = value + tok[at, :].astype(f32)
        mid[at, :] = value
        center = jnp.mean(value, axis=-1, keepdims=True)
        centred = value - center
        spread = jnp.mean(centred * centred, axis=-1, keepdims=True)
        own[at, :] = (
            centred * lax.rsqrt(spread + 1e-05) * vec[0:1, :] + vec[1:2, :]
        ).astype(bf)

    reduce = Reduce(product, (po, pe, rc, sb, xr, yr), sems, 0, peer, prepare)
    exchange_and_gather(reduce, both_gathers(own, out, sems, local, peer), 16, body)
    for copy in kept:
        copy.wait()


def forward_exchange(nrm, wvs, sco, w, tok, vec, cid):
    _, r, d = nrm.shape
    width = w.shape[1]
    count = EXCHANGE_SEMS
    blocks = [((TP, r, width), t) for t in (bf, bf, f32, f32)]
    return pl.pallas_call(
        forward_kernel,
        out_shape=tuple(SDS(*b) for b in blocks) + (SDS((r, d), f32), SDS((TP, r, d), bf)),
        in_specs=[VMEM] * 6,
        out_specs=(ANY,) * 4 + (VMEM, ANY),
        scratch_shapes=[pltpu.VMEM(*b) for b in blocks]
        + reduce_scratch(r, d)
        + [
            pltpu.VMEM((r, d), bf),
            pltpu.SemaphoreType.DMA((count,)),
            pltpu.SemaphoreType.DMA((count,)),
            pltpu.SemaphoreType.DMA((18,)),
        ],
        compiler_params=pltpu.CompilerParams(
            collective_id=cid, has_side_effects=True, vmem_limit_bytes=60 << 20
        ),
        name="forward_exchange",
    )(nrm, wvs, sco, w, tok, vec)


def norm_kernel(x, gain, bias, out):
    step = 32

    @pl.loop(0, x.shape[1] // step)
    def _(j):
        at = pl.ds(pl.multiple_of(j * step, step), step)
        value = x[0, at, :].astype(f32)
        centred = value - jnp.mean(value, axis=-1, keepdims=True)
        spread = jnp.mean(centred * centred, axis=-1, keepdims=True)
        out[0, at, :] = (centred * lax.rsqrt(spread + 1e-05) * gain[...] + bias[...]).astype(bf)


def norm_rows(x, gain, bias):
    _, r, d = x.shape
    row = pl.BlockSpec((1, r, d), lambda k: (k, 0, 0))
    vec = pl.BlockSpec((1, d), lambda k: (0, 0))
    return pl.pallas_call(
        norm_kernel,
        grid=(TP,),
        out_shape=SDS(x.shape, bf),
        in_specs=[row, vec, vec],
        out_specs=row,
        compiler_params=pltpu.CompilerParams(vmem_limit_bytes=56 << 20),
        cost_estimate=pl.CostEstimate(
            flops=8 * x.size, bytes_accessed=4 * x.size, transcendentals=0
        ),
        name="norm_rows",
    )(x, gain, bias)


def scores_kernel(x, w, cosine, sine, mask, q_out, k_out, sco, w_out):
    two, r, kh = q_out.shape
    half = kh // 2
    w_out[...] = w[...]
    rows = x[...].reshape(two * r, x.shape[2])
    for j, out in enumerate((q_out, k_out)):
        y = jnp.dot(rows, w[:, j * kh : (j + 1) * kh], preferred_element_type=f32)
        for i in range(two):
            u, v = y[i * r : (i + 1) * r, :half], y[i * r : (i + 1) * r, half:]
            out[i, :, :half] = (u * cosine[i] - v * sine[i]).astype(bf)
            out[i, :, half:] = (v * cosine[i] + u * sine[i]).astype(bf)
    for i in range(two):
        plain = lax.dot_general(
            q_out[i], k_out[i], (((1,), (1,)), ((), ())), preferred_element_type=f32
        )
        sco[i] = (plain * mask[i]).astype(bf)


def rotated_and_scores(x, qko, cosine, sine, mask):
    _, r, d = x.shape
    pair = lambda k: (k, 0, 0)
    square = pl.BlockSpec((2, r, KH), pair)
    angle = pl.BlockSpec((2, r, KH // 2), pair)
    weights = pl.BlockSpec((d, 2 * KH), lambda k: (0, 0))
    return pl.pallas_call(
        scores_kernel,
        grid=(TP // 2,),
        out_shape=(SDS((TP, r, KH), bf), SDS((TP, r, KH), bf), SDS(mask.shape, bf), SDS((d, 2 * KH), bf)),
        in_specs=[pl.BlockSpec((2, r, d), pair), weights, angle, angle, pl.BlockSpec((2, r, r), pair)],
        out_specs=(square, square, pl.BlockSpec((2, r, r), pair), weights),
        compiler_params=pltpu.CompilerParams(vmem_limit_bytes=56 << 20),
        cost_estimate=pl.CostEstimate(
            flops=4 * TP * r * d * KH, bytes_accessed=16 << 20, transcendentals=0
        ),
        name="rotated_and_scores",
    )(x, qko, cosine, sine, mask)


def hidden_kernel(x, gu, hid, act_out, slope_out):
    width = hid.shape[2]
    step = 256

    @pl.loop(0, width // step)
    def _(j):
        at = pl.ds(pl.multiple_of(j * step, step), step)
        behind = pl.ds(pl.multiple_of(j * step + width, step), step)
        rows = x[...].reshape(-1, x.shape[2])
        first = jnp.dot(rows, gu[:, at], preferred_element_type=f32)
        second = jnp.dot(rows, gu[:, behind], preferred_element_type=f32)
        share = 0.5 * (1.0 + lax.erf(first * math.sqrt(0.5)))
        act = first * share
        slope = share + first * (jnp.exp(-0.5 * first * first) * (1.0 / math.sqrt(2.0 * math.pi)))
        block = hid.shape[:2] + (step,)
        hid[:, :, at] = (act * second).astype(bf).reshape(block)
        act_out[:, :, at] = act.reshape(block)
        slope_out[:, :, at] = (slope * second).reshape(block)


def hidden_units(x, gu):
    _, r, d = x.shape
    width = gu.shape[1] // 2
    row = pl.BlockSpec((2, r, width), lambda k: (k, 0, 0))
    return pl.pallas_call(
        hidden_kernel,
        grid=(TP // 2,),
        out_shape=tuple(SDS((TP, r, width), t) for t in (bf, f32, f32)),
        in_specs=[
            pl.BlockSpec((2, r, d), lambda k: (k, 0, 0)),
            pl.BlockSpec(gu.shape, lambda k: (0, 0)),
        ],
        out_specs=(row, row, row),
        compiler_params=pltpu.CompilerParams(vmem_limit_bytes=56 << 20),
        cost_estimate=pl.CostEstimate(
            flops=4 * TP * r * d * width, bytes_accessed=24 << 20, transcendentals=2 * TP * r * width
        ),
        name="hidden_units",
    )(x, gu)


def hidden_back_kernel(cot, down, act, slope, out):
    width = act.shape[2]
    step = 256

    @pl.loop(0, width // step)
    def _(j):
        at = pl.ds(pl.multiple_of(j * step, step), step)
        behind = pl.ds(pl.multiple_of(j * step + width, step), step)
        grad = lax.dot_general(
            cot[...].reshape(-1, cot.shape[2]), down[at, :], (((1,), (1,)), ((), ())),
            preferred_element_type=f32,
        ).reshape(act.shape[:2] + (step,))
        out[:, :, at] = (grad * slope[:, :, at]).astype(bf)
        out[:, :, behind] = (grad * act[:, :, at]).astype(bf)


def hidden_back(cot, down, act, slope):
    _, r, d = cot.shape
    width = act.shape[2]
    row = pl.BlockSpec((2, r, width), lambda k: (k, 0, 0))
    return pl.pallas_call(
        hidden_back_kernel,
        grid=(TP // 2,),
        out_shape=SDS((TP, r, 2 * width), bf),
        in_specs=[
            pl.BlockSpec((2, r, d), lambda k: (k, 0, 0)),
            pl.BlockSpec(down.shape, lambda k: (0, 0)),
            row,
            row,
        ],
        out_specs=pl.BlockSpec((2, r, 2 * width), lambda k: (k, 0, 0)),
        compiler_params=pltpu.CompilerParams(vmem_limit_bytes=56 << 20),
        cost_estimate=pl.CostEstimate(
            flops=2 * TP * r * d * width, bytes_accessed=24 << 20, transcendentals=0
        ),
        name="hidden_back",
    )(cot, down, act, slope)


def backward_kernel(
    a, w, mid, cot, vec, gmid, out, sums, po, pe, rc, sb, xr, yr, own, acc, ssem, rsem, local
):
    _, peer = place()
    greet([peer(1), peer(2), peer(4)])
    sems = (ssem, rsem)
    acc[...] = jnp.zeros_like(acc)

    def body(at, g):
        value = mid[at, :]
        center = jnp.mean(value, axis=-1, keepdims=True)
        centred = value - center
        inv = lax.rsqrt(jnp.mean(centred * centred, axis=-1, keepdims=True) + 1e-05)
        hat = centred * inv
        acc[0] += g * hat
        acc[1] += g
        scaled = g * vec[0:1, :]
        mean_g = jnp.mean(scaled, axis=-1, keepdims=True)
        mean_gh = jnp.mean(scaled * hat, axis=-1, keepdims=True)
        grad = cot[at, :].astype(f32) + inv * (scaled - mean_g - hat * mean_gh)
        gmid[at, :] = grad
        own[at, :] = grad.astype(bf)

    reduce = Reduce(times(a, w, True), (po, pe, rc, sb, xr, yr), sems, 0, peer)
    exchange_and_gather(reduce, both_gathers(own, out, sems, local, peer), 16, body)
    sums[0:1, :] = jnp.sum(acc[0], axis=0, keepdims=True)
    sums[1:2, :] = jnp.sum(acc[1], axis=0, keepdims=True)


def backward_exchange(a, w, mid, cot, vec, cid):
    _, r, _ = a.shape
    c = w.shape[0]
    count = EXCHANGE_SEMS
    return pl.pallas_call(
        backward_kernel,
        out_shape=(SDS((r, c), f32), SDS((TP, r, c), bf), SDS((2, c), f32)),
        in_specs=[VMEM] * 5,
        out_specs=(VMEM, ANY, VMEM),
        scratch_shapes=reduce_scratch(r, c)
        + [
            pltpu.VMEM((r, c), bf),
            pltpu.VMEM((2, 16, c), f32),
            pltpu.SemaphoreType.DMA((count,)),
            pltpu.SemaphoreType.DMA((count,)),
            pltpu.SemaphoreType.DMA((2,)),
        ],
        compiler_params=pltpu.CompilerParams(
            collective_id=cid, has_side_effects=True, vmem_limit_bytes=52 << 20
        ),
        name="backward_exchange",
    )(a, w, mid, cot, vec)


def last_kernel(
    n, gqkv, gs, wqk, wvs, a2, w2, tok, gmid, gain, sums2, gtok, ffn, vec_out,
    po, pe, rc, sb, xr, yr, pe2, rc2, sb2, xr2, yr2, acc, vecs, near, far, part, ssem, rsem,
):
    dp = n // TP
    me, peer = place()
    g = lax.div(me, TP)
    width = vec_out.shape[1]
    others = [lax.rem(me + TP * j, n) for j in range(1, dp)]
    greet([peer(k) for k in range(1, TP)] + others)
    sems = (ssem, rsem)
    acc[...] = jnp.zeros_like(acc)
    nt = (((1,), (1,)), ((), ()))

    def product(i, odd, even):
        r, qk, v = gqkv.shape[1], wqk.shape[1], gs.shape[2]
        x, y = rows_of_pair(gqkv, i), rows_of_pair(gs, i)

        @pl.loop(0, even.shape[1] // TILE)
        def _(j):
            at = pl.ds(pl.multiple_of(j * TILE, TILE), TILE)
            z = lax.dot_general(x[:, :qk], wqk[at, :], nt, preferred_element_type=f32)
            z += lax.dot_general(x[:, qk:], wvs[at, :v], nt, preferred_element_type=f32)
            z += lax.dot_general(y, wvs[at, v:], nt, preferred_element_type=f32)
            even[:, at] = z[:r].astype(even.dtype)
            odd[:, at] = z[r:].astype(odd.dtype)

    one = Reduce(product, (po, pe, rc, sb, xr, yr), sems, 0, peer)
    one.run()
    for copy in one.core.values():
        copy.wait_send()
    one.sent = [copy for copy in one.sent if all(copy is not c for c in one.core.values())]
    two = Reduce(times(a2, w2, False), (po, pe2, rc2, sb2, xr2, yr2), sems, REDUCE_SEMS, peer)
    two.run()

    def body(at, grad):
        value = tok[at, :].astype(f32)
        center = jnp.mean(value, axis=-1, keepdims=True)
        centred = value - center
        inv = lax.rsqrt(jnp.mean(centred * centred, axis=-1, keepdims=True) + 1e-05)
        hat = centred * inv
        acc[0] += grad * hat
        acc[1] += grad
        scaled = grad * gain[...]
        mean_g = jnp.mean(scaled, axis=-1, keepdims=True)
        mean_gh = jnp.mean(scaled * hat, axis=-1, keepdims=True)
        gtok[at, :] = gmid[at, :] + inv * (scaled - mean_g - hat * mean_gh)

    for c in (0, 1):
        one.rows(c, 16, body)
    vecs[...] = jnp.zeros_like(vecs)
    vecs[0:1, :] = jnp.sum(acc[0], axis=0, keepdims=True)
    vecs[1:2, :] = jnp.sum(acc[1], axis=0, keepdims=True)
    vecs[2:4, :] = sums2[...]
    base = 2 * REDUCE_SEMS
    copies = []
    for j, dev in enumerate(others):
        at = pl.multiple_of(lax.div(dev, TP) * width, 128)
        copy = remote(vecs.at[:, pl.ds(at, width)], far.at[j], sems, base + j, dev)
        copy.start()
        copies.append(copy)

    def keep(at, value):
        ffn[at, :] = value

    two.rows(0, 32, keep)
    total = vecs[:, pl.ds(pl.multiple_of(g * width, 128), width)]
    for j, copy in enumerate(copies):
        copy.wait()
        total = total + far[j]
    part[...] = total
    copies = []
    for k in range(1, TP):
        copy = remote(part, near.at[k - 1], sems, base + dp + k - 1, peer(k))
        copy.start()
        copies.append(copy)
    two.rows(1, 32, keep)
    for k, copy in enumerate(copies):
        copy.wait()
        total = total + near[k]
    vec_out[...] = total
    one.finish()
    two.finish()


def last_exchange(n, gqkv, gs, wqk, wvs, a2, w2, tok, gmid, gain, sums2, cid):
    dp = n // TP
    _, r, _ = a2.shape
    c = w2.shape[1]
    width = c // dp
    count = 2 * REDUCE_SEMS + dp + TP
    return pl.pallas_call(
        functools.partial(last_kernel, n),
        out_shape=(SDS((r, c), f32), SDS((r, c), f32), SDS((8, width), f32)),
        in_specs=[VMEM] * 10,
        out_specs=(VMEM,) * 3,
        scratch_shapes=reduce_scratch(r, c)
        + reduce_scratch(r, c, bf)[1:]
        + [
            pltpu.VMEM((2, 16, c), f32),
            pltpu.VMEM((8, c), f32),
            pltpu.VMEM((TP - 1, 8, width), f32),
            pltpu.VMEM((dp, 8, width), f32),
            pltpu.VMEM((8, width), f32),
            pltpu.SemaphoreType.DMA((count,)),
            pltpu.SemaphoreType.DMA((count,)),
        ],
        compiler_params=pltpu.CompilerParams(
            collective_id=cid, has_side_effects=True, vmem_limit_bytes=ALL_VMEM
        ),
        name="last_exchange",
    )(gqkv, gs, wqk, wvs, a2, w2, tok, gmid, gain, sums2)


def gate_back_kernel(g_low, w, ret, swi, gret, gswi):
    r, width = gret.shape[1:]
    cols = w.shape[2]
    nt = (((1,), (1,)), ((), ()))
    grad = jnp.zeros((r, width), f32)
    for j in range(w.shape[0]):
        grad += lax.dot_general(
            g_low[0, :, j * cols : (j + 1) * cols], w[j], nt, preferred_element_type=f32
        )
    value, gate = ret[0], swi[0]
    centred = value - jnp.mean(value, axis=-1, keepdims=True)
    spread = jnp.mean(centred * centred, axis=-1, keepdims=True)
    inv = lax.rsqrt(jnp.maximum(spread, 0.25))
    share = 1.0 / (1.0 + jnp.exp(-gate))
    silu = gate * share
    gswi[0] = (grad * (centred * inv) * (share * (1.0 + gate * (1.0 - share)))).astype(bf)
    grad = grad * silu
    pull = jnp.mean(grad * centred, axis=-1, keepdims=True)
    pull = jnp.where(spread > 0.25, inv * inv * inv * pull, 0.0)
    grad = grad * inv - centred * pull
    gret[0] = (grad - jnp.mean(grad, axis=-1, keepdims=True)).astype(bf)


def gate_back(g_low, w, ret, swi):
    _, r, d = g_low.shape
    width = ret.shape[2]
    row = pl.BlockSpec((1, r, width), lambda k: (k, 0, 0))
    return pl.pallas_call(
        gate_back_kernel,
        grid=(TP,),
        out_shape=(SDS(ret.shape, bf), SDS(ret.shape, bf)),
        in_specs=[
            pl.BlockSpec((1, r, d), lambda k: (k, 0, 0)),
            pl.BlockSpec(w.shape, lambda k: (0, 0, 0)),
            row,
            row,
        ],
        out_specs=(row, row),
        compiler_params=pltpu.CompilerParams(vmem_limit_bytes=56 << 20),
        cost_estimate=pl.CostEstimate(
            flops=2 * TP * r * d * width, bytes_accessed=22 << 20, transcendentals=TP * r * width
        ),
        name="gate_back",
    )(g_low, w, ret, swi)


def scores_back_kernel(sco, mask, q, k, v, gret, cosine, sine, out):
    nt, tn = (((1,), (1,)), ((), ())), (((0,), (0,)), ((), ()))
    kh = q.shape[2]
    half = kh // 2
    out[0, :, 2 * kh :] = lax.dot_general(
        sco[0], gret[0], tn, preferred_element_type=f32
    ).astype(bf)
    grad = lax.dot_general(gret[0], v[0], nt, preferred_element_type=f32)
    grad = (grad * mask[0]).astype(bf)
    gq = jnp.dot(grad, k[0], preferred_element_type=f32)
    gk = lax.dot_general(grad, q[0], tn, preferred_element_type=f32)
    for i, g in enumerate((gq, gk)):
        u, w = g[:, :half], g[:, half:]
        at = i * kh
        out[0, :, at : at + half] = (u * cosine[0] + w * sine[0]).astype(bf)
        out[0, :, at + half : at + kh] = (w * cosine[0] - u * sine[0]).astype(bf)


def scores_back(sco, mask, q, k, v, gret, cosine, sine):
    _, r, kh = q.shape
    arrays = (sco, mask, q, k, v, gret, cosine, sine)
    width = 2 * kh + v.shape[2]
    spec = [pl.BlockSpec((1,) + x.shape[1:], lambda i: (i, 0, 0)) for x in arrays]
    return pl.pallas_call(
        scores_back_kernel,
        grid=(TP,),
        out_shape=SDS((TP, r, width), bf),
        in_specs=spec,
        out_specs=pl.BlockSpec((1, r, width), lambda i: (i, 0, 0)),
        compiler_params=pltpu.CompilerParams(vmem_limit_bytes=56 << 20),
        cost_estimate=pl.CostEstimate(
            flops=4 * TP * r * r * (kh + v.shape[2]), bytes_accessed=16 << 20, transcendentals=0
        ),
        name="scores_back",
    )(*arrays)


def tp_groups(n):
    return [[g * TP + t for t in range(TP)] for g in range(n // TP)]


def dp_groups(n):
    return [[g * TP + t for g in range(n // TP)] for t in range(TP)]


def plane_a2a(x, n):
    return lax.all_to_all(x, AXIS, 0, 0, axis_index_groups=tp_groups(n), tiled=True)


def dp_gather(x, n):
    return lax.all_gather(x, AXIS, axis=0, tiled=True, axis_index_groups=dp_groups(n))


def dp_reduce(x, n):
    return lax.psum_scatter(
        x, AXIS, scatter_dimension=0, tiled=True, axis_index_groups=dp_groups(n)
    )


def seq_positions(lengths, rows):
    ends = jnp.cumsum(lengths, axis=1)
    starts = ends - lengths
    index = jnp.arange(rows, dtype=jnp.int32)
    segment = jnp.sum((index[None, :, None] >= ends[:, None, :]).astype(jnp.int32), axis=2)
    member = segment[:, :, None] == jnp.arange(lengths.shape[1], dtype=jnp.int32)
    offset = index[None, :] - jnp.sum(jnp.where(member, starts[:, None, :], 0), axis=2)
    return segment, offset


def rotary_tables(offset):
    half = KH // 2
    freq = jnp.exp(-math.log(10000.0) * jnp.arange(half, dtype=f32) / half)
    angle = offset.astype(f32)[..., None] * freq
    return jnp.cos(angle), jnp.sin(angle)


def decay_mask(segment, offset, head):
    diff = offset[:, :, None] - offset[:, None, :]
    valid = (segment[:, :, None] == segment[:, None, :]) & (diff >= 0)
    steps = jnp.where(valid, diff, 0).astype(f32)
    log = jnp.log(1.0 - jnp.exp2(-5.0 - head.astype(f32)))
    return jnp.where(valid, jnp.exp(log * steps), 0.0) / math.sqrt(KH)


def dot_tn(a, b):
    return lax.dot_general(a, b, (((0,), (0,)), ((), ())), preferred_element_type=f32)


def col_blocks(w):
    r, c = w.shape
    return w.reshape(r, TP, c // TP).transpose(1, 0, 2).reshape(TP * r, c // TP)


def join_kernel(widths, parts, x, *outs):
    at = 0
    for out, width in zip(outs, widths):
        piece = width // parts
        for t in range(TP):
            for p in range(parts):
                to = (p * TP + t) * piece
                out[:, to : to + piece] = x[t, :, at + p * piece : at + (p + 1) * piece].astype(f32)
        at += width


def join(x, widths, parts=1):
    r = x.shape[1]
    if any(width // parts % 128 for width in widths):
        made, at = [], 0
        for width in widths:
            part = x[:, :, at : at + width].reshape(TP, r, parts, width // parts)
            made.append(part.transpose(1, 2, 0, 3).reshape(r, TP * width).astype(f32))
            at += width
        return made
    return pl.pallas_call(
        functools.partial(join_kernel, widths, parts),
        out_shape=tuple(SDS((r, TP * width), f32) for width in widths),
        in_specs=[VMEM],
        out_specs=tuple(VMEM for _ in widths),
        compiler_params=pltpu.CompilerParams(vmem_limit_bytes=8 << 20),
        cost_estimate=pl.CostEstimate(flops=0, bytes_accessed=6 * x.size, transcendentals=0),
        name="join",
    )(x)


def after(x, *deps):
    return lax.optimization_barrier((x,) + deps)[0]


def on_device(n, tokens, lengths, gain1, bias1, wq, wk, wv, ws, wo, gain2, bias2, wg, wu, wd, cot):
    rows, d = tokens.shape
    ff = wg.shape[1]
    dp = n // TP
    shard = d // n
    unit = ff // n
    me = lax.axis_index(AXIS)
    head = lax.rem(me, TP)

    def ff_blocks(w):
        return w.reshape(shard, dp, TP, unit).transpose(2, 0, 1, 3).reshape(TP, shard, dp * unit)

    lens = jnp.pad(lengths[0].astype(f32), (0, shard - lengths.shape[1]))
    vec = jnp.stack([v.astype(f32) for v in (gain1, bias1, gain2, bias2)] + [lens])
    vec = jnp.pad(vec, ((0, 3), (0, 128 - shard)))
    qko_blk = first_exchange(wq, wk, wo, 1)
    qko = dp_gather(qko_blk.reshape(TP * shard, 4 * KH), n)
    tok_all, vec_all, wd_all = second_exchange(n, after(tokens, qko_blk), vec, wd, 2)
    gu_in = jnp.concatenate([ff_blocks(wg), ff_blocks(wu)], axis=2)
    vs_blk, gu_blk = third_exchange(after(wv, tok_all), ws, gu_in, 3)
    vs = dp_gather(vs_blk.reshape(TP * shard, 2 * VH), n)
    gu = dp_gather(gu_blk.reshape(TP * shard, 2 * dp * unit), n)
    gain1f, bias1f, gain2f, bias2f = (
        vec_all[:, :, i, :shard].reshape(1, d) for i in range(4)
    )
    vec2 = jnp.concatenate([gain2f, bias2f], axis=0)
    mine = lax.dynamic_slice_in_dim(vec_all, lax.div(me, TP), 1, 0)[0, :, 4, :3]
    order = jnp.arange(TP, dtype=jnp.int32)
    pick = (order[None, :] == (order[:, None] ^ head)).astype(f32)
    len_all = jnp.sum(pick[:, :, None] * mine[None], axis=1).astype(jnp.int32)
    segment, offset = seq_positions(len_all, rows)
    cosine, sine = rotary_tables(offset)
    mask = decay_mask(segment, offset, head)

    normed = norm_rows(tok_all, gain1f, bias1f)
    q_rot, k_rot, scores, qk = rotated_and_scores(normed, qko, cosine, sine, mask)
    cot_all, out_blk, wd_all = fourth_exchange(
        n, after(cot, scores), qko.reshape(n, shard, 4 * KH), 2 * KH, wd, wd_all, 4
    )
    out_blk = out_blk.reshape(TP, VH, d // TP)
    down = wd_all.reshape(dp * wd.shape[0], d)
    v_low, mixed, retained, swish_in, middle, normed2 = forward_exchange(
        normed, vs, scores, out_blk, tokens, vec2, 5
    )
    hidden, act, slope = hidden_units(normed2, gu)
    normed2 = normed2.reshape(TP * rows, d)
    normed = normed.reshape(TP * rows, d)
    down_grad = dot_tn(hidden.reshape(TP * rows, dp * unit), cot_all.reshape(TP * rows, d)).astype(bf)
    g_down = dp_reduce(down_grad, n)

    g_fs = hidden_back(cot_all, down, act, slope)
    gu_grad = dot_tn(normed2, g_fs.reshape(TP * rows, 2 * dp * unit)).astype(bf)
    g_gu = dp_reduce(gu_grad, n)
    g_middle, g_low, sums2 = backward_exchange(g_fs, gu, middle, cot, vec2, 6)

    g_retained, g_swish = gate_back(g_low, out_blk, retained, swish_in)
    g_low = g_low.reshape(TP * rows, d)
    swish_grad = dot_tn(normed, g_swish.reshape(TP * rows, VH)).astype(bf)
    g_swi = dp_reduce(swish_grad, n)
    out_grad = dot_tn(mixed.reshape(TP * rows, VH), g_low).astype(bf)
    out_grad = plane_a2a(col_blocks(out_grad), n)
    g_qkv = scores_back(scores, mask, q_rot, k_rot, v_low, g_retained, cosine, sine)
    qkv_grad = dot_tn(normed, g_qkv.reshape(TP * rows, 2 * KH + VH)).astype(bf)
    g_qkv_own = dp_reduce(qkv_grad, n)
    g_out = dp_reduce(out_grad, n)
    grad_tokens, ffn, g_vecs = last_exchange(
        n, g_qkv, g_swish, qk, vs, hidden, down, tokens, g_middle, gain1f, sums2, 7
    )
    layer_out = (middle + ffn).astype(bf)

    g_vecs = lax.dynamic_slice_in_dim(g_vecs, head * shard, shard, 1)
    grad_d = g_down.astype(f32)
    g_gu = plane_a2a(g_gu, n)
    grad_g, grad_u = join(g_gu.reshape(TP, shard, 2 * dp * unit), (dp * unit,) * 2, dp)
    g_swi = plane_a2a(g_swi, n)
    (grad_s,) = join(g_swi.reshape(TP, shard, VH), (VH,))
    g_qkv_own = plane_a2a(g_qkv_own, n)
    grad_q, grad_k, grad_v = join(g_qkv_own.reshape(TP, shard, 2 * KH + VH), (KH, KH, VH))
    g_out = plane_a2a(g_out, n)
    (grad_o,) = join(g_out.reshape(TP, wo.shape[0], d // TP), (d // TP,))
    return (
        layer_out, grad_tokens, g_vecs[0], g_vecs[1], grad_q, grad_k, grad_v, grad_s, grad_o,
        g_vecs[2], g_vecs[3], grad_g, grad_u, grad_d,
    )


def solution(mesh):
    n = mesh.shape[AXIS]
    row, vec = P(AXIS, None), P(AXIS)
    ins = (row, row, vec, vec, row, row, row, row, row, vec, vec, row, row, row, row)
    outs = (row, row, vec, vec, row, row, row, row, row, vec, vec, row, row, row)

    def body(*args):
        return on_device(n, *args)

    return jax.shard_map(body, mesh=mesh, in_specs=ins, out_specs=outs, check_vma=False)
```

```python
import functools
import math

import jax
import jax.numpy as jnp
from jax import lax
from jax.experimental import pallas as pl
from jax.experimental.pallas import tpu as pltpu
from jax.sharding import PartitionSpec as P


KH = 256
VH = 512
TP = 8
AXIS = "fsdp"
MESH = pl.DeviceIdType.MESH
ANY = pl.BlockSpec(memory_space=pl.ANY)
VMEM = pl.BlockSpec(memory_space=pltpu.VMEM)
bf = jnp.bfloat16
f32 = jnp.float32
SDS = jax.ShapeDtypeStruct
ALL_VMEM = 67043328


def place():
    me = lax.axis_index(AXIS)
    steps = [s - 2 * s * lax.rem(lax.div(me, s), 2) for s in (1, 2, 4)]

    def peer(k):
        out = me
        for bit, step in enumerate(steps):
            if k >> bit & 1:
                out = out + step
        return out

    return me, peer


def greet(peers):
    barrier = pltpu.get_barrier_semaphore()
    for p in peers:
        pl.semaphore_signal(barrier, inc=1, device_id=(p,), device_id_type=MESH)
    return lambda: pl.semaphore_wait(barrier, len(peers))


def meet(peers):
    greet(peers)()


def remote(src, dst, sems, i, dev):
    return pltpu.make_async_remote_copy(
        src_ref=src, dst_ref=dst, send_sem=sems[0].at[i], recv_sem=sems[1].at[i],
        device_id=(dev,), device_id_type=MESH,
    )


GATHER_SEMS = 13


class Gather:
    def __init__(self, own, out, start, size, sems, base, local, peer):
        self.own, self.out, self.sems, self.base, self.local = own, out, sems, base, local
        h = size // 2
        self.all, self.top, self.bot = pl.ds(start, size), pl.ds(start, h), pl.ds(start + h, h)
        self.pc, self.px, self.py = peer(1), peer(2), peer(4)
        self.made = []

    def send(self, src, dst, dev):
        copy = remote(src, dst, self.sems, self.base + len(self.made), dev)
        copy.start()
        self.made.append(copy)
        return copy

    def pass_on(self, k, at):
        self.core.append(self.send(self.out.at[k, at], self.out.at[k + 1, at], self.pc))

    def start(self):
        own, out, top, bot = self.own, self.out, self.top, self.bot
        self.x0 = self.send(own.at[bot], out.at[2, bot], self.px)
        self.y0 = self.send(own.at[top], out.at[4, top], self.py)
        self.x1 = self.send(own.at[top], out.at[2, top], self.px)
        self.y1 = self.send(own.at[bot], out.at[4, bot], self.py)
        self.core = [self.send(own.at[self.all], out.at[1, self.all], self.pc)]
        self.keep = pltpu.make_async_copy(own.at[self.all], out.at[0, self.all], self.local)
        self.keep.start()

    def forward(self):
        out, top, bot = self.out, self.top, self.bot
        self.x0.wait_recv()
        self.fy = self.send(out.at[2, bot], out.at[6, bot], self.py)
        self.pass_on(2, bot)
        self.y0.wait_recv()
        self.fx = self.send(out.at[4, top], out.at[6, top], self.px)
        self.pass_on(4, top)
        self.x1.wait_recv()
        self.pass_on(2, top)
        self.y1.wait_recv()
        self.pass_on(4, bot)

    def finish(self):
        self.fy.wait_recv()
        self.pass_on(6, self.bot)
        self.fx.wait_recv()
        self.pass_on(6, self.top)
        for copy in self.core:
            copy.wait_recv()
        for copy in self.made:
            copy.wait_send()
        self.keep.wait()


def send_columns(src, out, cols, at, sems, base, local, t, peer, rows=None):
    copies = []
    rows = slice(None) if rows is None else rows

    def block(q):
        if len(src.shape) == 3:
            return src.at[q]
        return src.at[rows, pl.ds(pl.multiple_of(q * cols, 128), cols)]

    for k in range(1, TP):
        dev = peer(k)
        copy = remote(
            block(lax.rem(dev, TP)), out.at[t, :, pl.ds(at, cols)], sems, base + k - 1, dev
        )
        copy.start()
        copies.append(copy)
    keep = pltpu.make_async_copy(block(t), out.at[t, :, pl.ds(at, cols)], local)
    keep.start()
    return copies, keep


def finish(parts):
    for copies, keep in parts:
        for copy in copies:
            copy.wait()
        keep.wait()


def exchange_call(
    kernel, outs, args, sems, locals_, cid, specs=None, out_specs=None, vmem=12 << 20
):
    return pl.pallas_call(
        kernel,
        out_shape=outs,
        in_specs=specs or [VMEM] * len(args),
        out_specs=out_specs or tuple(ANY for _ in outs),
        scratch_shapes=[
            pltpu.SemaphoreType.DMA((sems,)),
            pltpu.SemaphoreType.DMA((sems,)),
            pltpu.SemaphoreType.DMA((locals_,)),
        ],
        compiler_params=pltpu.CompilerParams(
            collective_id=cid, has_side_effects=True, vmem_limit_bytes=vmem
        ),
    )(*args)


def first_kernel(wq, wk, wo, out, ssem, rsem, local):
    me, peer = place()
    t = lax.rem(me, TP)
    meet([peer(k) for k in range(1, TP)])
    sems = (ssem, rsem)
    shard, cq, co = wq.shape[0], wq.shape[1] // TP, wo.shape[1] // TP
    low, high = pl.ds(0, shard), pl.ds(shard, shard)
    finish([
        send_columns(wq, out, cq, 0, sems, 0, local.at[0], t, peer),
        send_columns(wk, out, cq, cq, sems, 7, local.at[1], t, peer),
        send_columns(wo, out, co, 2 * cq, sems, 14, local.at[2], t, peer, low),
        send_columns(wo, out, co, 2 * cq + co, sems, 21, local.at[3], t, peer, high),
    ])


def first_exchange(wq, wk, wo, cid):
    width = 2 * wq.shape[1] // TP + 2 * wo.shape[1] // TP
    outs = (SDS((TP, wq.shape[0], width), bf),)
    return exchange_call(first_kernel, outs, (wq, wk, wo), 28, 4, cid)[0]


def others_along(n):
    me = lax.axis_index(AXIS)
    return [lax.rem(me + TP * j, n) for j in range(1, n // TP)]


def second_kernel(n, tok, vec, tok_out, vec_out, ssem, rsem, local):
    me, peer = place()
    t, g = lax.rem(me, TP), lax.div(me, TP)
    others = others_along(n)
    meet([peer(k) for k in range(1, TP)] + others)
    sems = (ssem, rsem)
    base = GATHER_SEMS
    far = []
    keep = pltpu.make_async_copy(vec, vec_out.at[g, t], local.at[1])
    keep.start()
    for j, dev in enumerate(others):
        copy = remote(vec, vec_out.at[g, t], sems, base + TP + j, dev)
        copy.start()
        far.append(copy)
    gather = Gather(tok, tok_out, 0, tok.shape[0], sems, 0, local.at[0], peer)
    gather.start()
    for copy in far:
        copy.wait()
    keep.wait()
    near = []
    for k in range(1, TP):
        copy = remote(vec_out.at[:, t], vec_out.at[:, t], sems, base + k, peer(k))
        copy.start()
        near.append(copy)
    gather.forward()
    gather.finish()
    for copy in near:
        copy.wait()


def second_exchange(n, tok, vec, cid):
    outs = (SDS((TP,) + tok.shape, bf), SDS((n // TP, TP) + vec.shape, f32))
    kernel = functools.partial(second_kernel, n)
    sems = GATHER_SEMS + TP + n // TP
    return exchange_call(kernel, outs, (tok, vec), sems, 2, cid)


def third_kernel(wv, ws, gu, tok, gain, bias, out, gu_out, nrm, ssem, rsem, local):
    me, peer = place()
    t = lax.rem(me, TP)
    meet([peer(k) for k in range(1, TP)])
    sems = (ssem, rsem)
    cols = wv.shape[1] // TP
    parts = [
        send_columns(wv, out, cols, 0, sems, 0, local.at[0], t, peer),
        send_columns(ws, out, cols, cols, sems, 7, local.at[1], t, peer),
        send_columns(gu, gu_out, gu.shape[2], 0, sems, 14, local.at[2], t, peer),
    ]
    step, r = 16, tok.shape[1]

    def norm(j, _):
        k = lax.div(j, r // step)
        at = pl.ds(pl.multiple_of(lax.rem(j, r // step) * step, step), step)
        value = tok[k, at, :].astype(f32)
        centred = value - jnp.mean(value, axis=-1, keepdims=True)
        spread = jnp.mean(centred * centred, axis=-1, keepdims=True)
        nrm[k, at, :] = (centred * lax.rsqrt(spread + 1e-05) * gain[...] + bias[...]).astype(bf)
        return 0

    lax.fori_loop(0, TP * r // step, norm, 0, unroll=4)
    finish(parts)


def third_exchange(wv, ws, gu, tok, gain, bias, cid):
    outs = (
        SDS((TP, wv.shape[0], 2 * wv.shape[1] // TP), bf),
        SDS(gu.shape, bf),
        SDS(tok.shape, bf),
    )
    return exchange_call(
        third_kernel, outs, (wv, ws, gu, tok, gain, bias), 21, 3, cid,
        out_specs=(ANY, ANY, VMEM), vmem=32 << 20,
    )


def fourth_kernel(
    n, cot, qko, nrm, cosine, sine, mask, cot_out, o_out, q_out, k_out, sco, w, ssem, rsem, local
):
    me, peer = place()
    t = lax.rem(me, TP)
    meet([peer(k) for k in range(1, TP)])
    sems = (ssem, rsem)
    share, cols = n // TP, o_out.shape[4]
    _, r, kh = q_out.shape
    half = kh // 2
    weights = pltpu.make_async_copy(qko.at[:, :, pl.ds(0, 2 * kh)], w, local.at[3])
    weights.start()
    gather = Gather(cot, cot_out, 0, cot.shape[0], sems, 0, local.at[0], peer)
    gather.start()
    copies, keeps = [], []

    def part(p, which):
        return qko.at[pl.ds(p * share, share), :, pl.ds(2 * kh + which * cols, cols)]

    for which in (0, 1):
        for k in range(1, TP):
            dev = peer(k)
            copy = remote(
                part(lax.rem(dev, TP), which), o_out.at[t, :, which], sems,
                GATHER_SEMS + which * TP + k, dev,
            )
            copy.start()
            copies.append(copy)
        keep = pltpu.make_async_copy(part(t, which), o_out.at[t, :, which], local.at[1 + which])
        keep.start()
        keeps.append(keep)
    weights.wait()

    def products(pairs):
        @pl.loop(*pairs)
        def _(j):
            rows = nrm[pl.ds(2 * j, 2)].reshape(2 * r, nrm.shape[2])
            for at, out in ((0, q_out), (kh, k_out)):
                y = jnp.dot(
                    rows, w[:, :, at : at + kh].reshape(nrm.shape[2], kh),
                    preferred_element_type=f32,
                )
                for i in (0, 1):
                    u, v = y[i * r : (i + 1) * r, :half], y[i * r : (i + 1) * r, half:]
                    cos, sin = cosine[2 * j + i], sine[2 * j + i]
                    out[2 * j + i, :, :half] = (u * cos - v * sin).astype(bf)
                    out[2 * j + i, :, half:] = (v * cos + u * sin).astype(bf)
            for i in (0, 1):
                plain = lax.dot_general(
                    q_out[2 * j + i], k_out[2 * j + i], (((1,), (1,)), ((), ())),
                    preferred_element_type=f32,
                )
                sco[2 * j + i] = (plain * mask[2 * j + i]).astype(bf)

    products((0, TP // 2))
    gather.forward()
    gather.finish()
    for copy in copies:
        copy.wait()
    for keep in keeps:
        keep.wait()


def fourth_exchange(n, cot, qko, nrm, cosine, sine, mask, cid):
    _, shard, width = qko.shape
    cols = (width - 2 * KH) // 2
    r = cot.shape[0]
    outs = (
        SDS((TP,) + cot.shape, bf),
        SDS((TP, n // TP, 2, shard, cols), bf),
        SDS((TP, r, KH), bf),
        SDS((TP, r, KH), bf),
        SDS(mask.shape, bf),
        SDS((n, shard, 2 * KH), bf),
    )
    kernel = functools.partial(fourth_kernel, n)
    return exchange_call(
        kernel, outs, (cot, qko, nrm, cosine, sine, mask),
        GATHER_SEMS + 2 * TP, 4, cid,
        specs=[VMEM, ANY, VMEM, VMEM, VMEM, VMEM],
        out_specs=(ANY, ANY, VMEM, VMEM, VMEM, VMEM), vmem=40 << 20,
    )


REDUCE_SEMS = 16
TILE = 256


class Reduce:
    def __init__(self, product, bufs, sems, base, peer, prepare=None, enter=None):
        self.product, self.prepare, self.sems, self.base = product, prepare, sems, base
        self.enter = enter
        self.po, self.pe, self.rc, self.sb, self.xr, self.yr = bufs
        self.pc, self.px, self.py = peer(1), peer(2), peer(4)
        self.q = self.pe.shape[1] // 4
        self.sent, self.core, self.got = [], {}, ({}, {})

    def send(self, src, dst, dev, i):
        copy = remote(src, dst, self.sems, self.base + i, dev)
        copy.start()
        self.sent.append(copy)
        return copy

    def ready(self, i):
        if self.prepare is not None:
            self.prepare(2 * i)

    def pair(self, i):
        self.product(i, self.po.at[i], self.pe.at[i])
        if self.enter is not None:
            self.enter()
            self.enter = None
        self.core[i] = self.send(self.po.at[i], self.rc.at[i], self.pc, i)

    def add(self, c, i, lower, out, more=None):
        step = 16

        @pl.loop(0, self.q // step)
        def _(j):
            there = pl.ds(pl.multiple_of(j * step, step), step)
            here = pl.ds(pl.multiple_of(j * step + (2 * c + lower) * self.q, step), step)
            total = self.pe[i, here, :].astype(f32) + self.rc[i, here, :].astype(f32)
            if more is not None:
                total = total + more[there, :].astype(f32)
            self.sb[c, out, there, :] = total.astype(bf)

    def link(self, c, slot, name, ring, at, dev):
        self.got[c][name] = self.send(
            self.sb.at[c, slot], ring.at[c, at], dev, 4 + 6 * c + slot
        )

    def six(self, c):
        self.add(c, 3, 0, 0)
        self.link(c, 0, "x6", self.xr, 0, self.px)
        self.add(c, 3, 1, 1)
        self.link(c, 1, "y6", self.yr, 0, self.py)

    def two(self, c):
        self.add(c, 1, 0, 2)
        self.link(c, 2, "x2", self.xr, 1, self.px)

    def four(self, c):
        self.add(c, 2, 1, 3)
        self.link(c, 3, "y4", self.yr, 1, self.py)

    def onward(self, c):
        self.got[c]["x6"].wait_recv()
        self.add(c, 2, 0, 4, self.xr.at[c, 0])
        self.link(c, 4, "y4b", self.yr, 2, self.py)
        self.got[c]["y6"].wait_recv()
        self.add(c, 1, 1, 5, self.yr.at[c, 0])
        self.link(c, 5, "x2b", self.xr, 2, self.px)

    def run(self):
        self.ready(3)
        self.pair(3)
        stages = ((1, 3, self.six), (2, 1, self.two), (0, 2, self.four))
        for following, now, stage in stages:
            self.ready(following)
            if self.prepare is None:
                self.pair(following)
            self.core[now].wait_recv()
            for c in (0, 1):
                stage(c)
            if self.prepare is not None:
                self.pair(following)
        for c in (0, 1):
            self.onward(c)

    def rows(self, c, step, body):
        if c == 0:
            self.core[0].wait_recv()
        for name in ("x2", "y4", "y4b", "x2b"):
            self.got[c][name].wait_recv()
        for lower in (0, 1):
            near, far = (self.yr, self.xr) if lower else (self.xr, self.yr)

            @pl.loop(0, self.q // step)
            def _(j, lower=lower, near=near, far=far):
                there = pl.ds(pl.multiple_of(j * step, step), step)
                here = pl.ds(pl.multiple_of(j * step + (2 * c + lower) * self.q, step), step)
                body(
                    here,
                    self.pe[0, here, :].astype(f32)
                    + self.rc[0, here, :].astype(f32)
                    + near[c, 1, there, :].astype(f32)
                    + far[c, 2, there, :].astype(f32),
                )

    def finish(self):
        for copy in self.sent:
            copy.wait_send()


def reduce_scratch(r, c, even=f32):
    q = r // 4
    return [
        pltpu.VMEM((4, r, c), bf),
        pltpu.VMEM((4, r, c), even),
        pltpu.VMEM((4, r, c), bf),
        pltpu.VMEM((2, 6, q, c), bf),
        pltpu.VMEM((2, 3, q, c), bf),
        pltpu.VMEM((2, 3, q, c), bf),
    ]


def rows_of_pair(a, i):
    two, r, k = 2, a.shape[1], a.shape[2]
    return a[pl.ds(2 * i, two)].reshape(two * r, k)


def times(a, w, nt):
    def product(i, odd, even):
        r = a.shape[1]

        @pl.loop(0, even.shape[1] // TILE)
        def _(j):
            at = pl.ds(pl.multiple_of(j * TILE, TILE), TILE)
            x = rows_of_pair(a, i)
            if nt:
                y = lax.dot_general(
                    x, w[at, :], (((1,), (1,)), ((), ())), preferred_element_type=f32
                )
            else:
                y = jnp.dot(x, w[:, at], preferred_element_type=f32)
            even[:, at] = y[:r].astype(even.dtype)
            odd[:, at] = y[r:].astype(odd.dtype)

    return product


def exchange_and_gather(reduce, gathers, step, body):
    reduce.run()
    for c in (0, 1):
        reduce.rows(c, step, body)
        gathers[c].start()
    for c in (0, 1):
        gathers[c].forward()
    for c in (0, 1):
        gathers[c].finish()
    reduce.finish()


def both_gathers(own, out, sems, local, peer):
    half = own.shape[0] // 2
    return [
        Gather(own, out, c * half, half, sems, REDUCE_SEMS + c * GATHER_SEMS, local.at[c], peer)
        for c in (0, 1)
    ]


EXCHANGE_SEMS = REDUCE_SEMS + 2 * GATHER_SEMS


def forward_kernel(
    nrm, wvs, sco, w, tok, vec, v_out, mix_out, ret_out, swi_out, mid, out,
    v_buf, mix_buf, ret_buf, swi_buf, po, pe, rc, sb, xr, yr, own, ssem, rsem, local,
):
    _, peer = place()
    enter = greet([peer(1), peer(2), peer(4)])
    sems = (ssem, rsem)
    r, width = v_buf.shape[1:]
    kept = []

    def prepare(first):
        two = pl.ds(first, 2)
        x = nrm[two].reshape(2 * r, nrm.shape[2])

        tiles = width // TILE

        @pl.loop(0, 2 * tiles)
        def _(j):
            at = pl.ds(pl.multiple_of(j * TILE, TILE), TILE)
            y = jnp.dot(x, wvs[:, at], preferred_element_type=f32)
            y = y.reshape(2, r, TILE)

            @pl.when(j < tiles)
            def _():
                v_buf[two, :, at] = y.astype(bf)

            @pl.when(j >= tiles)
            def _():
                swi_buf[two, :, pl.ds(pl.multiple_of(j * TILE - width, TILE), TILE)] = y

        @pl.loop(0, 2 * tiles)
        def _(j):
            k = first + lax.div(j, tiles)
            at = pl.ds(pl.multiple_of(lax.rem(j, tiles) * TILE, TILE), TILE)
            ret_buf[k, :, at] = jnp.dot(sco[k], v_buf[k, :, at], preferred_element_type=f32)

        @pl.loop(0, 2 * r // 32)
        def _(j):
            k = first + lax.div(j, r // 32)
            at = pl.ds(pl.multiple_of(lax.rem(j, r // 32) * 32, 32), 32)
            value = ret_buf[k, at, :]
            centred = value - jnp.mean(value, axis=-1, keepdims=True)
            spread = jnp.mean(centred * centred, axis=-1, keepdims=True)
            gate = swi_buf[k, at, :]
            gate = gate / (1.0 + jnp.exp(-gate))
            mix_buf[k, at, :] = (
                gate * (centred * lax.rsqrt(jnp.maximum(spread, 0.25)))
            ).astype(bf)

        for i, (src, dst) in enumerate(
            ((v_buf, v_out), (mix_buf, mix_out), (ret_buf, ret_out), (swi_buf, swi_out))
        ):
            copy = pltpu.make_async_copy(
                src.at[two], dst.at[two], local.at[2 + 2 * first + i]
            )
            copy.start()
            kept.append(copy)

    def product(i, odd, even):
        step = w.shape[2]

        @pl.loop(0, w.shape[0])
        def _(j):
            at = pl.ds(pl.multiple_of(j * step, step), step)
            y = jnp.dot(rows_of_pair(mix_buf, i), w[j], preferred_element_type=f32)
            even[:, at] = y[:r].astype(even.dtype)
            odd[:, at] = y[r:].astype(odd.dtype)

    def body(at, value):
        value = value + tok[at, :].astype(f32)
        mid[at, :] = value
        center = jnp.mean(value, axis=-1, keepdims=True)
        centred = value - center
        spread = jnp.mean(centred * centred, axis=-1, keepdims=True)
        own[at, :] = (
            centred * lax.rsqrt(spread + 1e-05) * vec[0:1, :] + vec[1:2, :]
        ).astype(bf)

    reduce = Reduce(product, (po, pe, rc, sb, xr, yr), sems, 0, peer, prepare, enter)
    exchange_and_gather(reduce, both_gathers(own, out, sems, local, peer), 16, body)
    for copy in kept:
        copy.wait()


def forward_exchange(nrm, wvs, sco, w, tok, vec, cid):
    _, r, d = nrm.shape
    width = w.shape[1]
    count = EXCHANGE_SEMS
    blocks = [((TP, r, width), t) for t in (bf, bf, f32, f32)]
    return pl.pallas_call(
        forward_kernel,
        out_shape=tuple(SDS(*b) for b in blocks) + (SDS((r, d), f32), SDS((TP, r, d), bf)),
        in_specs=[VMEM] * 6,
        out_specs=(ANY,) * 4 + (VMEM, ANY),
        scratch_shapes=[pltpu.VMEM(*b) for b in blocks]
        + reduce_scratch(r, d)
        + [
            pltpu.VMEM((r, d), bf),
            pltpu.SemaphoreType.DMA((count,)),
            pltpu.SemaphoreType.DMA((count,)),
            pltpu.SemaphoreType.DMA((18,)),
        ],
        compiler_params=pltpu.CompilerParams(
            collective_id=cid, has_side_effects=True, vmem_limit_bytes=60 << 20
        ),
        name="forward_exchange",
    )(nrm, wvs, sco, w, tok, vec)


def product_kernel(a, b, out, turned):
    turned[...] = a[...].reshape(-1, a.shape[-1]).T
    rows = turned.shape[1]

    @pl.loop(0, out.shape[1] // TILE)
    def _(j):
        at = pl.ds(pl.multiple_of(j * TILE, TILE), TILE)
        out[:, at] = jnp.dot(
            turned[...], b[:, :, at].reshape(rows, TILE), preferred_element_type=f32
        ).astype(bf)


def row_product(a, b):
    _, r, m = a.shape
    width = b.shape[2]
    tile = 512 if m >= 2048 else 256
    return pl.pallas_call(
        product_kernel,
        grid=(m // tile,),
        out_shape=SDS((m, width), bf),
        in_specs=[
            pl.BlockSpec((TP, r, tile), lambda i: (0, 0, i)),
            pl.BlockSpec((TP, r, width), lambda i: (0, 0, 0)),
        ],
        out_specs=pl.BlockSpec((tile, width), lambda i: (i, 0)),
        scratch_shapes=[pltpu.VMEM((tile, TP * r), bf)],
        compiler_params=pltpu.CompilerParams(vmem_limit_bytes=56 << 20),
        cost_estimate=pl.CostEstimate(
            flops=2 * TP * r * m * width,
            bytes_accessed=2 * (a.size + b.size + m * width),
            transcendentals=0,
        ),
        name="row_product",
    )(a, b)


def hidden_kernel(x, gu, hid, act_out, slope_out):
    width = hid.shape[2]
    step = 256

    @pl.loop(0, width // step)
    def _(j):
        at = pl.ds(pl.multiple_of(j * step, step), step)
        behind = pl.ds(pl.multiple_of(j * step + width, step), step)
        rows = x[...].reshape(-1, x.shape[2])
        first = jnp.dot(rows, gu[:, at], preferred_element_type=f32)
        second = jnp.dot(rows, gu[:, behind], preferred_element_type=f32)
        share = 0.5 * (1.0 + lax.erf(first * math.sqrt(0.5)))
        act = first * share
        slope = share + first * (jnp.exp(-0.5 * first * first) * (1.0 / math.sqrt(2.0 * math.pi)))
        block = hid.shape[:2] + (step,)
        hid[:, :, at] = (act * second).astype(bf).reshape(block)
        act_out[:, :, at] = act.reshape(block)
        slope_out[:, :, at] = (slope * second).reshape(block)


def hidden_units(x, gu):
    _, r, d = x.shape
    width = gu.shape[1] // 2
    row = pl.BlockSpec((2, r, width), lambda k: (k, 0, 0))
    return pl.pallas_call(
        hidden_kernel,
        grid=(TP // 2,),
        out_shape=tuple(SDS((TP, r, width), t) for t in (bf, f32, f32)),
        in_specs=[
            pl.BlockSpec((2, r, d), lambda k: (k, 0, 0)),
            pl.BlockSpec(gu.shape, lambda k: (0, 0)),
        ],
        out_specs=(row, row, row),
        compiler_params=pltpu.CompilerParams(vmem_limit_bytes=56 << 20),
        cost_estimate=pl.CostEstimate(
            flops=4 * TP * r * d * width, bytes_accessed=24 << 20, transcendentals=2 * TP * r * width
        ),
        name="hidden_units",
    )(x, gu)


def hidden_back_kernel(cot, down, act, slope, out):
    width = act.shape[2]
    step = 256

    @pl.loop(0, width // step)
    def _(j):
        at = pl.ds(pl.multiple_of(j * step, step), step)
        behind = pl.ds(pl.multiple_of(j * step + width, step), step)
        grad = lax.dot_general(
            cot[...].reshape(-1, cot.shape[2]), down[at, :], (((1,), (1,)), ((), ())),
            preferred_element_type=f32,
        ).reshape(act.shape[:2] + (step,))
        out[:, :, at] = (grad * slope[:, :, at]).astype(bf)
        out[:, :, behind] = (grad * act[:, :, at]).astype(bf)


def hidden_back(cot, down, act, slope):
    _, r, d = cot.shape
    width = act.shape[2]
    row = pl.BlockSpec((2, r, width), lambda k: (k, 0, 0))
    return pl.pallas_call(
        hidden_back_kernel,
        grid=(TP // 2,),
        out_shape=SDS((TP, r, 2 * width), bf),
        in_specs=[
            pl.BlockSpec((2, r, d), lambda k: (k, 0, 0)),
            pl.BlockSpec(down.shape, lambda k: (0, 0)),
            row,
            row,
        ],
        out_specs=pl.BlockSpec((2, r, 2 * width), lambda k: (k, 0, 0)),
        compiler_params=pltpu.CompilerParams(vmem_limit_bytes=56 << 20),
        cost_estimate=pl.CostEstimate(
            flops=2 * TP * r * d * width, bytes_accessed=24 << 20, transcendentals=0
        ),
        name="hidden_back",
    )(cot, down, act, slope)


def backward_kernel(
    a, w, mid, cot, vec, gmid, out, sums, po, pe, rc, sb, xr, yr, own, acc, ssem, rsem, local
):
    _, peer = place()
    enter = greet([peer(1), peer(2), peer(4)])
    sems = (ssem, rsem)
    acc[...] = jnp.zeros_like(acc)

    def body(at, g):
        value = mid[at, :]
        center = jnp.mean(value, axis=-1, keepdims=True)
        centred = value - center
        inv = lax.rsqrt(jnp.mean(centred * centred, axis=-1, keepdims=True) + 1e-05)
        hat = centred * inv
        acc[0] += g * hat
        acc[1] += g
        scaled = g * vec[0:1, :]
        mean_g = jnp.mean(scaled, axis=-1, keepdims=True)
        mean_gh = jnp.mean(scaled * hat, axis=-1, keepdims=True)
        grad = cot[at, :].astype(f32) + inv * (scaled - mean_g - hat * mean_gh)
        gmid[at, :] = grad
        own[at, :] = grad.astype(bf)

    reduce = Reduce(times(a, w, True), (po, pe, rc, sb, xr, yr), sems, 0, peer, enter=enter)
    exchange_and_gather(reduce, both_gathers(own, out, sems, local, peer), 16, body)
    sums[0:1, :] = jnp.sum(acc[0], axis=0, keepdims=True)
    sums[1:2, :] = jnp.sum(acc[1], axis=0, keepdims=True)


def backward_exchange(a, w, mid, cot, vec, cid):
    _, r, _ = a.shape
    c = w.shape[0]
    count = EXCHANGE_SEMS
    return pl.pallas_call(
        backward_kernel,
        out_shape=(SDS((r, c), f32), SDS((TP, r, c), bf), SDS((2, c), f32)),
        in_specs=[VMEM] * 5,
        out_specs=(VMEM, ANY, VMEM),
        scratch_shapes=reduce_scratch(r, c)
        + [
            pltpu.VMEM((r, c), bf),
            pltpu.VMEM((2, 16, c), f32),
            pltpu.SemaphoreType.DMA((count,)),
            pltpu.SemaphoreType.DMA((count,)),
            pltpu.SemaphoreType.DMA((2,)),
        ],
        compiler_params=pltpu.CompilerParams(
            collective_id=cid, has_side_effects=True, vmem_limit_bytes=52 << 20
        ),
        name="backward_exchange",
    )(a, w, mid, cot, vec)


def last_kernel(
    n, gqkv, gs, wqk, wvs, a2, w2, tok, gmid, gain, sums2, gtok, ffn, vec_out,
    po, pe, rc, sb, xr, yr, pe2, rc2, sb2, xr2, yr2, acc, vecs, near, far, part, ssem, rsem,
):
    dp = n // TP
    me, peer = place()
    g = lax.div(me, TP)
    width = vec_out.shape[1]
    others = [lax.rem(me + TP * j, n) for j in range(1, dp)]
    enter = greet([peer(k) for k in range(1, TP)] + others)
    sems = (ssem, rsem)
    acc[...] = jnp.zeros_like(acc)
    nt = (((1,), (1,)), ((), ()))

    def product(i, odd, even):
        r, qk, v = gqkv.shape[1], wqk.shape[1], gs.shape[2]
        x, y = rows_of_pair(gqkv, i), rows_of_pair(gs, i)

        @pl.loop(0, even.shape[1] // TILE)
        def _(j):
            at = pl.ds(pl.multiple_of(j * TILE, TILE), TILE)
            z = lax.dot_general(x[:, :qk], wqk[at, :], nt, preferred_element_type=f32)
            z += lax.dot_general(x[:, qk:], wvs[at, :v], nt, preferred_element_type=f32)
            z += lax.dot_general(y, wvs[at, v:], nt, preferred_element_type=f32)
            even[:, at] = z[:r].astype(even.dtype)
            odd[:, at] = z[r:].astype(odd.dtype)

    one = Reduce(product, (po, pe, rc, sb, xr, yr), sems, 0, peer, enter=enter)
    one.run()
    for copy in one.core.values():
        copy.wait_send()
    one.sent = [copy for copy in one.sent if all(copy is not c for c in one.core.values())]
    two = Reduce(times(a2, w2, False), (po, pe2, rc2, sb2, xr2, yr2), sems, REDUCE_SEMS, peer)
    two.run()

    def body(at, grad):
        value = tok[at, :].astype(f32)
        center = jnp.mean(value, axis=-1, keepdims=True)
        centred = value - center
        inv = lax.rsqrt(jnp.mean(centred * centred, axis=-1, keepdims=True) + 1e-05)
        hat = centred * inv
        acc[0] += grad * hat
        acc[1] += grad
        scaled = grad * gain[...]
        mean_g = jnp.mean(scaled, axis=-1, keepdims=True)
        mean_gh = jnp.mean(scaled * hat, axis=-1, keepdims=True)
        gtok[at, :] = gmid[at, :] + inv * (scaled - mean_g - hat * mean_gh)

    for c in (0, 1):
        one.rows(c, 16, body)
    vecs[...] = jnp.zeros_like(vecs)
    vecs[0:1, :] = jnp.sum(acc[0], axis=0, keepdims=True)
    vecs[1:2, :] = jnp.sum(acc[1], axis=0, keepdims=True)
    vecs[2:4, :] = sums2[...]
    base = 2 * REDUCE_SEMS
    copies = []
    for j, dev in enumerate(others):
        at = pl.multiple_of(lax.div(dev, TP) * width, 128)
        copy = remote(vecs.at[:, pl.ds(at, width)], far.at[j], sems, base + j, dev)
        copy.start()
        copies.append(copy)

    def keep(at, value):
        ffn[at, :] = value

    two.rows(0, 16, keep)
    total = vecs[:, pl.ds(pl.multiple_of(g * width, 128), width)]
    for j, copy in enumerate(copies):
        copy.wait()
        total = total + far[j]
    part[...] = total
    copies = []
    for k in range(1, TP):
        copy = remote(part, near.at[k - 1], sems, base + dp + k - 1, peer(k))
        copy.start()
        copies.append(copy)
    two.rows(1, 16, keep)
    for k, copy in enumerate(copies):
        copy.wait()
        total = total + near[k]
    vec_out[...] = total
    one.finish()
    two.finish()


def last_exchange(n, gqkv, gs, wqk, wvs, a2, w2, tok, gmid, gain, sums2, cid):
    dp = n // TP
    _, r, _ = a2.shape
    c = w2.shape[1]
    width = c // dp
    count = 2 * REDUCE_SEMS + dp + TP
    return pl.pallas_call(
        functools.partial(last_kernel, n),
        out_shape=(SDS((r, c), f32), SDS((r, c), f32), SDS((8, width), f32)),
        in_specs=[VMEM] * 10,
        out_specs=(VMEM,) * 3,
        scratch_shapes=reduce_scratch(r, c)
        + reduce_scratch(r, c, bf)[1:]
        + [
            pltpu.VMEM((2, 16, c), f32),
            pltpu.VMEM((8, c), f32),
            pltpu.VMEM((TP - 1, 8, width), f32),
            pltpu.VMEM((dp, 8, width), f32),
            pltpu.VMEM((8, width), f32),
            pltpu.SemaphoreType.DMA((count,)),
            pltpu.SemaphoreType.DMA((count,)),
        ],
        compiler_params=pltpu.CompilerParams(
            collective_id=cid, has_side_effects=True, vmem_limit_bytes=ALL_VMEM
        ),
        name="last_exchange",
    )(gqkv, gs, wqk, wvs, a2, w2, tok, gmid, gain, sums2)


def gate_back_kernel(g_low, w, ret, swi, gret, gswi, whole, back):
    two, r, _ = gret.shape
    cols = w.shape[2]

    @pl.when(pl.program_id(0) == 0)
    def _():
        for j in range(w.shape[0]):
            whole[:, j * cols : (j + 1) * cols] = w[j]

    back[...] = lax.dot_general(
        g_low[...].reshape(two * r, g_low.shape[2]), whole[...], (((1,), (1,)), ((), ())),
        preferred_element_type=f32,
    )
    step = 32
    for i in range(two):

        @pl.loop(0, r // step)
        def _(j, i=i):
            at = pl.ds(pl.multiple_of(j * step, step), step)
            value, gate = ret[i, at, :], swi[i, at, :]
            grad = back[pl.ds(pl.multiple_of(i * r + j * step, step), step), :]
            centred = value - jnp.mean(value, axis=-1, keepdims=True)
            spread = jnp.mean(centred * centred, axis=-1, keepdims=True)
            inv = lax.rsqrt(jnp.maximum(spread, 0.25))
            share = 1.0 / (1.0 + jnp.exp(-gate))
            silu = gate * share
            gswi[i, at, :] = (
                grad * (centred * inv) * (share * (1.0 + gate * (1.0 - share)))
            ).astype(bf)
            grad = grad * silu
            pull = jnp.mean(grad * centred, axis=-1, keepdims=True)
            pull = jnp.where(spread > 0.25, inv * inv * inv * pull, 0.0)
            grad = grad * inv - centred * pull
            gret[i, at, :] = (grad - jnp.mean(grad, axis=-1, keepdims=True)).astype(bf)


def gate_back(g_low, w, ret, swi):
    _, r, d = g_low.shape
    width = ret.shape[2]
    row = pl.BlockSpec((2, r, width), lambda k: (k, 0, 0))
    return pl.pallas_call(
        gate_back_kernel,
        grid=(TP // 2,),
        out_shape=(SDS(ret.shape, bf), SDS(ret.shape, bf)),
        in_specs=[
            pl.BlockSpec((2, r, d), lambda k: (k, 0, 0)),
            pl.BlockSpec(w.shape, lambda k: (0, 0, 0)),
            row,
            row,
        ],
        out_specs=(row, row),
        scratch_shapes=[pltpu.VMEM((width, d), bf), pltpu.VMEM((2 * r, width), f32)],
        compiler_params=pltpu.CompilerParams(vmem_limit_bytes=56 << 20),
        cost_estimate=pl.CostEstimate(
            flops=2 * TP * r * d * width, bytes_accessed=22 << 20, transcendentals=TP * r * width
        ),
        name="gate_back",
    )(g_low, w, ret, swi)


def scores_back_kernel(sco, mask, q, k, v, gret, cosine, sine, out):
    nt, tn = (((1,), (1,)), ((), ())), (((0,), (0,)), ((), ()))
    kh = q.shape[2]
    half = kh // 2
    out[0, :, 2 * kh :] = lax.dot_general(
        sco[0], gret[0], tn, preferred_element_type=f32
    ).astype(bf)
    grad = lax.dot_general(gret[0], v[0], nt, preferred_element_type=f32)
    grad = (grad * mask[0]).astype(bf)
    gq = jnp.dot(grad, k[0], preferred_element_type=f32)
    gk = lax.dot_general(grad, q[0], tn, preferred_element_type=f32)
    for i, g in enumerate((gq, gk)):
        u, w = g[:, :half], g[:, half:]
        at = i * kh
        out[0, :, at : at + half] = (u * cosine[0] + w * sine[0]).astype(bf)
        out[0, :, at + half : at + kh] = (w * cosine[0] - u * sine[0]).astype(bf)


def scores_back(sco, mask, q, k, v, gret, cosine, sine):
    _, r, kh = q.shape
    arrays = (sco, mask, q, k, v, gret, cosine, sine)
    width = 2 * kh + v.shape[2]
    spec = [pl.BlockSpec((1,) + x.shape[1:], lambda i: (i, 0, 0)) for x in arrays]
    return pl.pallas_call(
        scores_back_kernel,
        grid=(TP,),
        out_shape=SDS((TP, r, width), bf),
        in_specs=spec,
        out_specs=pl.BlockSpec((1, r, width), lambda i: (i, 0, 0)),
        compiler_params=pltpu.CompilerParams(vmem_limit_bytes=56 << 20),
        cost_estimate=pl.CostEstimate(
            flops=4 * TP * r * r * (kh + v.shape[2]), bytes_accessed=16 << 20, transcendentals=0
        ),
        name="scores_back",
    )(*arrays)


def tp_groups(n):
    return [[g * TP + t for t in range(TP)] for g in range(n // TP)]


def dp_groups(n):
    return [[g * TP + t for g in range(n // TP)] for t in range(TP)]


def plane_a2a(x, n):
    return lax.all_to_all(x, AXIS, 0, 0, axis_index_groups=tp_groups(n), tiled=True)


def dp_gather(x, n):
    return lax.all_gather(x, AXIS, axis=0, tiled=True, axis_index_groups=dp_groups(n))


def dp_reduce(x, n):
    return lax.psum_scatter(
        x, AXIS, scatter_dimension=0, tiled=True, axis_index_groups=dp_groups(n)
    )


def seq_positions(lengths, rows):
    ends = jnp.cumsum(lengths, axis=1)
    starts = ends - lengths
    index = jnp.arange(rows, dtype=jnp.int32)
    segment = jnp.sum((index[None, :, None] >= ends[:, None, :]).astype(jnp.int32), axis=2)
    member = segment[:, :, None] == jnp.arange(lengths.shape[1], dtype=jnp.int32)
    offset = index[None, :] - jnp.sum(jnp.where(member, starts[:, None, :], 0), axis=2)
    return segment, offset


def rotary_tables(offset):
    half = KH // 2
    freq = jnp.exp(-math.log(10000.0) * jnp.arange(half, dtype=f32) / half)
    angle = offset.astype(f32)[..., None] * freq
    return jnp.cos(angle), jnp.sin(angle)


def decay_mask(segment, offset, head):
    diff = offset[:, :, None] - offset[:, None, :]
    valid = (segment[:, :, None] == segment[:, None, :]) & (diff >= 0)
    steps = jnp.where(valid, diff, 0).astype(f32)
    log = jnp.log(1.0 - jnp.exp2(-5.0 - head.astype(f32)))
    return jnp.where(valid, jnp.exp(log * steps), 0.0) / math.sqrt(KH)


def col_blocks(w):
    r, c = w.shape
    return w.reshape(r, TP, c // TP).transpose(1, 0, 2).reshape(TP * r, c // TP)


def join_kernel(widths, parts, x, *outs):
    at = 0
    for out, width in zip(outs, widths):
        piece = width // parts
        for t in range(TP):
            for p in range(parts):
                to = (p * TP + t) * piece
                out[:, to : to + piece] = x[t, :, at + p * piece : at + (p + 1) * piece].astype(f32)
        at += width


def join(x, widths, parts=1):
    r = x.shape[1]
    if any(width // parts % 128 for width in widths):
        made, at = [], 0
        for width in widths:
            part = x[:, :, at : at + width].reshape(TP, r, parts, width // parts)
            made.append(part.transpose(1, 2, 0, 3).reshape(r, TP * width).astype(f32))
            at += width
        return made
    return pl.pallas_call(
        functools.partial(join_kernel, widths, parts),
        out_shape=tuple(SDS((r, TP * width), f32) for width in widths),
        in_specs=[VMEM],
        out_specs=tuple(VMEM for _ in widths),
        compiler_params=pltpu.CompilerParams(vmem_limit_bytes=8 << 20),
        cost_estimate=pl.CostEstimate(flops=0, bytes_accessed=6 * x.size, transcendentals=0),
        name="join",
    )(x)


def after(x, *deps):
    return lax.optimization_barrier((x,) + deps)[0]


def on_device(n, tokens, lengths, gain1, bias1, wq, wk, wv, ws, wo, gain2, bias2, wg, wu, wd, cot):
    rows, d = tokens.shape
    ff = wg.shape[1]
    dp = n // TP
    shard = d // n
    unit = ff // n
    me = lax.axis_index(AXIS)
    head = lax.rem(me, TP)

    def ff_blocks(w):
        return w.reshape(shard, dp, TP, unit).transpose(2, 0, 1, 3).reshape(TP, shard, dp * unit)

    lens = jnp.pad(lengths[0].astype(f32), (0, shard - lengths.shape[1]))
    vec = jnp.stack([v.astype(f32) for v in (gain1, bias1, gain2, bias2)] + [lens])
    vec = jnp.pad(vec, ((0, 3), (0, 128 - shard)))
    qko_blk = first_exchange(wq, wk, wo, 1)
    qko = dp_gather(qko_blk.reshape(TP * shard, 4 * KH), n)
    tok_all, vec_all = second_exchange(n, after(tokens, qko_blk), vec, 2)
    gain1f, bias1f, gain2f, bias2f = (
        vec_all[:, :, i, :shard].reshape(1, d) for i in range(4)
    )
    vec2 = jnp.concatenate([gain2f, bias2f], axis=0)
    gu_in = jnp.concatenate([ff_blocks(wg), ff_blocks(wu)], axis=2)
    vs_blk, gu_blk, normed = third_exchange(wv, ws, gu_in, tok_all, gain1f, bias1f, 3)
    vs = dp_gather(vs_blk.reshape(TP * shard, 2 * VH), n)
    gu = dp_gather(gu_blk.reshape(TP * shard, 2 * dp * unit), n)
    down = dp_gather(wd, n)

    mine = lax.dynamic_slice_in_dim(vec_all, lax.div(me, TP), 1, 0)[0, :, 4, :3]
    order = jnp.arange(TP, dtype=jnp.int32)
    pick = (order[None, :] == (order[:, None] ^ head)).astype(f32)
    len_all = jnp.sum(pick[:, :, None] * mine[None], axis=1).astype(jnp.int32)
    segment, offset = seq_positions(len_all, rows)
    cosine, sine = rotary_tables(offset)
    mask = decay_mask(segment, offset, head)

    cot_all, out_blk, q_rot, k_rot, scores, qk = fourth_exchange(
        n, cot, qko.reshape(n, shard, 4 * KH), normed, cosine, sine, mask, 4
    )
    out_blk = out_blk.reshape(TP, VH, d // TP)
    qk = qk.reshape(d, 2 * KH)
    v_low, mixed, retained, swish_in, middle, normed2 = forward_exchange(
        normed, vs, scores, out_blk, tokens, vec2, 5
    )
    hidden, act, slope = hidden_units(normed2, gu)
    down_grad = row_product(hidden, cot_all)
    g_down = dp_reduce(down_grad, n)

    g_fs = hidden_back(cot_all, down, act, slope)
    gu_grad = row_product(normed2, g_fs)
    g_gu = dp_reduce(gu_grad, n)
    g_middle, g_low, sums2 = backward_exchange(g_fs, gu, middle, cot, vec2, 6)

    g_retained, g_swish = gate_back(g_low, out_blk, retained, swish_in)
    swish_grad = row_product(normed, g_swish)
    g_swi = dp_reduce(swish_grad, n)
    out_grad = row_product(mixed, g_low)
    out_grad = plane_a2a(col_blocks(out_grad), n)
    g_qkv = scores_back(scores, mask, q_rot, k_rot, v_low, g_retained, cosine, sine)
    qkv_grad = row_product(normed, g_qkv)
    g_qkv_own = dp_reduce(qkv_grad, n)
    g_out = dp_reduce(out_grad, n)
    grad_tokens, ffn, g_vecs = last_exchange(
        n, g_qkv, g_swish, qk, vs, hidden, down, tokens, g_middle, gain1f, sums2, 7
    )
    layer_out = (middle + ffn).astype(bf)

    g_vecs = lax.dynamic_slice_in_dim(g_vecs, head * shard, shard, 1)
    grad_d = g_down.astype(f32)
    g_gu = plane_a2a(g_gu, n)
    grad_g, grad_u = join(g_gu.reshape(TP, shard, 2 * dp * unit), (dp * unit,) * 2, dp)
    g_swi = plane_a2a(g_swi, n)
    (grad_s,) = join(g_swi.reshape(TP, shard, VH), (VH,))
    g_qkv_own = plane_a2a(g_qkv_own, n)
    grad_q, grad_k, grad_v = join(g_qkv_own.reshape(TP, shard, 2 * KH + VH), (KH, KH, VH))
    g_out = plane_a2a(g_out, n)
    (grad_o,) = join(g_out.reshape(TP, wo.shape[0], d // TP), (d // TP,))
    return (
        layer_out, grad_tokens, g_vecs[0], g_vecs[1], grad_q, grad_k, grad_v, grad_s, grad_o,
        g_vecs[2], g_vecs[3], grad_g, grad_u, grad_d,
    )


def solution(mesh):
    n = mesh.shape[AXIS]
    row, vec = P(AXIS, None), P(AXIS)
    ins = (row, row, vec, vec, row, row, row, row, row, vec, vec, row, row, row, row)
    outs = (row, row, vec, vec, row, row, row, row, row, vec, vec, row, row, row)

    def body(*args):
        return on_device(n, *args)

    return jax.shard_map(body, mesh=mesh, in_specs=ins, out_specs=outs, check_vma=False)
```

```python
import functools
import math

import jax
import jax.numpy as jnp
from jax import lax
from jax.experimental import pallas as pl
from jax.experimental.pallas import tpu as pltpu
from jax.sharding import PartitionSpec as P


KH = 256
VH = 512
TP = 8
AXIS = "fsdp"
MESH = pl.DeviceIdType.MESH
ANY = pl.BlockSpec(memory_space=pl.ANY)
VMEM = pl.BlockSpec(memory_space=pltpu.VMEM)
bf = jnp.bfloat16
f32 = jnp.float32
SDS = jax.ShapeDtypeStruct
ALL_VMEM = 67043328


def place():
    me = lax.axis_index(AXIS)
    steps = [s - 2 * s * lax.rem(lax.div(me, s), 2) for s in (1, 2, 4)]

    def peer(k):
        out = me
        for bit, step in enumerate(steps):
            if k >> bit & 1:
                out = out + step
        return out

    return me, peer


def greet(peers):
    barrier = pltpu.get_barrier_semaphore()
    for p in peers:
        pl.semaphore_signal(barrier, inc=1, device_id=(p,), device_id_type=MESH)
    return lambda: pl.semaphore_wait(barrier, len(peers))


def meet(peers):
    greet(peers)()


def remote(src, dst, sems, i, dev):
    return pltpu.make_async_remote_copy(
        src_ref=src, dst_ref=dst, send_sem=sems[0].at[i], recv_sem=sems[1].at[i],
        device_id=(dev,), device_id_type=MESH,
    )


GATHER_SEMS = 13


class Gather:
    def __init__(self, own, out, start, size, sems, base, local, peer):
        self.own, self.out, self.sems, self.base, self.local = own, out, sems, base, local
        h = size // 2
        self.all, self.top, self.bot = pl.ds(start, size), pl.ds(start, h), pl.ds(start + h, h)
        self.pc, self.px, self.py = peer(1), peer(2), peer(4)
        self.made = []

    def send(self, src, dst, dev):
        copy = remote(src, dst, self.sems, self.base + len(self.made), dev)
        copy.start()
        self.made.append(copy)
        return copy

    def pass_on(self, k, at):
        self.core.append(self.send(self.out.at[k, at], self.out.at[k + 1, at], self.pc))

    def start(self):
        own, out, top, bot = self.own, self.out, self.top, self.bot
        self.x0 = self.send(own.at[bot], out.at[2, bot], self.px)
        self.y0 = self.send(own.at[top], out.at[4, top], self.py)
        self.x1 = self.send(own.at[top], out.at[2, top], self.px)
        self.y1 = self.send(own.at[bot], out.at[4, bot], self.py)
        self.core = [self.send(own.at[self.all], out.at[1, self.all], self.pc)]
        self.keep = pltpu.make_async_copy(own.at[self.all], out.at[0, self.all], self.local)
        self.keep.start()

    def forward(self):
        out, top, bot = self.out, self.top, self.bot
        self.x0.wait_recv()
        self.fy = self.send(out.at[2, bot], out.at[6, bot], self.py)
        self.pass_on(2, bot)
        self.y0.wait_recv()
        self.fx = self.send(out.at[4, top], out.at[6, top], self.px)
        self.pass_on(4, top)
        self.x1.wait_recv()
        self.pass_on(2, top)
        self.y1.wait_recv()
        self.pass_on(4, bot)

    def finish(self):
        self.fy.wait_recv()
        self.pass_on(6, self.bot)
        self.fx.wait_recv()
        self.pass_on(6, self.top)
        for copy in self.core:
            copy.wait_recv()
        for copy in self.made:
            copy.wait_send()
        self.keep.wait()


def send_columns(src, out, cols, at, sems, base, local, t, peer, rows=None):
    copies = []
    rows = slice(None) if rows is None else rows

    def block(q):
        if len(src.shape) == 3:
            return src.at[q]
        return src.at[rows, pl.ds(pl.multiple_of(q * cols, 128), cols)]

    for k in range(1, TP):
        dev = peer(k)
        copy = remote(
            block(lax.rem(dev, TP)), out.at[t, :, pl.ds(at, cols)], sems, base + k - 1, dev
        )
        copy.start()
        copies.append(copy)
    keep = pltpu.make_async_copy(block(t), out.at[t, :, pl.ds(at, cols)], local)
    keep.start()
    return copies, keep


def finish(parts):
    for copies, keep in parts:
        for copy in copies:
            copy.wait()
        keep.wait()


def exchange_call(
    kernel, outs, args, sems, locals_, cid, specs=None, out_specs=None, vmem=12 << 20
):
    return pl.pallas_call(
        kernel,
        out_shape=outs,
        in_specs=specs or [VMEM] * len(args),
        out_specs=out_specs or tuple(ANY for _ in outs),
        scratch_shapes=[
            pltpu.SemaphoreType.DMA((sems,)),
            pltpu.SemaphoreType.DMA((sems,)),
            pltpu.SemaphoreType.DMA((locals_,)),
        ],
        compiler_params=pltpu.CompilerParams(
            collective_id=cid, has_side_effects=True, vmem_limit_bytes=vmem
        ),
    )(*args)


def first_kernel(wq, wk, wo, out, ssem, rsem, local):
    me, peer = place()
    t = lax.rem(me, TP)
    meet([peer(k) for k in range(1, TP)])
    sems = (ssem, rsem)
    shard, cq, co = wq.shape[0], wq.shape[1] // TP, wo.shape[1] // TP
    low, high = pl.ds(0, shard), pl.ds(shard, shard)
    finish([
        send_columns(wq, out, cq, 0, sems, 0, local.at[0], t, peer),
        send_columns(wk, out, cq, cq, sems, 7, local.at[1], t, peer),
        send_columns(wo, out, co, 2 * cq, sems, 14, local.at[2], t, peer, low),
        send_columns(wo, out, co, 2 * cq + co, sems, 21, local.at[3], t, peer, high),
    ])


def first_exchange(wq, wk, wo, cid):
    width = 2 * wq.shape[1] // TP + 2 * wo.shape[1] // TP
    outs = (SDS((TP, wq.shape[0], width), bf),)
    return exchange_call(first_kernel, outs, (wq, wk, wo), 28, 4, cid)[0]


def others_along(n):
    me = lax.axis_index(AXIS)
    return [lax.rem(me + TP * j, n) for j in range(1, n // TP)]


def second_kernel(n, tok, vec, tok_out, vec_out, ssem, rsem, local):
    me, peer = place()
    t, g = lax.rem(me, TP), lax.div(me, TP)
    others = others_along(n)
    meet([peer(k) for k in range(1, TP)] + others)
    sems = (ssem, rsem)
    base = GATHER_SEMS
    far = []
    keep = pltpu.make_async_copy(vec, vec_out.at[g, t], local.at[1])
    keep.start()
    for j, dev in enumerate(others):
        copy = remote(vec, vec_out.at[g, t], sems, base + TP + j, dev)
        copy.start()
        far.append(copy)
    gather = Gather(tok, tok_out, 0, tok.shape[0], sems, 0, local.at[0], peer)
    gather.start()
    for copy in far:
        copy.wait()
    keep.wait()
    near = []
    for k in range(1, TP):
        copy = remote(vec_out.at[:, t], vec_out.at[:, t], sems, base + k, peer(k))
        copy.start()
        near.append(copy)
    gather.forward()
    gather.finish()
    for copy in near:
        copy.wait()


def second_exchange(n, tok, vec, cid):
    outs = (SDS((TP,) + tok.shape, bf), SDS((n // TP, TP) + vec.shape, f32))
    kernel = functools.partial(second_kernel, n)
    sems = GATHER_SEMS + TP + n // TP
    return exchange_call(kernel, outs, (tok, vec), sems, 2, cid)


def third_kernel(wv, ws, gu, tok, gain, bias, out, gu_out, nrm, ssem, rsem, local):
    me, peer = place()
    t = lax.rem(me, TP)
    meet([peer(k) for k in range(1, TP)])
    sems = (ssem, rsem)
    cols = wv.shape[1] // TP
    parts = [
        send_columns(wv, out, cols, 0, sems, 0, local.at[0], t, peer),
        send_columns(ws, out, cols, cols, sems, 7, local.at[1], t, peer),
        send_columns(gu, gu_out, gu.shape[2], 0, sems, 14, local.at[2], t, peer),
    ]
    step, r = 16, tok.shape[1]

    def norm(j, _):
        k = lax.div(j, r // step)
        at = pl.ds(pl.multiple_of(lax.rem(j, r // step) * step, step), step)
        value = tok[k, at, :].astype(f32)
        centred = value - jnp.mean(value, axis=-1, keepdims=True)
        spread = jnp.mean(centred * centred, axis=-1, keepdims=True)
        nrm[k, at, :] = (centred * lax.rsqrt(spread + 1e-05) * gain[...] + bias[...]).astype(bf)
        return 0

    lax.fori_loop(0, TP * r // step, norm, 0, unroll=4)
    finish(parts)


def third_exchange(wv, ws, gu, tok, gain, bias, cid):
    outs = (
        SDS((TP, wv.shape[0], 2 * wv.shape[1] // TP), bf),
        SDS(gu.shape, bf),
        SDS(tok.shape, bf),
    )
    return exchange_call(
        third_kernel, outs, (wv, ws, gu, tok, gain, bias), 21, 3, cid,
        out_specs=(ANY, ANY, VMEM), vmem=32 << 20,
    )


def fourth_kernel(
    n, cot, qko, nrm, cosine, sine, mask, cot_out, o_out, q_out, k_out, sco, w, ssem, rsem, local
):
    me, peer = place()
    t = lax.rem(me, TP)
    meet([peer(k) for k in range(1, TP)])
    sems = (ssem, rsem)
    share, cols = n // TP, o_out.shape[4]
    _, r, kh = q_out.shape
    half = kh // 2
    weights = pltpu.make_async_copy(qko.at[:, :, pl.ds(0, 2 * kh)], w, local.at[3])
    weights.start()
    gather = Gather(cot, cot_out, 0, cot.shape[0], sems, 0, local.at[0], peer)
    gather.start()
    copies, keeps = [], []

    def part(p, which):
        return qko.at[pl.ds(p * share, share), :, pl.ds(2 * kh + which * cols, cols)]

    for which in (0, 1):
        for k in range(1, TP):
            dev = peer(k)
            copy = remote(
                part(lax.rem(dev, TP), which), o_out.at[t, :, which], sems,
                GATHER_SEMS + which * TP + k, dev,
            )
            copy.start()
            copies.append(copy)
        keep = pltpu.make_async_copy(part(t, which), o_out.at[t, :, which], local.at[1 + which])
        keep.start()
        keeps.append(keep)
    weights.wait()

    def products(pairs):
        @pl.loop(*pairs)
        def _(j):
            rows = nrm[pl.ds(2 * j, 2)].reshape(2 * r, nrm.shape[2])
            for at, out in ((0, q_out), (kh, k_out)):
                y = jnp.dot(
                    rows, w[:, :, at : at + kh].reshape(nrm.shape[2], kh),
                    preferred_element_type=f32,
                )
                for i in (0, 1):
                    u, v = y[i * r : (i + 1) * r, :half], y[i * r : (i + 1) * r, half:]
                    cos, sin = cosine[2 * j + i], sine[2 * j + i]
                    out[2 * j + i, :, :half] = (u * cos - v * sin).astype(bf)
                    out[2 * j + i, :, half:] = (v * cos + u * sin).astype(bf)
            for i in (0, 1):
                plain = lax.dot_general(
                    q_out[2 * j + i], k_out[2 * j + i], (((1,), (1,)), ((), ())),
                    preferred_element_type=f32,
                )
                sco[2 * j + i] = (plain * mask[2 * j + i]).astype(bf)

    products((0, TP // 2))
    gather.forward()
    gather.finish()
    for copy in copies:
        copy.wait()
    for keep in keeps:
        keep.wait()


def fourth_exchange(n, cot, qko, nrm, cosine, sine, mask, cid):
    _, shard, width = qko.shape
    cols = (width - 2 * KH) // 2
    r = cot.shape[0]
    outs = (
        SDS((TP,) + cot.shape, bf),
        SDS((TP, n // TP, 2, shard, cols), bf),
        SDS((TP, r, KH), bf),
        SDS((TP, r, KH), bf),
        SDS(mask.shape, bf),
        SDS((n, shard, 2 * KH), bf),
    )
    kernel = functools.partial(fourth_kernel, n)
    return exchange_call(
        kernel, outs, (cot, qko, nrm, cosine, sine, mask),
        GATHER_SEMS + 2 * TP, 4, cid,
        specs=[VMEM, ANY, VMEM, VMEM, VMEM, VMEM],
        out_specs=(ANY, ANY, VMEM, VMEM, VMEM, VMEM), vmem=40 << 20,
    )


REDUCE_SEMS = 16
TILE = 256


class Reduce:
    def __init__(self, product, bufs, sems, base, peer, prepare=None, enter=None):
        self.product, self.prepare, self.sems, self.base = product, prepare, sems, base
        self.enter = enter
        self.po, self.pe, self.rc, self.sb, self.ring = bufs
        self.pc, self.px, self.py = peer(1), peer(2), peer(4)
        self.q = self.pe.shape[1] // 4
        self.sent, self.core, self.got = [], {}, ({}, {})

    def send(self, src, dst, dev, i):
        copy = remote(src, dst, self.sems, self.base + i, dev)
        copy.start()
        self.sent.append(copy)
        return copy

    def ready(self, i):
        if self.prepare is not None:
            self.prepare(2 * i)

    def pair(self, i):
        self.product(i, self.po.at[i], self.pe.at[i])
        if self.enter is not None:
            self.enter()
            self.enter = None
        self.core[i] = self.send(self.po.at[i], self.rc.at[i], self.pc, i)

    def add(self, halves, i, lower, out, more=None):
        step = 16
        steps = self.q // step
        first, count = halves

        @pl.loop(first * steps, (first + count) * steps)
        def _(j):
            c = lax.div(j, steps)
            there = pl.ds(pl.multiple_of(lax.rem(j, steps) * step, step), step)
            here = pl.ds(
                pl.multiple_of(lax.rem(j, steps) * step + (2 * c + lower) * self.q, step), step
            )
            total = self.pe[i, here, :].astype(f32) + self.rc[i, here, :].astype(f32)
            if more is not None:
                total = total + self.ring[more, c, 0, there, :].astype(f32)
            self.sb[c, out, there, :] = total.astype(bf)

    def link(self, c, slot, name, ring, at, dev):
        self.got[c][name] = self.send(
            self.sb.at[c, slot], self.ring.at[ring, c, at], dev, 4 + 6 * c + slot
        )

    def both(self, slot, name, i, lower, ring, at, dev):
        self.add((0, 2), i, lower, slot)
        for c in (0, 1):
            self.link(c, slot, name, ring, at, dev)

    def six(self):
        self.both(0, "x6", 3, 0, 0, 0, self.px)
        self.both(1, "y6", 3, 1, 1, 0, self.py)

    def two(self):
        self.both(2, "x2", 1, 0, 0, 1, self.px)

    def four(self):
        self.both(3, "y4", 2, 1, 1, 1, self.py)

    def onward(self, c):
        self.got[c]["x6"].wait_recv()
        self.add((c, 1), 2, 0, 4, 0)
        self.link(c, 4, "y4b", 1, 2, self.py)
        self.got[c]["y6"].wait_recv()
        self.add((c, 1), 1, 1, 5, 1)
        self.link(c, 5, "x2b", 0, 2, self.px)

    def run(self):
        self.ready(3)
        self.pair(3)
        stages = ((1, 3, self.six), (2, 1, self.two), (0, 2, self.four))
        for following, now, stage in stages:
            self.ready(following)
            if self.prepare is None:
                self.pair(following)
            self.core[now].wait_recv()
            stage()
            if self.prepare is not None:
                self.pair(following)
        for c in (0, 1):
            self.onward(c)

    def rows(self, c, step, body):
        if c == 0:
            self.core[0].wait_recv()
        for name in ("x2", "y4", "y4b", "x2b"):
            self.got[c][name].wait_recv()
        steps = self.q // step

        @pl.loop(0, 2 * steps)
        def _(j):
            lower = lax.div(j, steps)
            there = pl.ds(pl.multiple_of(lax.rem(j, steps) * step, step), step)
            here = pl.ds(pl.multiple_of(j * step + 2 * c * self.q, step), step)
            body(
                here,
                self.pe[0, here, :].astype(f32)
                + self.rc[0, here, :].astype(f32)
                + self.ring[lower, c, 1, there, :].astype(f32)
                + self.ring[1 - lower, c, 2, there, :].astype(f32),
            )

    def finish(self):
        for copy in self.sent:
            copy.wait_send()


def reduce_scratch(r, c, even=f32):
    q = r // 4
    return [
        pltpu.VMEM((4, r, c), bf),
        pltpu.VMEM((4, r, c), even),
        pltpu.VMEM((4, r, c), bf),
        pltpu.VMEM((2, 6, q, c), bf),
        pltpu.VMEM((2, 2, 3, q, c), bf),
    ]


def rows_of_pair(a, i):
    two, r, k = 2, a.shape[1], a.shape[2]
    return a[pl.ds(2 * i, two)].reshape(two * r, k)


def times(a, w, nt):
    def product(i, odd, even):
        r = a.shape[1]

        @pl.loop(0, even.shape[1] // TILE)
        def _(j):
            at = pl.ds(pl.multiple_of(j * TILE, TILE), TILE)
            x = rows_of_pair(a, i)
            if nt:
                y = lax.dot_general(
                    x, w[at, :], (((1,), (1,)), ((), ())), preferred_element_type=f32
                )
            else:
                y = jnp.dot(x, w[:, at], preferred_element_type=f32)
            even[:, at] = y[:r].astype(even.dtype)
            odd[:, at] = y[r:].astype(odd.dtype)

    return product


def exchange_and_gather(reduce, gathers, step, body):
    reduce.run()
    for c in (0, 1):
        reduce.rows(c, step, body)
        gathers[c].start()
    for c in (0, 1):
        gathers[c].forward()
    for c in (0, 1):
        gathers[c].finish()
    reduce.finish()


def both_gathers(own, out, sems, local, peer):
    half = own.shape[0] // 2
    return [
        Gather(own, out, c * half, half, sems, REDUCE_SEMS + c * GATHER_SEMS, local.at[c], peer)
        for c in (0, 1)
    ]


EXCHANGE_SEMS = REDUCE_SEMS + 2 * GATHER_SEMS


def forward_kernel(
    nrm, wvs, sco, w, tok, vec, v_out, mix_out, ret_out, swi_out, mid, out,
    v_buf, mix_buf, ret_buf, swi_buf, po, pe, rc, sb, ring, own, ssem, rsem, local,
):
    _, peer = place()
    enter = greet([peer(1), peer(2), peer(4)])
    sems = (ssem, rsem)
    r, width = v_buf.shape[1:]
    kept = []

    def prepare(first):
        two = pl.ds(first, 2)
        x = nrm[two].reshape(2 * r, nrm.shape[2])

        tiles = width // TILE

        @pl.loop(0, 2 * tiles)
        def _(j):
            at = pl.ds(pl.multiple_of(j * TILE, TILE), TILE)
            y = jnp.dot(x, wvs[:, at], preferred_element_type=f32)
            y = y.reshape(2, r, TILE)

            @pl.when(j < tiles)
            def _():
                v_buf[two, :, at] = y.astype(bf)

            @pl.when(j >= tiles)
            def _():
                swi_buf[two, :, pl.ds(pl.multiple_of(j * TILE - width, TILE), TILE)] = y

        @pl.loop(0, 2 * tiles)
        def _(j):
            k = first + lax.div(j, tiles)
            at = pl.ds(pl.multiple_of(lax.rem(j, tiles) * TILE, TILE), TILE)
            ret_buf[k, :, at] = jnp.dot(sco[k], v_buf[k, :, at], preferred_element_type=f32)

        @pl.loop(0, 2 * r // 32)
        def _(j):
            k = first + lax.div(j, r // 32)
            at = pl.ds(pl.multiple_of(lax.rem(j, r // 32) * 32, 32), 32)
            value = ret_buf[k, at, :]
            centred = value - jnp.mean(value, axis=-1, keepdims=True)
            spread = jnp.mean(centred * centred, axis=-1, keepdims=True)
            gate = swi_buf[k, at, :]
            gate = gate / (1.0 + jnp.exp(-gate))
            mix_buf[k, at, :] = (
                gate * (centred * lax.rsqrt(jnp.maximum(spread, 0.25)))
            ).astype(bf)

        for i, (src, dst) in enumerate(
            ((v_buf, v_out), (mix_buf, mix_out), (ret_buf, ret_out), (swi_buf, swi_out))
        ):
            copy = pltpu.make_async_copy(
                src.at[two], dst.at[two], local.at[2 + 2 * first + i]
            )
            copy.start()
            kept.append(copy)

    def product(i, odd, even):
        step = w.shape[2]

        @pl.loop(0, w.shape[0])
        def _(j):
            at = pl.ds(pl.multiple_of(j * step, step), step)
            y = jnp.dot(rows_of_pair(mix_buf, i), w[j], preferred_element_type=f32)
            even[:, at] = y[:r].astype(even.dtype)
            odd[:, at] = y[r:].astype(odd.dtype)

    def body(at, value):
        value = value + tok[at, :].astype(f32)
        mid[at, :] = value
        center = jnp.mean(value, axis=-1, keepdims=True)
        centred = value - center
        spread = jnp.mean(centred * centred, axis=-1, keepdims=True)
        own[at, :] = (
            centred * lax.rsqrt(spread + 1e-05) * vec[0:1, :] + vec[1:2, :]
        ).astype(bf)

    reduce = Reduce(product, (po, pe, rc, sb, ring), sems, 0, peer, prepare, enter)
    exchange_and_gather(reduce, both_gathers(own, out, sems, local, peer), 16, body)
    for copy in kept:
        copy.wait()


def forward_exchange(nrm, wvs, sco, w, tok, vec, cid):
    _, r, d = nrm.shape
    width = w.shape[1]
    count = EXCHANGE_SEMS
    blocks = [((TP, r, width), t) for t in (bf, bf, f32, f32)]
    return pl.pallas_call(
        forward_kernel,
        out_shape=tuple(SDS(*b) for b in blocks) + (SDS((r, d), f32), SDS((TP, r, d), bf)),
        in_specs=[VMEM] * 6,
        out_specs=(ANY,) * 4 + (VMEM, ANY),
        scratch_shapes=[pltpu.VMEM(*b) for b in blocks]
        + reduce_scratch(r, d)
        + [
            pltpu.VMEM((r, d), bf),
            pltpu.SemaphoreType.DMA((count,)),
            pltpu.SemaphoreType.DMA((count,)),
            pltpu.SemaphoreType.DMA((18,)),
        ],
        compiler_params=pltpu.CompilerParams(
            collective_id=cid, has_side_effects=True, vmem_limit_bytes=60 << 20
        ),
        name="forward_exchange",
    )(nrm, wvs, sco, w, tok, vec)


def product_kernel(a, b, out):
    a, b = a[...].reshape(-1, a.shape[-1]), b[...].reshape(-1, b.shape[-1])
    out[...] = lax.dot_general(
        a, b, (((0,), (0,)), ((), ())), preferred_element_type=f32
    ).astype(bf)


def row_product(a, b):
    _, r, m = a.shape
    width = b.shape[2]
    tile, part = 512 if m >= 2048 else 256, min(width, 1024)
    return pl.pallas_call(
        product_kernel,
        grid=(width // part, m // tile),
        out_shape=SDS((m, width), bf),
        in_specs=[
            pl.BlockSpec((TP, r, tile), lambda j, i: (0, 0, i)),
            pl.BlockSpec((TP, r, part), lambda j, i: (0, 0, j)),
        ],
        out_specs=pl.BlockSpec((tile, part), lambda j, i: (i, j)),
        compiler_params=pltpu.CompilerParams(vmem_limit_bytes=56 << 20),
        cost_estimate=pl.CostEstimate(
            flops=2 * TP * r * m * width,
            bytes_accessed=2 * (a.size + b.size + m * width),
            transcendentals=0,
        ),
        name="row_product",
    )(a, b)


def hidden_kernel(x, gu, hid, act_out, slope_out):
    width = hid.shape[2]
    step = 256

    @pl.loop(0, width // step)
    def _(j):
        at = pl.ds(pl.multiple_of(j * step, step), step)
        behind = pl.ds(pl.multiple_of(j * step + width, step), step)
        rows = x[...].reshape(-1, x.shape[2])
        first = jnp.dot(rows, gu[:, at], preferred_element_type=f32)
        second = jnp.dot(rows, gu[:, behind], preferred_element_type=f32)
        share = 0.5 * (1.0 + lax.erf(first * math.sqrt(0.5)))
        act = first * share
        slope = share + first * (jnp.exp(-0.5 * first * first) * (1.0 / math.sqrt(2.0 * math.pi)))
        block = hid.shape[:2] + (step,)
        hid[:, :, at] = (act * second).astype(bf).reshape(block)
        act_out[:, :, at] = act.reshape(block)
        slope_out[:, :, at] = (slope * second).reshape(block)


def hidden_units(x, gu):
    _, r, d = x.shape
    width = gu.shape[1] // 2
    row = pl.BlockSpec((2, r, width), lambda k: (k, 0, 0))
    return pl.pallas_call(
        hidden_kernel,
        grid=(TP // 2,),
        out_shape=tuple(SDS((TP, r, width), t) for t in (bf, f32, f32)),
        in_specs=[
            pl.BlockSpec((2, r, d), lambda k: (k, 0, 0)),
            pl.BlockSpec(gu.shape, lambda k: (0, 0)),
        ],
        out_specs=(row, row, row),
        compiler_params=pltpu.CompilerParams(vmem_limit_bytes=56 << 20),
        cost_estimate=pl.CostEstimate(
            flops=4 * TP * r * d * width, bytes_accessed=24 << 20, transcendentals=2 * TP * r * width
        ),
        name="hidden_units",
    )(x, gu)


def hidden_back_kernel(cot, down, act, slope, out):
    width = act.shape[2]
    step = 256

    @pl.loop(0, width // step)
    def _(j):
        at = pl.ds(pl.multiple_of(j * step, step), step)
        behind = pl.ds(pl.multiple_of(j * step + width, step), step)
        grad = lax.dot_general(
            cot[...].reshape(-1, cot.shape[2]), down[at, :], (((1,), (1,)), ((), ())),
            preferred_element_type=f32,
        ).reshape(act.shape[:2] + (step,))
        out[:, :, at] = (grad * slope[:, :, at]).astype(bf)
        out[:, :, behind] = (grad * act[:, :, at]).astype(bf)


def hidden_back(cot, down, act, slope):
    _, r, d = cot.shape
    width = act.shape[2]
    row = pl.BlockSpec((2, r, width), lambda k: (k, 0, 0))
    return pl.pallas_call(
        hidden_back_kernel,
        grid=(TP // 2,),
        out_shape=SDS((TP, r, 2 * width), bf),
        in_specs=[
            pl.BlockSpec((2, r, d), lambda k: (k, 0, 0)),
            pl.BlockSpec(down.shape, lambda k: (0, 0)),
            row,
            row,
        ],
        out_specs=pl.BlockSpec((2, r, 2 * width), lambda k: (k, 0, 0)),
        compiler_params=pltpu.CompilerParams(vmem_limit_bytes=56 << 20),
        cost_estimate=pl.CostEstimate(
            flops=2 * TP * r * d * width, bytes_accessed=24 << 20, transcendentals=0
        ),
        name="hidden_back",
    )(cot, down, act, slope)


def backward_kernel(
    a, w, mid, cot, vec, gmid, out, sums, po, pe, rc, sb, ring, own, acc, ssem, rsem, local
):
    _, peer = place()
    enter = greet([peer(1), peer(2), peer(4)])
    sems = (ssem, rsem)
    acc[...] = jnp.zeros_like(acc)

    def body(at, g):
        value = mid[at, :]
        center = jnp.mean(value, axis=-1, keepdims=True)
        centred = value - center
        inv = lax.rsqrt(jnp.mean(centred * centred, axis=-1, keepdims=True) + 1e-05)
        hat = centred * inv
        acc[0] += g * hat
        acc[1] += g
        scaled = g * vec[0:1, :]
        mean_g = jnp.mean(scaled, axis=-1, keepdims=True)
        mean_gh = jnp.mean(scaled * hat, axis=-1, keepdims=True)
        grad = cot[at, :].astype(f32) + inv * (scaled - mean_g - hat * mean_gh)
        gmid[at, :] = grad
        own[at, :] = grad.astype(bf)

    reduce = Reduce(times(a, w, True), (po, pe, rc, sb, ring), sems, 0, peer, enter=enter)
    exchange_and_gather(reduce, both_gathers(own, out, sems, local, peer), 16, body)
    sums[0:1, :] = jnp.sum(acc[0], axis=0, keepdims=True)
    sums[1:2, :] = jnp.sum(acc[1], axis=0, keepdims=True)


def backward_exchange(a, w, mid, cot, vec, cid):
    _, r, _ = a.shape
    c = w.shape[0]
    count = EXCHANGE_SEMS
    return pl.pallas_call(
        backward_kernel,
        out_shape=(SDS((r, c), f32), SDS((TP, r, c), bf), SDS((2, c), f32)),
        in_specs=[VMEM] * 5,
        out_specs=(VMEM, ANY, VMEM),
        scratch_shapes=reduce_scratch(r, c)
        + [
            pltpu.VMEM((r, c), bf),
            pltpu.VMEM((2, 16, c), f32),
            pltpu.SemaphoreType.DMA((count,)),
            pltpu.SemaphoreType.DMA((count,)),
            pltpu.SemaphoreType.DMA((2,)),
        ],
        compiler_params=pltpu.CompilerParams(
            collective_id=cid, has_side_effects=True, vmem_limit_bytes=52 << 20
        ),
        name="backward_exchange",
    )(a, w, mid, cot, vec)


def last_kernel(
    n, gqkv, gs, wqk, wvs, a2, w2, tok, gmid, gain, sums2, gtok, ffn, vec_out,
    po, pe, rc, sb, ring, pe2, rc2, sb2, ring2, acc, vecs, near, far, part, ssem, rsem,
):
    dp = n // TP
    me, peer = place()
    g = lax.div(me, TP)
    width = vec_out.shape[1]
    others = [lax.rem(me + TP * j, n) for j in range(1, dp)]
    enter = greet([peer(k) for k in range(1, TP)] + others)
    sems = (ssem, rsem)
    acc[...] = jnp.zeros_like(acc)
    nt = (((1,), (1,)), ((), ()))

    def product(i, odd, even):
        r, qk, v = gqkv.shape[1], wqk.shape[1], gs.shape[2]
        x, y = rows_of_pair(gqkv, i), rows_of_pair(gs, i)

        @pl.loop(0, even.shape[1] // TILE)
        def _(j):
            at = pl.ds(pl.multiple_of(j * TILE, TILE), TILE)
            z = lax.dot_general(x[:, :qk], wqk[at, :], nt, preferred_element_type=f32)
            z += lax.dot_general(x[:, qk:], wvs[at, :v], nt, preferred_element_type=f32)
            z += lax.dot_general(y, wvs[at, v:], nt, preferred_element_type=f32)
            even[:, at] = z[:r].astype(even.dtype)
            odd[:, at] = z[r:].astype(odd.dtype)

    one = Reduce(product, (po, pe, rc, sb, ring), sems, 0, peer, enter=enter)
    one.run()
    for copy in one.core.values():
        copy.wait_send()
    one.sent = [copy for copy in one.sent if all(copy is not c for c in one.core.values())]
    two = Reduce(times(a2, w2, False), (po, pe2, rc2, sb2, ring2), sems, REDUCE_SEMS, peer)
    two.run()

    def body(at, grad):
        value = tok[at, :].astype(f32)
        center = jnp.mean(value, axis=-1, keepdims=True)
        centred = value - center
        inv = lax.rsqrt(jnp.mean(centred * centred, axis=-1, keepdims=True) + 1e-05)
        hat = centred * inv
        acc[0] += grad * hat
        acc[1] += grad
        scaled = grad * gain[...]
        mean_g = jnp.mean(scaled, axis=-1, keepdims=True)
        mean_gh = jnp.mean(scaled * hat, axis=-1, keepdims=True)
        gtok[at, :] = gmid[at, :] + inv * (scaled - mean_g - hat * mean_gh)

    for c in (0, 1):
        one.rows(c, 16, body)
    vecs[...] = jnp.zeros_like(vecs)
    vecs[0:1, :] = jnp.sum(acc[0], axis=0, keepdims=True)
    vecs[1:2, :] = jnp.sum(acc[1], axis=0, keepdims=True)
    vecs[2:4, :] = sums2[...]
    base = 2 * REDUCE_SEMS
    copies = []
    for j, dev in enumerate(others):
        at = pl.multiple_of(lax.div(dev, TP) * width, 128)
        copy = remote(vecs.at[:, pl.ds(at, width)], far.at[j], sems, base + j, dev)
        copy.start()
        copies.append(copy)

    def keep(at, value):
        ffn[at, :] = value

    two.rows(0, 16, keep)
    total = vecs[:, pl.ds(pl.multiple_of(g * width, 128), width)]
    for j, copy in enumerate(copies):
        copy.wait()
        total = total + far[j]
    part[...] = total
    copies = []
    for k in range(1, TP):
        copy = remote(part, near.at[k - 1], sems, base + dp + k - 1, peer(k))
        copy.start()
        copies.append(copy)
    two.rows(1, 16, keep)
    for k, copy in enumerate(copies):
        copy.wait()
        total = total + near[k]
    vec_out[...] = total
    one.finish()
    two.finish()


def last_exchange(n, gqkv, gs, wqk, wvs, a2, w2, tok, gmid, gain, sums2, cid):
    dp = n // TP
    _, r, _ = a2.shape
    c = w2.shape[1]
    width = c // dp
    count = 2 * REDUCE_SEMS + dp + TP
    return pl.pallas_call(
        functools.partial(last_kernel, n),
        out_shape=(SDS((r, c), f32), SDS((r, c), f32), SDS((8, width), f32)),
        in_specs=[VMEM] * 10,
        out_specs=(VMEM,) * 3,
        scratch_shapes=reduce_scratch(r, c)
        + reduce_scratch(r, c, bf)[1:]
        + [
            pltpu.VMEM((2, 16, c), f32),
            pltpu.VMEM((8, c), f32),
            pltpu.VMEM((TP - 1, 8, width), f32),
            pltpu.VMEM((dp, 8, width), f32),
            pltpu.VMEM((8, width), f32),
            pltpu.SemaphoreType.DMA((count,)),
            pltpu.SemaphoreType.DMA((count,)),
        ],
        compiler_params=pltpu.CompilerParams(
            collective_id=cid, has_side_effects=True, vmem_limit_bytes=ALL_VMEM
        ),
        name="last_exchange",
    )(gqkv, gs, wqk, wvs, a2, w2, tok, gmid, gain, sums2)


def gate_back_kernel(g_low, w, ret, swi, gret, gswi, whole):
    cols = w.shape[2]

    @pl.when(pl.program_id(0) == 0)
    def _():
        for j in range(w.shape[0]):
            whole[:, j * cols : (j + 1) * cols] = w[j]

    grad = lax.dot_general(
        g_low[0], whole[...], (((1,), (1,)), ((), ())), preferred_element_type=f32
    )
    value, gate = ret[0], swi[0]
    centred = value - jnp.mean(value, axis=-1, keepdims=True)
    spread = jnp.mean(centred * centred, axis=-1, keepdims=True)
    inv = lax.rsqrt(jnp.maximum(spread, 0.25))
    share = 1.0 / (1.0 + jnp.exp(-gate))
    silu = gate * share
    gswi[0] = (grad * (centred * inv) * (share * (1.0 + gate * (1.0 - share)))).astype(bf)
    grad = grad * silu
    pull = jnp.mean(grad * centred, axis=-1, keepdims=True)
    pull = jnp.where(spread > 0.25, inv * inv * inv * pull, 0.0)
    grad = grad * inv - centred * pull
    gret[0] = (grad - jnp.mean(grad, axis=-1, keepdims=True)).astype(bf)


def gate_back(g_low, w, ret, swi):
    _, r, d = g_low.shape
    width = ret.shape[2]
    row = pl.BlockSpec((1, r, width), lambda k: (k, 0, 0))
    return pl.pallas_call(
        gate_back_kernel,
        grid=(TP,),
        out_shape=(SDS(ret.shape, bf), SDS(ret.shape, bf)),
        in_specs=[
            pl.BlockSpec((1, r, d), lambda k: (k, 0, 0)),
            pl.BlockSpec(w.shape, lambda k: (0, 0, 0)),
            row,
            row,
        ],
        out_specs=(row, row),
        scratch_shapes=[pltpu.VMEM((width, d), bf)],
        compiler_params=pltpu.CompilerParams(vmem_limit_bytes=56 << 20),
        cost_estimate=pl.CostEstimate(
            flops=2 * TP * r * d * width, bytes_accessed=22 << 20, transcendentals=TP * r * width
        ),
        name="gate_back",
    )(g_low, w, ret, swi)


def scores_back_kernel(sco, mask, q, k, v, gret, cosine, sine, out):
    nt, tn = (((1,), (1,)), ((), ())), (((0,), (0,)), ((), ()))
    kh = q.shape[2]
    half = kh // 2
    out[0, :, 2 * kh :] = lax.dot_general(
        sco[0], gret[0], tn, preferred_element_type=f32
    ).astype(bf)
    grad = lax.dot_general(gret[0], v[0], nt, preferred_element_type=f32)
    grad = (grad * mask[0]).astype(bf)
    gq = jnp.dot(grad, k[0], preferred_element_type=f32)
    gk = lax.dot_general(grad, q[0], tn, preferred_element_type=f32)
    for i, g in enumerate((gq, gk)):
        u, w = g[:, :half], g[:, half:]
        at = i * kh
        out[0, :, at : at + half] = (u * cosine[0] + w * sine[0]).astype(bf)
        out[0, :, at + half : at + kh] = (w * cosine[0] - u * sine[0]).astype(bf)


def scores_back(sco, mask, q, k, v, gret, cosine, sine):
    _, r, kh = q.shape
    arrays = (sco, mask, q, k, v, gret, cosine, sine)
    width = 2 * kh + v.shape[2]
    spec = [pl.BlockSpec((1,) + x.shape[1:], lambda i: (i, 0, 0)) for x in arrays]
    return pl.pallas_call(
        scores_back_kernel,
        grid=(TP,),
        out_shape=SDS((TP, r, width), bf),
        in_specs=spec,
        out_specs=pl.BlockSpec((1, r, width), lambda i: (i, 0, 0)),
        compiler_params=pltpu.CompilerParams(vmem_limit_bytes=56 << 20),
        cost_estimate=pl.CostEstimate(
            flops=4 * TP * r * r * (kh + v.shape[2]), bytes_accessed=16 << 20, transcendentals=0
        ),
        name="scores_back",
    )(*arrays)


def tp_groups(n):
    return [[g * TP + t for t in range(TP)] for g in range(n // TP)]


def dp_groups(n):
    return [[g * TP + t for g in range(n // TP)] for t in range(TP)]


def plane_a2a(x, n):
    return lax.all_to_all(x, AXIS, 0, 0, axis_index_groups=tp_groups(n), tiled=True)


def dp_gather(x, n):
    return lax.all_gather(x, AXIS, axis=0, tiled=True, axis_index_groups=dp_groups(n))


def dp_reduce(x, n):
    return lax.psum_scatter(
        x, AXIS, scatter_dimension=0, tiled=True, axis_index_groups=dp_groups(n)
    )


def seq_positions(lengths, rows):
    ends = jnp.cumsum(lengths, axis=1)
    starts = ends - lengths
    index = jnp.arange(rows, dtype=jnp.int32)
    segment = jnp.sum((index[None, :, None] >= ends[:, None, :]).astype(jnp.int32), axis=2)
    member = segment[:, :, None] == jnp.arange(lengths.shape[1], dtype=jnp.int32)
    offset = index[None, :] - jnp.sum(jnp.where(member, starts[:, None, :], 0), axis=2)
    return segment, offset


def rotary_tables(offset):
    half = KH // 2
    freq = jnp.exp(-math.log(10000.0) * jnp.arange(half, dtype=f32) / half)
    angle = offset.astype(f32)[..., None] * freq
    return jnp.cos(angle), jnp.sin(angle)


def decay_mask(segment, offset, head):
    diff = offset[:, :, None] - offset[:, None, :]
    valid = (segment[:, :, None] == segment[:, None, :]) & (diff >= 0)
    steps = jnp.where(valid, diff, 0).astype(f32)
    log = jnp.log(1.0 - jnp.exp2(-5.0 - head.astype(f32)))
    return jnp.where(valid, jnp.exp(log * steps), 0.0) / math.sqrt(KH)


def col_blocks(w):
    r, c = w.shape
    return w.reshape(r, TP, c // TP).transpose(1, 0, 2).reshape(TP * r, c // TP)


def join_kernel(widths, parts, x, *outs):
    at = 0
    for out, width in zip(outs, widths):
        piece = width // parts
        for t in range(TP):
            for p in range(parts):
                to = (p * TP + t) * piece
                out[:, to : to + piece] = x[t, :, at + p * piece : at + (p + 1) * piece].astype(f32)
        at += width


def join(x, widths, parts=1):
    r = x.shape[1]
    if any(width // parts % 128 for width in widths):
        made, at = [], 0
        for width in widths:
            part = x[:, :, at : at + width].reshape(TP, r, parts, width // parts)
            made.append(part.transpose(1, 2, 0, 3).reshape(r, TP * width).astype(f32))
            at += width
        return made
    return pl.pallas_call(
        functools.partial(join_kernel, widths, parts),
        out_shape=tuple(SDS((r, TP * width), f32) for width in widths),
        in_specs=[VMEM],
        out_specs=tuple(VMEM for _ in widths),
        compiler_params=pltpu.CompilerParams(vmem_limit_bytes=8 << 20),
        cost_estimate=pl.CostEstimate(flops=0, bytes_accessed=6 * x.size, transcendentals=0),
        name="join",
    )(x)


def after(x, *deps):
    return lax.optimization_barrier((x,) + deps)[0]


def on_device(n, tokens, lengths, gain1, bias1, wq, wk, wv, ws, wo, gain2, bias2, wg, wu, wd, cot):
    rows, d = tokens.shape
    ff = wg.shape[1]
    dp = n // TP
    shard = d // n
    unit = ff // n
    me = lax.axis_index(AXIS)
    head = lax.rem(me, TP)

    def ff_blocks(w):
        return w.reshape(shard, dp, TP, unit).transpose(2, 0, 1, 3).reshape(TP, shard, dp * unit)

    lens = jnp.pad(lengths[0].astype(f32), (0, shard - lengths.shape[1]))
    vec = jnp.stack([v.astype(f32) for v in (gain1, bias1, gain2, bias2)] + [lens])
    vec = jnp.pad(vec, ((0, 3), (0, 128 - shard)))
    qko_blk = first_exchange(wq, wk, wo, 1)
    qko = dp_gather(qko_blk.reshape(TP * shard, 4 * KH), n)
    tok_all, vec_all = second_exchange(n, after(tokens, qko_blk), vec, 2)
    gain1f, bias1f, gain2f, bias2f = (
        vec_all[:, :, i, :shard].reshape(1, d) for i in range(4)
    )
    vec2 = jnp.concatenate([gain2f, bias2f], axis=0)
    gu_in = jnp.concatenate([ff_blocks(wg), ff_blocks(wu)], axis=2)
    vs_blk, gu_blk, normed = third_exchange(wv, ws, gu_in, tok_all, gain1f, bias1f, 3)
    vs = dp_gather(vs_blk.reshape(TP * shard, 2 * VH), n)
    gu = dp_gather(gu_blk.reshape(TP * shard, 2 * dp * unit), n)
    down = dp_gather(wd, n)

    mine = lax.dynamic_slice_in_dim(vec_all, lax.div(me, TP), 1, 0)[0, :, 4, :3]
    order = jnp.arange(TP, dtype=jnp.int32)
    pick = (order[None, :] == (order[:, None] ^ head)).astype(f32)
    len_all = jnp.sum(pick[:, :, None] * mine[None], axis=1).astype(jnp.int32)
    segment, offset = seq_positions(len_all, rows)
    cosine, sine = rotary_tables(offset)
    mask = decay_mask(segment, offset, head)

    cot_all, out_blk, q_rot, k_rot, scores, qk = fourth_exchange(
        n, cot, qko.reshape(n, shard, 4 * KH), normed, cosine, sine, mask, 4
    )
    out_blk = out_blk.reshape(TP, VH, d // TP)
    qk = qk.reshape(d, 2 * KH)
    v_low, mixed, retained, swish_in, middle, normed2 = forward_exchange(
        normed, vs, scores, out_blk, tokens, vec2, 5
    )
    hidden, act, slope = hidden_units(normed2, gu)
    down_grad = row_product(hidden, cot_all)
    g_down = dp_reduce(down_grad, n)

    g_fs = hidden_back(cot_all, down, act, slope)
    gu_grad = row_product(normed2, g_fs)
    g_gu = dp_reduce(gu_grad, n)
    g_middle, g_low, sums2 = backward_exchange(g_fs, gu, middle, cot, vec2, 6)

    g_retained, g_swish = gate_back(g_low, out_blk, retained, swish_in)
    swish_grad = row_product(normed, g_swish)
    g_swi = dp_reduce(swish_grad, n)
    out_grad = row_product(mixed, g_low)
    out_grad = plane_a2a(col_blocks(out_grad), n)
    g_qkv = scores_back(scores, mask, q_rot, k_rot, v_low, g_retained, cosine, sine)
    qkv_grad = row_product(normed, g_qkv)
    g_qkv_own = dp_reduce(qkv_grad, n)
    g_out = dp_reduce(out_grad, n)
    grad_tokens, ffn, g_vecs = last_exchange(
        n, g_qkv, g_swish, qk, vs, hidden, down, tokens, g_middle, gain1f, sums2, 7
    )
    layer_out = (middle + ffn).astype(bf)

    g_vecs = lax.dynamic_slice_in_dim(g_vecs, head * shard, shard, 1)
    grad_d = g_down.astype(f32)
    g_gu = plane_a2a(g_gu, n)
    grad_g, grad_u = join(g_gu.reshape(TP, shard, 2 * dp * unit), (dp * unit,) * 2, dp)
    g_swi = plane_a2a(g_swi, n)
    (grad_s,) = join(g_swi.reshape(TP, shard, VH), (VH,))
    g_qkv_own = plane_a2a(g_qkv_own, n)
    grad_q, grad_k, grad_v = join(g_qkv_own.reshape(TP, shard, 2 * KH + VH), (KH, KH, VH))
    g_out = plane_a2a(g_out, n)
    (grad_o,) = join(g_out.reshape(TP, wo.shape[0], d // TP), (d // TP,))
    return (
        layer_out, grad_tokens, g_vecs[0], g_vecs[1], grad_q, grad_k, grad_v, grad_s, grad_o,
        g_vecs[2], g_vecs[3], grad_g, grad_u, grad_d,
    )


def solution(mesh):
    n = mesh.shape[AXIS]
    row, vec = P(AXIS, None), P(AXIS)
    ins = (row, row, vec, vec, row, row, row, row, row, vec, vec, row, row, row, row)
    outs = (row, row, vec, vec, row, row, row, row, row, vec, vec, row, row, row)

    def body(*args):
        return on_device(n, *args)

    return jax.shard_map(body, mesh=mesh, in_specs=ins, out_specs=outs, check_vma=False)
```

```python
import functools
import math

import jax
import jax.numpy as jnp
from jax import lax
from jax.experimental import pallas as pl
from jax.experimental.pallas import tpu as pltpu
from jax.sharding import PartitionSpec as P


KH = 256
VH = 512
TP = 8
AXIS = "fsdp"
MESH = pl.DeviceIdType.MESH
ANY = pl.BlockSpec(memory_space=pl.ANY)
VMEM = pl.BlockSpec(memory_space=pltpu.VMEM)
bf = jnp.bfloat16
f32 = jnp.float32
SDS = jax.ShapeDtypeStruct
ALL_VMEM = 67043328


def place():
    me = lax.axis_index(AXIS)
    steps = [s - 2 * s * lax.rem(lax.div(me, s), 2) for s in (1, 2, 4)]

    def peer(k):
        out = me
        for bit, step in enumerate(steps):
            if k >> bit & 1:
                out = out + step
        return out

    return me, peer


def greet(peers):
    barrier = pltpu.get_barrier_semaphore()
    for p in peers:
        pl.semaphore_signal(barrier, inc=1, device_id=(p,), device_id_type=MESH)
    return lambda: pl.semaphore_wait(barrier, len(peers))


def meet(peers):
    greet(peers)()


def remote(src, dst, sems, i, dev):
    return pltpu.make_async_remote_copy(
        src_ref=src, dst_ref=dst, send_sem=sems[0].at[i], recv_sem=sems[1].at[i],
        device_id=(dev,), device_id_type=MESH,
    )


GATHER_SEMS = 13


class Gather:
    def __init__(self, own, out, start, size, sems, base, local, peer):
        self.own, self.out, self.sems, self.base, self.local = own, out, sems, base, local
        h = size // 2
        self.all, self.top, self.bot = pl.ds(start, size), pl.ds(start, h), pl.ds(start + h, h)
        self.pc, self.px, self.py = peer(1), peer(2), peer(4)
        self.made = []

    def send(self, src, dst, dev):
        copy = remote(src, dst, self.sems, self.base + len(self.made), dev)
        copy.start()
        self.made.append(copy)
        return copy

    def pass_on(self, k, at):
        self.core.append(self.send(self.out.at[k, at], self.out.at[k + 1, at], self.pc))

    def start(self):
        own, out, top, bot = self.own, self.out, self.top, self.bot
        self.x0 = self.send(own.at[bot], out.at[2, bot], self.px)
        self.y0 = self.send(own.at[top], out.at[4, top], self.py)
        self.x1 = self.send(own.at[top], out.at[2, top], self.px)
        self.y1 = self.send(own.at[bot], out.at[4, bot], self.py)
        self.core = [self.send(own.at[self.all], out.at[1, self.all], self.pc)]
        self.keep = pltpu.make_async_copy(own.at[self.all], out.at[0, self.all], self.local)
        self.keep.start()

    def forward(self):
        out, top, bot = self.out, self.top, self.bot
        self.x0.wait_recv()
        self.fy = self.send(out.at[2, bot], out.at[6, bot], self.py)
        self.pass_on(2, bot)
        self.y0.wait_recv()
        self.fx = self.send(out.at[4, top], out.at[6, top], self.px)
        self.pass_on(4, top)
        self.x1.wait_recv()
        self.pass_on(2, top)
        self.y1.wait_recv()
        self.pass_on(4, bot)

    def finish(self):
        self.fy.wait_recv()
        self.pass_on(6, self.bot)
        self.fx.wait_recv()
        self.pass_on(6, self.top)
        for copy in self.core:
            copy.wait_recv()
        for copy in self.made:
            copy.wait_send()
        self.keep.wait()


def send_columns(src, out, cols, at, sems, base, local, t, peer, rows=None):
    copies = []
    rows = slice(None) if rows is None else rows

    def block(q):
        if len(src.shape) == 3:
            return src.at[q]
        return src.at[rows, pl.ds(pl.multiple_of(q * cols, 128), cols)]

    for k in range(1, TP):
        dev = peer(k)
        copy = remote(
            block(lax.rem(dev, TP)), out.at[t, :, pl.ds(at, cols)], sems, base + k - 1, dev
        )
        copy.start()
        copies.append(copy)
    keep = pltpu.make_async_copy(block(t), out.at[t, :, pl.ds(at, cols)], local)
    keep.start()
    return copies, keep


def finish(parts):
    for copies, keep in parts:
        for copy in copies:
            copy.wait()
        keep.wait()


def exchange_call(
    kernel, outs, args, sems, locals_, cid, specs=None, out_specs=None, vmem=12 << 20
):
    return pl.pallas_call(
        kernel,
        out_shape=outs,
        in_specs=specs or [VMEM] * len(args),
        out_specs=out_specs or tuple(ANY for _ in outs),
        scratch_shapes=[
            pltpu.SemaphoreType.DMA((sems,)),
            pltpu.SemaphoreType.DMA((sems,)),
            pltpu.SemaphoreType.DMA((locals_,)),
        ],
        compiler_params=pltpu.CompilerParams(
            collective_id=cid, has_side_effects=True, vmem_limit_bytes=vmem
        ),
    )(*args)


def first_kernel(wq, wk, wo, out, ssem, rsem, local):
    me, peer = place()
    t = lax.rem(me, TP)
    meet([peer(k) for k in range(1, TP)])
    sems = (ssem, rsem)
    shard, cq, co = wq.shape[0], wq.shape[1] // TP, wo.shape[1] // TP
    low, high = pl.ds(0, shard), pl.ds(shard, shard)
    finish([
        send_columns(wq, out, cq, 0, sems, 0, local.at[0], t, peer),
        send_columns(wk, out, cq, cq, sems, 7, local.at[1], t, peer),
        send_columns(wo, out, co, 2 * cq, sems, 14, local.at[2], t, peer, low),
        send_columns(wo, out, co, 2 * cq + co, sems, 21, local.at[3], t, peer, high),
    ])


def first_exchange(wq, wk, wo, cid):
    width = 2 * wq.shape[1] // TP + 2 * wo.shape[1] // TP
    outs = (SDS((TP, wq.shape[0], width), bf),)
    return exchange_call(first_kernel, outs, (wq, wk, wo), 28, 4, cid)[0]


def others_along(n):
    me = lax.axis_index(AXIS)
    return [lax.rem(me + TP * j, n) for j in range(1, n // TP)]


def second_kernel(n, tok, vec, tok_out, vec_out, ssem, rsem, local):
    me, peer = place()
    t, g = lax.rem(me, TP), lax.div(me, TP)
    others = others_along(n)
    meet([peer(k) for k in range(1, TP)] + others)
    sems = (ssem, rsem)
    base = GATHER_SEMS
    far = []
    keep = pltpu.make_async_copy(vec, vec_out.at[g, t], local.at[1])
    keep.start()
    for j, dev in enumerate(others):
        copy = remote(vec, vec_out.at[g, t], sems, base + TP + j, dev)
        copy.start()
        far.append(copy)
    gather = Gather(tok, tok_out, 0, tok.shape[0], sems, 0, local.at[0], peer)
    gather.start()
    for copy in far:
        copy.wait()
    keep.wait()
    near = []
    for k in range(1, TP):
        copy = remote(vec_out.at[:, t], vec_out.at[:, t], sems, base + k, peer(k))
        copy.start()
        near.append(copy)
    gather.forward()
    gather.finish()
    for copy in near:
        copy.wait()


def second_exchange(n, tok, vec, cid):
    outs = (SDS((TP,) + tok.shape, bf), SDS((n // TP, TP) + vec.shape, f32))
    kernel = functools.partial(second_kernel, n)
    sems = GATHER_SEMS + TP + n // TP
    return exchange_call(kernel, outs, (tok, vec), sems, 2, cid)


def third_kernel(wv, ws, gu, tok, gain, bias, out, gu_out, nrm, ssem, rsem, local):
    me, peer = place()
    t = lax.rem(me, TP)
    meet([peer(k) for k in range(1, TP)])
    sems = (ssem, rsem)
    cols = wv.shape[1] // TP
    parts = [
        send_columns(wv, out, cols, 0, sems, 0, local.at[0], t, peer),
        send_columns(ws, out, cols, cols, sems, 7, local.at[1], t, peer),
        send_columns(gu, gu_out, gu.shape[2], 0, sems, 14, local.at[2], t, peer),
    ]
    step, r = 16, tok.shape[1]

    def norm(j, _):
        k = lax.div(j, r // step)
        at = pl.ds(pl.multiple_of(lax.rem(j, r // step) * step, step), step)
        value = tok[k, at, :].astype(f32)
        centred = value - jnp.mean(value, axis=-1, keepdims=True)
        spread = jnp.mean(centred * centred, axis=-1, keepdims=True)
        nrm[k, at, :] = (centred * lax.rsqrt(spread + 1e-05) * gain[...] + bias[...]).astype(bf)
        return 0

    lax.fori_loop(0, TP * r // step, norm, 0, unroll=4)
    finish(parts)


def third_exchange(wv, ws, gu, tok, gain, bias, cid):
    outs = (
        SDS((TP, wv.shape[0], 2 * wv.shape[1] // TP), bf),
        SDS(gu.shape, bf),
        SDS(tok.shape, bf),
    )
    return exchange_call(
        third_kernel, outs, (wv, ws, gu, tok, gain, bias), 21, 3, cid,
        out_specs=(ANY, ANY, VMEM), vmem=32 << 20,
    )


def fourth_kernel(
    n, cot, qko, nrm, cosine, sine, mask, cot_out, o_out, q_out, k_out, sco, w, ssem, rsem, local
):
    me, peer = place()
    t = lax.rem(me, TP)
    meet([peer(k) for k in range(1, TP)])
    sems = (ssem, rsem)
    share, cols = n // TP, o_out.shape[4]
    _, r, kh = q_out.shape
    half = kh // 2
    weights = pltpu.make_async_copy(qko.at[:, :, pl.ds(0, 2 * kh)], w, local.at[3])
    weights.start()
    gather = Gather(cot, cot_out, 0, cot.shape[0], sems, 0, local.at[0], peer)
    gather.start()
    copies, keeps = [], []

    def part(p, which):
        return qko.at[pl.ds(p * share, share), :, pl.ds(2 * kh + which * cols, cols)]

    for which in (0, 1):
        for k in range(1, TP):
            dev = peer(k)
            copy = remote(
                part(lax.rem(dev, TP), which), o_out.at[t, :, which], sems,
                GATHER_SEMS + which * TP + k, dev,
            )
            copy.start()
            copies.append(copy)
        keep = pltpu.make_async_copy(part(t, which), o_out.at[t, :, which], local.at[1 + which])
        keep.start()
        keeps.append(keep)
    weights.wait()

    def products(pairs):
        @pl.loop(*pairs)
        def _(j):
            rows = nrm[pl.ds(2 * j, 2)].reshape(2 * r, nrm.shape[2])
            for at, out in ((0, q_out), (kh, k_out)):
                y = jnp.dot(
                    rows, w[:, :, at : at + kh].reshape(nrm.shape[2], kh),
                    preferred_element_type=f32,
                )
                for i in (0, 1):
                    u, v = y[i * r : (i + 1) * r, :half], y[i * r : (i + 1) * r, half:]
                    cos, sin = cosine[2 * j + i], sine[2 * j + i]
                    out[2 * j + i, :, :half] = (u * cos - v * sin).astype(bf)
                    out[2 * j + i, :, half:] = (v * cos + u * sin).astype(bf)
            for i in (0, 1):
                plain = lax.dot_general(
                    q_out[2 * j + i], k_out[2 * j + i], (((1,), (1,)), ((), ())),
                    preferred_element_type=f32,
                )
                sco[2 * j + i] = (plain * mask[2 * j + i]).astype(bf)

    products((0, TP // 2))
    gather.forward()
    gather.finish()
    for copy in copies:
        copy.wait()
    for keep in keeps:
        keep.wait()


def fourth_exchange(n, cot, qko, nrm, cosine, sine, mask, cid):
    _, shard, width = qko.shape
    cols = (width - 2 * KH) // 2
    r = cot.shape[0]
    outs = (
        SDS((TP,) + cot.shape, bf),
        SDS((TP, n // TP, 2, shard, cols), bf),
        SDS((TP, r, KH), bf),
        SDS((TP, r, KH), bf),
        SDS(mask.shape, bf),
        SDS((n, shard, 2 * KH), bf),
    )
    kernel = functools.partial(fourth_kernel, n)
    return exchange_call(
        kernel, outs, (cot, qko, nrm, cosine, sine, mask),
        GATHER_SEMS + 2 * TP, 4, cid,
        specs=[VMEM, ANY, VMEM, VMEM, VMEM, VMEM],
        out_specs=(ANY, ANY, VMEM, VMEM, VMEM, VMEM), vmem=40 << 20,
    )


REDUCE_SEMS = 16
WIDE = 1024


class Reduce:
    def __init__(self, product, bufs, sems, base, peer, prepare=None, enter=None):
        self.product, self.prepare, self.sems, self.base = product, prepare, sems, base
        self.enter = enter
        self.po, self.pe, self.rc, self.sb, self.ring = bufs
        self.pc = peer(1)
        px, py = peer(2), peer(4)
        self.slots = ((0, 0, px), (1, 0, py), (0, 1, px), (1, 1, py), (1, 2, py), (0, 2, px))
        self.q = self.pe.shape[1] // 4
        self.waiting = True

    def core(self, i):
        return remote(self.po.at[i], self.rc.at[i], self.sems, self.base + i, self.pc)

    def link(self, c, slot):
        axis, at, dev = self.slots[slot]
        return remote(
            self.sb.at[c, slot], self.ring.at[axis, c, at], self.sems,
            self.base + 4 + 6 * c + slot, dev,
        )

    def add(self, halves, i, lower, out, more=None):
        step = 16
        steps = self.q // step
        first, count = halves

        @pl.loop(first * steps, (first + count) * steps)
        def _(j):
            c = lax.div(j, steps)
            there = pl.ds(pl.multiple_of(lax.rem(j, steps) * step, step), step)
            here = pl.ds(
                pl.multiple_of(lax.rem(j, steps) * step + (2 * c + lower) * self.q, step), step
            )
            total = self.pe[i, here, :].astype(f32) + self.rc[i, here, :].astype(f32)
            if more is not None:
                total = total + self.ring[more, c, 0, there, :].astype(f32)
            self.sb[c, out, there, :] = total.astype(bf)

    def both(self, slot, i, lower):
        self.add((0, 2), i, lower, slot)
        for c in (0, 1):
            self.link(c, slot).start()

    def six(self):
        self.core(3).wait_recv()
        self.both(0, 3, 0)
        self.both(1, 3, 1)

    def two(self):
        self.core(1).wait_recv()
        self.both(2, 1, 0)

    def four(self):
        self.core(2).wait_recv()
        self.both(3, 2, 1)

    def onward(self, c):
        self.link(c, 0).wait_recv()
        self.add((c, 1), 2, 0, 4, 0)
        self.link(c, 4).start()
        self.link(c, 1).wait_recv()
        self.add((c, 1), 1, 1, 5, 1)
        self.link(c, 5).start()

    def pair(self, it, i):
        self.product(it, i, self.po.at[i], self.pe.at[i])
        self.core(i).start()

    def run(self):
        if self.enter is not None:
            self.enter()

        @pl.loop(0, 4)
        def _(it):
            i = pair_at(it)
            if self.prepare is not None:
                self.prepare(it, i)
            else:
                self.pair(it, i)
            for k, stage in ((1, self.six), (2, self.two), (3, self.four)):
                pl.when(it == k)(stage)
            if self.prepare is not None:
                self.pair(it, i)

        for c in (0, 1):
            self.onward(c)

    def rows(self, c, step, body, unroll=2):
        if c == 0:
            self.core(0).wait_recv()
        for slot in (2, 3, 4, 5):
            self.link(c, slot).wait_recv()
        steps = self.q // step

        def some(j, _):
            lower = lax.div(j, steps)
            there = pl.ds(pl.multiple_of(lax.rem(j, steps) * step, step), step)
            here = pl.ds(pl.multiple_of(j * step + 2 * c * self.q, step), step)
            body(
                here,
                self.pe[0, here, :].astype(f32)
                + self.rc[0, here, :].astype(f32)
                + self.ring[lower, c, 1, there, :].astype(f32)
                + self.ring[1 - lower, c, 2, there, :].astype(f32),
            )
            return 0

        lax.fori_loop(0, 2 * steps, some, 0, unroll=unroll)

    def core_sent(self):
        for i in range(4):
            self.core(i).wait_send()
        self.waiting = False

    def finish(self):
        if self.waiting:
            self.core_sent()
        for c in (0, 1):
            for slot in range(6):
                self.link(c, slot).wait_send()


def pair_at(it):
    return it + 3 * (1 - lax.div(it + 2, 3)) - 3 * lax.div(it, 3)


class Load:
    def __init__(self, sems):
        self.sems, self.count = sems, 0

    def whole(self, src, dst):
        copy = pltpu.make_async_copy(src, dst, self.sems.at[self.count])
        self.count += 1
        copy.start()
        return copy.wait

    def paired(self, src, dst):
        base = self.count
        self.count += 4

        def piece(i):
            two = pl.ds(2 * i, 2)
            return pltpu.make_async_copy(src.at[two], dst.at[two], self.sems.at[base + i])

        return piece


def reduce_scratch(r, c, even=f32):
    q = r // 4
    return [
        pltpu.VMEM((4, r, c), bf),
        pltpu.VMEM((4, r, c), even),
        pltpu.VMEM((4, r, c), bf),
        pltpu.VMEM((2, 6, q, c), bf),
        pltpu.VMEM((2, 2, 3, q, c), bf),
    ]


def rows_of_pair(a, i):
    two, r, k = 2, a.shape[1], a.shape[2]
    return a[pl.ds(2 * i, two)].reshape(two * r, k)


def times(a, w, nt, arrive):
    def product(it, i, odd, even):
        r = a.shape[1]
        arrive(it, i)

        @pl.loop(0, even.shape[1] // WIDE)
        def _(j):
            at = pl.ds(pl.multiple_of(j * WIDE, WIDE), WIDE)
            x = rows_of_pair(a, i)
            if nt:
                y = lax.dot_general(
                    x, w[at, :], (((1,), (1,)), ((), ())), preferred_element_type=f32
                )
            else:
                y = jnp.dot(x, w[:, at], preferred_element_type=f32)
            even[:, at] = y[:r].astype(even.dtype)
            odd[:, at] = y[r:].astype(odd.dtype)

    return product


def exchange_and_gather(reduce, gathers, step, body, arrivals):
    reduce.run()
    for arrive in arrivals:
        arrive()
    for c in (0, 1):
        reduce.rows(c, step, body)
        gathers[c].start()
    for c in (0, 1):
        gathers[c].forward()
    for c in (0, 1):
        gathers[c].finish()
    reduce.finish()


def both_gathers(own, out, sems, local, peer):
    half = own.shape[0] // 2
    return [
        Gather(own, out, c * half, half, sems, REDUCE_SEMS + c * GATHER_SEMS, local.at[c], peer)
        for c in (0, 1)
    ]


EXCHANGE_SEMS = REDUCE_SEMS + 2 * GATHER_SEMS


def forward_kernel(
    nrm_in, wvs_in, sco, w_in, tok_in, vec, v_out, mix_out, ret_out, swi_out, mid, out,
    nrm, wvs, w, tok, v_buf, mix_buf, ret_buf, swi_buf, po, pe, rc, sb, ring, own,
    ssem, rsem, local, load,
):
    _, peer = place()
    enter = greet([peer(1), peer(2), peer(4)])
    sems = (ssem, rsem)
    r, width = v_buf.shape[1:]
    loads = Load(load)
    nrm_piece = loads.paired(nrm_in, nrm)
    nrm_piece(3).start()
    wvs_here = loads.whole(wvs_in, wvs)
    w_here = loads.whole(w_in, w)
    for i in (1, 2, 0):
        nrm_piece(i).start()
    tok_here = loads.whole(tok_in, tok)
    kept = ((v_buf, v_out), (mix_buf, mix_out), (ret_buf, ret_out), (swi_buf, swi_out))

    def keep(i):
        two = pl.ds(2 * i, 2)
        return [
            pltpu.make_async_copy(src.at[two], dst.at[two], local.at[2 + 4 * i + j])
            for j, (src, dst) in enumerate(kept)
        ]

    def prepare(it, i):
        first = 2 * i
        two = pl.ds(first, 2)
        pl.when(it == 0)(wvs_here)
        nrm_piece(i).wait()
        x = nrm[two].reshape(2 * r, nrm.shape[2])
        v = jnp.dot(x, wvs[:, :width], preferred_element_type=f32).astype(bf)
        v_buf[two] = v.reshape(2, r, width)
        for k in (0, 1):
            ret_buf[first + k] = jnp.dot(
                sco[first + k], v[k * r : (k + 1) * r], preferred_element_type=f32
            )
        s = jnp.dot(x, wvs[:, width:], preferred_element_type=f32)
        swi_buf[two] = s.reshape(2, r, width)

        def gated(j, _):
            k = first + lax.div(j, r // 32)
            at = pl.ds(pl.multiple_of(lax.rem(j, r // 32) * 32, 32), 32)
            value = ret_buf[k, at, :]
            centred = value - jnp.mean(value, axis=-1, keepdims=True)
            spread = jnp.mean(centred * centred, axis=-1, keepdims=True)
            gate = swi_buf[k, at, :]
            gate = gate / (1.0 + jnp.exp(-gate))
            mix_buf[k, at, :] = (
                gate * (centred * lax.rsqrt(jnp.maximum(spread, 0.25)))
            ).astype(bf)
            return 0

        lax.fori_loop(0, 2 * r // 32, gated, 0, unroll=4)
        for copy in keep(i):
            copy.start()

    def product(it, i, odd, even):
        step = w.shape[2]
        pl.when(it == 0)(w_here)

        def columns(j, _):
            at = pl.ds(pl.multiple_of(j * step, step), step)
            y = jnp.dot(rows_of_pair(mix_buf, i), w[j], preferred_element_type=f32)
            even[:, at] = y[:r].astype(even.dtype)
            odd[:, at] = y[r:].astype(odd.dtype)
            return 0

        lax.fori_loop(0, w.shape[0], columns, 0, unroll=4)

    def body(at, value):
        value = value + tok[at, :].astype(f32)
        mid[at, :] = value
        center = jnp.mean(value, axis=-1, keepdims=True)
        centred = value - center
        spread = jnp.mean(centred * centred, axis=-1, keepdims=True)
        own[at, :] = (
            centred * lax.rsqrt(spread + 1e-05) * vec[0:1, :] + vec[1:2, :]
        ).astype(bf)

    reduce = Reduce(product, (po, pe, rc, sb, ring), sems, 0, peer, prepare, enter)
    exchange_and_gather(reduce, both_gathers(own, out, sems, local, peer), 16, body, (tok_here,))
    for i in range(4):
        for copy in keep(i):
            copy.wait()


def forward_exchange(nrm, wvs, sco, w, tok, vec, cid):
    _, r, d = nrm.shape
    width = w.shape[1]
    count = EXCHANGE_SEMS
    blocks = [((TP, r, width), t) for t in (bf, bf, f32, f32)]
    return pl.pallas_call(
        forward_kernel,
        out_shape=tuple(SDS(*b) for b in blocks) + (SDS((r, d), f32), SDS((TP, r, d), bf)),
        in_specs=[ANY, ANY, VMEM, ANY, ANY, VMEM],
        out_specs=(ANY,) * 4 + (VMEM, ANY),
        scratch_shapes=[pltpu.VMEM(x.shape, x.dtype) for x in (nrm, wvs, w, tok)]
        + [pltpu.VMEM(*b) for b in blocks]
        + reduce_scratch(r, d)
        + [
            pltpu.VMEM((r, d), bf),
            pltpu.SemaphoreType.DMA((count,)),
            pltpu.SemaphoreType.DMA((count,)),
            pltpu.SemaphoreType.DMA((18,)),
            pltpu.SemaphoreType.DMA((7,)),
        ],
        compiler_params=pltpu.CompilerParams(
            collective_id=cid, has_side_effects=True, vmem_limit_bytes=60 << 20
        ),
        name="forward_exchange",
    )(nrm, wvs, sco, w, tok, vec)


def product_kernel(a, b, out):
    a, b = a[...].reshape(-1, a.shape[-1]), b[...].reshape(-1, b.shape[-1])
    out[...] = lax.dot_general(
        a, b, (((0,), (0,)), ((), ())), preferred_element_type=f32
    ).astype(bf)


def row_product(a, b):
    _, r, m = a.shape
    width = b.shape[2]
    tile, part = 512 if m >= 2048 else 256, min(width, 1024)
    return pl.pallas_call(
        product_kernel,
        grid=(width // part, m // tile),
        out_shape=SDS((m, width), bf),
        in_specs=[
            pl.BlockSpec((TP, r, tile), lambda j, i: (0, 0, i)),
            pl.BlockSpec((TP, r, part), lambda j, i: (0, 0, j)),
        ],
        out_specs=pl.BlockSpec((tile, part), lambda j, i: (i, j)),
        compiler_params=pltpu.CompilerParams(vmem_limit_bytes=56 << 20),
        cost_estimate=pl.CostEstimate(
            flops=2 * TP * r * m * width,
            bytes_accessed=2 * (a.size + b.size + m * width),
            transcendentals=0,
        ),
        name="row_product",
    )(a, b)


def hidden_kernel(x, gu, hid, act_out, slope_out):
    width = hid.shape[2]
    step = 256

    @pl.loop(0, width // step)
    def _(j):
        at = pl.ds(pl.multiple_of(j * step, step), step)
        behind = pl.ds(pl.multiple_of(j * step + width, step), step)
        rows = x[...].reshape(-1, x.shape[2])
        first = jnp.dot(rows, gu[:, at], preferred_element_type=f32)
        second = jnp.dot(rows, gu[:, behind], preferred_element_type=f32)
        share = 0.5 * (1.0 + lax.erf(first * math.sqrt(0.5)))
        act = first * share
        slope = share + first * (jnp.exp(-0.5 * first * first) * (1.0 / math.sqrt(2.0 * math.pi)))
        block = hid.shape[:2] + (step,)
        hid[:, :, at] = (act * second).astype(bf).reshape(block)
        act_out[:, :, at] = act.reshape(block)
        slope_out[:, :, at] = (slope * second).reshape(block)


def hidden_units(x, gu):
    _, r, d = x.shape
    width = gu.shape[1] // 2
    row = pl.BlockSpec((2, r, width), lambda k: (k, 0, 0))
    return pl.pallas_call(
        hidden_kernel,
        grid=(TP // 2,),
        out_shape=tuple(SDS((TP, r, width), t) for t in (bf, f32, f32)),
        in_specs=[
            pl.BlockSpec((2, r, d), lambda k: (k, 0, 0)),
            pl.BlockSpec(gu.shape, lambda k: (0, 0)),
        ],
        out_specs=(row, row, row),
        compiler_params=pltpu.CompilerParams(vmem_limit_bytes=56 << 20),
        cost_estimate=pl.CostEstimate(
            flops=4 * TP * r * d * width, bytes_accessed=24 << 20, transcendentals=2 * TP * r * width
        ),
        name="hidden_units",
    )(x, gu)


def hidden_back_kernel(cot, down, act, slope, out):
    width = act.shape[2]
    step = 256

    @pl.loop(0, width // step)
    def _(j):
        at = pl.ds(pl.multiple_of(j * step, step), step)
        behind = pl.ds(pl.multiple_of(j * step + width, step), step)
        grad = lax.dot_general(
            cot[...].reshape(-1, cot.shape[2]), down[at, :], (((1,), (1,)), ((), ())),
            preferred_element_type=f32,
        ).reshape(act.shape[:2] + (step,))
        out[:, :, at] = (grad * slope[:, :, at]).astype(bf)
        out[:, :, behind] = (grad * act[:, :, at]).astype(bf)


def hidden_back(cot, down, act, slope):
    _, r, d = cot.shape
    width = act.shape[2]
    row = pl.BlockSpec((2, r, width), lambda k: (k, 0, 0))
    return pl.pallas_call(
        hidden_back_kernel,
        grid=(TP // 2,),
        out_shape=SDS((TP, r, 2 * width), bf),
        in_specs=[
            pl.BlockSpec((2, r, d), lambda k: (k, 0, 0)),
            pl.BlockSpec(down.shape, lambda k: (0, 0)),
            row,
            row,
        ],
        out_specs=pl.BlockSpec((2, r, 2 * width), lambda k: (k, 0, 0)),
        compiler_params=pltpu.CompilerParams(vmem_limit_bytes=56 << 20),
        cost_estimate=pl.CostEstimate(
            flops=2 * TP * r * d * width, bytes_accessed=24 << 20, transcendentals=0
        ),
        name="hidden_back",
    )(cot, down, act, slope)


def backward_kernel(
    a_in, w_in, mid_in, cot_in, vec, gmid, out, sums,
    a, w, mid, cot, po, pe, rc, sb, ring, own, acc, ssem, rsem, local, load,
):
    _, peer = place()
    enter = greet([peer(1), peer(2), peer(4)])
    sems = (ssem, rsem)
    loads = Load(load)
    piece = loads.paired(a_in, a)
    piece(3).start()
    w_here = loads.whole(w_in, w)
    for i in (1, 2, 0):
        piece(i).start()
    arrivals = (loads.whole(mid_in, mid), loads.whole(cot_in, cot))

    def arrive(it, i):
        pl.when(it == 0)(w_here)
        piece(i).wait()

    acc[...] = jnp.zeros_like(acc)

    def body(at, g):
        value = mid[at, :]
        center = jnp.mean(value, axis=-1, keepdims=True)
        centred = value - center
        inv = lax.rsqrt(jnp.mean(centred * centred, axis=-1, keepdims=True) + 1e-05)
        hat = centred * inv
        acc[0] += g * hat
        acc[1] += g
        scaled = g * vec[0:1, :]
        mean_g = jnp.mean(scaled, axis=-1, keepdims=True)
        mean_gh = jnp.mean(scaled * hat, axis=-1, keepdims=True)
        grad = cot[at, :].astype(f32) + inv * (scaled - mean_g - hat * mean_gh)
        gmid[at, :] = grad
        own[at, :] = grad.astype(bf)

    reduce = Reduce(
        times(a, w, True, arrive), (po, pe, rc, sb, ring), sems, 0, peer, enter=enter
    )
    exchange_and_gather(reduce, both_gathers(own, out, sems, local, peer), 16, body, arrivals)
    sums[0:1, :] = jnp.sum(acc[0], axis=0, keepdims=True)
    sums[1:2, :] = jnp.sum(acc[1], axis=0, keepdims=True)


def backward_exchange(a, w, mid, cot, vec, cid):
    _, r, _ = a.shape
    c = w.shape[0]
    count = EXCHANGE_SEMS
    return pl.pallas_call(
        backward_kernel,
        out_shape=(SDS((r, c), f32), SDS((TP, r, c), bf), SDS((2, c), f32)),
        in_specs=[ANY] * 4 + [VMEM],
        out_specs=(VMEM, ANY, VMEM),
        scratch_shapes=[pltpu.VMEM(x.shape, x.dtype) for x in (a, w, mid, cot)]
        + reduce_scratch(r, c)
        + [
            pltpu.VMEM((r, c), bf),
            pltpu.VMEM((2, 16, c), f32),
            pltpu.SemaphoreType.DMA((count,)),
            pltpu.SemaphoreType.DMA((count,)),
            pltpu.SemaphoreType.DMA((2,)),
            pltpu.SemaphoreType.DMA((7,)),
        ],
        compiler_params=pltpu.CompilerParams(
            collective_id=cid, has_side_effects=True, vmem_limit_bytes=52 << 20
        ),
        name="backward_exchange",
    )(a, w, mid, cot, vec)


def last_kernel(
    n, gqkv_in, gs_in, wqk_in, wvs_in, a2_in, w2_in, tok_in, gmid_in, gain, sums2,
    gtok, ffn, vec_out, gqkv, gs, wqk, wvs, a2, w2, tok, gmid,
    po, pe, rc, sb, ring, pe2, rc2, sb2, ring2, acc, vecs, near, far, part, ssem, rsem, load,
):
    dp = n // TP
    me, peer = place()
    g = lax.div(me, TP)
    width = vec_out.shape[1]
    others = [lax.rem(me + TP * j, n) for j in range(1, dp)]
    enter = greet([peer(k) for k in range(1, TP)] + others)
    sems = (ssem, rsem)
    loads = Load(load)
    pieces = loads.paired(gqkv_in, gqkv), loads.paired(gs_in, gs)
    for piece in pieces:
        piece(3).start()
    weights = loads.whole(wqk_in, wqk), loads.whole(wvs_in, wvs)
    for i in (1, 2, 0):
        for piece in pieces:
            piece(i).start()
    second = loads.whole(a2_in, a2), loads.whole(w2_in, w2)
    arrivals = loads.whole(tok_in, tok), loads.whole(gmid_in, gmid)

    def all_here(waits):
        def wait():
            for one in waits:
                one()

        return wait

    acc[...] = jnp.zeros_like(acc)
    nt = (((1,), (1,)), ((), ()))

    def product(it, i, odd, even):
        r, qk, v = gqkv.shape[1], wqk.shape[1], gs.shape[2]
        pl.when(it == 0)(all_here(weights))
        for piece in pieces:
            piece(i).wait()
        x, y = rows_of_pair(gqkv, i), rows_of_pair(gs, i)

        @pl.loop(0, even.shape[1] // WIDE)
        def _(j):
            at = pl.ds(pl.multiple_of(j * WIDE, WIDE), WIDE)
            z = lax.dot_general(x[:, :qk], wqk[at, :], nt, preferred_element_type=f32)
            z += lax.dot_general(x[:, qk:], wvs[at, :v], nt, preferred_element_type=f32)
            z += lax.dot_general(y, wvs[at, v:], nt, preferred_element_type=f32)
            even[:, at] = z[:r].astype(even.dtype)
            odd[:, at] = z[r:].astype(odd.dtype)

    one = Reduce(product, (po, pe, rc, sb, ring), sems, 0, peer, enter=enter)
    one.run()
    one.core_sent()

    def arrive(it, _):
        pl.when(it == 0)(all_here(second))

    two = Reduce(times(a2, w2, False, arrive), (po, pe2, rc2, sb2, ring2), sems, REDUCE_SEMS, peer)
    two.run()

    def body(at, grad):
        value = tok[at, :].astype(f32)
        center = jnp.mean(value, axis=-1, keepdims=True)
        centred = value - center
        inv = lax.rsqrt(jnp.mean(centred * centred, axis=-1, keepdims=True) + 1e-05)
        hat = centred * inv
        acc[0] += grad * hat
        acc[1] += grad
        scaled = grad * gain[...]
        mean_g = jnp.mean(scaled, axis=-1, keepdims=True)
        mean_gh = jnp.mean(scaled * hat, axis=-1, keepdims=True)
        gtok[at, :] = gmid[at, :] + inv * (scaled - mean_g - hat * mean_gh)

    all_here(arrivals)()
    for c in (0, 1):
        one.rows(c, 16, body)
    vecs[...] = jnp.zeros_like(vecs)
    vecs[0:1, :] = jnp.sum(acc[0], axis=0, keepdims=True)
    vecs[1:2, :] = jnp.sum(acc[1], axis=0, keepdims=True)
    vecs[2:4, :] = sums2[...]
    base = 2 * REDUCE_SEMS
    copies = []
    for j, dev in enumerate(others):
        at = pl.multiple_of(lax.div(dev, TP) * width, 128)
        copy = remote(vecs.at[:, pl.ds(at, width)], far.at[j], sems, base + j, dev)
        copy.start()
        copies.append(copy)

    def keep(at, value):
        ffn[at, :] = value

    two.rows(0, 16, keep)
    total = vecs[:, pl.ds(pl.multiple_of(g * width, 128), width)]
    for j, copy in enumerate(copies):
        copy.wait()
        total = total + far[j]
    part[...] = total
    copies = []
    for k in range(1, TP):
        copy = remote(part, near.at[k - 1], sems, base + dp + k - 1, peer(k))
        copy.start()
        copies.append(copy)
    two.rows(1, 16, keep)
    for k, copy in enumerate(copies):
        copy.wait()
        total = total + near[k]
    vec_out[...] = total
    one.finish()
    two.finish()


def last_exchange(n, gqkv, gs, wqk, wvs, a2, w2, tok, gmid, gain, sums2, cid):
    dp = n // TP
    _, r, _ = a2.shape
    c = w2.shape[1]
    width = c // dp
    count = 2 * REDUCE_SEMS + dp + TP
    return pl.pallas_call(
        functools.partial(last_kernel, n),
        out_shape=(SDS((r, c), f32), SDS((r, c), f32), SDS((8, width), f32)),
        in_specs=[ANY] * 8 + [VMEM] * 2,
        out_specs=(VMEM,) * 3,
        scratch_shapes=[
            pltpu.VMEM(x.shape, x.dtype) for x in (gqkv, gs, wqk, wvs, a2, w2, tok, gmid)
        ]
        + reduce_scratch(r, c)
        + reduce_scratch(r, c, bf)[1:]
        + [
            pltpu.VMEM((2, 16, c), f32),
            pltpu.VMEM((8, c), f32),
            pltpu.VMEM((TP - 1, 8, width), f32),
            pltpu.VMEM((dp, 8, width), f32),
            pltpu.VMEM((8, width), f32),
            pltpu.SemaphoreType.DMA((count,)),
            pltpu.SemaphoreType.DMA((count,)),
            pltpu.SemaphoreType.DMA((14,)),
        ],
        compiler_params=pltpu.CompilerParams(
            collective_id=cid, has_side_effects=True, vmem_limit_bytes=ALL_VMEM
        ),
        name="last_exchange",
    )(gqkv, gs, wqk, wvs, a2, w2, tok, gmid, gain, sums2)


def gate_back_kernel(g_low, w, ret, swi, gret, gswi, whole):
    cols = w.shape[2]

    @pl.when(pl.program_id(0) == 0)
    def _():
        for j in range(w.shape[0]):
            whole[:, j * cols : (j + 1) * cols] = w[j]

    grad = lax.dot_general(
        g_low[0], whole[...], (((1,), (1,)), ((), ())), preferred_element_type=f32
    )
    value, gate = ret[0], swi[0]
    centred = value - jnp.mean(value, axis=-1, keepdims=True)
    spread = jnp.mean(centred * centred, axis=-1, keepdims=True)
    inv = lax.rsqrt(jnp.maximum(spread, 0.25))
    share = 1.0 / (1.0 + jnp.exp(-gate))
    silu = gate * share
    gswi[0] = (grad * (centred * inv) * (share * (1.0 + gate * (1.0 - share)))).astype(bf)
    grad = grad * silu
    pull = jnp.mean(grad * centred, axis=-1, keepdims=True)
    pull = jnp.where(spread > 0.25, inv * inv * inv * pull, 0.0)
    grad = grad * inv - centred * pull
    gret[0] = (grad - jnp.mean(grad, axis=-1, keepdims=True)).astype(bf)


def gate_back(g_low, w, ret, swi):
    _, r, d = g_low.shape
    width = ret.shape[2]
    row = pl.BlockSpec((1, r, width), lambda k: (k, 0, 0))
    return pl.pallas_call(
        gate_back_kernel,
        grid=(TP,),
        out_shape=(SDS(ret.shape, bf), SDS(ret.shape, bf)),
        in_specs=[
            pl.BlockSpec((1, r, d), lambda k: (k, 0, 0)),
            pl.BlockSpec(w.shape, lambda k: (0, 0, 0)),
            row,
            row,
        ],
        out_specs=(row, row),
        scratch_shapes=[pltpu.VMEM((width, d), bf)],
        compiler_params=pltpu.CompilerParams(vmem_limit_bytes=56 << 20),
        cost_estimate=pl.CostEstimate(
            flops=2 * TP * r * d * width, bytes_accessed=22 << 20, transcendentals=TP * r * width
        ),
        name="gate_back",
    )(g_low, w, ret, swi)


def scores_back_kernel(sco, mask, q, k, v, gret, cosine, sine, out):
    nt, tn = (((1,), (1,)), ((), ())), (((0,), (0,)), ((), ()))
    kh = q.shape[2]
    half = kh // 2
    out[0, :, 2 * kh :] = lax.dot_general(
        sco[0], gret[0], tn, preferred_element_type=f32
    ).astype(bf)
    grad = lax.dot_general(gret[0], v[0], nt, preferred_element_type=f32)
    grad = (grad * mask[0]).astype(bf)
    gq = jnp.dot(grad, k[0], preferred_element_type=f32)
    gk = lax.dot_general(grad, q[0], tn, preferred_element_type=f32)
    for i, g in enumerate((gq, gk)):
        u, w = g[:, :half], g[:, half:]
        at = i * kh
        out[0, :, at : at + half] = (u * cosine[0] + w * sine[0]).astype(bf)
        out[0, :, at + half : at + kh] = (w * cosine[0] - u * sine[0]).astype(bf)


def scores_back(sco, mask, q, k, v, gret, cosine, sine):
    _, r, kh = q.shape
    arrays = (sco, mask, q, k, v, gret, cosine, sine)
    width = 2 * kh + v.shape[2]
    spec = [pl.BlockSpec((1,) + x.shape[1:], lambda i: (i, 0, 0)) for x in arrays]
    return pl.pallas_call(
        scores_back_kernel,
        grid=(TP,),
        out_shape=SDS((TP, r, width), bf),
        in_specs=spec,
        out_specs=pl.BlockSpec((1, r, width), lambda i: (i, 0, 0)),
        compiler_params=pltpu.CompilerParams(vmem_limit_bytes=56 << 20),
        cost_estimate=pl.CostEstimate(
            flops=4 * TP * r * r * (kh + v.shape[2]), bytes_accessed=16 << 20, transcendentals=0
        ),
        name="scores_back",
    )(*arrays)


def tp_groups(n):
    return [[g * TP + t for t in range(TP)] for g in range(n // TP)]


def dp_groups(n):
    return [[g * TP + t for g in range(n // TP)] for t in range(TP)]


def plane_a2a(x, n):
    return lax.all_to_all(x, AXIS, 0, 0, axis_index_groups=tp_groups(n), tiled=True)


def dp_gather(x, n):
    return lax.all_gather(x, AXIS, axis=0, tiled=True, axis_index_groups=dp_groups(n))


def dp_reduce(x, n):
    return lax.psum_scatter(
        x, AXIS, scatter_dimension=0, tiled=True, axis_index_groups=dp_groups(n)
    )


def seq_positions(lengths, rows):
    ends = jnp.cumsum(lengths, axis=1)
    starts = ends - lengths
    index = jnp.arange(rows, dtype=jnp.int32)
    segment = jnp.sum((index[None, :, None] >= ends[:, None, :]).astype(jnp.int32), axis=2)
    member = segment[:, :, None] == jnp.arange(lengths.shape[1], dtype=jnp.int32)
    offset = index[None, :] - jnp.sum(jnp.where(member, starts[:, None, :], 0), axis=2)
    return segment, offset


def rotary_tables(offset):
    half = KH // 2
    freq = jnp.exp(-math.log(10000.0) * jnp.arange(half, dtype=f32) / half)
    angle = offset.astype(f32)[..., None] * freq
    return jnp.cos(angle), jnp.sin(angle)


def decay_mask(segment, offset, head):
    diff = offset[:, :, None] - offset[:, None, :]
    valid = (segment[:, :, None] == segment[:, None, :]) & (diff >= 0)
    steps = jnp.where(valid, diff, 0).astype(f32)
    log = jnp.log(1.0 - jnp.exp2(-5.0 - head.astype(f32)))
    return jnp.where(valid, jnp.exp(log * steps), 0.0) / math.sqrt(KH)


def col_blocks(w):
    r, c = w.shape
    return w.reshape(r, TP, c // TP).transpose(1, 0, 2).reshape(TP * r, c // TP)


def join_kernel(widths, parts, x, *outs):
    at = 0
    for out, width in zip(outs, widths):
        piece = width // parts
        for t in range(TP):
            for p in range(parts):
                to = (p * TP + t) * piece
                out[:, to : to + piece] = x[t, :, at + p * piece : at + (p + 1) * piece].astype(f32)
        at += width


def join(x, widths, parts=1):
    r = x.shape[1]
    if any(width // parts % 128 for width in widths):
        made, at = [], 0
        for width in widths:
            part = x[:, :, at : at + width].reshape(TP, r, parts, width // parts)
            made.append(part.transpose(1, 2, 0, 3).reshape(r, TP * width).astype(f32))
            at += width
        return made
    return pl.pallas_call(
        functools.partial(join_kernel, widths, parts),
        out_shape=tuple(SDS((r, TP * width), f32) for width in widths),
        in_specs=[VMEM],
        out_specs=tuple(VMEM for _ in widths),
        compiler_params=pltpu.CompilerParams(vmem_limit_bytes=8 << 20),
        cost_estimate=pl.CostEstimate(flops=0, bytes_accessed=6 * x.size, transcendentals=0),
        name="join",
    )(x)


def after(x, *deps):
    return lax.optimization_barrier((x,) + deps)[0]


def on_device(n, tokens, lengths, gain1, bias1, wq, wk, wv, ws, wo, gain2, bias2, wg, wu, wd, cot):
    rows, d = tokens.shape
    ff = wg.shape[1]
    dp = n // TP
    shard = d // n
    unit = ff // n
    me = lax.axis_index(AXIS)
    head = lax.rem(me, TP)

    def ff_blocks(w):
        return w.reshape(shard, dp, TP, unit).transpose(2, 0, 1, 3).reshape(TP, shard, dp * unit)

    lens = jnp.pad(lengths[0].astype(f32), (0, shard - lengths.shape[1]))
    vec = jnp.stack([v.astype(f32) for v in (gain1, bias1, gain2, bias2)] + [lens])
    vec = jnp.pad(vec, ((0, 3), (0, 128 - shard)))
    qko_blk = first_exchange(wq, wk, wo, 1)
    qko = dp_gather(qko_blk.reshape(TP * shard, 4 * KH), n)
    tok_all, vec_all = second_exchange(n, after(tokens, qko_blk), vec, 2)
    gain1f, bias1f, gain2f, bias2f = (
        vec_all[:, :, i, :shard].reshape(1, d) for i in range(4)
    )
    vec2 = jnp.concatenate([gain2f, bias2f], axis=0)
    gu_in = jnp.concatenate([ff_blocks(wg), ff_blocks(wu)], axis=2)
    vs_blk, gu_blk, normed = third_exchange(wv, ws, gu_in, tok_all, gain1f, bias1f, 3)
    vs = dp_gather(vs_blk.reshape(TP * shard, 2 * VH), n)
    gu = dp_gather(gu_blk.reshape(TP * shard, 2 * dp * unit), n)
    down = dp_gather(wd, n)

    mine = lax.dynamic_slice_in_dim(vec_all, lax.div(me, TP), 1, 0)[0, :, 4, :3]
    order = jnp.arange(TP, dtype=jnp.int32)
    pick = (order[None, :] == (order[:, None] ^ head)).astype(f32)
    len_all = jnp.sum(pick[:, :, None] * mine[None], axis=1).astype(jnp.int32)
    segment, offset = seq_positions(len_all, rows)
    cosine, sine = rotary_tables(offset)
    mask = decay_mask(segment, offset, head)

    cot_all, out_blk, q_rot, k_rot, scores, qk = fourth_exchange(
        n, cot, qko.reshape(n, shard, 4 * KH), normed, cosine, sine, mask, 4
    )
    out_blk = out_blk.reshape(TP, VH, d // TP)
    qk = qk.reshape(d, 2 * KH)
    v_low, mixed, retained, swish_in, middle, normed2 = forward_exchange(
        normed, vs, scores, out_blk, tokens, vec2, 5
    )
    hidden, act, slope = hidden_units(normed2, gu)
    down_grad = row_product(hidden, cot_all)
    g_down = dp_reduce(down_grad, n)

    g_fs = hidden_back(cot_all, down, act, slope)
    gu_grad = row_product(normed2, g_fs)
    g_gu = dp_reduce(gu_grad, n)
    g_middle, g_low, sums2 = backward_exchange(g_fs, gu, middle, cot, vec2, 6)

    g_retained, g_swish = gate_back(g_low, out_blk, retained, swish_in)
    swish_grad = row_product(normed, g_swish)
    g_swi = dp_reduce(swish_grad, n)
    out_grad = row_product(mixed, g_low)
    out_grad = plane_a2a(col_blocks(out_grad), n)
    g_qkv = scores_back(scores, mask, q_rot, k_rot, v_low, g_retained, cosine, sine)
    qkv_grad = row_product(normed, g_qkv)
    g_qkv_own = dp_reduce(qkv_grad, n)
    g_out = dp_reduce(out_grad, n)
    grad_tokens, ffn, g_vecs = last_exchange(
        n, g_qkv, g_swish, qk, vs, hidden, down, tokens, g_middle, gain1f, sums2, 7
    )
    layer_out = (middle + ffn).astype(bf)

    g_vecs = lax.dynamic_slice_in_dim(g_vecs, head * shard, shard, 1)
    grad_d = g_down.astype(f32)
    g_gu = plane_a2a(g_gu, n)
    grad_g, grad_u = join(g_gu.reshape(TP, shard, 2 * dp * unit), (dp * unit,) * 2, dp)
    g_swi = plane_a2a(g_swi, n)
    (grad_s,) = join(g_swi.reshape(TP, shard, VH), (VH,))
    g_qkv_own = plane_a2a(g_qkv_own, n)
    grad_q, grad_k, grad_v = join(g_qkv_own.reshape(TP, shard, 2 * KH + VH), (KH, KH, VH))
    g_out = plane_a2a(g_out, n)
    (grad_o,) = join(g_out.reshape(TP, wo.shape[0], d // TP), (d // TP,))
    return (
        layer_out, grad_tokens, g_vecs[0], g_vecs[1], grad_q, grad_k, grad_v, grad_s, grad_o,
        g_vecs[2], g_vecs[3], grad_g, grad_u, grad_d,
    )


def solution(mesh):
    n = mesh.shape[AXIS]
    row, vec = P(AXIS, None), P(AXIS)
    ins = (row, row, vec, vec, row, row, row, row, row, vec, vec, row, row, row, row)
    outs = (row, row, vec, vec, row, row, row, row, row, vec, vec, row, row, row)

    def body(*args):
        return on_device(n, *args)

    return jax.shard_map(body, mesh=mesh, in_specs=ins, out_specs=outs, check_vma=False)
```

```python
import functools
import math

import jax
import jax.numpy as jnp
from jax import lax
from jax.experimental import pallas as pl
from jax.experimental.pallas import tpu as pltpu
from jax.sharding import PartitionSpec as P


HEADS = 8
KH = 256
VH = 512
TP = 8
AXIS = "fsdp"
MESH = pl.DeviceIdType.MESH
ANY = pl.BlockSpec(memory_space=pl.ANY)
VMEM = pl.BlockSpec(memory_space=pltpu.VMEM)
bf = jnp.bfloat16
f32 = jnp.float32
SDS = jax.ShapeDtypeStruct
ALL_VMEM = 67043328


def place():
    me = lax.axis_index(AXIS)
    steps = [s - 2 * s * lax.rem(lax.div(me, s), 2) for s in (1, 2, 4)]

    def peer(k):
        out = me
        for bit, step in enumerate(steps):
            if k >> bit & 1:
                out = out + step
        return out

    return me, peer


def greet(peers):
    barrier = pltpu.get_barrier_semaphore()
    for p in peers:
        pl.semaphore_signal(barrier, inc=1, device_id=(p,), device_id_type=MESH)
    return lambda: pl.semaphore_wait(barrier, len(peers))


def meet(peers):
    greet(peers)()


def remote(src, dst, sems, i, dev):
    return pltpu.make_async_remote_copy(
        src_ref=src, dst_ref=dst, send_sem=sems[0].at[i], recv_sem=sems[1].at[i],
        device_id=(dev,), device_id_type=MESH,
    )


GATHER_SEMS = 13


class Gather:
    def __init__(self, own, out, start, size, sems, base, local, peer):
        self.own, self.out, self.sems, self.base, self.local = own, out, sems, base, local
        h = size // 2
        self.all, self.top, self.bot = pl.ds(start, size), pl.ds(start, h), pl.ds(start + h, h)
        self.pc, self.px, self.py = peer(1), peer(2), peer(4)
        self.made = []

    def send(self, src, dst, dev):
        copy = remote(src, dst, self.sems, self.base + len(self.made), dev)
        copy.start()
        self.made.append(copy)
        return copy

    def pass_on(self, k, at):
        self.core.append(self.send(self.out.at[k, at], self.out.at[k + 1, at], self.pc))

    def start(self):
        own, out, top, bot = self.own, self.out, self.top, self.bot
        self.x0 = self.send(own.at[bot], out.at[2, bot], self.px)
        self.y0 = self.send(own.at[top], out.at[4, top], self.py)
        self.x1 = self.send(own.at[top], out.at[2, top], self.px)
        self.y1 = self.send(own.at[bot], out.at[4, bot], self.py)
        self.core = [self.send(own.at[self.all], out.at[1, self.all], self.pc)]
        self.keep = pltpu.make_async_copy(own.at[self.all], out.at[0, self.all], self.local)
        self.keep.start()

    def forward(self):
        out, top, bot = self.out, self.top, self.bot
        self.x0.wait_recv()
        self.fy = self.send(out.at[2, bot], out.at[6, bot], self.py)
        self.pass_on(2, bot)
        self.y0.wait_recv()
        self.fx = self.send(out.at[4, top], out.at[6, top], self.px)
        self.pass_on(4, top)
        self.x1.wait_recv()
        self.pass_on(2, top)
        self.y1.wait_recv()
        self.pass_on(4, bot)

    def finish(self):
        self.fy.wait_recv()
        self.pass_on(6, self.bot)
        self.fx.wait_recv()
        self.pass_on(6, self.top)
        for copy in self.core:
            copy.wait_recv()
        for copy in self.made:
            copy.wait_send()
        self.keep.wait()


def send_columns(src, out, cols, at, sems, base, local, t, peer, rows=None):
    copies = []
    rows = slice(None) if rows is None else rows

    def block(q):
        if len(src.shape) == 3:
            return src.at[q]
        return src.at[rows, pl.ds(pl.multiple_of(q * cols, 128), cols)]

    for k in range(1, TP):
        dev = peer(k)
        copy = remote(
            block(lax.rem(dev, TP)), out.at[t, :, pl.ds(at, cols)], sems, base + k - 1, dev
        )
        copy.start()
        copies.append(copy)
    keep = pltpu.make_async_copy(block(t), out.at[t, :, pl.ds(at, cols)], local)
    keep.start()
    return copies, keep


def finish(parts):
    for copies, keep in parts:
        for copy in copies:
            copy.wait()
        keep.wait()


def exchange_call(
    kernel, outs, args, sems, locals_, cid, specs=None, out_specs=None, vmem=12 << 20
):
    return pl.pallas_call(
        kernel,
        out_shape=outs,
        in_specs=specs or [VMEM] * len(args),
        out_specs=out_specs or tuple(ANY for _ in outs),
        scratch_shapes=[
            pltpu.SemaphoreType.DMA((sems,)),
            pltpu.SemaphoreType.DMA((sems,)),
            pltpu.SemaphoreType.DMA((locals_,)),
        ],
        compiler_params=pltpu.CompilerParams(
            collective_id=cid, has_side_effects=True, vmem_limit_bytes=vmem
        ),
    )(*args)


def first_kernel(wq, wk, wo, out, ssem, rsem, local):
    me, peer = place()
    t = lax.rem(me, TP)
    meet([peer(k) for k in range(1, TP)])
    sems = (ssem, rsem)
    shard, cq, co = wq.shape[0], wq.shape[1] // TP, wo.shape[1] // TP
    low, high = pl.ds(0, shard), pl.ds(shard, shard)
    finish([
        send_columns(wq, out, cq, 0, sems, 0, local.at[0], t, peer),
        send_columns(wk, out, cq, cq, sems, 7, local.at[1], t, peer),
        send_columns(wo, out, co, 2 * cq, sems, 14, local.at[2], t, peer, low),
        send_columns(wo, out, co, 2 * cq + co, sems, 21, local.at[3], t, peer, high),
    ])


def first_exchange(wq, wk, wo, cid):
    width = 2 * wq.shape[1] // TP + 2 * wo.shape[1] // TP
    outs = (SDS((TP, wq.shape[0], width), bf),)
    return exchange_call(first_kernel, outs, (wq, wk, wo), 28, 4, cid)[0]


def others_along(n):
    me = lax.axis_index(AXIS)
    return [lax.rem(me + TP * j, n) for j in range(1, n // TP)]


def second_kernel(n, tok, vec, tok_out, vec_out, ssem, rsem, local):
    me, peer = place()
    t, g = lax.rem(me, TP), lax.div(me, TP)
    others = others_along(n)
    meet([peer(k) for k in range(1, TP)] + others)
    sems = (ssem, rsem)
    base = GATHER_SEMS
    far = []
    keep = pltpu.make_async_copy(vec, vec_out.at[g, t], local.at[1])
    keep.start()
    for j, dev in enumerate(others):
        copy = remote(vec, vec_out.at[g, t], sems, base + TP + j, dev)
        copy.start()
        far.append(copy)
    gather = Gather(tok, tok_out, 0, tok.shape[0], sems, 0, local.at[0], peer)
    gather.start()
    for copy in far:
        copy.wait()
    keep.wait()
    near = []
    for k in range(1, TP):
        copy = remote(vec_out.at[:, t], vec_out.at[:, t], sems, base + k, peer(k))
        copy.start()
        near.append(copy)
    gather.forward()
    gather.finish()
    for copy in near:
        copy.wait()


def second_exchange(n, tok, vec, cid):
    outs = (SDS((TP,) + tok.shape, bf), SDS((n // TP, TP) + vec.shape, f32))
    kernel = functools.partial(second_kernel, n)
    sems = GATHER_SEMS + TP + n // TP
    return exchange_call(kernel, outs, (tok, vec), sems, 2, cid)


def third_kernel(wv, ws, gu, tok, gain, bias, out, gu_out, nrm, ssem, rsem, local):
    me, peer = place()
    t = lax.rem(me, TP)
    meet([peer(k) for k in range(1, TP)])
    sems = (ssem, rsem)
    cols = wv.shape[1] // TP
    parts = [
        send_columns(wv, out, cols, 0, sems, 0, local.at[0], t, peer),
        send_columns(ws, out, cols, cols, sems, 7, local.at[1], t, peer),
        send_columns(gu, gu_out, gu.shape[2], 0, sems, 14, local.at[2], t, peer),
    ]
    step, r = 16, tok.shape[1]

    def norm(j, _):
        k = lax.div(j, r // step)
        at = pl.ds(pl.multiple_of(lax.rem(j, r // step) * step, step), step)
        value = tok[k, at, :].astype(f32)
        centred = value - jnp.mean(value, axis=-1, keepdims=True)
        spread = jnp.mean(centred * centred, axis=-1, keepdims=True)
        nrm[k, at, :] = (centred * lax.rsqrt(spread + 1e-05) * gain[...] + bias[...]).astype(bf)
        return 0

    lax.fori_loop(0, TP * r // step, norm, 0, unroll=4)
    finish(parts)


def third_exchange(wv, ws, gu, tok, gain, bias, cid):
    outs = (
        SDS((TP, wv.shape[0], 2 * wv.shape[1] // TP), bf),
        SDS(gu.shape, bf),
        SDS(tok.shape, bf),
    )
    return exchange_call(
        third_kernel, outs, (wv, ws, gu, tok, gain, bias), 21, 3, cid,
        out_specs=(ANY, ANY, VMEM), vmem=32 << 20,
    )


def fourth_kernel(
    n, cot, qko, nrm, cosine, sine, mask, cot_out, o_out, q_out, k_out, sco, w, ssem, rsem, local
):
    me, peer = place()
    t = lax.rem(me, TP)
    meet([peer(k) for k in range(1, TP)])
    sems = (ssem, rsem)
    share, cols = n // TP, o_out.shape[4]
    _, r, kh = q_out.shape
    half = kh // 2
    weights = pltpu.make_async_copy(qko.at[:, :, pl.ds(0, 2 * kh)], w, local.at[3])
    weights.start()
    gather = Gather(cot, cot_out, 0, cot.shape[0], sems, 0, local.at[0], peer)
    gather.start()
    copies, keeps = [], []

    def part(p, which):
        return qko.at[pl.ds(p * share, share), :, pl.ds(2 * kh + which * cols, cols)]

    for which in (0, 1):
        for k in range(1, TP):
            dev = peer(k)
            copy = remote(
                part(lax.rem(dev, TP), which), o_out.at[t, :, which], sems,
                GATHER_SEMS + which * TP + k, dev,
            )
            copy.start()
            copies.append(copy)
        keep = pltpu.make_async_copy(part(t, which), o_out.at[t, :, which], local.at[1 + which])
        keep.start()
        keeps.append(keep)
    weights.wait()

    def products(pairs):
        @pl.loop(*pairs)
        def _(j):
            rows = nrm[pl.ds(2 * j, 2)].reshape(2 * r, nrm.shape[2])
            for at, out in ((0, q_out), (kh, k_out)):
                y = jnp.dot(
                    rows, w[:, :, at : at + kh].reshape(nrm.shape[2], kh),
                    preferred_element_type=f32,
                )
                for i in (0, 1):
                    u, v = y[i * r : (i + 1) * r, :half], y[i * r : (i + 1) * r, half:]
                    cos, sin = cosine[2 * j + i], sine[2 * j + i]
                    out[2 * j + i, :, :half] = (u * cos - v * sin).astype(bf)
                    out[2 * j + i, :, half:] = (v * cos + u * sin).astype(bf)
            for i in (0, 1):
                plain = lax.dot_general(
                    q_out[2 * j + i], k_out[2 * j + i], (((1,), (1,)), ((), ())),
                    preferred_element_type=f32,
                )
                sco[2 * j + i] = (plain * mask[2 * j + i]).astype(bf)

    products((0, TP // 2))
    gather.forward()
    gather.finish()
    for copy in copies:
        copy.wait()
    for keep in keeps:
        keep.wait()


def fourth_exchange(n, cot, qko, nrm, cosine, sine, mask, cid):
    _, shard, width = qko.shape
    cols = (width - 2 * KH) // 2
    r = cot.shape[0]
    outs = (
        SDS((TP,) + cot.shape, bf),
        SDS((TP, n // TP, 2, shard, cols), bf),
        SDS((TP, r, KH), bf),
        SDS((TP, r, KH), bf),
        SDS(mask.shape, bf),
        SDS((n, shard, 2 * KH), bf),
    )
    kernel = functools.partial(fourth_kernel, n)
    return exchange_call(
        kernel, outs, (cot, qko, nrm, cosine, sine, mask),
        GATHER_SEMS + 2 * TP, 4, cid,
        specs=[VMEM, ANY, VMEM, VMEM, VMEM, VMEM],
        out_specs=(ANY, ANY, VMEM, VMEM, VMEM, VMEM), vmem=40 << 20,
    )


REDUCE_SEMS = 16
WIDE = 1024


class Reduce:
    def __init__(self, product, bufs, sems, base, peer, prepare=None, enter=None):
        self.product, self.prepare, self.sems, self.base = product, prepare, sems, base
        self.enter = enter
        self.po, self.pe, self.rc, self.sb, self.ring = bufs
        self.pc = peer(1)
        px, py = peer(2), peer(4)
        self.slots = ((0, 0, px), (1, 0, py), (0, 1, px), (1, 1, py), (1, 2, py), (0, 2, px))
        self.q = self.pe.shape[1] // 4
        self.waiting = True

    def core(self, i):
        return remote(self.po.at[i], self.rc.at[i], self.sems, self.base + i, self.pc)

    def link(self, c, slot):
        axis, at, dev = self.slots[slot]
        return remote(
            self.sb.at[c, slot], self.ring.at[axis, c, at], self.sems,
            self.base + 4 + 6 * c + slot, dev,
        )

    def add(self, halves, i, lower, out, more=None):
        step = 16
        steps = self.q // step
        first, count = halves

        @pl.loop(first * steps, (first + count) * steps)
        def _(j):
            c = lax.div(j, steps)
            there = pl.ds(pl.multiple_of(lax.rem(j, steps) * step, step), step)
            here = pl.ds(
                pl.multiple_of(lax.rem(j, steps) * step + (2 * c + lower) * self.q, step), step
            )
            total = self.pe[i, here, :].astype(f32) + self.rc[i, here, :].astype(f32)
            if more is not None:
                total = total + self.ring[more, c, 0, there, :].astype(f32)
            self.sb[c, out, there, :] = total.astype(bf)

    def both(self, slot, i, lower):
        self.add((0, 2), i, lower, slot)
        for c in (0, 1):
            self.link(c, slot).start()

    def six(self):
        self.core(3).wait_recv()
        self.both(0, 3, 0)
        self.both(1, 3, 1)

    def two(self):
        self.core(1).wait_recv()
        self.both(2, 1, 0)

    def four(self):
        self.core(2).wait_recv()
        self.both(3, 2, 1)

    def onward(self, c):
        self.link(c, 0).wait_recv()
        self.add((c, 1), 2, 0, 4, 0)
        self.link(c, 4).start()
        self.link(c, 1).wait_recv()
        self.add((c, 1), 1, 1, 5, 1)
        self.link(c, 5).start()

    def pair(self, it, i):
        self.product(it, i, self.po.at[i], self.pe.at[i])
        self.core(i).start()

    def run(self):
        if self.enter is not None:
            self.enter()

        @pl.loop(0, 4)
        def _(it):
            i = pair_at(it)
            if self.prepare is not None:
                self.prepare(it, i)
            else:
                self.pair(it, i)
            for k, stage in ((1, self.six), (2, self.two), (3, self.four)):
                pl.when(it == k)(stage)
            if self.prepare is not None:
                self.pair(it, i)

        for c in (0, 1):
            self.onward(c)

    def rows(self, c, step, body, unroll=2):
        if c == 0:
            self.core(0).wait_recv()
        for slot in (2, 3, 4, 5):
            self.link(c, slot).wait_recv()
        steps = self.q // step

        def some(j, _):
            lower = lax.div(j, steps)
            there = pl.ds(pl.multiple_of(lax.rem(j, steps) * step, step), step)
            here = pl.ds(pl.multiple_of(j * step + 2 * c * self.q, step), step)
            body(
                here,
                self.pe[0, here, :].astype(f32)
                + self.rc[0, here, :].astype(f32)
                + self.ring[lower, c, 1, there, :].astype(f32)
                + self.ring[1 - lower, c, 2, there, :].astype(f32),
            )
            return 0

        lax.fori_loop(0, 2 * steps, some, 0, unroll=unroll)

    def core_sent(self):
        for i in range(4):
            self.core(i).wait_send()
        self.waiting = False

    def finish(self):
        if self.waiting:
            self.core_sent()
        for c in (0, 1):
            for slot in range(6):
                self.link(c, slot).wait_send()


def pair_at(it):
    return it + 3 * (1 - lax.div(it + 2, 3)) - 3 * lax.div(it, 3)


class Load:
    def __init__(self, sems):
        self.sems, self.count = sems, 0

    def whole(self, src, dst):
        copy = pltpu.make_async_copy(src, dst, self.sems.at[self.count])
        self.count += 1
        copy.start()
        return copy.wait

    def paired(self, src, dst):
        base = self.count
        self.count += 4

        def piece(i):
            two = pl.ds(2 * i, 2)
            return pltpu.make_async_copy(src.at[two], dst.at[two], self.sems.at[base + i])

        return piece


def reduce_scratch(r, c, even=f32):
    q = r // 4
    return [
        pltpu.VMEM((4, r, c), bf),
        pltpu.VMEM((4, r, c), even),
        pltpu.VMEM((4, r, c), bf),
        pltpu.VMEM((2, 6, q, c), bf),
        pltpu.VMEM((2, 2, 3, q, c), bf),
    ]


def rows_of_pair(a, i):
    two, r, k = 2, a.shape[1], a.shape[2]
    return a[pl.ds(2 * i, two)].reshape(two * r, k)


def times(a, w, nt, arrive):
    def product(it, i, odd, even):
        r = a.shape[1]
        arrive(it, i)

        @pl.loop(0, even.shape[1] // WIDE)
        def _(j):
            at = pl.ds(pl.multiple_of(j * WIDE, WIDE), WIDE)
            x = rows_of_pair(a, i)
            if nt:
                y = lax.dot_general(
                    x, w[at, :], (((1,), (1,)), ((), ())), preferred_element_type=f32
                )
            else:
                y = jnp.dot(x, w[:, at], preferred_element_type=f32)
            even[:, at] = y[:r].astype(even.dtype)
            odd[:, at] = y[r:].astype(odd.dtype)

    return product


def exchange_and_gather(reduce, gathers, step, body, arrivals):
    reduce.run()
    for arrive in arrivals:
        arrive()
    for c in (0, 1):
        reduce.rows(c, step, body)
        gathers[c].start()
    for c in (0, 1):
        gathers[c].forward()
    for c in (0, 1):
        gathers[c].finish()
    reduce.finish()


def both_gathers(own, out, sems, local, peer):
    half = own.shape[0] // 2
    return [
        Gather(own, out, c * half, half, sems, REDUCE_SEMS + c * GATHER_SEMS, local.at[c], peer)
        for c in (0, 1)
    ]


EXCHANGE_SEMS = REDUCE_SEMS + 2 * GATHER_SEMS


def forward_kernel(
    nrm_in, wvs_in, sco, w_in, tok_in, vec, v_out, mix_out, ret_out, swi_out, mid, out,
    nrm, wvs, w, tok, v_buf, mix_buf, ret_buf, swi_buf, po, pe, rc, sb, ring, own,
    ssem, rsem, local, load,
):
    _, peer = place()
    enter = greet([peer(1), peer(2), peer(4)])
    sems = (ssem, rsem)
    r, width = v_buf.shape[1:]
    loads = Load(load)
    nrm_piece = loads.paired(nrm_in, nrm)
    nrm_piece(3).start()
    wvs_here = loads.whole(wvs_in, wvs)
    w_here = loads.whole(w_in, w)
    for i in (1, 2, 0):
        nrm_piece(i).start()
    tok_here = loads.whole(tok_in, tok)
    kept = ((v_buf, v_out), (mix_buf, mix_out), (ret_buf, ret_out), (swi_buf, swi_out))

    def keep(i):
        two = pl.ds(2 * i, 2)
        return [
            pltpu.make_async_copy(src.at[two], dst.at[two], local.at[2 + 4 * i + j])
            for j, (src, dst) in enumerate(kept)
        ]

    def prepare(it, i):
        first = 2 * i
        two = pl.ds(first, 2)
        pl.when(it == 0)(wvs_here)
        nrm_piece(i).wait()
        x = nrm[two].reshape(2 * r, nrm.shape[2])
        v = jnp.dot(x, wvs[:, :width], preferred_element_type=f32).astype(bf)
        v_buf[two] = v.reshape(2, r, width)
        for k in (0, 1):
            ret_buf[first + k] = jnp.dot(
                sco[first + k], v[k * r : (k + 1) * r], preferred_element_type=f32
            )
        s = jnp.dot(x, wvs[:, width:], preferred_element_type=f32)
        swi_buf[two] = s.reshape(2, r, width)

        def gated(j, _):
            k = first + lax.div(j, r // 32)
            at = pl.ds(pl.multiple_of(lax.rem(j, r // 32) * 32, 32), 32)
            value = ret_buf[k, at, :]
            centred = value - jnp.mean(value, axis=-1, keepdims=True)
            spread = jnp.mean(centred * centred, axis=-1, keepdims=True)
            gate = swi_buf[k, at, :]
            gate = gate / (1.0 + jnp.exp(-gate))
            mix_buf[k, at, :] = (
                gate * (centred * lax.rsqrt(jnp.maximum(spread, 0.25)))
            ).astype(bf)
            return 0

        lax.fori_loop(0, 2 * r // 32, gated, 0, unroll=4)
        for copy in keep(i):
            copy.start()

    def product(it, i, odd, even):
        step = w.shape[2]
        pl.when(it == 0)(w_here)

        def columns(j, _):
            at = pl.ds(pl.multiple_of(j * step, step), step)
            y = jnp.dot(rows_of_pair(mix_buf, i), w[j], preferred_element_type=f32)
            even[:, at] = y[:r].astype(even.dtype)
            odd[:, at] = y[r:].astype(odd.dtype)
            return 0

        lax.fori_loop(0, w.shape[0], columns, 0, unroll=4)

    def body(at, value):
        value = value + tok[at, :].astype(f32)
        mid[at, :] = value
        center = jnp.mean(value, axis=-1, keepdims=True)
        centred = value - center
        spread = jnp.mean(centred * centred, axis=-1, keepdims=True)
        own[at, :] = (
            centred * lax.rsqrt(spread + 1e-05) * vec[0:1, :] + vec[1:2, :]
        ).astype(bf)

    reduce = Reduce(product, (po, pe, rc, sb, ring), sems, 0, peer, prepare, enter)
    exchange_and_gather(reduce, both_gathers(own, out, sems, local, peer), 16, body, (tok_here,))
    for i in range(4):
        for copy in keep(i):
            copy.wait()


def forward_exchange(nrm, wvs, sco, w, tok, vec, cid):
    _, r, d = nrm.shape
    width = w.shape[1]
    count = EXCHANGE_SEMS
    blocks = [((TP, r, width), t) for t in (bf, bf, f32, f32)]
    return pl.pallas_call(
        forward_kernel,
        out_shape=tuple(SDS(*b) for b in blocks) + (SDS((r, d), f32), SDS((TP, r, d), bf)),
        in_specs=[ANY, ANY, VMEM, ANY, ANY, VMEM],
        out_specs=(ANY,) * 4 + (VMEM, ANY),
        scratch_shapes=[pltpu.VMEM(x.shape, x.dtype) for x in (nrm, wvs, w, tok)]
        + [pltpu.VMEM(*b) for b in blocks]
        + reduce_scratch(r, d)
        + [
            pltpu.VMEM((r, d), bf),
            pltpu.SemaphoreType.DMA((count,)),
            pltpu.SemaphoreType.DMA((count,)),
            pltpu.SemaphoreType.DMA((18,)),
            pltpu.SemaphoreType.DMA((7,)),
        ],
        compiler_params=pltpu.CompilerParams(
            collective_id=cid, has_side_effects=True, vmem_limit_bytes=60 << 20
        ),
        name="forward_exchange",
    )(nrm, wvs, sco, w, tok, vec)


def product_kernel(a, b, out):
    a, b = a[...].reshape(-1, a.shape[-1]), b[...].reshape(-1, b.shape[-1])
    out[...] = lax.dot_general(
        a, b, (((0,), (0,)), ((), ())), preferred_element_type=f32
    ).astype(bf)


def row_product(a, b):
    _, r, m = a.shape
    width = b.shape[2]
    tile, part = 512 if m >= 2048 else 256, min(width, 1024)
    return pl.pallas_call(
        product_kernel,
        grid=(width // part, m // tile),
        out_shape=SDS((m, width), bf),
        in_specs=[
            pl.BlockSpec((TP, r, tile), lambda j, i: (0, 0, i)),
            pl.BlockSpec((TP, r, part), lambda j, i: (0, 0, j)),
        ],
        out_specs=pl.BlockSpec((tile, part), lambda j, i: (i, j)),
        compiler_params=pltpu.CompilerParams(vmem_limit_bytes=56 << 20),
        cost_estimate=pl.CostEstimate(
            flops=2 * TP * r * m * width,
            bytes_accessed=2 * (a.size + b.size + m * width),
            transcendentals=0,
        ),
        name="row_product",
    )(a, b)


def hidden_kernel(x, gu, hid, act_out, slope_out):
    width = hid.shape[2]
    step = 256

    @pl.loop(0, width // step)
    def _(j):
        at = pl.ds(pl.multiple_of(j * step, step), step)
        behind = pl.ds(pl.multiple_of(j * step + width, step), step)
        rows = x[...].reshape(-1, x.shape[2])
        first = jnp.dot(rows, gu[:, at], preferred_element_type=f32)
        second = jnp.dot(rows, gu[:, behind], preferred_element_type=f32)
        share = 0.5 * (1.0 + lax.erf(first * math.sqrt(0.5)))
        act = first * share
        slope = share + first * (jnp.exp(-0.5 * first * first) * (1.0 / math.sqrt(2.0 * math.pi)))
        block = hid.shape[:2] + (step,)
        hid[:, :, at] = (act * second).astype(bf).reshape(block)
        act_out[:, :, at] = act.reshape(block)
        slope_out[:, :, at] = (slope * second).reshape(block)


def hidden_units(x, gu):
    _, r, d = x.shape
    width = gu.shape[1] // 2
    row = pl.BlockSpec((2, r, width), lambda k: (k, 0, 0))
    return pl.pallas_call(
        hidden_kernel,
        grid=(TP // 2,),
        out_shape=tuple(SDS((TP, r, width), t) for t in (bf, f32, f32)),
        in_specs=[
            pl.BlockSpec((2, r, d), lambda k: (k, 0, 0)),
            pl.BlockSpec(gu.shape, lambda k: (0, 0)),
        ],
        out_specs=(row, row, row),
        compiler_params=pltpu.CompilerParams(vmem_limit_bytes=56 << 20),
        cost_estimate=pl.CostEstimate(
            flops=4 * TP * r * d * width, bytes_accessed=24 << 20, transcendentals=2 * TP * r * width
        ),
        name="hidden_units",
    )(x, gu)


def hidden_back_kernel(cot, down, act, slope, out):
    width = act.shape[2]
    step = 256

    @pl.loop(0, width // step)
    def _(j):
        at = pl.ds(pl.multiple_of(j * step, step), step)
        behind = pl.ds(pl.multiple_of(j * step + width, step), step)
        grad = lax.dot_general(
            cot[...].reshape(-1, cot.shape[2]), down[at, :], (((1,), (1,)), ((), ())),
            preferred_element_type=f32,
        ).reshape(act.shape[:2] + (step,))
        out[:, :, at] = (grad * slope[:, :, at]).astype(bf)
        out[:, :, behind] = (grad * act[:, :, at]).astype(bf)


def hidden_back(cot, down, act, slope):
    _, r, d = cot.shape
    width = act.shape[2]
    row = pl.BlockSpec((2, r, width), lambda k: (k, 0, 0))
    return pl.pallas_call(
        hidden_back_kernel,
        grid=(TP // 2,),
        out_shape=SDS((TP, r, 2 * width), bf),
        in_specs=[
            pl.BlockSpec((2, r, d), lambda k: (k, 0, 0)),
            pl.BlockSpec(down.shape, lambda k: (0, 0)),
            row,
            row,
        ],
        out_specs=pl.BlockSpec((2, r, 2 * width), lambda k: (k, 0, 0)),
        compiler_params=pltpu.CompilerParams(vmem_limit_bytes=56 << 20),
        cost_estimate=pl.CostEstimate(
            flops=2 * TP * r * d * width, bytes_accessed=24 << 20, transcendentals=0
        ),
        name="hidden_back",
    )(cot, down, act, slope)


def backward_kernel(
    a_in, w_in, mid_in, cot_in, vec, gmid, out, sums,
    a, w, mid, cot, po, pe, rc, sb, ring, own, acc, ssem, rsem, local, load,
):
    _, peer = place()
    enter = greet([peer(1), peer(2), peer(4)])
    sems = (ssem, rsem)
    loads = Load(load)
    piece = loads.paired(a_in, a)
    piece(3).start()
    w_here = loads.whole(w_in, w)
    for i in (1, 2, 0):
        piece(i).start()
    arrivals = (loads.whole(mid_in, mid), loads.whole(cot_in, cot))

    def arrive(it, i):
        pl.when(it == 0)(w_here)
        piece(i).wait()

    acc[...] = jnp.zeros_like(acc)

    def body(at, g):
        value = mid[at, :]
        center = jnp.mean(value, axis=-1, keepdims=True)
        centred = value - center
        inv = lax.rsqrt(jnp.mean(centred * centred, axis=-1, keepdims=True) + 1e-05)
        hat = centred * inv
        acc[0] += g * hat
        acc[1] += g
        scaled = g * vec[0:1, :]
        mean_g = jnp.mean(scaled, axis=-1, keepdims=True)
        mean_gh = jnp.mean(scaled * hat, axis=-1, keepdims=True)
        grad = cot[at, :].astype(f32) + inv * (scaled - mean_g - hat * mean_gh)
        gmid[at, :] = grad
        own[at, :] = grad.astype(bf)

    reduce = Reduce(
        times(a, w, True, arrive), (po, pe, rc, sb, ring), sems, 0, peer, enter=enter
    )
    exchange_and_gather(reduce, both_gathers(own, out, sems, local, peer), 16, body, arrivals)
    sums[0:1, :] = jnp.sum(acc[0], axis=0, keepdims=True)
    sums[1:2, :] = jnp.sum(acc[1], axis=0, keepdims=True)


def backward_exchange(a, w, mid, cot, vec, cid):
    _, r, _ = a.shape
    c = w.shape[0]
    count = EXCHANGE_SEMS
    return pl.pallas_call(
        backward_kernel,
        out_shape=(SDS((r, c), f32), SDS((TP, r, c), bf), SDS((2, c), f32)),
        in_specs=[ANY] * 4 + [VMEM],
        out_specs=(VMEM, ANY, VMEM),
        scratch_shapes=[pltpu.VMEM(x.shape, x.dtype) for x in (a, w, mid, cot)]
        + reduce_scratch(r, c)
        + [
            pltpu.VMEM((r, c), bf),
            pltpu.VMEM((2, 16, c), f32),
            pltpu.SemaphoreType.DMA((count,)),
            pltpu.SemaphoreType.DMA((count,)),
            pltpu.SemaphoreType.DMA((2,)),
            pltpu.SemaphoreType.DMA((7,)),
        ],
        compiler_params=pltpu.CompilerParams(
            collective_id=cid, has_side_effects=True, vmem_limit_bytes=52 << 20
        ),
        name="backward_exchange",
    )(a, w, mid, cot, vec)


def last_kernel(
    n, gqkv_in, gs_in, wqk_in, wvs_in, a2_in, w2_in, tok_in, gmid_in, gain, sums2,
    gtok, ffn, vec_out, gqkv, gs, wqk, wvs, a2, w2, tok, gmid,
    po, pe, rc, sb, ring, pe2, rc2, sb2, ring2, acc, vecs, near, far, part, ssem, rsem, load,
):
    dp = n // TP
    me, peer = place()
    g = lax.div(me, TP)
    width = vec_out.shape[1]
    others = [lax.rem(me + TP * j, n) for j in range(1, dp)]
    enter = greet([peer(k) for k in range(1, TP)] + others)
    sems = (ssem, rsem)
    loads = Load(load)
    pieces = loads.paired(gqkv_in, gqkv), loads.paired(gs_in, gs)
    for piece in pieces:
        piece(3).start()
    weights = loads.whole(wqk_in, wqk), loads.whole(wvs_in, wvs)
    for i in (1, 2, 0):
        for piece in pieces:
            piece(i).start()
    second = loads.whole(a2_in, a2), loads.whole(w2_in, w2)
    arrivals = loads.whole(tok_in, tok), loads.whole(gmid_in, gmid)

    def all_here(waits):
        def wait():
            for one in waits:
                one()

        return wait

    acc[...] = jnp.zeros_like(acc)
    nt = (((1,), (1,)), ((), ()))

    def product(it, i, odd, even):
        r, qk, v = gqkv.shape[1], wqk.shape[1], gs.shape[2]
        pl.when(it == 0)(all_here(weights))
        for piece in pieces:
            piece(i).wait()
        x, y = rows_of_pair(gqkv, i), rows_of_pair(gs, i)

        @pl.loop(0, even.shape[1] // WIDE)
        def _(j):
            at = pl.ds(pl.multiple_of(j * WIDE, WIDE), WIDE)
            z = lax.dot_general(x[:, :qk], wqk[at, :], nt, preferred_element_type=f32)
            z += lax.dot_general(x[:, qk:], wvs[at, :v], nt, preferred_element_type=f32)
            z += lax.dot_general(y, wvs[at, v:], nt, preferred_element_type=f32)
            even[:, at] = z[:r].astype(even.dtype)
            odd[:, at] = z[r:].astype(odd.dtype)

    one = Reduce(product, (po, pe, rc, sb, ring), sems, 0, peer, enter=enter)
    one.run()
    one.core_sent()

    def arrive(it, _):
        pl.when(it == 0)(all_here(second))

    two = Reduce(times(a2, w2, False, arrive), (po, pe2, rc2, sb2, ring2), sems, REDUCE_SEMS, peer)
    two.run()

    def body(at, grad):
        value = tok[at, :].astype(f32)
        center = jnp.mean(value, axis=-1, keepdims=True)
        centred = value - center
        inv = lax.rsqrt(jnp.mean(centred * centred, axis=-1, keepdims=True) + 1e-05)
        hat = centred * inv
        acc[0] += grad * hat
        acc[1] += grad
        scaled = grad * gain[...]
        mean_g = jnp.mean(scaled, axis=-1, keepdims=True)
        mean_gh = jnp.mean(scaled * hat, axis=-1, keepdims=True)
        gtok[at, :] = gmid[at, :] + inv * (scaled - mean_g - hat * mean_gh)

    all_here(arrivals)()
    for c in (0, 1):
        one.rows(c, 16, body)
    vecs[...] = jnp.zeros_like(vecs)
    vecs[0:1, :] = jnp.sum(acc[0], axis=0, keepdims=True)
    vecs[1:2, :] = jnp.sum(acc[1], axis=0, keepdims=True)
    vecs[2:4, :] = sums2[...]
    base = 2 * REDUCE_SEMS
    copies = []
    for j, dev in enumerate(others):
        at = pl.multiple_of(lax.div(dev, TP) * width, 128)
        copy = remote(vecs.at[:, pl.ds(at, width)], far.at[j], sems, base + j, dev)
        copy.start()
        copies.append(copy)

    def keep(at, value):
        ffn[at, :] = value

    two.rows(0, 16, keep)
    total = vecs[:, pl.ds(pl.multiple_of(g * width, 128), width)]
    for j, copy in enumerate(copies):
        copy.wait()
        total = total + far[j]
    part[...] = total
    copies = []
    for k in range(1, TP):
        copy = remote(part, near.at[k - 1], sems, base + dp + k - 1, peer(k))
        copy.start()
        copies.append(copy)
    two.rows(1, 16, keep)
    for k, copy in enumerate(copies):
        copy.wait()
        total = total + near[k]
    vec_out[...] = total
    one.finish()
    two.finish()


def last_exchange(n, gqkv, gs, wqk, wvs, a2, w2, tok, gmid, gain, sums2, cid):
    dp = n // TP
    _, r, _ = a2.shape
    c = w2.shape[1]
    width = c // dp
    count = 2 * REDUCE_SEMS + dp + TP
    return pl.pallas_call(
        functools.partial(last_kernel, n),
        out_shape=(SDS((r, c), f32), SDS((r, c), f32), SDS((8, width), f32)),
        in_specs=[ANY] * 8 + [VMEM] * 2,
        out_specs=(VMEM,) * 3,
        scratch_shapes=[
            pltpu.VMEM(x.shape, x.dtype) for x in (gqkv, gs, wqk, wvs, a2, w2, tok, gmid)
        ]
        + reduce_scratch(r, c)
        + reduce_scratch(r, c, bf)[1:]
        + [
            pltpu.VMEM((2, 16, c), f32),
            pltpu.VMEM((8, c), f32),
            pltpu.VMEM((TP - 1, 8, width), f32),
            pltpu.VMEM((dp, 8, width), f32),
            pltpu.VMEM((8, width), f32),
            pltpu.SemaphoreType.DMA((count,)),
            pltpu.SemaphoreType.DMA((count,)),
            pltpu.SemaphoreType.DMA((14,)),
        ],
        compiler_params=pltpu.CompilerParams(
            collective_id=cid, has_side_effects=True, vmem_limit_bytes=ALL_VMEM
        ),
        name="last_exchange",
    )(gqkv, gs, wqk, wvs, a2, w2, tok, gmid, gain, sums2)


def gate_back_kernel(g_low, w, ret, swi, gret, gswi, whole):
    cols = w.shape[2]

    @pl.when(pl.program_id(0) == 0)
    def _():
        for j in range(w.shape[0]):
            whole[:, j * cols : (j + 1) * cols] = w[j]

    two, r, _ = gret.shape
    grads = lax.dot_general(
        g_low[...].reshape(two * r, g_low.shape[2]), whole[...], (((1,), (1,)), ((), ())),
        preferred_element_type=f32,
    )
    for i in range(two):
        grad, value, gate = grads[i * r : (i + 1) * r], ret[i], swi[i]
        centred = value - jnp.mean(value, axis=-1, keepdims=True)
        spread = jnp.mean(centred * centred, axis=-1, keepdims=True)
        inv = lax.rsqrt(jnp.maximum(spread, 0.25))
        share = 1.0 / (1.0 + jnp.exp(-gate))
        silu = gate * share
        gswi[i] = (grad * (centred * inv) * (share * (1.0 + gate * (1.0 - share)))).astype(bf)
        grad = grad * silu
        pull = jnp.mean(grad * centred, axis=-1, keepdims=True)
        pull = jnp.where(spread > 0.25, inv * inv * inv * pull, 0.0)
        grad = grad * inv - centred * pull
        gret[i] = (grad - jnp.mean(grad, axis=-1, keepdims=True)).astype(bf)


def gate_back(g_low, w, ret, swi):
    _, r, d = g_low.shape
    width = ret.shape[2]
    row = pl.BlockSpec((2, r, width), lambda k: (k, 0, 0))
    return pl.pallas_call(
        gate_back_kernel,
        grid=(TP // 2,),
        out_shape=(SDS(ret.shape, bf), SDS(ret.shape, bf)),
        in_specs=[
            pl.BlockSpec((2, r, d), lambda k: (k, 0, 0)),
            pl.BlockSpec(w.shape, lambda k: (0, 0, 0)),
            row,
            row,
        ],
        out_specs=(row, row),
        scratch_shapes=[pltpu.VMEM((width, d), bf)],
        compiler_params=pltpu.CompilerParams(vmem_limit_bytes=56 << 20),
        cost_estimate=pl.CostEstimate(
            flops=2 * TP * r * d * width, bytes_accessed=22 << 20, transcendentals=TP * r * width
        ),
        name="gate_back",
    )(g_low, w, ret, swi)


def scores_back_kernel(sco, mask, q, k, v, gret, cosine, sine, out):
    nt, tn = (((1,), (1,)), ((), ())), (((0,), (0,)), ((), ()))
    kh = q.shape[2]
    half = kh // 2
    out[0, :, 2 * kh :] = lax.dot_general(
        sco[0], gret[0], tn, preferred_element_type=f32
    ).astype(bf)
    grad = lax.dot_general(gret[0], v[0], nt, preferred_element_type=f32)
    grad = (grad * mask[0]).astype(bf)
    gq = jnp.dot(grad, k[0], preferred_element_type=f32)
    gk = lax.dot_general(grad, q[0], tn, preferred_element_type=f32)
    for i, g in enumerate((gq, gk)):
        u, w = g[:, :half], g[:, half:]
        at = i * kh
        out[0, :, at : at + half] = (u * cosine[0] + w * sine[0]).astype(bf)
        out[0, :, at + half : at + kh] = (w * cosine[0] - u * sine[0]).astype(bf)


def scores_back(sco, mask, q, k, v, gret, cosine, sine):
    _, r, kh = q.shape
    arrays = (sco, mask, q, k, v, gret, cosine, sine)
    width = 2 * kh + v.shape[2]
    spec = [pl.BlockSpec((1,) + x.shape[1:], lambda i: (i, 0, 0)) for x in arrays]
    return pl.pallas_call(
        scores_back_kernel,
        grid=(TP,),
        out_shape=SDS((TP, r, width), bf),
        in_specs=spec,
        out_specs=pl.BlockSpec((1, r, width), lambda i: (i, 0, 0)),
        compiler_params=pltpu.CompilerParams(vmem_limit_bytes=56 << 20),
        cost_estimate=pl.CostEstimate(
            flops=4 * TP * r * r * (kh + v.shape[2]), bytes_accessed=16 << 20, transcendentals=0
        ),
        name="scores_back",
    )(*arrays)


def tp_groups(n):
    return [[g * TP + t for t in range(TP)] for g in range(n // TP)]


def dp_groups(n):
    return [[g * TP + t for g in range(n // TP)] for t in range(TP)]


def plane_a2a(x, n):
    return lax.all_to_all(x, AXIS, 0, 0, axis_index_groups=tp_groups(n), tiled=True)


def spread_rows(x, n):
    rows = x.shape[0] // 4
    t = lax.rem(lax.axis_index(AXIS), TP)
    got = []
    for m in range(4):
        chunk = lax.dynamic_slice_in_dim(x, lax.rem(lax.div(t, 2) + m, 4) * rows, rows, 0)
        pairs = [
            (g * TP + h, g * TP + 4 * (h % 2) + (h // 2 + m) % 4)
            for g in range(n // TP)
            for h in range(TP)
        ]
        got.append(lax.ppermute(chunk, AXIS, pairs))
    turned = jnp.concatenate(got[::-1] * 2, axis=0)
    return lax.dynamic_slice_in_dim(turned, (3 - lax.rem(t, 4)) * rows, 4 * rows, 0)


def dp_gather(x, n):
    return lax.all_gather(x, AXIS, axis=0, tiled=True, axis_index_groups=dp_groups(n))


def dp_reduce(x, n):
    return lax.psum_scatter(
        x, AXIS, scatter_dimension=0, tiled=True, axis_index_groups=dp_groups(n)
    )


def seq_positions(lengths, rows):
    ends = jnp.cumsum(lengths, axis=1)
    starts = ends - lengths
    index = jnp.arange(rows, dtype=jnp.int32)
    segment = jnp.sum((index[None, :, None] >= ends[:, None, :]).astype(jnp.int32), axis=2)
    member = segment[:, :, None] == jnp.arange(lengths.shape[1], dtype=jnp.int32)
    offset = index[None, :] - jnp.sum(jnp.where(member, starts[:, None, :], 0), axis=2)
    return segment, offset


def rotary_tables(offset):
    half = KH // 2
    freq = jnp.exp(-math.log(10000.0) * jnp.arange(half, dtype=f32) / half)
    angle = offset.astype(f32)[..., None] * freq
    return jnp.cos(angle), jnp.sin(angle)


def decay_mask(segment, offset, head):
    diff = offset[:, :, None] - offset[:, None, :]
    valid = (segment[:, :, None] == segment[:, None, :]) & (diff >= 0)
    steps = jnp.where(valid, diff, 0).astype(f32)
    log = jnp.log(1.0 - jnp.exp2(-5.0 - head.astype(f32)))
    return jnp.where(valid, jnp.exp(log * steps), 0.0) / math.sqrt(KH)


def col_blocks(w):
    r, c = w.shape
    return w.reshape(r, TP, c // TP).transpose(1, 0, 2).reshape(TP * r, c // TP)


def join_kernel(widths, parts, x, *outs):
    at = 0
    for out, width in zip(outs, widths):
        piece = width // parts
        for t in range(TP):
            for p in range(parts):
                to = (p * TP + t) * piece
                out[:, to : to + piece] = x[t, :, at + p * piece : at + (p + 1) * piece].astype(f32)
        at += width


def join(x, widths, parts=1):
    r = x.shape[1]
    if any(width // parts % 128 for width in widths):
        made, at = [], 0
        for width in widths:
            part = x[:, :, at : at + width].reshape(TP, r, parts, width // parts)
            made.append(part.transpose(1, 2, 0, 3).reshape(r, TP * width).astype(f32))
            at += width
        return made
    return pl.pallas_call(
        functools.partial(join_kernel, widths, parts),
        out_shape=tuple(SDS((r, TP * width), f32) for width in widths),
        in_specs=[VMEM],
        out_specs=tuple(VMEM for _ in widths),
        compiler_params=pltpu.CompilerParams(vmem_limit_bytes=8 << 20),
        cost_estimate=pl.CostEstimate(flops=0, bytes_accessed=6 * x.size, transcendentals=0),
        name="join",
    )(x)


def after(x, *deps):
    return lax.optimization_barrier((x,) + deps)[0]


def on_device(n, tokens, lengths, gain1, bias1, wq, wk, wv, ws, wo, gain2, bias2, wg, wu, wd, cot):
    rows, d = tokens.shape
    ff = wg.shape[1]
    dp = n // TP
    shard = d // n
    unit = ff // n
    me = lax.axis_index(AXIS)
    head = lax.rem(me, TP)

    def ff_blocks(w):
        return w.reshape(shard, dp, TP, unit).transpose(2, 0, 1, 3).reshape(TP, shard, dp * unit)

    lens = jnp.pad(lengths[0].astype(f32), (0, shard - lengths.shape[1]))
    vec = jnp.stack([v.astype(f32) for v in (gain1, bias1, gain2, bias2)] + [lens])
    vec = jnp.pad(vec, ((0, 3), (0, 128 - shard)))
    qko_blk = first_exchange(wq, wk, wo, 1)
    qko = dp_gather(qko_blk.reshape(TP * shard, 4 * KH), n)
    tok_all, vec_all = second_exchange(n, after(tokens, qko_blk), vec, 2)
    gain1f, bias1f, gain2f, bias2f = (
        vec_all[:, :, i, :shard].reshape(1, d) for i in range(4)
    )
    vec2 = jnp.concatenate([gain2f, bias2f], axis=0)
    gu_in = jnp.concatenate([ff_blocks(wg), ff_blocks(wu)], axis=2)
    vs_blk, gu_blk, normed = third_exchange(wv, ws, gu_in, tok_all, gain1f, bias1f, 3)
    vs = dp_gather(vs_blk.reshape(TP * shard, 2 * VH), n)
    gu = dp_gather(gu_blk.reshape(TP * shard, 2 * dp * unit), n)
    down = dp_gather(wd, n)

    mine = lax.dynamic_slice_in_dim(vec_all, lax.div(me, TP), 1, 0)[0, :, 4, :3]
    order = jnp.arange(TP, dtype=jnp.int32)
    pick = (order[None, :] == (order[:, None] ^ head)).astype(f32)
    len_all = jnp.sum(pick[:, :, None] * mine[None], axis=1).astype(jnp.int32)
    segment, offset = seq_positions(len_all, rows)
    cosine, sine = rotary_tables(offset)
    mask = decay_mask(segment, offset, head)

    cot_all, out_blk, q_rot, k_rot, scores, qk = fourth_exchange(
        n, cot, qko.reshape(n, shard, 4 * KH), normed, cosine, sine, mask, 4
    )
    out_blk = out_blk.reshape(TP, VH, d // TP)
    qk = qk.reshape(d, 2 * KH)
    v_low, mixed, retained, swish_in, middle, normed2 = forward_exchange(
        normed, vs, scores, out_blk, tokens, vec2, 5
    )
    hidden, act, slope = hidden_units(normed2, gu)
    down_grad = row_product(hidden, cot_all)
    g_down = dp_reduce(down_grad, n)

    g_fs = hidden_back(cot_all, down, act, slope)
    gu_grad = row_product(normed2, g_fs)
    g_gu = dp_reduce(gu_grad, n)
    g_middle, g_low, sums2 = backward_exchange(g_fs, gu, middle, cot, vec2, 6)

    g_retained, g_swish = gate_back(g_low, out_blk, retained, swish_in)
    swish_grad = row_product(normed, g_swish)
    g_swi = dp_reduce(swish_grad, n)
    out_grad = row_product(mixed, g_low)
    spread = wo.shape[0] * HEADS == VH * 2
    if spread:
        out_grad = spread_rows(out_grad, n)
    else:
        out_grad = plane_a2a(col_blocks(out_grad), n)
    g_qkv = scores_back(scores, mask, q_rot, k_rot, v_low, g_retained, cosine, sine)
    qkv_grad = row_product(normed, g_qkv)
    g_qkv_own = dp_reduce(qkv_grad, n)
    g_out = dp_reduce(out_grad, n)
    grad_tokens, ffn, g_vecs = last_exchange(
        n, g_qkv, g_swish, qk, vs, hidden, down, tokens, g_middle, gain1f, sums2, 7
    )
    layer_out = (middle + ffn).astype(bf)

    g_vecs = lax.dynamic_slice_in_dim(g_vecs, head * shard, shard, 1)
    grad_d = g_down.astype(f32)
    g_gu = plane_a2a(g_gu, n)
    grad_g, grad_u = join(g_gu.reshape(TP, shard, 2 * dp * unit), (dp * unit,) * 2, dp)
    g_swi = plane_a2a(g_swi, n)
    (grad_s,) = join(g_swi.reshape(TP, shard, VH), (VH,))
    g_qkv_own = plane_a2a(g_qkv_own, n)
    grad_q, grad_k, grad_v = join(g_qkv_own.reshape(TP, shard, 2 * KH + VH), (KH, KH, VH))
    if spread:
        grad_o = g_out.astype(f32)
    else:
        g_out = plane_a2a(g_out, n)
        (grad_o,) = join(g_out.reshape(TP, wo.shape[0], d // TP), (d // TP,))
    return (
        layer_out, grad_tokens, g_vecs[0], g_vecs[1], grad_q, grad_k, grad_v, grad_s, grad_o,
        g_vecs[2], g_vecs[3], grad_g, grad_u, grad_d,
    )


def solution(mesh):
    n = mesh.shape[AXIS]
    row, vec = P(AXIS, None), P(AXIS)
    ins = (row, row, vec, vec, row, row, row, row, row, vec, vec, row, row, row, row)
    outs = (row, row, vec, vec, row, row, row, row, row, vec, vec, row, row, row)

    def body(*args):
        return on_device(n, *args)

    return jax.shard_map(body, mesh=mesh, in_specs=ins, out_specs=outs, check_vma=False)
```

```python
import functools
import math

import jax
import jax.numpy as jnp
from jax import lax
from jax.experimental import pallas as pl
from jax.experimental.pallas import tpu as pltpu
from jax.sharding import PartitionSpec as P


HEADS = 8
KH = 256
VH = 512
TP = 8
AXIS = "fsdp"
MESH = pl.DeviceIdType.MESH
ANY = pl.BlockSpec(memory_space=pl.ANY)
VMEM = pl.BlockSpec(memory_space=pltpu.VMEM)
bf = jnp.bfloat16
f32 = jnp.float32
SDS = jax.ShapeDtypeStruct
ALL_VMEM = 67043328


def place():
    me = lax.axis_index(AXIS)
    steps = [s - 2 * s * lax.rem(lax.div(me, s), 2) for s in (1, 2, 4)]

    def peer(k):
        out = me
        for bit, step in enumerate(steps):
            if k >> bit & 1:
                out = out + step
        return out

    return me, peer


def greet(peers):
    barrier = pltpu.get_barrier_semaphore()
    for p in peers:
        pl.semaphore_signal(barrier, inc=1, device_id=(p,), device_id_type=MESH)
    return lambda: pl.semaphore_wait(barrier, len(peers))


def meet(peers):
    greet(peers)()


def remote(src, dst, sems, i, dev):
    return pltpu.make_async_remote_copy(
        src_ref=src, dst_ref=dst, send_sem=sems[0].at[i], recv_sem=sems[1].at[i],
        device_id=(dev,), device_id_type=MESH,
    )


GATHER_SEMS = 13


class Gather:
    def __init__(self, own, out, start, size, sems, base, local, peer):
        self.own, self.out, self.sems, self.base, self.local = own, out, sems, base, local
        h = size // 2
        self.all, self.top, self.bot = pl.ds(start, size), pl.ds(start, h), pl.ds(start + h, h)
        self.pc, self.px, self.py = peer(1), peer(2), peer(4)
        self.made = []

    def send(self, src, dst, dev):
        copy = remote(src, dst, self.sems, self.base + len(self.made), dev)
        copy.start()
        self.made.append(copy)
        return copy

    def pass_on(self, k, at):
        self.core.append(self.send(self.out.at[k, at], self.out.at[k + 1, at], self.pc))

    def start(self):
        own, out, top, bot = self.own, self.out, self.top, self.bot
        self.x0 = self.send(own.at[bot], out.at[2, bot], self.px)
        self.y0 = self.send(own.at[top], out.at[4, top], self.py)
        self.x1 = self.send(own.at[top], out.at[2, top], self.px)
        self.y1 = self.send(own.at[bot], out.at[4, bot], self.py)
        self.core = [self.send(own.at[self.all], out.at[1, self.all], self.pc)]
        self.keep = pltpu.make_async_copy(own.at[self.all], out.at[0, self.all], self.local)
        self.keep.start()

    def forward(self):
        out, top, bot = self.out, self.top, self.bot
        self.x0.wait_recv()
        self.fy = self.send(out.at[2, bot], out.at[6, bot], self.py)
        self.pass_on(2, bot)
        self.y0.wait_recv()
        self.fx = self.send(out.at[4, top], out.at[6, top], self.px)
        self.pass_on(4, top)
        self.x1.wait_recv()
        self.pass_on(2, top)
        self.y1.wait_recv()
        self.pass_on(4, bot)

    def finish(self):
        self.fy.wait_recv()
        self.pass_on(6, self.bot)
        self.fx.wait_recv()
        self.pass_on(6, self.top)
        for copy in self.core:
            copy.wait_recv()
        for copy in self.made:
            copy.wait_send()
        self.keep.wait()


def send_columns(src, out, cols, at, sems, base, local, t, peer, rows=None):
    copies = []
    rows = slice(None) if rows is None else rows

    def block(q):
        if len(src.shape) == 3:
            return src.at[q]
        return src.at[rows, pl.ds(pl.multiple_of(q * cols, 128), cols)]

    for k in range(1, TP):
        dev = peer(k)
        copy = remote(
            block(lax.rem(dev, TP)), out.at[t, :, pl.ds(at, cols)], sems, base + k - 1, dev
        )
        copy.start()
        copies.append(copy)
    keep = pltpu.make_async_copy(block(t), out.at[t, :, pl.ds(at, cols)], local)
    keep.start()
    return copies, keep


def finish(parts):
    for copies, keep in parts:
        for copy in copies:
            copy.wait()
        keep.wait()


def exchange_call(
    kernel, outs, args, sems, locals_, cid, specs=None, out_specs=None, vmem=12 << 20
):
    return pl.pallas_call(
        kernel,
        out_shape=outs,
        in_specs=specs or [VMEM] * len(args),
        out_specs=out_specs or tuple(ANY for _ in outs),
        scratch_shapes=[
            pltpu.SemaphoreType.DMA((sems,)),
            pltpu.SemaphoreType.DMA((sems,)),
            pltpu.SemaphoreType.DMA((locals_,)),
        ],
        compiler_params=pltpu.CompilerParams(
            collective_id=cid, has_side_effects=True, vmem_limit_bytes=vmem
        ),
    )(*args)


def first_kernel(n, wq, wk, wo, wd, out, wd_out, ssem, rsem, local):
    me, peer = place()
    t, g = lax.rem(me, TP), lax.div(me, TP)
    others = others_along(n)
    meet([peer(k) for k in range(1, TP)] + others)
    sems = (ssem, rsem)
    shard, cq, co = wq.shape[0], wq.shape[1] // TP, wo.shape[1] // TP
    low, high = pl.ds(0, shard), pl.ds(shard, shard)
    along = [remote(wd, wd_out.at[g], sems, 28 + j, dev) for j, dev in enumerate(others)]
    for copy in along:
        copy.start()
    keep = pltpu.make_async_copy(wd, wd_out.at[g], local.at[4])
    keep.start()
    finish([
        send_columns(wq, out, cq, 0, sems, 0, local.at[0], t, peer),
        send_columns(wk, out, cq, cq, sems, 7, local.at[1], t, peer),
        send_columns(wo, out, co, 2 * cq, sems, 14, local.at[2], t, peer, low),
        send_columns(wo, out, co, 2 * cq + co, sems, 21, local.at[3], t, peer, high),
        (along, keep),
    ])


def first_exchange(n, wq, wk, wo, wd, cid):
    width = 2 * wq.shape[1] // TP + 2 * wo.shape[1] // TP
    outs = (SDS((TP, wq.shape[0], width), bf), SDS((n // TP,) + wd.shape, bf))
    kernel = functools.partial(first_kernel, n)
    return exchange_call(kernel, outs, (wq, wk, wo, wd), 28 + n // TP, 5, cid)


def others_along(n):
    me = lax.axis_index(AXIS)
    return [lax.rem(me + TP * j, n) for j in range(1, n // TP)]


def second_kernel(n, tok, vec, tok_out, vec_out, ssem, rsem, local):
    me, peer = place()
    t, g = lax.rem(me, TP), lax.div(me, TP)
    others = others_along(n)
    meet([peer(k) for k in range(1, TP)] + others)
    sems = (ssem, rsem)
    base = GATHER_SEMS
    far = []
    keep = pltpu.make_async_copy(vec, vec_out.at[g, t], local.at[1])
    keep.start()
    for j, dev in enumerate(others):
        copy = remote(vec, vec_out.at[g, t], sems, base + TP + j, dev)
        copy.start()
        far.append(copy)
    gather = Gather(tok, tok_out, 0, tok.shape[0], sems, 0, local.at[0], peer)
    gather.start()
    for copy in far:
        copy.wait()
    keep.wait()
    near = []
    for k in range(1, TP):
        copy = remote(vec_out.at[:, t], vec_out.at[:, t], sems, base + k, peer(k))
        copy.start()
        near.append(copy)
    gather.forward()
    gather.finish()
    for copy in near:
        copy.wait()


def second_exchange(n, tok, vec, cid):
    outs = (SDS((TP,) + tok.shape, bf), SDS((n // TP, TP) + vec.shape, f32))
    kernel = functools.partial(second_kernel, n)
    sems = GATHER_SEMS + TP + n // TP
    return exchange_call(kernel, outs, (tok, vec), sems, 2, cid)


def third_kernel(wv, ws, gu, tok, gain, bias, out, gu_out, nrm, ssem, rsem, local):
    me, peer = place()
    t = lax.rem(me, TP)
    meet([peer(k) for k in range(1, TP)])
    sems = (ssem, rsem)
    cols = wv.shape[1] // TP
    parts = [
        send_columns(wv, out, cols, 0, sems, 0, local.at[0], t, peer),
        send_columns(ws, out, cols, cols, sems, 7, local.at[1], t, peer),
        send_columns(gu, gu_out, gu.shape[2], 0, sems, 14, local.at[2], t, peer),
    ]
    step, r = 16, tok.shape[1]

    def norm(j, _):
        k = lax.div(j, r // step)
        at = pl.ds(pl.multiple_of(lax.rem(j, r // step) * step, step), step)
        value = tok[k, at, :].astype(f32)
        centred = value - jnp.mean(value, axis=-1, keepdims=True)
        spread = jnp.mean(centred * centred, axis=-1, keepdims=True)
        nrm[k, at, :] = (centred * lax.rsqrt(spread + 1e-05) * gain[...] + bias[...]).astype(bf)
        return 0

    lax.fori_loop(0, TP * r // step, norm, 0, unroll=4)
    finish(parts)


def third_exchange(wv, ws, gu, tok, gain, bias, cid):
    outs = (
        SDS((TP, wv.shape[0], 2 * wv.shape[1] // TP), bf),
        SDS(gu.shape, bf),
        SDS(tok.shape, bf),
    )
    return exchange_call(
        third_kernel, outs, (wv, ws, gu, tok, gain, bias), 21, 3, cid,
        out_specs=(ANY, ANY, VMEM), vmem=32 << 20,
    )


def fourth_kernel(
    n, cot, qko, nrm, cosine, sine, mask, cot_out, o_out, q_out, k_out, sco, w, ssem, rsem, local
):
    me, peer = place()
    t = lax.rem(me, TP)
    meet([peer(k) for k in range(1, TP)])
    sems = (ssem, rsem)
    share, cols = n // TP, o_out.shape[4]
    _, r, kh = q_out.shape
    half = kh // 2
    weights = pltpu.make_async_copy(qko.at[:, :, pl.ds(0, 2 * kh)], w, local.at[3])
    weights.start()
    gather = Gather(cot, cot_out, 0, cot.shape[0], sems, 0, local.at[0], peer)
    gather.start()
    copies, keeps = [], []

    def part(p, which):
        return qko.at[pl.ds(p * share, share), :, pl.ds(2 * kh + which * cols, cols)]

    for which in (0, 1):
        for k in range(1, TP):
            dev = peer(k)
            copy = remote(
                part(lax.rem(dev, TP), which), o_out.at[t, :, which], sems,
                GATHER_SEMS + which * TP + k, dev,
            )
            copy.start()
            copies.append(copy)
        keep = pltpu.make_async_copy(part(t, which), o_out.at[t, :, which], local.at[1 + which])
        keep.start()
        keeps.append(keep)
    weights.wait()

    def products(pairs):
        @pl.loop(*pairs)
        def _(j):
            rows = nrm[pl.ds(2 * j, 2)].reshape(2 * r, nrm.shape[2])
            for at, out in ((0, q_out), (kh, k_out)):
                y = jnp.dot(
                    rows, w[:, :, at : at + kh].reshape(nrm.shape[2], kh),
                    preferred_element_type=f32,
                )
                for i in (0, 1):
                    u, v = y[i * r : (i + 1) * r, :half], y[i * r : (i + 1) * r, half:]
                    cos, sin = cosine[2 * j + i], sine[2 * j + i]
                    out[2 * j + i, :, :half] = (u * cos - v * sin).astype(bf)
                    out[2 * j + i, :, half:] = (v * cos + u * sin).astype(bf)
            for i in (0, 1):
                plain = lax.dot_general(
                    q_out[2 * j + i], k_out[2 * j + i], (((1,), (1,)), ((), ())),
                    preferred_element_type=f32,
                )
                sco[2 * j + i] = (plain * mask[2 * j + i]).astype(bf)

    products((0, TP // 2))
    gather.forward()
    gather.finish()
    for copy in copies:
        copy.wait()
    for keep in keeps:
        keep.wait()


def fourth_exchange(n, cot, qko, nrm, cosine, sine, mask, cid):
    _, shard, width = qko.shape
    cols = (width - 2 * KH) // 2
    r = cot.shape[0]
    outs = (
        SDS((TP,) + cot.shape, bf),
        SDS((TP, n // TP, 2, shard, cols), bf),
        SDS((TP, r, KH), bf),
        SDS((TP, r, KH), bf),
        SDS(mask.shape, bf),
        SDS((n, shard, 2 * KH), bf),
    )
    kernel = functools.partial(fourth_kernel, n)
    return exchange_call(
        kernel, outs, (cot, qko, nrm, cosine, sine, mask),
        GATHER_SEMS + 2 * TP, 4, cid,
        specs=[VMEM, ANY, VMEM, VMEM, VMEM, VMEM],
        out_specs=(ANY, ANY, VMEM, VMEM, VMEM, VMEM), vmem=40 << 20,
    )


REDUCE_SEMS = 16
WIDE = 1024


class Reduce:
    def __init__(self, product, bufs, sems, base, peer, prepare=None, enter=None):
        self.product, self.prepare, self.sems, self.base = product, prepare, sems, base
        self.enter = enter
        self.po, self.pe, self.rc, self.sb, self.ring = bufs
        self.pc = peer(1)
        px, py = peer(2), peer(4)
        self.slots = ((0, 0, px), (1, 0, py), (0, 1, px), (1, 1, py), (1, 2, py), (0, 2, px))
        self.q = self.pe.shape[1] // 4
        self.waiting = True

    def core(self, i):
        return remote(self.po.at[i], self.rc.at[i], self.sems, self.base + i, self.pc)

    def link(self, c, slot):
        axis, at, dev = self.slots[slot]
        return remote(
            self.sb.at[c, slot], self.ring.at[axis, c, at], self.sems,
            self.base + 4 + 6 * c + slot, dev,
        )

    def add(self, halves, i, lower, out, more=None):
        step = 16
        steps = self.q // step
        first, count = halves

        @pl.loop(first * steps, (first + count) * steps)
        def _(j):
            c = lax.div(j, steps)
            there = pl.ds(pl.multiple_of(lax.rem(j, steps) * step, step), step)
            here = pl.ds(
                pl.multiple_of(lax.rem(j, steps) * step + (2 * c + lower) * self.q, step), step
            )
            total = self.pe[i, here, :].astype(f32) + self.rc[i, here, :].astype(f32)
            if more is not None:
                total = total + self.ring[more, c, 0, there, :].astype(f32)
            self.sb[c, out, there, :] = total.astype(bf)

    def both(self, slot, i, lower):
        self.add((0, 2), i, lower, slot)
        for c in (0, 1):
            self.link(c, slot).start()

    def six(self):
        self.core(3).wait_recv()
        self.both(0, 3, 0)
        self.both(1, 3, 1)

    def two(self):
        self.core(1).wait_recv()
        self.both(2, 1, 0)

    def four(self):
        self.core(2).wait_recv()
        self.both(3, 2, 1)

    def onward(self, c):
        self.link(c, 0).wait_recv()
        self.add((c, 1), 2, 0, 4, 0)
        self.link(c, 4).start()
        self.link(c, 1).wait_recv()
        self.add((c, 1), 1, 1, 5, 1)
        self.link(c, 5).start()

    def pair(self, it, i):
        self.product(it, i, self.po.at[i], self.pe.at[i])
        self.core(i).start()

    def run(self):
        if self.enter is not None:
            self.enter()

        @pl.loop(0, 4)
        def _(it):
            i = pair_at(it)
            if self.prepare is not None:
                self.prepare(it, i)
            else:
                self.pair(it, i)
            for k, stage in ((1, self.six), (2, self.two), (3, self.four)):
                pl.when(it == k)(stage)
            if self.prepare is not None:
                self.pair(it, i)

        for c in (0, 1):
            self.onward(c)

    def rows(self, c, step, body, unroll=2):
        if c == 0:
            self.core(0).wait_recv()
        for slot in (2, 3, 4, 5):
            self.link(c, slot).wait_recv()
        steps = self.q // step

        def some(j, _):
            lower = lax.div(j, steps)
            there = pl.ds(pl.multiple_of(lax.rem(j, steps) * step, step), step)
            here = pl.ds(pl.multiple_of(j * step + 2 * c * self.q, step), step)
            body(
                here,
                self.pe[0, here, :].astype(f32)
                + self.rc[0, here, :].astype(f32)
                + self.ring[lower, c, 1, there, :].astype(f32)
                + self.ring[1 - lower, c, 2, there, :].astype(f32),
            )
            return 0

        lax.fori_loop(0, 2 * steps, some, 0, unroll=unroll)

    def core_sent(self):
        for i in range(4):
            self.core(i).wait_send()
        self.waiting = False

    def finish(self):
        if self.waiting:
            self.core_sent()
        for c in (0, 1):
            for slot in range(6):
                self.link(c, slot).wait_send()


def pair_at(it):
    return it + 3 * (1 - lax.div(it + 2, 3)) - 3 * lax.div(it, 3)


class Load:
    def __init__(self, sems):
        self.sems, self.count = sems, 0

    def whole(self, src, dst):
        copy = pltpu.make_async_copy(src, dst, self.sems.at[self.count])
        self.count += 1
        copy.start()
        return copy.wait

    def paired(self, src, dst):
        base = self.count
        self.count += 4

        def piece(i):
            two = pl.ds(2 * i, 2)
            return pltpu.make_async_copy(src.at[two], dst.at[two], self.sems.at[base + i])

        return piece


def reduce_scratch(r, c, even=f32):
    q = r // 4
    return [
        pltpu.VMEM((4, r, c), bf),
        pltpu.VMEM((4, r, c), even),
        pltpu.VMEM((4, r, c), bf),
        pltpu.VMEM((2, 6, q, c), bf),
        pltpu.VMEM((2, 2, 3, q, c), bf),
    ]


def rows_of_pair(a, i):
    two, r, k = 2, a.shape[1], a.shape[2]
    return a[pl.ds(2 * i, two)].reshape(two * r, k)


def times(a, w, nt, arrive):
    def product(it, i, odd, even):
        r = a.shape[1]
        arrive(it, i)

        @pl.loop(0, even.shape[1] // WIDE)
        def _(j):
            at = pl.ds(pl.multiple_of(j * WIDE, WIDE), WIDE)
            x = rows_of_pair(a, i)
            if nt:
                y = lax.dot_general(
                    x, w[at, :], (((1,), (1,)), ((), ())), preferred_element_type=f32
                )
            else:
                y = jnp.dot(x, w[:, at], preferred_element_type=f32)
            even[:, at] = y[:r].astype(even.dtype)
            odd[:, at] = y[r:].astype(odd.dtype)

    return product


def exchange_and_gather(reduce, gathers, step, body, arrivals):
    reduce.run()
    for arrive in arrivals:
        arrive()
    for c in (0, 1):
        reduce.rows(c, step, body)
        gathers[c].start()
    for c in (0, 1):
        gathers[c].forward()
    for c in (0, 1):
        gathers[c].finish()
    reduce.finish()


def both_gathers(own, out, sems, local, peer):
    half = own.shape[0] // 2
    return [
        Gather(own, out, c * half, half, sems, REDUCE_SEMS + c * GATHER_SEMS, local.at[c], peer)
        for c in (0, 1)
    ]


EXCHANGE_SEMS = REDUCE_SEMS + 2 * GATHER_SEMS


def forward_kernel(
    nrm_in, wvs_in, sco, w_in, tok_in, vec, v_out, mix_out, ret_out, swi_out, mid, out,
    nrm, wvs, w, tok, v_buf, mix_buf, ret_buf, swi_buf, po, pe, rc, sb, ring, own,
    ssem, rsem, local, load,
):
    _, peer = place()
    enter = greet([peer(1), peer(2), peer(4)])
    sems = (ssem, rsem)
    r, width = v_buf.shape[1:]
    loads = Load(load)
    nrm_piece = loads.paired(nrm_in, nrm)
    nrm_piece(3).start()
    wvs_here = loads.whole(wvs_in, wvs)
    w_here = loads.whole(w_in, w)
    for i in (1, 2, 0):
        nrm_piece(i).start()
    tok_here = loads.whole(tok_in, tok)
    kept = ((v_buf, v_out), (mix_buf, mix_out), (ret_buf, ret_out), (swi_buf, swi_out))

    def keep(i):
        two = pl.ds(2 * i, 2)
        return [
            pltpu.make_async_copy(src.at[two], dst.at[two], local.at[2 + 4 * i + j])
            for j, (src, dst) in enumerate(kept)
        ]

    def prepare(it, i):
        first = 2 * i
        two = pl.ds(first, 2)
        pl.when(it == 0)(wvs_here)
        nrm_piece(i).wait()
        x = nrm[two].reshape(2 * r, nrm.shape[2])
        v = jnp.dot(x, wvs[:, :width], preferred_element_type=f32).astype(bf)
        v_buf[two] = v.reshape(2, r, width)
        for k in (0, 1):
            ret_buf[first + k] = jnp.dot(
                sco[first + k], v[k * r : (k + 1) * r], preferred_element_type=f32
            )
        s = jnp.dot(x, wvs[:, width:], preferred_element_type=f32)
        swi_buf[two] = s.reshape(2, r, width)

        def gated(j, _):
            k = first + lax.div(j, r // 32)
            at = pl.ds(pl.multiple_of(lax.rem(j, r // 32) * 32, 32), 32)
            value = ret_buf[k, at, :]
            centred = value - jnp.mean(value, axis=-1, keepdims=True)
            spread = jnp.mean(centred * centred, axis=-1, keepdims=True)
            gate = swi_buf[k, at, :]
            gate = gate / (1.0 + jnp.exp(-gate))
            mix_buf[k, at, :] = (
                gate * (centred * lax.rsqrt(jnp.maximum(spread, 0.25)))
            ).astype(bf)
            return 0

        lax.fori_loop(0, 2 * r // 32, gated, 0, unroll=4)
        for copy in keep(i):
            copy.start()

    def product(it, i, odd, even):
        step = w.shape[2]
        pl.when(it == 0)(w_here)

        def columns(j, _):
            at = pl.ds(pl.multiple_of(j * step, step), step)
            y = jnp.dot(rows_of_pair(mix_buf, i), w[j], preferred_element_type=f32)
            even[:, at] = y[:r].astype(even.dtype)
            odd[:, at] = y[r:].astype(odd.dtype)
            return 0

        lax.fori_loop(0, w.shape[0], columns, 0, unroll=4)

    def body(at, value):
        value = value + tok[at, :].astype(f32)
        mid[at, :] = value
        center = jnp.mean(value, axis=-1, keepdims=True)
        centred = value - center
        spread = jnp.mean(centred * centred, axis=-1, keepdims=True)
        own[at, :] = (
            centred * lax.rsqrt(spread + 1e-05) * vec[0:1, :] + vec[1:2, :]
        ).astype(bf)

    reduce = Reduce(product, (po, pe, rc, sb, ring), sems, 0, peer, prepare, enter)
    exchange_and_gather(reduce, both_gathers(own, out, sems, local, peer), 16, body, (tok_here,))
    for i in range(4):
        for copy in keep(i):
            copy.wait()


def forward_exchange(nrm, wvs, sco, w, tok, vec, cid):
    _, r, d = nrm.shape
    width = w.shape[1]
    count = EXCHANGE_SEMS
    blocks = [((TP, r, width), t) for t in (bf, bf, f32, f32)]
    return pl.pallas_call(
        forward_kernel,
        out_shape=tuple(SDS(*b) for b in blocks) + (SDS((r, d), f32), SDS((TP, r, d), bf)),
        in_specs=[ANY, ANY, VMEM, ANY, ANY, VMEM],
        out_specs=(ANY,) * 4 + (VMEM, ANY),
        scratch_shapes=[pltpu.VMEM(x.shape, x.dtype) for x in (nrm, wvs, w, tok)]
        + [pltpu.VMEM(*b) for b in blocks]
        + reduce_scratch(r, d)
        + [
            pltpu.VMEM((r, d), bf),
            pltpu.SemaphoreType.DMA((count,)),
            pltpu.SemaphoreType.DMA((count,)),
            pltpu.SemaphoreType.DMA((18,)),
            pltpu.SemaphoreType.DMA((7,)),
        ],
        compiler_params=pltpu.CompilerParams(
            collective_id=cid, has_side_effects=True, vmem_limit_bytes=60 << 20
        ),
        name="forward_exchange",
    )(nrm, wvs, sco, w, tok, vec)


def product_kernel(a, b, out):
    a, b = a[...].reshape(-1, a.shape[-1]), b[...].reshape(-1, b.shape[-1])
    out[...] = lax.dot_general(
        a, b, (((0,), (0,)), ((), ())), preferred_element_type=f32
    ).astype(bf)


def row_product(a, b):
    _, r, m = a.shape
    width = b.shape[2]
    tile, part = 512 if m >= 2048 else 256, min(width, 1024)
    return pl.pallas_call(
        product_kernel,
        grid=(width // part, m // tile),
        out_shape=SDS((m, width), bf),
        in_specs=[
            pl.BlockSpec((TP, r, tile), lambda j, i: (0, 0, i)),
            pl.BlockSpec((TP, r, part), lambda j, i: (0, 0, j)),
        ],
        out_specs=pl.BlockSpec((tile, part), lambda j, i: (i, j)),
        compiler_params=pltpu.CompilerParams(vmem_limit_bytes=56 << 20),
        cost_estimate=pl.CostEstimate(
            flops=2 * TP * r * m * width,
            bytes_accessed=2 * (a.size + b.size + m * width),
            transcendentals=0,
        ),
        name="row_product",
    )(a, b)


def hidden_kernel(x, gu, hid, act_out, slope_out):
    width = hid.shape[2]
    step = 256

    @pl.loop(0, width // step)
    def _(j):
        at = pl.ds(pl.multiple_of(j * step, step), step)
        behind = pl.ds(pl.multiple_of(j * step + width, step), step)
        rows = x[...].reshape(-1, x.shape[2])
        first = jnp.dot(rows, gu[:, at], preferred_element_type=f32)
        second = jnp.dot(rows, gu[:, behind], preferred_element_type=f32)
        share = 0.5 * (1.0 + lax.erf(first * math.sqrt(0.5)))
        act = first * share
        slope = share + first * (jnp.exp(-0.5 * first * first) * (1.0 / math.sqrt(2.0 * math.pi)))
        block = hid.shape[:2] + (step,)
        hid[:, :, at] = (act * second).astype(bf).reshape(block)
        act_out[:, :, at] = act.reshape(block)
        slope_out[:, :, at] = (slope * second).reshape(block)


def hidden_units(x, gu):
    _, r, d = x.shape
    width = gu.shape[1] // 2
    row = pl.BlockSpec((2, r, width), lambda k: (k, 0, 0))
    return pl.pallas_call(
        hidden_kernel,
        grid=(TP // 2,),
        out_shape=tuple(SDS((TP, r, width), t) for t in (bf, f32, f32)),
        in_specs=[
            pl.BlockSpec((2, r, d), lambda k: (k, 0, 0)),
            pl.BlockSpec(gu.shape, lambda k: (0, 0)),
        ],
        out_specs=(row, row, row),
        compiler_params=pltpu.CompilerParams(vmem_limit_bytes=56 << 20),
        cost_estimate=pl.CostEstimate(
            flops=4 * TP * r * d * width, bytes_accessed=24 << 20, transcendentals=2 * TP * r * width
        ),
        name="hidden_units",
    )(x, gu)


def hidden_back_kernel(cot, d0, d1, act, slope, out, down):
    width = act.shape[2]
    step = 256
    early, rows = d0.shape[1], d0.shape[1] + d1.shape[1]

    @pl.when(pl.program_id(0) == 0)
    def _():
        for g in range(d0.shape[0]):
            down[g * rows : g * rows + early] = d0[g]
            down[g * rows + early : (g + 1) * rows] = d1[g]

    @pl.loop(0, width // step)
    def _(j):
        at = pl.ds(pl.multiple_of(j * step, step), step)
        behind = pl.ds(pl.multiple_of(j * step + width, step), step)
        grad = lax.dot_general(
            cot[...].reshape(-1, cot.shape[2]), down[at, :], (((1,), (1,)), ((), ())),
            preferred_element_type=f32,
        ).reshape(act.shape[:2] + (step,))
        out[:, :, at] = (grad * slope[:, :, at]).astype(bf)
        out[:, :, behind] = (grad * act[:, :, at]).astype(bf)


def hidden_back(cot, d0, d1, act, slope):
    _, r, d = cot.shape
    width = act.shape[2]
    row = pl.BlockSpec((2, r, width), lambda k: (k, 0, 0))
    return pl.pallas_call(
        hidden_back_kernel,
        grid=(TP // 2,),
        out_shape=SDS((TP, r, 2 * width), bf),
        in_specs=[
            pl.BlockSpec((2, r, d), lambda k: (k, 0, 0)),
            pl.BlockSpec(d0.shape, lambda k: (0, 0, 0)),
            pl.BlockSpec(d1.shape, lambda k: (0, 0, 0)),
            row,
            row,
        ],
        scratch_shapes=[pltpu.VMEM((width, d), bf)],
        out_specs=pl.BlockSpec((2, r, 2 * width), lambda k: (k, 0, 0)),
        compiler_params=pltpu.CompilerParams(vmem_limit_bytes=56 << 20),
        cost_estimate=pl.CostEstimate(
            flops=2 * TP * r * d * width, bytes_accessed=24 << 20, transcendentals=0
        ),
        name="hidden_back",
    )(cot, d0, d1, act, slope)


def backward_kernel(
    a_in, w_in, mid_in, cot_in, vec, gmid, out, sums,
    a, w, mid, cot, po, pe, rc, sb, ring, own, acc, ssem, rsem, local, load,
):
    _, peer = place()
    enter = greet([peer(1), peer(2), peer(4)])
    sems = (ssem, rsem)
    loads = Load(load)
    piece = loads.paired(a_in, a)
    piece(3).start()
    w_here = loads.whole(w_in, w)
    for i in (1, 2, 0):
        piece(i).start()
    arrivals = (loads.whole(mid_in, mid), loads.whole(cot_in, cot))

    def arrive(it, i):
        pl.when(it == 0)(w_here)
        piece(i).wait()

    acc[...] = jnp.zeros_like(acc)

    def body(at, g):
        value = mid[at, :]
        center = jnp.mean(value, axis=-1, keepdims=True)
        centred = value - center
        inv = lax.rsqrt(jnp.mean(centred * centred, axis=-1, keepdims=True) + 1e-05)
        hat = centred * inv
        acc[0] += g * hat
        acc[1] += g
        scaled = g * vec[0:1, :]
        mean_g = jnp.mean(scaled, axis=-1, keepdims=True)
        mean_gh = jnp.mean(scaled * hat, axis=-1, keepdims=True)
        grad = cot[at, :].astype(f32) + inv * (scaled - mean_g - hat * mean_gh)
        gmid[at, :] = grad
        own[at, :] = grad.astype(bf)

    reduce = Reduce(
        times(a, w, True, arrive), (po, pe, rc, sb, ring), sems, 0, peer, enter=enter
    )
    exchange_and_gather(reduce, both_gathers(own, out, sems, local, peer), 16, body, arrivals)
    sums[0:1, :] = jnp.sum(acc[0], axis=0, keepdims=True)
    sums[1:2, :] = jnp.sum(acc[1], axis=0, keepdims=True)


def backward_exchange(a, w, mid, cot, vec, cid):
    _, r, _ = a.shape
    c = w.shape[0]
    count = EXCHANGE_SEMS
    return pl.pallas_call(
        backward_kernel,
        out_shape=(SDS((r, c), f32), SDS((TP, r, c), bf), SDS((2, c), f32)),
        in_specs=[ANY] * 4 + [VMEM],
        out_specs=(VMEM, ANY, VMEM),
        scratch_shapes=[pltpu.VMEM(x.shape, x.dtype) for x in (a, w, mid, cot)]
        + reduce_scratch(r, c)
        + [
            pltpu.VMEM((r, c), bf),
            pltpu.VMEM((2, 16, c), f32),
            pltpu.SemaphoreType.DMA((count,)),
            pltpu.SemaphoreType.DMA((count,)),
            pltpu.SemaphoreType.DMA((2,)),
            pltpu.SemaphoreType.DMA((7,)),
        ],
        compiler_params=pltpu.CompilerParams(
            collective_id=cid, has_side_effects=True, vmem_limit_bytes=52 << 20
        ),
        name="backward_exchange",
    )(a, w, mid, cot, vec)


def last_kernel(
    n, gqkv_in, gs_in, wqk_in, wvs_in, a2_in, d0, d1, tok_in, gmid_in, gain, sums2,
    gtok, ffn, vec_out, gqkv, gs, wqk, wvs, a2, w2, tok, gmid,
    po, pe, rc, sb, ring, pe2, rc2, sb2, ring2, acc, vecs, near, far, part, ssem, rsem, load,
):
    dp = n // TP
    me, peer = place()
    g = lax.div(me, TP)
    width = vec_out.shape[1]
    others = [lax.rem(me + TP * j, n) for j in range(1, dp)]
    enter = greet([peer(k) for k in range(1, TP)] + others)
    sems = (ssem, rsem)
    loads = Load(load)
    pieces = loads.paired(gqkv_in, gqkv), loads.paired(gs_in, gs)
    for piece in pieces:
        piece(3).start()
    weights = loads.whole(wqk_in, wqk), loads.whole(wvs_in, wvs)
    for i in (1, 2, 0):
        for piece in pieces:
            piece(i).start()
    second = [loads.whole(a2_in, a2)]
    early, rows = d0.shape[1], d0.shape[1] + d1.shape[1]
    for k in range(dp):
        second.append(loads.whole(d0.at[k], w2.at[pl.ds(k * rows, early)]))
        second.append(loads.whole(d1.at[k], w2.at[pl.ds(k * rows + early, rows - early)]))
    arrivals = loads.whole(tok_in, tok), loads.whole(gmid_in, gmid)

    def all_here(waits):
        def wait():
            for one in waits:
                one()

        return wait

    acc[...] = jnp.zeros_like(acc)
    nt = (((1,), (1,)), ((), ()))

    def product(it, i, odd, even):
        r, qk, v = gqkv.shape[1], wqk.shape[1], gs.shape[2]
        pl.when(it == 0)(all_here(weights))
        for piece in pieces:
            piece(i).wait()
        x, y = rows_of_pair(gqkv, i), rows_of_pair(gs, i)

        @pl.loop(0, even.shape[1] // WIDE)
        def _(j):
            at = pl.ds(pl.multiple_of(j * WIDE, WIDE), WIDE)
            z = lax.dot_general(x[:, :qk], wqk[at, :], nt, preferred_element_type=f32)
            z += lax.dot_general(x[:, qk:], wvs[at, :v], nt, preferred_element_type=f32)
            z += lax.dot_general(y, wvs[at, v:], nt, preferred_element_type=f32)
            even[:, at] = z[:r].astype(even.dtype)
            odd[:, at] = z[r:].astype(odd.dtype)

    one = Reduce(product, (po, pe, rc, sb, ring), sems, 0, peer, enter=enter)
    one.run()
    one.core_sent()

    def arrive(it, _):
        pl.when(it == 0)(all_here(second))

    two = Reduce(times(a2, w2, False, arrive), (po, pe2, rc2, sb2, ring2), sems, REDUCE_SEMS, peer)
    two.run()

    def body(at, grad):
        value = tok[at, :].astype(f32)
        center = jnp.mean(value, axis=-1, keepdims=True)
        centred = value - center
        inv = lax.rsqrt(jnp.mean(centred * centred, axis=-1, keepdims=True) + 1e-05)
        hat = centred * inv
        acc[0] += grad * hat
        acc[1] += grad
        scaled = grad * gain[...]
        mean_g = jnp.mean(scaled, axis=-1, keepdims=True)
        mean_gh = jnp.mean(scaled * hat, axis=-1, keepdims=True)
        gtok[at, :] = gmid[at, :] + inv * (scaled - mean_g - hat * mean_gh)

    all_here(arrivals)()
    for c in (0, 1):
        one.rows(c, 16, body)
    vecs[...] = jnp.zeros_like(vecs)
    vecs[0:1, :] = jnp.sum(acc[0], axis=0, keepdims=True)
    vecs[1:2, :] = jnp.sum(acc[1], axis=0, keepdims=True)
    vecs[2:4, :] = sums2[...]
    base = 2 * REDUCE_SEMS
    copies = []
    for j, dev in enumerate(others):
        at = pl.multiple_of(lax.div(dev, TP) * width, 128)
        copy = remote(vecs.at[:, pl.ds(at, width)], far.at[j], sems, base + j, dev)
        copy.start()
        copies.append(copy)

    def keep(at, value):
        ffn[at, :] = value

    two.rows(0, 16, keep)
    total = vecs[:, pl.ds(pl.multiple_of(g * width, 128), width)]
    for j, copy in enumerate(copies):
        copy.wait()
        total = total + far[j]
    part[...] = total
    copies = []
    for k in range(1, TP):
        copy = remote(part, near.at[k - 1], sems, base + dp + k - 1, peer(k))
        copy.start()
        copies.append(copy)
    two.rows(1, 16, keep)
    for k, copy in enumerate(copies):
        copy.wait()
        total = total + near[k]
    vec_out[...] = total
    one.finish()
    two.finish()


def last_exchange(n, gqkv, gs, wqk, wvs, a2, d0, d1, tok, gmid, gain, sums2, cid):
    dp = n // TP
    _, r, _ = a2.shape
    c = d0.shape[2]
    width = c // dp
    count = 2 * REDUCE_SEMS + dp + TP
    return pl.pallas_call(
        functools.partial(last_kernel, n),
        out_shape=(SDS((r, c), f32), SDS((r, c), f32), SDS((8, width), f32)),
        in_specs=[ANY] * 9 + [VMEM] * 2,
        out_specs=(VMEM,) * 3,
        scratch_shapes=[
            pltpu.VMEM(x.shape, x.dtype)
            for x in (gqkv, gs, wqk, wvs, a2, SDS((a2.shape[2], c), bf), tok, gmid)
        ]
        + reduce_scratch(r, c)
        + reduce_scratch(r, c, bf)[1:]
        + [
            pltpu.VMEM((2, 16, c), f32),
            pltpu.VMEM((8, c), f32),
            pltpu.VMEM((TP - 1, 8, width), f32),
            pltpu.VMEM((dp, 8, width), f32),
            pltpu.VMEM((8, width), f32),
            pltpu.SemaphoreType.DMA((count,)),
            pltpu.SemaphoreType.DMA((count,)),
            pltpu.SemaphoreType.DMA((13 + 2 * dp,)),
        ],
        compiler_params=pltpu.CompilerParams(
            collective_id=cid, has_side_effects=True, vmem_limit_bytes=ALL_VMEM
        ),
        name="last_exchange",
    )(gqkv, gs, wqk, wvs, a2, d0, d1, tok, gmid, gain, sums2)


def gate_back_kernel(g_low, w, ret, swi, gret, gswi, whole):
    cols = w.shape[2]

    @pl.when(pl.program_id(0) == 0)
    def _():
        for j in range(w.shape[0]):
            whole[:, j * cols : (j + 1) * cols] = w[j]

    two, r, _ = gret.shape
    grads = lax.dot_general(
        g_low[...].reshape(two * r, g_low.shape[2]), whole[...], (((1,), (1,)), ((), ())),
        preferred_element_type=f32,
    )
    for i in range(two):
        grad, value, gate = grads[i * r : (i + 1) * r], ret[i], swi[i]
        centred = value - jnp.mean(value, axis=-1, keepdims=True)
        spread = jnp.mean(centred * centred, axis=-1, keepdims=True)
        inv = lax.rsqrt(jnp.maximum(spread, 0.25))
        share = 1.0 / (1.0 + jnp.exp(-gate))
        silu = gate * share
        gswi[i] = (grad * (centred * inv) * (share * (1.0 + gate * (1.0 - share)))).astype(bf)
        grad = grad * silu
        pull = jnp.mean(grad * centred, axis=-1, keepdims=True)
        pull = jnp.where(spread > 0.25, inv * inv * inv * pull, 0.0)
        grad = grad * inv - centred * pull
        gret[i] = (grad - jnp.mean(grad, axis=-1, keepdims=True)).astype(bf)


def gate_back(g_low, w, ret, swi):
    _, r, d = g_low.shape
    width = ret.shape[2]
    row = pl.BlockSpec((2, r, width), lambda k: (k, 0, 0))
    return pl.pallas_call(
        gate_back_kernel,
        grid=(TP // 2,),
        out_shape=(SDS(ret.shape, bf), SDS(ret.shape, bf)),
        in_specs=[
            pl.BlockSpec((2, r, d), lambda k: (k, 0, 0)),
            pl.BlockSpec(w.shape, lambda k: (0, 0, 0)),
            row,
            row,
        ],
        out_specs=(row, row),
        scratch_shapes=[pltpu.VMEM((width, d), bf)],
        compiler_params=pltpu.CompilerParams(vmem_limit_bytes=56 << 20),
        cost_estimate=pl.CostEstimate(
            flops=2 * TP * r * d * width, bytes_accessed=22 << 20, transcendentals=TP * r * width
        ),
        name="gate_back",
    )(g_low, w, ret, swi)


def scores_back_kernel(sco, mask, q, k, v, gret, cosine, sine, out):
    nt, tn = (((1,), (1,)), ((), ())), (((0,), (0,)), ((), ()))
    kh = q.shape[2]
    half = kh // 2
    out[0, :, 2 * kh :] = lax.dot_general(
        sco[0], gret[0], tn, preferred_element_type=f32
    ).astype(bf)
    grad = lax.dot_general(gret[0], v[0], nt, preferred_element_type=f32)
    grad = (grad * mask[0]).astype(bf)
    gq = jnp.dot(grad, k[0], preferred_element_type=f32)
    gk = lax.dot_general(grad, q[0], tn, preferred_element_type=f32)
    for i, g in enumerate((gq, gk)):
        u, w = g[:, :half], g[:, half:]
        at = i * kh
        out[0, :, at : at + half] = (u * cosine[0] + w * sine[0]).astype(bf)
        out[0, :, at + half : at + kh] = (w * cosine[0] - u * sine[0]).astype(bf)


def scores_back(sco, mask, q, k, v, gret, cosine, sine):
    _, r, kh = q.shape
    arrays = (sco, mask, q, k, v, gret, cosine, sine)
    width = 2 * kh + v.shape[2]
    spec = [pl.BlockSpec((1,) + x.shape[1:], lambda i: (i, 0, 0)) for x in arrays]
    return pl.pallas_call(
        scores_back_kernel,
        grid=(TP,),
        out_shape=SDS((TP, r, width), bf),
        in_specs=spec,
        out_specs=pl.BlockSpec((1, r, width), lambda i: (i, 0, 0)),
        compiler_params=pltpu.CompilerParams(vmem_limit_bytes=56 << 20),
        cost_estimate=pl.CostEstimate(
            flops=4 * TP * r * r * (kh + v.shape[2]), bytes_accessed=16 << 20, transcendentals=0
        ),
        name="scores_back",
    )(*arrays)


def spread_kernel(a, b, out, turned, made, ssem, rsem, local):
    me, peer = place()
    t = lax.rem(me, TP)
    first = me - t
    place_of, low = lax.div(t, 2), lax.rem(t, 2)
    sems = (ssem, rsem)
    enter = greet([peer(k) for k in range(1, TP)])
    turned[...] = a[...].reshape(-1, a.shape[2]).T
    rows, tile = out.shape[1], 512
    enter()
    copies = []
    for j in range(out.shape[2] // tile):
        at = pl.ds(j * tile, tile)
        made[:, at] = jnp.dot(
            turned[...], b[:, :, at].reshape(turned.shape[1], tile), preferred_element_type=f32
        ).astype(bf)
        for m in range(4):
            chunk = lax.rem(place_of + m, 4)
            dev = first + 4 * low + chunk
            src = made.at[pl.ds(pl.multiple_of(chunk * rows, rows), rows), at]
            dst = out.at[place_of, :, at]
            i = 4 * j + m
            away = remote(src, dst, sems, i, dev)
            here = pltpu.make_async_copy(src, dst, local.at[i])
            pl.when(dev != me)(away.start)
            pl.when(dev == me)(here.start)
            copies.append((dev, away, here))
    for dev, away, here in copies:
        pl.when(dev != me)(away.wait)
        pl.when(dev == me)(here.wait)


def spread_product(a, b, cid):
    _, r, m = a.shape
    width = b.shape[2]
    count = 4 * (width // 512)
    return pl.pallas_call(
        spread_kernel,
        out_shape=SDS((4, m // 4, width), bf),
        in_specs=[VMEM, VMEM],
        out_specs=ANY,
        scratch_shapes=[
            pltpu.VMEM((m, TP * r), bf),
            pltpu.VMEM((m, width), bf),
            pltpu.SemaphoreType.DMA((count,)),
            pltpu.SemaphoreType.DMA((count,)),
            pltpu.SemaphoreType.DMA((count,)),
        ],
        compiler_params=pltpu.CompilerParams(
            collective_id=cid, has_side_effects=True, vmem_limit_bytes=32 << 20
        ),
        name="spread_product",
    )(a, b)


def tp_groups(n):
    return [[g * TP + t for t in range(TP)] for g in range(n // TP)]


def dp_groups(n):
    return [[g * TP + t for g in range(n // TP)] for t in range(TP)]


def plane_a2a(x, n):
    return lax.all_to_all(x, AXIS, 0, 0, axis_index_groups=tp_groups(n), tiled=True)


def dp_gather(x, n):
    return lax.all_gather(x, AXIS, axis=0, tiled=True, axis_index_groups=dp_groups(n))


def dp_reduce(x, n):
    return lax.psum_scatter(
        x, AXIS, scatter_dimension=0, tiled=True, axis_index_groups=dp_groups(n)
    )


def seq_positions(lengths, rows):
    ends = jnp.cumsum(lengths, axis=1)
    starts = ends - lengths
    index = jnp.arange(rows, dtype=jnp.int32)
    segment = jnp.sum((index[None, :, None] >= ends[:, None, :]).astype(jnp.int32), axis=2)
    member = segment[:, :, None] == jnp.arange(lengths.shape[1], dtype=jnp.int32)
    offset = index[None, :] - jnp.sum(jnp.where(member, starts[:, None, :], 0), axis=2)
    return segment, offset


def rotary_tables(offset):
    half = KH // 2
    freq = jnp.exp(-math.log(10000.0) * jnp.arange(half, dtype=f32) / half)
    angle = offset.astype(f32)[..., None] * freq
    return jnp.cos(angle), jnp.sin(angle)


def decay_mask(segment, offset, head):
    diff = offset[:, :, None] - offset[:, None, :]
    valid = (segment[:, :, None] == segment[:, None, :]) & (diff >= 0)
    steps = jnp.where(valid, diff, 0).astype(f32)
    log = jnp.log(1.0 - jnp.exp2(-5.0 - head.astype(f32)))
    return jnp.where(valid, jnp.exp(log * steps), 0.0) / math.sqrt(KH)


def col_blocks(w):
    r, c = w.shape
    return w.reshape(r, TP, c // TP).transpose(1, 0, 2).reshape(TP * r, c // TP)


def join_kernel(widths, parts, x, *outs):
    at = 0
    for out, width in zip(outs, widths):
        piece = width // parts
        for t in range(TP):
            for p in range(parts):
                to = (p * TP + t) * piece
                out[:, to : to + piece] = x[t, :, at + p * piece : at + (p + 1) * piece].astype(f32)
        at += width


def join(x, widths, parts=1):
    r = x.shape[1]
    if any(width // parts % 128 for width in widths):
        made, at = [], 0
        for width in widths:
            part = x[:, :, at : at + width].reshape(TP, r, parts, width // parts)
            made.append(part.transpose(1, 2, 0, 3).reshape(r, TP * width).astype(f32))
            at += width
        return made
    return pl.pallas_call(
        functools.partial(join_kernel, widths, parts),
        out_shape=tuple(SDS((r, TP * width), f32) for width in widths),
        in_specs=[VMEM],
        out_specs=tuple(VMEM for _ in widths),
        compiler_params=pltpu.CompilerParams(vmem_limit_bytes=8 << 20),
        cost_estimate=pl.CostEstimate(flops=0, bytes_accessed=6 * x.size, transcendentals=0),
        name="join",
    )(x)


def after(x, *deps):
    return lax.optimization_barrier((x,) + deps)[0]


def on_device(n, tokens, lengths, gain1, bias1, wq, wk, wv, ws, wo, gain2, bias2, wg, wu, wd, cot):
    rows, d = tokens.shape
    ff = wg.shape[1]
    dp = n // TP
    shard = d // n
    unit = ff // n
    me = lax.axis_index(AXIS)
    head = lax.rem(me, TP)

    def ff_blocks(w):
        return w.reshape(shard, dp, TP, unit).transpose(2, 0, 1, 3).reshape(TP, shard, dp * unit)

    lens = jnp.pad(lengths[0].astype(f32), (0, shard - lengths.shape[1]))
    vec = jnp.stack([v.astype(f32) for v in (gain1, bias1, gain2, bias2)] + [lens])
    vec = jnp.pad(vec, ((0, 3), (0, 128 - shard)))
    early = max(16, wd.shape[0] // 4)
    qko_blk, d0 = first_exchange(n, wq, wk, wo, wd[:early], 1)
    qko = dp_gather(qko_blk.reshape(TP * shard, 4 * KH), n)
    tok_all, vec_all = second_exchange(n, after(tokens, qko_blk), vec, 2)
    gain1f, bias1f, gain2f, bias2f = (
        vec_all[:, :, i, :shard].reshape(1, d) for i in range(4)
    )
    vec2 = jnp.concatenate([gain2f, bias2f], axis=0)
    gu_in = jnp.concatenate([ff_blocks(wg), ff_blocks(wu)], axis=2)
    vs_blk, gu_blk, normed = third_exchange(wv, ws, gu_in, tok_all, gain1f, bias1f, 3)
    vs = dp_gather(vs_blk.reshape(TP * shard, 2 * VH), n)
    gu = dp_gather(gu_blk.reshape(TP * shard, 2 * dp * unit), n)
    down = d0, dp_gather(wd[early:], n).reshape(dp, wd.shape[0] - early, d)

    mine = lax.dynamic_slice_in_dim(vec_all, lax.div(me, TP), 1, 0)[0, :, 4, :3]
    order = jnp.arange(TP, dtype=jnp.int32)
    pick = (order[None, :] == (order[:, None] ^ head)).astype(f32)
    len_all = jnp.sum(pick[:, :, None] * mine[None], axis=1).astype(jnp.int32)
    segment, offset = seq_positions(len_all, rows)
    cosine, sine = rotary_tables(offset)
    mask = decay_mask(segment, offset, head)

    cot_all, out_blk, q_rot, k_rot, scores, qk = fourth_exchange(
        n, cot, qko.reshape(n, shard, 4 * KH), normed, cosine, sine, mask, 4
    )
    out_blk = out_blk.reshape(TP, VH, d // TP)
    qk = qk.reshape(d, 2 * KH)
    v_low, mixed, retained, swish_in, middle, normed2 = forward_exchange(
        normed, vs, scores, out_blk, tokens, vec2, 5
    )
    hidden, act, slope = hidden_units(normed2, gu)
    down_grad = row_product(hidden, cot_all)
    g_down = dp_reduce(down_grad, n)

    g_fs = hidden_back(cot_all, *down, act, slope)
    gu_grad = row_product(normed2, g_fs)
    g_gu = dp_reduce(gu_grad, n)
    g_middle, g_low, sums2 = backward_exchange(g_fs, gu, middle, cot, vec2, 6)

    g_retained, g_swish = gate_back(g_low, out_blk, retained, swish_in)
    swish_grad = row_product(normed, g_swish)
    g_swi = dp_reduce(swish_grad, n)
    spread = wo.shape[0] * HEADS == VH * 2
    if spread:
        out_grad = spread_product(mixed, g_low, 8).reshape(VH, d)
    else:
        out_grad = row_product(mixed, g_low)
        out_grad = plane_a2a(col_blocks(out_grad), n)
    g_qkv = scores_back(scores, mask, q_rot, k_rot, v_low, g_retained, cosine, sine)
    qkv_grad = row_product(normed, g_qkv)
    g_qkv_own = dp_reduce(qkv_grad, n)
    g_out = dp_reduce(out_grad, n)
    grad_tokens, ffn, g_vecs = last_exchange(
        n, g_qkv, g_swish, qk, vs, hidden, *down, tokens, g_middle, gain1f, sums2, 7
    )
    layer_out = (middle + ffn).astype(bf)

    g_vecs = lax.dynamic_slice_in_dim(g_vecs, head * shard, shard, 1)
    grad_d = g_down.astype(f32)
    g_gu = plane_a2a(g_gu, n)
    grad_g, grad_u = join(g_gu.reshape(TP, shard, 2 * dp * unit), (dp * unit,) * 2, dp)
    g_swi = plane_a2a(g_swi, n)
    (grad_s,) = join(g_swi.reshape(TP, shard, VH), (VH,))
    g_qkv_own = plane_a2a(g_qkv_own, n)
    grad_q, grad_k, grad_v = join(g_qkv_own.reshape(TP, shard, 2 * KH + VH), (KH, KH, VH))
    if spread:
        grad_o = g_out.astype(f32)
    else:
        g_out = plane_a2a(g_out, n)
        (grad_o,) = join(g_out.reshape(TP, wo.shape[0], d // TP), (d // TP,))
    return (
        layer_out, grad_tokens, g_vecs[0], g_vecs[1], grad_q, grad_k, grad_v, grad_s, grad_o,
        g_vecs[2], g_vecs[3], grad_g, grad_u, grad_d,
    )


def solution(mesh):
    n = mesh.shape[AXIS]
    row, vec = P(AXIS, None), P(AXIS)
    ins = (row, row, vec, vec, row, row, row, row, row, vec, vec, row, row, row, row)
    outs = (row, row, vec, vec, row, row, row, row, row, vec, vec, row, row, row)

    def body(*args):
        return on_device(n, *args)

    return jax.shard_map(body, mesh=mesh, in_specs=ins, out_specs=outs, check_vma=False)
```

```python
import functools
import math

import jax
import jax.numpy as jnp
from jax import lax
from jax.experimental import pallas as pl
from jax.experimental.pallas import tpu as pltpu
from jax.sharding import PartitionSpec as P


HEADS = 8
KH = 256
VH = 512
TP = 8
AXIS = "fsdp"
MESH = pl.DeviceIdType.MESH
ANY = pl.BlockSpec(memory_space=pl.ANY)
VMEM = pl.BlockSpec(memory_space=pltpu.VMEM)
bf = jnp.bfloat16
f32 = jnp.float32
SDS = jax.ShapeDtypeStruct
ALL_VMEM = 67043328


def place():
    me = lax.axis_index(AXIS)
    steps = [s - 2 * s * lax.rem(lax.div(me, s), 2) for s in (1, 2, 4)]

    def peer(k):
        out = me
        for bit, step in enumerate(steps):
            if k >> bit & 1:
                out = out + step
        return out

    return me, peer


def greet(peers):
    barrier = pltpu.get_barrier_semaphore()
    for p in peers:
        pl.semaphore_signal(barrier, inc=1, device_id=(p,), device_id_type=MESH)
    return lambda: pl.semaphore_wait(barrier, len(peers))


def meet(peers):
    greet(peers)()


def remote(src, dst, sems, i, dev):
    return pltpu.make_async_remote_copy(
        src_ref=src, dst_ref=dst, send_sem=sems[0].at[i], recv_sem=sems[1].at[i],
        device_id=(dev,), device_id_type=MESH,
    )


GATHER_SEMS = 13


class Gather:
    def __init__(self, own, out, start, size, sems, base, local, peer):
        self.own, self.out, self.sems, self.base, self.local = own, out, sems, base, local
        h = size // 2
        self.all, self.top, self.bot = pl.ds(start, size), pl.ds(start, h), pl.ds(start + h, h)
        self.pc, self.px, self.py = peer(1), peer(2), peer(4)
        self.made = []

    def send(self, src, dst, dev):
        copy = remote(src, dst, self.sems, self.base + len(self.made), dev)
        copy.start()
        self.made.append(copy)
        return copy

    def pass_on(self, k, at):
        self.core.append(self.send(self.out.at[k, at], self.out.at[k + 1, at], self.pc))

    def start(self):
        own, out, top, bot = self.own, self.out, self.top, self.bot
        self.x0 = self.send(own.at[bot], out.at[2, bot], self.px)
        self.y0 = self.send(own.at[top], out.at[4, top], self.py)
        self.x1 = self.send(own.at[top], out.at[2, top], self.px)
        self.y1 = self.send(own.at[bot], out.at[4, bot], self.py)
        self.core = [self.send(own.at[self.all], out.at[1, self.all], self.pc)]
        self.keep = pltpu.make_async_copy(own.at[self.all], out.at[0, self.all], self.local)
        self.keep.start()

    def forward(self):
        out, top, bot = self.out, self.top, self.bot
        self.x0.wait_recv()
        self.fy = self.send(out.at[2, bot], out.at[6, bot], self.py)
        self.pass_on(2, bot)
        self.y0.wait_recv()
        self.fx = self.send(out.at[4, top], out.at[6, top], self.px)
        self.pass_on(4, top)
        self.x1.wait_recv()
        self.pass_on(2, top)
        self.y1.wait_recv()
        self.pass_on(4, bot)

    def finish(self):
        self.fy.wait_recv()
        self.pass_on(6, self.bot)
        self.fx.wait_recv()
        self.pass_on(6, self.top)
        for copy in self.core:
            copy.wait_recv()
        for copy in self.made:
            copy.wait_send()
        self.keep.wait()


def send_columns(src, out, cols, at, sems, base, local, t, peer, rows=None):
    copies = []
    rows = slice(None) if rows is None else rows

    def block(q):
        if len(src.shape) == 3:
            return src.at[q]
        return src.at[rows, pl.ds(pl.multiple_of(q * cols, 128), cols)]

    for k in range(1, TP):
        dev = peer(k)
        copy = remote(
            block(lax.rem(dev, TP)), out.at[t, :, pl.ds(at, cols)], sems, base + k - 1, dev
        )
        copy.start()
        copies.append(copy)
    keep = pltpu.make_async_copy(block(t), out.at[t, :, pl.ds(at, cols)], local)
    keep.start()
    return copies, keep


def finish(parts):
    for copies, keep in parts:
        for copy in copies:
            copy.wait()
        keep.wait()


def exchange_call(
    kernel, outs, args, sems, locals_, cid, specs=None, out_specs=None, vmem=12 << 20
):
    return pl.pallas_call(
        kernel,
        out_shape=outs,
        in_specs=specs or [VMEM] * len(args),
        out_specs=out_specs or tuple(ANY for _ in outs),
        scratch_shapes=[
            pltpu.SemaphoreType.DMA((sems,)),
            pltpu.SemaphoreType.DMA((sems,)),
            pltpu.SemaphoreType.DMA((locals_,)),
        ],
        compiler_params=pltpu.CompilerParams(
            collective_id=cid, has_side_effects=True, vmem_limit_bytes=vmem
        ),
    )(*args)


def first_kernel(n, wq, wk, wo, wd, out, wd_out, ssem, rsem, local):
    me, peer = place()
    t, g = lax.rem(me, TP), lax.div(me, TP)
    others = others_along(n)
    meet([peer(k) for k in range(1, TP)] + others)
    sems = (ssem, rsem)
    shard, cq, co = wq.shape[0], wq.shape[1] // TP, wo.shape[1] // TP
    low, high = pl.ds(0, shard), pl.ds(shard, shard)
    wd = wd.at[pl.ds(0, wd_out.shape[1])]
    along = [remote(wd, wd_out.at[g], sems, 28 + j, dev) for j, dev in enumerate(others)]
    for copy in along:
        copy.start()
    keep = pltpu.make_async_copy(wd, wd_out.at[g], local.at[4])
    keep.start()
    finish([
        send_columns(wq, out, cq, 0, sems, 0, local.at[0], t, peer),
        send_columns(wk, out, cq, cq, sems, 7, local.at[1], t, peer),
        send_columns(wo, out, co, 2 * cq, sems, 14, local.at[2], t, peer, low),
        send_columns(wo, out, co, 2 * cq + co, sems, 21, local.at[3], t, peer, high),
        (along, keep),
    ])


def first_exchange(n, wq, wk, wo, wd, early, cid):
    width = 2 * wq.shape[1] // TP + 2 * wo.shape[1] // TP
    outs = (SDS((TP, wq.shape[0], width), bf), SDS((n // TP, early, wd.shape[1]), bf))
    kernel = functools.partial(first_kernel, n)
    return exchange_call(kernel, outs, (wq, wk, wo, wd), 28 + n // TP, 5, cid)


def others_along(n):
    me = lax.axis_index(AXIS)
    return [lax.rem(me + TP * j, n) for j in range(1, n // TP)]


def second_kernel(n, tok, vec, tok_out, vec_out, ssem, rsem, local):
    me, peer = place()
    t, g = lax.rem(me, TP), lax.div(me, TP)
    others = others_along(n)
    meet([peer(k) for k in range(1, TP)] + others)
    sems = (ssem, rsem)
    base = GATHER_SEMS
    far = []
    keep = pltpu.make_async_copy(vec, vec_out.at[g, t], local.at[1])
    keep.start()
    for j, dev in enumerate(others):
        copy = remote(vec, vec_out.at[g, t], sems, base + TP + j, dev)
        copy.start()
        far.append(copy)
    gather = Gather(tok, tok_out, 0, tok.shape[0], sems, 0, local.at[0], peer)
    gather.start()
    for copy in far:
        copy.wait()
    keep.wait()
    near = []
    for k in range(1, TP):
        copy = remote(vec_out.at[:, t], vec_out.at[:, t], sems, base + k, peer(k))
        copy.start()
        near.append(copy)
    gather.forward()
    gather.finish()
    for copy in near:
        copy.wait()


def second_exchange(n, tok, vec, cid):
    outs = (SDS((TP,) + tok.shape, bf), SDS((n // TP, TP) + vec.shape, f32))
    kernel = functools.partial(second_kernel, n)
    sems = GATHER_SEMS + TP + n // TP
    return exchange_call(kernel, outs, (tok, vec), sems, 2, cid)


def third_kernel(wv, ws, gu, tok, gain, bias, out, gu_out, nrm, ssem, rsem, local):
    me, peer = place()
    t = lax.rem(me, TP)
    meet([peer(k) for k in range(1, TP)])
    sems = (ssem, rsem)
    cols = wv.shape[1] // TP
    parts = [
        send_columns(wv, out, cols, 0, sems, 0, local.at[0], t, peer),
        send_columns(ws, out, cols, cols, sems, 7, local.at[1], t, peer),
        send_columns(gu, gu_out, gu.shape[2], 0, sems, 14, local.at[2], t, peer),
    ]
    step, r = 16, tok.shape[1]

    def norm(j, _):
        k = lax.div(j, r // step)
        at = pl.ds(pl.multiple_of(lax.rem(j, r // step) * step, step), step)
        value = tok[k, at, :].astype(f32)
        centred = value - jnp.mean(value, axis=-1, keepdims=True)
        spread = jnp.mean(centred * centred, axis=-1, keepdims=True)
        nrm[k, at, :] = (centred * lax.rsqrt(spread + 1e-05) * gain[...] + bias[...]).astype(bf)
        return 0

    lax.fori_loop(0, TP * r // step, norm, 0, unroll=4)
    finish(parts)


def third_exchange(wv, ws, gu, tok, gain, bias, cid):
    outs = (
        SDS((TP, wv.shape[0], 2 * wv.shape[1] // TP), bf),
        SDS(gu.shape, bf),
        SDS(tok.shape, bf),
    )
    return exchange_call(
        third_kernel, outs, (wv, ws, gu, tok, gain, bias), 21, 3, cid,
        out_specs=(ANY, ANY, VMEM), vmem=32 << 20,
    )


def fourth_kernel(
    n, cot, qko, nrm, cosine, sine, mask, cot_out, o_out, q_out, k_out, sco, w, ssem, rsem, local
):
    me, peer = place()
    t = lax.rem(me, TP)
    meet([peer(k) for k in range(1, TP)])
    sems = (ssem, rsem)
    share, cols = n // TP, o_out.shape[4]
    _, r, kh = q_out.shape
    half = kh // 2
    weights = pltpu.make_async_copy(qko.at[:, :, pl.ds(0, 2 * kh)], w, local.at[3])
    weights.start()
    gather = Gather(cot, cot_out, 0, cot.shape[0], sems, 0, local.at[0], peer)
    gather.start()
    copies, keeps = [], []

    def part(p, which):
        return qko.at[pl.ds(p * share, share), :, pl.ds(2 * kh + which * cols, cols)]

    for which in (0, 1):
        for k in range(1, TP):
            dev = peer(k)
            copy = remote(
                part(lax.rem(dev, TP), which), o_out.at[t, :, which], sems,
                GATHER_SEMS + which * TP + k, dev,
            )
            copy.start()
            copies.append(copy)
        keep = pltpu.make_async_copy(part(t, which), o_out.at[t, :, which], local.at[1 + which])
        keep.start()
        keeps.append(keep)
    weights.wait()

    def products(pairs):
        @pl.loop(*pairs)
        def _(j):
            rows = nrm[pl.ds(2 * j, 2)].reshape(2 * r, nrm.shape[2])
            for at, out in ((0, q_out), (kh, k_out)):
                y = jnp.dot(
                    rows, w[:, :, at : at + kh].reshape(nrm.shape[2], kh),
                    preferred_element_type=f32,
                )
                for i in (0, 1):
                    u, v = y[i * r : (i + 1) * r, :half], y[i * r : (i + 1) * r, half:]
                    cos, sin = cosine[2 * j + i], sine[2 * j + i]
                    out[2 * j + i, :, :half] = (u * cos - v * sin).astype(bf)
                    out[2 * j + i, :, half:] = (v * cos + u * sin).astype(bf)
            for i in (0, 1):
                plain = lax.dot_general(
                    q_out[2 * j + i], k_out[2 * j + i], (((1,), (1,)), ((), ())),
                    preferred_element_type=f32,
                )
                sco[2 * j + i] = (plain * mask[2 * j + i]).astype(bf)

    products((0, TP // 2))
    gather.forward()
    gather.finish()
    for copy in copies:
        copy.wait()
    for keep in keeps:
        keep.wait()


def fourth_exchange(n, cot, qko, nrm, cosine, sine, mask, cid):
    _, shard, width = qko.shape
    cols = (width - 2 * KH) // 2
    r = cot.shape[0]
    outs = (
        SDS((TP,) + cot.shape, bf),
        SDS((TP, n // TP, 2, shard, cols), bf),
        SDS((TP, r, KH), bf),
        SDS((TP, r, KH), bf),
        SDS(mask.shape, bf),
        SDS((n, shard, 2 * KH), bf),
    )
    kernel = functools.partial(fourth_kernel, n)
    return exchange_call(
        kernel, outs, (cot, qko, nrm, cosine, sine, mask),
        GATHER_SEMS + 2 * TP, 4, cid,
        specs=[VMEM, ANY, VMEM, VMEM, VMEM, VMEM],
        out_specs=(ANY, ANY, VMEM, VMEM, VMEM, VMEM), vmem=40 << 20,
    )


REDUCE_SEMS = 16
WIDE = 1024


class Reduce:
    def __init__(self, product, bufs, sems, base, peer, prepare=None, enter=None):
        self.product, self.prepare, self.sems, self.base = product, prepare, sems, base
        self.enter = enter
        self.po, self.pe, self.rc, self.sb, self.ring = bufs
        self.pc = peer(1)
        px, py = peer(2), peer(4)
        self.slots = ((0, 0, px), (1, 0, py), (0, 1, px), (1, 1, py), (1, 2, py), (0, 2, px))
        self.q = self.pe.shape[1] // 4
        self.waiting = True

    def core(self, i):
        return remote(self.po.at[i], self.rc.at[i], self.sems, self.base + i, self.pc)

    def link(self, c, slot):
        axis, at, dev = self.slots[slot]
        return remote(
            self.sb.at[c, slot], self.ring.at[axis, c, at], self.sems,
            self.base + 4 + 6 * c + slot, dev,
        )

    def add(self, halves, i, lower, out, more=None):
        step = 16
        steps = self.q // step
        first, count = halves

        @pl.loop(first * steps, (first + count) * steps)
        def _(j):
            c = lax.div(j, steps)
            there = pl.ds(pl.multiple_of(lax.rem(j, steps) * step, step), step)
            here = pl.ds(
                pl.multiple_of(lax.rem(j, steps) * step + (2 * c + lower) * self.q, step), step
            )
            total = self.pe[i, here, :].astype(f32) + self.rc[i, here, :].astype(f32)
            if more is not None:
                total = total + self.ring[more, c, 0, there, :].astype(f32)
            self.sb[c, out, there, :] = total.astype(bf)

    def both(self, slot, i, lower):
        self.add((0, 2), i, lower, slot)
        for c in (0, 1):
            self.link(c, slot).start()

    def six(self):
        self.core(3).wait_recv()
        self.both(0, 3, 0)
        self.both(1, 3, 1)

    def two(self):
        self.core(1).wait_recv()
        self.both(2, 1, 0)

    def four(self):
        self.core(2).wait_recv()
        self.both(3, 2, 1)

    def onward(self, c):
        self.link(c, 0).wait_recv()
        self.add((c, 1), 2, 0, 4, 0)
        self.link(c, 4).start()
        self.link(c, 1).wait_recv()
        self.add((c, 1), 1, 1, 5, 1)
        self.link(c, 5).start()

    def pair(self, it, i):
        self.product(it, i, self.po.at[i], self.pe.at[i])
        self.core(i).start()

    def run(self):
        if self.enter is not None:
            self.enter()

        @pl.loop(0, 4)
        def _(it):
            i = pair_at(it)
            if self.prepare is not None:
                self.prepare(it, i)
            else:
                self.pair(it, i)
            for k, stage in ((1, self.six), (2, self.two), (3, self.four)):
                pl.when(it == k)(stage)
            if self.prepare is not None:
                self.pair(it, i)

        for c in (0, 1):
            self.onward(c)

    def rows(self, c, step, body, unroll=2):
        if c == 0:
            self.core(0).wait_recv()
        for slot in (2, 3, 4, 5):
            self.link(c, slot).wait_recv()
        steps = self.q // step

        def some(j, _):
            lower = lax.div(j, steps)
            there = pl.ds(pl.multiple_of(lax.rem(j, steps) * step, step), step)
            here = pl.ds(pl.multiple_of(j * step + 2 * c * self.q, step), step)
            body(
                here,
                self.pe[0, here, :].astype(f32)
                + self.rc[0, here, :].astype(f32)
                + self.ring[lower, c, 1, there, :].astype(f32)
                + self.ring[1 - lower, c, 2, there, :].astype(f32),
            )
            return 0

        lax.fori_loop(0, 2 * steps, some, 0, unroll=unroll)

    def core_sent(self):
        for i in range(4):
            self.core(i).wait_send()
        self.waiting = False

    def finish(self):
        if self.waiting:
            self.core_sent()
        for c in (0, 1):
            for slot in range(6):
                self.link(c, slot).wait_send()


def pair_at(it):
    return it + 3 * (1 - lax.div(it + 2, 3)) - 3 * lax.div(it, 3)


class Load:
    def __init__(self, sems):
        self.sems, self.count = sems, 0

    def whole(self, src, dst):
        copy = pltpu.make_async_copy(src, dst, self.sems.at[self.count])
        self.count += 1
        copy.start()
        return copy.wait

    def paired(self, src, dst):
        base = self.count
        self.count += 4

        def piece(i):
            two = pl.ds(2 * i, 2)
            return pltpu.make_async_copy(src.at[two], dst.at[two], self.sems.at[base + i])

        return piece


def reduce_scratch(r, c, even=f32):
    q = r // 4
    return [
        pltpu.VMEM((4, r, c), bf),
        pltpu.VMEM((4, r, c), even),
        pltpu.VMEM((4, r, c), bf),
        pltpu.VMEM((2, 6, q, c), bf),
        pltpu.VMEM((2, 2, 3, q, c), bf),
    ]


def rows_of_pair(a, i):
    two, r, k = 2, a.shape[1], a.shape[2]
    return a[pl.ds(2 * i, two)].reshape(two * r, k)


def times(a, w, nt, arrive):
    def product(it, i, odd, even):
        r = a.shape[1]
        arrive(it, i)

        @pl.loop(0, even.shape[1] // WIDE)
        def _(j):
            at = pl.ds(pl.multiple_of(j * WIDE, WIDE), WIDE)
            x = rows_of_pair(a, i)
            if nt:
                y = lax.dot_general(
                    x, w[at, :], (((1,), (1,)), ((), ())), preferred_element_type=f32
                )
            else:
                y = jnp.dot(x, w[:, at], preferred_element_type=f32)
            even[:, at] = y[:r].astype(even.dtype)
            odd[:, at] = y[r:].astype(odd.dtype)

    return product


def exchange_and_gather(reduce, gathers, step, body, arrivals):
    reduce.run()
    for arrive in arrivals:
        arrive()
    for c in (0, 1):
        reduce.rows(c, step, body)
        gathers[c].start()
    for c in (0, 1):
        gathers[c].forward()
    for c in (0, 1):
        gathers[c].finish()
    reduce.finish()


def both_gathers(own, out, sems, local, peer):
    half = own.shape[0] // 2
    return [
        Gather(own, out, c * half, half, sems, REDUCE_SEMS + c * GATHER_SEMS, local.at[c], peer)
        for c in (0, 1)
    ]


EXCHANGE_SEMS = REDUCE_SEMS + 2 * GATHER_SEMS


def forward_kernel(
    nrm_in, wvs_in, sco, w_in, tok_in, vec, v_out, mix_out, ret_out, swi_out, mid, out,
    nrm, wvs, w, tok, v_buf, mix_buf, ret_buf, swi_buf, po, pe, rc, sb, ring, own,
    ssem, rsem, local, load,
):
    _, peer = place()
    enter = greet([peer(1), peer(2), peer(4)])
    sems = (ssem, rsem)
    r, width = v_buf.shape[1:]
    loads = Load(load)
    nrm_piece = loads.paired(nrm_in, nrm)
    nrm_piece(3).start()
    wvs_here = loads.whole(wvs_in, wvs)
    w_here = loads.whole(w_in, w)
    for i in (1, 2, 0):
        nrm_piece(i).start()
    tok_here = loads.whole(tok_in, tok)
    kept = ((v_buf, v_out), (mix_buf, mix_out), (ret_buf, ret_out), (swi_buf, swi_out))

    def keep(i):
        two = pl.ds(2 * i, 2)
        return [
            pltpu.make_async_copy(src.at[two], dst.at[two], local.at[2 + 4 * i + j])
            for j, (src, dst) in enumerate(kept)
        ]

    def prepare(it, i):
        first = 2 * i
        two = pl.ds(first, 2)
        pl.when(it == 0)(wvs_here)
        nrm_piece(i).wait()
        x = nrm[two].reshape(2 * r, nrm.shape[2])
        v = jnp.dot(x, wvs[:, :width], preferred_element_type=f32).astype(bf)
        v_buf[two] = v.reshape(2, r, width)
        for k in (0, 1):
            ret_buf[first + k] = jnp.dot(
                sco[first + k], v[k * r : (k + 1) * r], preferred_element_type=f32
            )
        s = jnp.dot(x, wvs[:, width:], preferred_element_type=f32)
        swi_buf[two] = s.reshape(2, r, width)

        def gated(j, _):
            k = first + lax.div(j, r // 32)
            at = pl.ds(pl.multiple_of(lax.rem(j, r // 32) * 32, 32), 32)
            value = ret_buf[k, at, :]
            centred = value - jnp.mean(value, axis=-1, keepdims=True)
            spread = jnp.mean(centred * centred, axis=-1, keepdims=True)
            gate = swi_buf[k, at, :]
            gate = gate / (1.0 + jnp.exp(-gate))
            mix_buf[k, at, :] = (
                gate * (centred * lax.rsqrt(jnp.maximum(spread, 0.25)))
            ).astype(bf)
            return 0

        lax.fori_loop(0, 2 * r // 32, gated, 0, unroll=4)
        for copy in keep(i):
            copy.start()

    def product(it, i, odd, even):
        step = w.shape[2]
        pl.when(it == 0)(w_here)

        def columns(j, _):
            at = pl.ds(pl.multiple_of(j * step, step), step)
            y = jnp.dot(rows_of_pair(mix_buf, i), w[j], preferred_element_type=f32)
            even[:, at] = y[:r].astype(even.dtype)
            odd[:, at] = y[r:].astype(odd.dtype)
            return 0

        lax.fori_loop(0, w.shape[0], columns, 0, unroll=2)

    def body(at, value):
        value = value + tok[at, :].astype(f32)
        mid[at, :] = value
        center = jnp.mean(value, axis=-1, keepdims=True)
        centred = value - center
        spread = jnp.mean(centred * centred, axis=-1, keepdims=True)
        own[at, :] = (
            centred * lax.rsqrt(spread + 1e-05) * vec[0:1, :] + vec[1:2, :]
        ).astype(bf)

    reduce = Reduce(product, (po, pe, rc, sb, ring), sems, 0, peer, prepare, enter)
    exchange_and_gather(reduce, both_gathers(own, out, sems, local, peer), 16, body, (tok_here,))
    for i in range(4):
        for copy in keep(i):
            copy.wait()


def forward_exchange(nrm, wvs, sco, w, tok, vec, cid):
    _, r, d = nrm.shape
    width = w.shape[1]
    count = EXCHANGE_SEMS
    blocks = [((TP, r, width), t) for t in (bf, bf, f32, f32)]
    return pl.pallas_call(
        forward_kernel,
        out_shape=tuple(SDS(*b) for b in blocks) + (SDS((r, d), f32), SDS((TP, r, d), bf)),
        in_specs=[ANY, ANY, VMEM, ANY, ANY, VMEM],
        out_specs=(ANY,) * 4 + (VMEM, ANY),
        scratch_shapes=[pltpu.VMEM(x.shape, x.dtype) for x in (nrm, wvs, w, tok)]
        + [pltpu.VMEM(*b) for b in blocks]
        + reduce_scratch(r, d)
        + [
            pltpu.VMEM((r, d), bf),
            pltpu.SemaphoreType.DMA((count,)),
            pltpu.SemaphoreType.DMA((count,)),
            pltpu.SemaphoreType.DMA((18,)),
            pltpu.SemaphoreType.DMA((7,)),
        ],
        compiler_params=pltpu.CompilerParams(
            collective_id=cid, has_side_effects=True, vmem_limit_bytes=60 << 20
        ),
        name="forward_exchange",
    )(nrm, wvs, sco, w, tok, vec)


def product_kernel(a, b, out):
    a, b = a[...].reshape(-1, a.shape[-1]), b[...].reshape(-1, b.shape[-1])
    out[...] = lax.dot_general(
        a, b, (((0,), (0,)), ((), ())), preferred_element_type=f32
    ).astype(bf)


def row_product(a, b):
    _, r, m = a.shape
    width = b.shape[2]
    tile, part = 512 if m >= 2048 else 256, min(width, 1024)
    return pl.pallas_call(
        product_kernel,
        grid=(width // part, m // tile),
        out_shape=SDS((m, width), bf),
        in_specs=[
            pl.BlockSpec((TP, r, tile), lambda j, i: (0, 0, i)),
            pl.BlockSpec((TP, r, part), lambda j, i: (0, 0, j)),
        ],
        out_specs=pl.BlockSpec((tile, part), lambda j, i: (i, j)),
        compiler_params=pltpu.CompilerParams(vmem_limit_bytes=56 << 20),
        cost_estimate=pl.CostEstimate(
            flops=2 * TP * r * m * width,
            bytes_accessed=2 * (a.size + b.size + m * width),
            transcendentals=0,
        ),
        name="row_product",
    )(a, b)


def hidden_kernel(x, gu, hid, act_out, slope_out):
    width = hid.shape[2]
    step = 256

    @pl.loop(0, width // step)
    def _(j):
        at = pl.ds(pl.multiple_of(j * step, step), step)
        behind = pl.ds(pl.multiple_of(j * step + width, step), step)
        rows = x[...].reshape(-1, x.shape[2])
        first = jnp.dot(rows, gu[:, at], preferred_element_type=f32)
        second = jnp.dot(rows, gu[:, behind], preferred_element_type=f32)
        share = 0.5 * (1.0 + lax.erf(first * math.sqrt(0.5)))
        act = first * share
        slope = share + first * (jnp.exp(-0.5 * first * first) * (1.0 / math.sqrt(2.0 * math.pi)))
        block = hid.shape[:2] + (step,)
        hid[:, :, at] = (act * second).astype(bf).reshape(block)
        act_out[:, :, at] = act.reshape(block)
        slope_out[:, :, at] = (slope * second).reshape(block)


def hidden_units(x, gu):
    _, r, d = x.shape
    width = gu.shape[1] // 2
    row = pl.BlockSpec((2, r, width), lambda k: (k, 0, 0))
    return pl.pallas_call(
        hidden_kernel,
        grid=(TP // 2,),
        out_shape=tuple(SDS((TP, r, width), t) for t in (bf, f32, f32)),
        in_specs=[
            pl.BlockSpec((2, r, d), lambda k: (k, 0, 0)),
            pl.BlockSpec(gu.shape, lambda k: (0, 0)),
        ],
        out_specs=(row, row, row),
        compiler_params=pltpu.CompilerParams(vmem_limit_bytes=56 << 20),
        cost_estimate=pl.CostEstimate(
            flops=4 * TP * r * d * width, bytes_accessed=24 << 20, transcendentals=2 * TP * r * width
        ),
        name="hidden_units",
    )(x, gu)


def hidden_back_kernel(cot, d0, d1, act, slope, out, down):
    width = act.shape[2]
    step = 512
    early, rows = d0.shape[1], d0.shape[1] + d1.shape[1]

    @pl.when(pl.program_id(0) == 0)
    def _():
        for g in range(d0.shape[0]):
            down[g * rows : g * rows + early] = d0[g]
            down[g * rows + early : (g + 1) * rows] = d1[g]

    @pl.loop(0, width // step)
    def _(j):
        at = pl.ds(pl.multiple_of(j * step, step), step)
        behind = pl.ds(pl.multiple_of(j * step + width, step), step)
        grad = lax.dot_general(
            cot[...].reshape(-1, cot.shape[2]), down[at, :], (((1,), (1,)), ((), ())),
            preferred_element_type=f32,
        ).reshape(act.shape[:2] + (step,))
        out[:, :, at] = (grad * slope[:, :, at]).astype(bf)
        out[:, :, behind] = (grad * act[:, :, at]).astype(bf)


def hidden_back(cot, d0, d1, act, slope):
    _, r, d = cot.shape
    width = act.shape[2]
    row = pl.BlockSpec((2, r, width), lambda k: (k, 0, 0))
    return pl.pallas_call(
        hidden_back_kernel,
        grid=(TP // 2,),
        out_shape=SDS((TP, r, 2 * width), bf),
        in_specs=[
            pl.BlockSpec((2, r, d), lambda k: (k, 0, 0)),
            pl.BlockSpec(d0.shape, lambda k: (0, 0, 0)),
            pl.BlockSpec(d1.shape, lambda k: (0, 0, 0)),
            row,
            row,
        ],
        scratch_shapes=[pltpu.VMEM((width, d), bf)],
        out_specs=pl.BlockSpec((2, r, 2 * width), lambda k: (k, 0, 0)),
        compiler_params=pltpu.CompilerParams(vmem_limit_bytes=56 << 20),
        cost_estimate=pl.CostEstimate(
            flops=2 * TP * r * d * width, bytes_accessed=24 << 20, transcendentals=0
        ),
        name="hidden_back",
    )(cot, d0, d1, act, slope)


def backward_kernel(
    a_in, w_in, mid_in, cot_in, vec, gmid, out, sums,
    a, w, mid, cot, po, pe, rc, sb, ring, own, acc, ssem, rsem, local, load,
):
    _, peer = place()
    enter = greet([peer(1), peer(2), peer(4)])
    sems = (ssem, rsem)
    loads = Load(load)
    piece = loads.paired(a_in, a)
    piece(3).start()
    w_here = loads.whole(w_in, w)
    for i in (1, 2, 0):
        piece(i).start()
    arrivals = (loads.whole(mid_in, mid), loads.whole(cot_in, cot))

    def arrive(it, i):
        pl.when(it == 0)(w_here)
        piece(i).wait()

    acc[...] = jnp.zeros_like(acc)

    def body(at, g):
        value = mid[at, :]
        center = jnp.mean(value, axis=-1, keepdims=True)
        centred = value - center
        inv = lax.rsqrt(jnp.mean(centred * centred, axis=-1, keepdims=True) + 1e-05)
        hat = centred * inv
        acc[0] += g * hat
        acc[1] += g
        scaled = g * vec[0:1, :]
        mean_g = jnp.mean(scaled, axis=-1, keepdims=True)
        mean_gh = jnp.mean(scaled * hat, axis=-1, keepdims=True)
        grad = cot[at, :].astype(f32) + inv * (scaled - mean_g - hat * mean_gh)
        gmid[at, :] = grad
        own[at, :] = grad.astype(bf)

    reduce = Reduce(
        times(a, w, True, arrive), (po, pe, rc, sb, ring), sems, 0, peer, enter=enter
    )
    exchange_and_gather(reduce, both_gathers(own, out, sems, local, peer), 16, body, arrivals)
    sums[0:1, :] = jnp.sum(acc[0], axis=0, keepdims=True)
    sums[1:2, :] = jnp.sum(acc[1], axis=0, keepdims=True)


def backward_exchange(a, w, mid, cot, vec, cid):
    _, r, _ = a.shape
    c = w.shape[0]
    count = EXCHANGE_SEMS
    return pl.pallas_call(
        backward_kernel,
        out_shape=(SDS((r, c), f32), SDS((TP, r, c), bf), SDS((2, c), f32)),
        in_specs=[ANY] * 4 + [VMEM],
        out_specs=(VMEM, ANY, VMEM),
        scratch_shapes=[pltpu.VMEM(x.shape, x.dtype) for x in (a, w, mid, cot)]
        + reduce_scratch(r, c)
        + [
            pltpu.VMEM((r, c), bf),
            pltpu.VMEM((2, 16, c), f32),
            pltpu.SemaphoreType.DMA((count,)),
            pltpu.SemaphoreType.DMA((count,)),
            pltpu.SemaphoreType.DMA((2,)),
            pltpu.SemaphoreType.DMA((7,)),
        ],
        compiler_params=pltpu.CompilerParams(
            collective_id=cid, has_side_effects=True, vmem_limit_bytes=52 << 20
        ),
        name="backward_exchange",
    )(a, w, mid, cot, vec)


def last_kernel(
    n, gqkv_in, gs_in, wqk_in, wvs_in, a2_in, d0, d1, tok_in, gain, sums2,
    gtok, ffn, vec_out, gqkv, gs, wqk, wvs, a2, w2, tok,
    po, pe, rc, sb, ring, pe2, rc2, sb2, ring2, acc, vecs, near, far, part, ssem, rsem, load,
):
    dp = n // TP
    me, peer = place()
    g = lax.div(me, TP)
    width = vec_out.shape[1]
    others = [lax.rem(me + TP * j, n) for j in range(1, dp)]
    enter = greet([peer(k) for k in range(1, TP)] + others)
    sems = (ssem, rsem)
    loads = Load(load)
    pieces = loads.paired(gqkv_in, gqkv), loads.paired(gs_in, gs)
    for piece in pieces:
        piece(3).start()
    weights = loads.whole(wqk_in, wqk), loads.whole(wvs_in, wvs)
    for i in (1, 2, 0):
        for piece in pieces:
            piece(i).start()
    second = [loads.whole(a2_in, a2)]
    early, rows = d0.shape[1], d0.shape[1] + d1.shape[1]
    for k in range(dp):
        second.append(loads.whole(d0.at[k], w2.at[pl.ds(k * rows, early)]))
        second.append(loads.whole(d1.at[k], w2.at[pl.ds(k * rows + early, rows - early)]))
    arrivals = (loads.whole(tok_in, tok),)

    def all_here(waits):
        def wait():
            for one in waits:
                one()

        return wait

    acc[...] = jnp.zeros_like(acc)
    nt = (((1,), (1,)), ((), ()))

    def product(it, i, odd, even):
        r, qk, v = gqkv.shape[1], wqk.shape[1], gs.shape[2]
        pl.when(it == 0)(all_here(weights))
        for piece in pieces:
            piece(i).wait()
        x, y = rows_of_pair(gqkv, i), rows_of_pair(gs, i)

        @pl.loop(0, even.shape[1] // WIDE)
        def _(j):
            at = pl.ds(pl.multiple_of(j * WIDE, WIDE), WIDE)
            z = lax.dot_general(x[:, :qk], wqk[at, :], nt, preferred_element_type=f32)
            z += lax.dot_general(x[:, qk:], wvs[at, :v], nt, preferred_element_type=f32)
            z += lax.dot_general(y, wvs[at, v:], nt, preferred_element_type=f32)
            even[:, at] = z[:r].astype(even.dtype)
            odd[:, at] = z[r:].astype(odd.dtype)

    one = Reduce(product, (po, pe, rc, sb, ring), sems, 0, peer, enter=enter)
    one.run()
    one.core_sent()

    def arrive(it, _):
        pl.when(it == 0)(all_here(second))

    two = Reduce(times(a2, w2, False, arrive), (po, pe2, rc2, sb2, ring2), sems, REDUCE_SEMS, peer)
    two.run()

    def body(at, grad):
        value = tok[at, :].astype(f32)
        center = jnp.mean(value, axis=-1, keepdims=True)
        centred = value - center
        inv = lax.rsqrt(jnp.mean(centred * centred, axis=-1, keepdims=True) + 1e-05)
        hat = centred * inv
        acc[0] += grad * hat
        acc[1] += grad
        scaled = grad * gain[...]
        mean_g = jnp.mean(scaled, axis=-1, keepdims=True)
        mean_gh = jnp.mean(scaled * hat, axis=-1, keepdims=True)
        gtok[at, :] = inv * (scaled - mean_g - hat * mean_gh)

    all_here(arrivals)()
    for c in (0, 1):
        one.rows(c, 16, body)
    vecs[...] = jnp.zeros_like(vecs)
    vecs[0:1, :] = jnp.sum(acc[0], axis=0, keepdims=True)
    vecs[1:2, :] = jnp.sum(acc[1], axis=0, keepdims=True)
    vecs[2:4, :] = sums2[...]
    base = 2 * REDUCE_SEMS
    copies = []
    for j, dev in enumerate(others):
        at = pl.multiple_of(lax.div(dev, TP) * width, 128)
        copy = remote(vecs.at[:, pl.ds(at, width)], far.at[j], sems, base + j, dev)
        copy.start()
        copies.append(copy)

    def keep(at, value):
        ffn[at, :] = value

    two.rows(0, 16, keep)
    total = vecs[:, pl.ds(pl.multiple_of(g * width, 128), width)]
    for j, copy in enumerate(copies):
        copy.wait()
        total = total + far[j]
    part[...] = total
    copies = []
    for k in range(1, TP):
        copy = remote(part, near.at[k - 1], sems, base + dp + k - 1, peer(k))
        copy.start()
        copies.append(copy)
    two.rows(1, 16, keep)
    for k, copy in enumerate(copies):
        copy.wait()
        total = total + near[k]
    vec_out[...] = total
    one.finish()
    two.finish()


def last_exchange(n, gqkv, gs, wqk, wvs, a2, d0, d1, tok, gain, sums2, cid):
    dp = n // TP
    _, r, _ = a2.shape
    c = d0.shape[2]
    width = c // dp
    count = 2 * REDUCE_SEMS + dp + TP
    return pl.pallas_call(
        functools.partial(last_kernel, n),
        out_shape=(SDS((r, c), f32), SDS((r, c), f32), SDS((8, width), f32)),
        in_specs=[ANY] * 8 + [VMEM] * 2,
        out_specs=(VMEM,) * 3,
        scratch_shapes=[
            pltpu.VMEM(x.shape, x.dtype)
            for x in (gqkv, gs, wqk, wvs, a2, SDS((a2.shape[2], c), bf), tok)
        ]
        + reduce_scratch(r, c)
        + reduce_scratch(r, c, bf)[1:]
        + [
            pltpu.VMEM((2, 16, c), f32),
            pltpu.VMEM((8, c), f32),
            pltpu.VMEM((TP - 1, 8, width), f32),
            pltpu.VMEM((dp, 8, width), f32),
            pltpu.VMEM((8, width), f32),
            pltpu.SemaphoreType.DMA((count,)),
            pltpu.SemaphoreType.DMA((count,)),
            pltpu.SemaphoreType.DMA((12 + 2 * dp,)),
        ],
        compiler_params=pltpu.CompilerParams(
            collective_id=cid, has_side_effects=True, vmem_limit_bytes=ALL_VMEM
        ),
        name="last_exchange",
    )(gqkv, gs, wqk, wvs, a2, d0, d1, tok, gain, sums2)


def gate_back_kernel(g_low, w, ret, swi, gret, gswi, whole):
    cols = w.shape[2]

    @pl.when(pl.program_id(0) == 0)
    def _():
        for j in range(w.shape[0]):
            whole[:, j * cols : (j + 1) * cols] = w[j]

    two, r, _ = gret.shape
    grads = lax.dot_general(
        g_low[...].reshape(two * r, g_low.shape[2]), whole[...], (((1,), (1,)), ((), ())),
        preferred_element_type=f32,
    )
    for i in range(two):
        grad, value, gate = grads[i * r : (i + 1) * r], ret[i], swi[i]
        centred = value - jnp.mean(value, axis=-1, keepdims=True)
        spread = jnp.mean(centred * centred, axis=-1, keepdims=True)
        inv = lax.rsqrt(jnp.maximum(spread, 0.25))
        share = 1.0 / (1.0 + jnp.exp(-gate))
        silu = gate * share
        gswi[i] = (grad * (centred * inv) * (share * (1.0 + gate * (1.0 - share)))).astype(bf)
        grad = grad * silu
        pull = jnp.mean(grad * centred, axis=-1, keepdims=True)
        pull = jnp.where(spread > 0.25, inv * inv * inv * pull, 0.0)
        grad = grad * inv - centred * pull
        gret[i] = (grad - jnp.mean(grad, axis=-1, keepdims=True)).astype(bf)


def gate_back(g_low, w, ret, swi):
    _, r, d = g_low.shape
    width = ret.shape[2]
    row = pl.BlockSpec((2, r, width), lambda k: (k, 0, 0))
    return pl.pallas_call(
        gate_back_kernel,
        grid=(TP // 2,),
        out_shape=(SDS(ret.shape, bf), SDS(ret.shape, bf)),
        in_specs=[
            pl.BlockSpec((2, r, d), lambda k: (k, 0, 0)),
            pl.BlockSpec(w.shape, lambda k: (0, 0, 0)),
            row,
            row,
        ],
        out_specs=(row, row),
        scratch_shapes=[pltpu.VMEM((width, d), bf)],
        compiler_params=pltpu.CompilerParams(vmem_limit_bytes=56 << 20),
        cost_estimate=pl.CostEstimate(
            flops=2 * TP * r * d * width, bytes_accessed=22 << 20, transcendentals=TP * r * width
        ),
        name="gate_back",
    )(g_low, w, ret, swi)


def scores_back_kernel(sco, mask, q, k, v, gret, cosine, sine, out):
    nt, tn = (((1,), (1,)), ((), ())), (((0,), (0,)), ((), ()))
    kh = q.shape[2]
    half = kh // 2
    out[0, :, 2 * kh :] = lax.dot_general(
        sco[0], gret[0], tn, preferred_element_type=f32
    ).astype(bf)
    grad = lax.dot_general(gret[0], v[0], nt, preferred_element_type=f32)
    grad = (grad * mask[0]).astype(bf)
    gq = jnp.dot(grad, k[0], preferred_element_type=f32)
    gk = lax.dot_general(grad, q[0], tn, preferred_element_type=f32)
    for i, g in enumerate((gq, gk)):
        u, w = g[:, :half], g[:, half:]
        at = i * kh
        out[0, :, at : at + half] = (u * cosine[0] + w * sine[0]).astype(bf)
        out[0, :, at + half : at + kh] = (w * cosine[0] - u * sine[0]).astype(bf)


def scores_back(sco, mask, q, k, v, gret, cosine, sine):
    _, r, kh = q.shape
    arrays = (sco, mask, q, k, v, gret, cosine, sine)
    width = 2 * kh + v.shape[2]
    spec = [pl.BlockSpec((1,) + x.shape[1:], lambda i: (i, 0, 0)) for x in arrays]
    return pl.pallas_call(
        scores_back_kernel,
        grid=(TP,),
        out_shape=SDS((TP, r, width), bf),
        in_specs=spec,
        out_specs=pl.BlockSpec((1, r, width), lambda i: (i, 0, 0)),
        compiler_params=pltpu.CompilerParams(vmem_limit_bytes=56 << 20),
        cost_estimate=pl.CostEstimate(
            flops=4 * TP * r * r * (kh + v.shape[2]), bytes_accessed=16 << 20, transcendentals=0
        ),
        name="scores_back",
    )(*arrays)


def spread_kernel(a_in, b_in, out, a, b, turned, made, ssem, rsem, local, load):
    me, peer = place()
    t = lax.rem(me, TP)
    place_of, low = lax.div(t, 2), lax.rem(t, 2)
    sems = (ssem, rsem)
    enter = greet([peer(k) for k in range(1, TP)])
    rows, tile = out.shape[1], 512
    tiles = out.shape[2] // tile

    def columns(j):
        return pl.ds(pl.multiple_of(j * tile, tile), tile)

    def piece(j):
        return pltpu.make_async_copy(
            b_in.at[:, :, columns(j)], b.at[:, :, columns(j)], load.at[1 + j]
        )

    def sends(j, act):
        for m in range(4):
            chunk = lax.rem(place_of + m, 4)
            dev = me - t + 4 * low + chunk
            src = made.at[pl.ds(pl.multiple_of(chunk * rows, rows), rows), columns(j)]
            dst = out.at[place_of, :, columns(j)]
            i = 4 * j + m
            away = remote(src, dst, sems, i, dev)
            here = pltpu.make_async_copy(src, dst, local.at[i])
            pl.when(dev != me)(getattr(away, act))
            pl.when(dev == me)(getattr(here, act))

    whole = pltpu.make_async_copy(a_in, a, load.at[0])
    whole.start()
    for j in range(tiles):
        piece(j).start()
    whole.wait()
    turned[...] = a[...].reshape(-1, a.shape[2]).T
    enter()

    @pl.loop(0, tiles)
    def _(j):
        piece(j).wait()
        made[:, columns(j)] = jnp.dot(
            turned[...], b[:, :, columns(j)].reshape(turned.shape[1], tile),
            preferred_element_type=f32,
        ).astype(bf)
        sends(j, "start")

    @pl.loop(0, tiles)
    def _(j):
        sends(j, "wait")


def spread_product(a, b, cid):
    _, r, m = a.shape
    width = b.shape[2]
    count = 4 * (width // 512)
    return pl.pallas_call(
        spread_kernel,
        out_shape=SDS((4, m // 4, width), bf),
        in_specs=[ANY, ANY],
        out_specs=ANY,
        scratch_shapes=[
            pltpu.VMEM(a.shape, bf),
            pltpu.VMEM(b.shape, bf),
            pltpu.VMEM((m, TP * r), bf),
            pltpu.VMEM((m, width), bf),
            pltpu.SemaphoreType.DMA((count,)),
            pltpu.SemaphoreType.DMA((count,)),
            pltpu.SemaphoreType.DMA((count,)),
            pltpu.SemaphoreType.DMA((1 + width // 512,)),
        ],
        compiler_params=pltpu.CompilerParams(
            collective_id=cid, has_side_effects=True, vmem_limit_bytes=ALL_VMEM
        ),
        name="spread_product",
    )(a, b)


def tp_groups(n):
    return [[g * TP + t for t in range(TP)] for g in range(n // TP)]


def dp_groups(n):
    return [[g * TP + t for g in range(n // TP)] for t in range(TP)]


def plane_a2a(x, n):
    return lax.all_to_all(x, AXIS, 0, 0, axis_index_groups=tp_groups(n), tiled=True)


def dp_gather(x, n):
    return lax.all_gather(x, AXIS, axis=0, tiled=True, axis_index_groups=dp_groups(n))


def dp_reduce(x, n):
    return lax.psum_scatter(
        x, AXIS, scatter_dimension=0, tiled=True, axis_index_groups=dp_groups(n)
    )


def seq_positions(lengths, rows):
    ends = jnp.cumsum(lengths, axis=1)
    starts = ends - lengths
    index = jnp.arange(rows, dtype=jnp.int32)
    segment = jnp.sum((index[None, :, None] >= ends[:, None, :]).astype(jnp.int32), axis=2)
    member = segment[:, :, None] == jnp.arange(lengths.shape[1], dtype=jnp.int32)
    offset = index[None, :] - jnp.sum(jnp.where(member, starts[:, None, :], 0), axis=2)
    return segment, offset


def rotary_tables(offset):
    half = KH // 2
    freq = jnp.exp(-math.log(10000.0) * jnp.arange(half, dtype=f32) / half)
    angle = offset.astype(f32)[..., None] * freq
    return jnp.cos(angle), jnp.sin(angle)


def decay_mask(segment, offset, head):
    diff = offset[:, :, None] - offset[:, None, :]
    valid = (segment[:, :, None] == segment[:, None, :]) & (diff >= 0)
    steps = jnp.where(valid, diff, 0).astype(f32)
    log = jnp.log(1.0 - jnp.exp2(-5.0 - head.astype(f32)))
    return jnp.where(valid, jnp.exp(log * steps), 0.0) / math.sqrt(KH)


def col_blocks(w):
    r, c = w.shape
    return w.reshape(r, TP, c // TP).transpose(1, 0, 2).reshape(TP * r, c // TP)


def join_kernel(widths, parts, x, *outs):
    at = 0
    for out, width in zip(outs, widths):
        piece = width // parts
        for t in range(TP):
            for p in range(parts):
                to = (p * TP + t) * piece
                out[:, to : to + piece] = x[t, :, at + p * piece : at + (p + 1) * piece].astype(f32)
        at += width


def join(x, widths, parts=1):
    r = x.shape[1]
    if any(width // parts % 128 for width in widths):
        made, at = [], 0
        for width in widths:
            part = x[:, :, at : at + width].reshape(TP, r, parts, width // parts)
            made.append(part.transpose(1, 2, 0, 3).reshape(r, TP * width).astype(f32))
            at += width
        return made
    return pl.pallas_call(
        functools.partial(join_kernel, widths, parts),
        out_shape=tuple(SDS((r, TP * width), f32) for width in widths),
        in_specs=[VMEM],
        out_specs=tuple(VMEM for _ in widths),
        compiler_params=pltpu.CompilerParams(vmem_limit_bytes=8 << 20),
        cost_estimate=pl.CostEstimate(flops=0, bytes_accessed=6 * x.size, transcendentals=0),
        name="join",
    )(x)


def after(x, *deps):
    return lax.optimization_barrier((x,) + deps)[0]


def on_device(n, tokens, lengths, gain1, bias1, wq, wk, wv, ws, wo, gain2, bias2, wg, wu, wd, cot):
    rows, d = tokens.shape
    ff = wg.shape[1]
    dp = n // TP
    shard = d // n
    unit = ff // n
    me = lax.axis_index(AXIS)
    head = lax.rem(me, TP)

    def ff_blocks(w):
        return w.reshape(shard, dp, TP, unit).transpose(2, 0, 1, 3).reshape(TP, shard, dp * unit)

    lens = jnp.pad(lengths[0].astype(f32), (0, shard - lengths.shape[1]))
    vec = jnp.stack([v.astype(f32) for v in (gain1, bias1, gain2, bias2)] + [lens])
    vec = jnp.pad(vec, ((0, 3), (0, 128 - shard)))
    early = max(16, wd.shape[0] // 4)
    qko_blk, d0 = first_exchange(n, wq, wk, wo, wd, early, 1)
    qko = dp_gather(qko_blk.reshape(TP * shard, 4 * KH), n)
    tok_all, vec_all = second_exchange(n, after(tokens, qko_blk), vec, 2)
    gain1f, bias1f, gain2f, bias2f = (
        vec_all[:, :, i, :shard].reshape(1, d) for i in range(4)
    )
    vec2 = jnp.concatenate([gain2f, bias2f], axis=0)
    gu_in = jnp.concatenate([ff_blocks(wg), ff_blocks(wu)], axis=2)
    vs_blk, gu_blk, normed = third_exchange(wv, ws, gu_in, tok_all, gain1f, bias1f, 3)
    vs = dp_gather(vs_blk.reshape(TP * shard, 2 * VH), n)
    gu = dp_gather(gu_blk.reshape(TP * shard, 2 * dp * unit), n)
    down = d0, dp_gather(wd[early:], n).reshape(dp, wd.shape[0] - early, d)

    mine = lax.dynamic_slice_in_dim(vec_all, lax.div(me, TP), 1, 0)[0, :, 4, :3]
    order = jnp.arange(TP, dtype=jnp.int32)
    pick = (order[None, :] == (order[:, None] ^ head)).astype(f32)
    len_all = jnp.sum(pick[:, :, None] * mine[None], axis=1).astype(jnp.int32)
    segment, offset = seq_positions(len_all, rows)
    cosine, sine = rotary_tables(offset)
    mask = decay_mask(segment, offset, head)

    cot_all, out_blk, q_rot, k_rot, scores, qk = fourth_exchange(
        n, cot, qko.reshape(n, shard, 4 * KH), normed, cosine, sine, mask, 4
    )
    out_blk = out_blk.reshape(TP, VH, d // TP)
    qk = qk.reshape(d, 2 * KH)
    v_low, mixed, retained, swish_in, middle, normed2 = forward_exchange(
        normed, vs, scores, out_blk, tokens, vec2, 5
    )
    hidden, act, slope = hidden_units(normed2, gu)
    down_grad = row_product(hidden, cot_all)
    g_down = dp_reduce(down_grad, n)

    g_fs = hidden_back(cot_all, *down, act, slope)
    gu_grad = row_product(normed2, g_fs)
    g_gu = dp_reduce(gu_grad, n)
    g_middle, g_low, sums2 = backward_exchange(g_fs, gu, middle, cot, vec2, 6)

    g_retained, g_swish = gate_back(g_low, out_blk, retained, swish_in)
    swish_grad = row_product(normed, g_swish)
    g_swi = dp_reduce(swish_grad, n)
    spread = wo.shape[0] * HEADS == VH * 2
    if spread:
        out_grad = spread_product(mixed, g_low, 8).reshape(VH, d)
    else:
        out_grad = row_product(mixed, g_low)
        out_grad = plane_a2a(col_blocks(out_grad), n)
    g_qkv = scores_back(scores, mask, q_rot, k_rot, v_low, g_retained, cosine, sine)
    qkv_grad = row_product(normed, g_qkv)
    g_qkv_own = dp_reduce(qkv_grad, n)
    g_out = dp_reduce(out_grad, n)
    grad_part, ffn, g_vecs = last_exchange(
        n, g_qkv, g_swish, qk, vs, hidden, *down, tokens, gain1f, sums2, 7
    )
    grad_tokens = g_middle + grad_part
    layer_out = (middle + ffn).astype(bf)

    g_vecs = lax.dynamic_slice_in_dim(g_vecs, head * shard, shard, 1)
    grad_d = g_down.astype(f32)
    g_gu = plane_a2a(g_gu, n)
    grad_g, grad_u = join(g_gu.reshape(TP, shard, 2 * dp * unit), (dp * unit,) * 2, dp)
    g_swi = plane_a2a(g_swi, n)
    (grad_s,) = join(g_swi.reshape(TP, shard, VH), (VH,))
    g_qkv_own = plane_a2a(g_qkv_own, n)
    grad_q, grad_k, grad_v = join(g_qkv_own.reshape(TP, shard, 2 * KH + VH), (KH, KH, VH))
    if spread:
        grad_o = g_out.astype(f32)
    else:
        g_out = plane_a2a(g_out, n)
        (grad_o,) = join(g_out.reshape(TP, wo.shape[0], d // TP), (d // TP,))
    return (
        layer_out, grad_tokens, g_vecs[0], g_vecs[1], grad_q, grad_k, grad_v, grad_s, grad_o,
        g_vecs[2], g_vecs[3], grad_g, grad_u, grad_d,
    )


def solution(mesh):
    n = mesh.shape[AXIS]
    row, vec = P(AXIS, None), P(AXIS)
    ins = (row, row, vec, vec, row, row, row, row, row, vec, vec, row, row, row, row)
    outs = (row, row, vec, vec, row, row, row, row, row, vec, vec, row, row, row)

    def body(*args):
        return on_device(n, *args)

    return jax.shard_map(body, mesh=mesh, in_specs=ins, out_specs=outs, check_vma=False)
```

```python
import functools
import math

import jax
import jax.numpy as jnp
from jax import lax
from jax.experimental import pallas as pl
from jax.experimental.pallas import tpu as pltpu
from jax.sharding import PartitionSpec as P


HEADS = 8
KH = 256
VH = 512
TP = 8
AXIS = "fsdp"
MESH = pl.DeviceIdType.MESH
ANY = pl.BlockSpec(memory_space=pl.ANY)
VMEM = pl.BlockSpec(memory_space=pltpu.VMEM)
bf = jnp.bfloat16
f32 = jnp.float32
SDS = jax.ShapeDtypeStruct
ALL_VMEM = 67043328


def place():
    me = lax.axis_index(AXIS)
    steps = [s - 2 * s * lax.rem(lax.div(me, s), 2) for s in (1, 2, 4)]

    def peer(k):
        out = me
        for bit, step in enumerate(steps):
            if k >> bit & 1:
                out = out + step
        return out

    return me, peer


def greet(peers):
    barrier = pltpu.get_barrier_semaphore()
    for p in peers:
        pl.semaphore_signal(barrier, inc=1, device_id=(p,), device_id_type=MESH)
    return lambda: pl.semaphore_wait(barrier, len(peers))


def meet(peers):
    greet(peers)()


def remote(src, dst, sems, i, dev):
    return pltpu.make_async_remote_copy(
        src_ref=src, dst_ref=dst, send_sem=sems[0].at[i], recv_sem=sems[1].at[i],
        device_id=(dev,), device_id_type=MESH,
    )


GATHER_SEMS = 13


class Gather:
    def __init__(self, own, out, start, size, sems, base, local, peer):
        self.own, self.out, self.sems, self.base, self.local = own, out, sems, base, local
        h = size // 2
        self.all, self.top, self.bot = pl.ds(start, size), pl.ds(start, h), pl.ds(start + h, h)
        self.pc, self.px, self.py = peer(1), peer(2), peer(4)
        self.made = []

    def send(self, src, dst, dev):
        copy = remote(src, dst, self.sems, self.base + len(self.made), dev)
        copy.start()
        self.made.append(copy)
        return copy

    def pass_on(self, k, at):
        self.core.append(self.send(self.out.at[k, at], self.out.at[k + 1, at], self.pc))

    def start(self):
        own, out, top, bot = self.own, self.out, self.top, self.bot
        self.x0 = self.send(own.at[bot], out.at[2, bot], self.px)
        self.y0 = self.send(own.at[top], out.at[4, top], self.py)
        self.x1 = self.send(own.at[top], out.at[2, top], self.px)
        self.y1 = self.send(own.at[bot], out.at[4, bot], self.py)
        self.core = [self.send(own.at[self.all], out.at[1, self.all], self.pc)]
        self.keep = pltpu.make_async_copy(own.at[self.all], out.at[0, self.all], self.local)
        self.keep.start()

    def forward(self):
        out, top, bot = self.out, self.top, self.bot
        self.x0.wait_recv()
        self.fy = self.send(out.at[2, bot], out.at[6, bot], self.py)
        self.pass_on(2, bot)
        self.y0.wait_recv()
        self.fx = self.send(out.at[4, top], out.at[6, top], self.px)
        self.pass_on(4, top)
        self.x1.wait_recv()
        self.pass_on(2, top)
        self.y1.wait_recv()
        self.pass_on(4, bot)

    def finish(self):
        self.fy.wait_recv()
        self.pass_on(6, self.bot)
        self.fx.wait_recv()
        self.pass_on(6, self.top)
        for copy in self.core:
            copy.wait_recv()
        for copy in self.made:
            copy.wait_send()
        self.keep.wait()


def send_columns(src, out, cols, at, sems, base, local, t, peer, rows=None):
    copies = []
    rows = slice(None) if rows is None else rows

    def block(q):
        if len(src.shape) == 3:
            return src.at[q]
        return src.at[rows, pl.ds(pl.multiple_of(q * cols, 128), cols)]

    for k in range(1, TP):
        dev = peer(k)
        copy = remote(
            block(lax.rem(dev, TP)), out.at[t, :, pl.ds(at, cols)], sems, base + k - 1, dev
        )
        copy.start()
        copies.append(copy)
    keep = pltpu.make_async_copy(block(t), out.at[t, :, pl.ds(at, cols)], local)
    keep.start()
    return copies, keep


def finish(parts):
    for copies, keep in parts:
        for copy in copies:
            copy.wait()
        keep.wait()


def exchange_call(
    kernel, outs, args, sems, locals_, cid, specs=None, out_specs=None, vmem=12 << 20
):
    return pl.pallas_call(
        kernel,
        out_shape=outs,
        in_specs=specs or [VMEM] * len(args),
        out_specs=out_specs or tuple(ANY for _ in outs),
        scratch_shapes=[
            pltpu.SemaphoreType.DMA((sems,)),
            pltpu.SemaphoreType.DMA((sems,)),
            pltpu.SemaphoreType.DMA((locals_,)),
        ],
        compiler_params=pltpu.CompilerParams(
            collective_id=cid, has_side_effects=True, vmem_limit_bytes=vmem
        ),
    )(*args)


def first_kernel(n, wq, wk, wo, wd, out, wd_out, ssem, rsem, local):
    me, peer = place()
    t, g = lax.rem(me, TP), lax.div(me, TP)
    others = others_along(n)
    meet([peer(k) for k in range(1, TP)] + others)
    sems = (ssem, rsem)
    shard, cq, co = wq.shape[0], wq.shape[1] // TP, wo.shape[1] // TP
    low, high = pl.ds(0, shard), pl.ds(shard, shard)
    wd = wd.at[pl.ds(0, wd_out.shape[1])]
    along = [remote(wd, wd_out.at[g], sems, 28 + j, dev) for j, dev in enumerate(others)]
    for copy in along:
        copy.start()
    keep = pltpu.make_async_copy(wd, wd_out.at[g], local.at[4])
    keep.start()
    finish([
        send_columns(wq, out, cq, 0, sems, 0, local.at[0], t, peer),
        send_columns(wk, out, cq, cq, sems, 7, local.at[1], t, peer),
        send_columns(wo, out, co, 2 * cq, sems, 14, local.at[2], t, peer, low),
        send_columns(wo, out, co, 2 * cq + co, sems, 21, local.at[3], t, peer, high),
        (along, keep),
    ])


def first_exchange(n, wq, wk, wo, wd, early, cid):
    width = 2 * wq.shape[1] // TP + 2 * wo.shape[1] // TP
    outs = (SDS((TP, wq.shape[0], width), bf), SDS((n // TP, early, wd.shape[1]), bf))
    kernel = functools.partial(first_kernel, n)
    return exchange_call(
        kernel, outs, (wq, wk, wo, wd), 28 + n // TP, 5, cid,
        specs=[ANY] * 4, vmem=ALL_VMEM,
    )


def others_along(n):
    me = lax.axis_index(AXIS)
    return [lax.rem(me + TP * j, n) for j in range(1, n // TP)]


def second_kernel(n, tok, vec, tok_out, vec_out, ssem, rsem, local):
    me, peer = place()
    t, g = lax.rem(me, TP), lax.div(me, TP)
    others = others_along(n)
    meet([peer(k) for k in range(1, TP)] + others)
    sems = (ssem, rsem)
    base = GATHER_SEMS
    far = []
    keep = pltpu.make_async_copy(vec, vec_out.at[g, t], local.at[1])
    keep.start()
    for j, dev in enumerate(others):
        copy = remote(vec, vec_out.at[g, t], sems, base + TP + j, dev)
        copy.start()
        far.append(copy)
    gather = Gather(tok, tok_out, 0, tok.shape[0], sems, 0, local.at[0], peer)
    gather.start()
    for copy in far:
        copy.wait()
    keep.wait()
    near = []
    for k in range(1, TP):
        copy = remote(vec_out.at[:, t], vec_out.at[:, t], sems, base + k, peer(k))
        copy.start()
        near.append(copy)
    gather.forward()
    gather.finish()
    for copy in near:
        copy.wait()


def second_exchange(n, tok, vec, cid):
    outs = (SDS((TP,) + tok.shape, bf), SDS((n // TP, TP) + vec.shape, f32))
    kernel = functools.partial(second_kernel, n)
    sems = GATHER_SEMS + TP + n // TP
    return exchange_call(kernel, outs, (tok, vec), sems, 2, cid)


def third_kernel(wv, ws, gu, tok, gain, bias, out, gu_out, nrm, ssem, rsem, local):
    me, peer = place()
    t = lax.rem(me, TP)
    meet([peer(k) for k in range(1, TP)])
    sems = (ssem, rsem)
    cols = wv.shape[1] // TP
    parts = [
        send_columns(wv, out, cols, 0, sems, 0, local.at[0], t, peer),
        send_columns(ws, out, cols, cols, sems, 7, local.at[1], t, peer),
        send_columns(gu, gu_out, gu.shape[2], 0, sems, 14, local.at[2], t, peer),
    ]
    step, r = 16, tok.shape[1]

    def norm(j, _):
        k = lax.div(j, r // step)
        at = pl.ds(pl.multiple_of(lax.rem(j, r // step) * step, step), step)
        value = tok[k, at, :].astype(f32)
        centred = value - jnp.mean(value, axis=-1, keepdims=True)
        spread = jnp.mean(centred * centred, axis=-1, keepdims=True)
        nrm[k, at, :] = (centred * lax.rsqrt(spread + 1e-05) * gain[...] + bias[...]).astype(bf)
        return 0

    lax.fori_loop(0, TP * r // step, norm, 0, unroll=4)
    finish(parts)


def third_exchange(wv, ws, gu, tok, gain, bias, cid):
    outs = (
        SDS((TP, wv.shape[0], 2 * wv.shape[1] // TP), bf),
        SDS(gu.shape, bf),
        SDS(tok.shape, bf),
    )
    return exchange_call(
        third_kernel, outs, (wv, ws, gu, tok, gain, bias), 21, 3, cid,
        out_specs=(ANY, ANY, VMEM), vmem=32 << 20,
    )


def fourth_kernel(
    n, cot, qko, nrm, cosine, sine, mask, cot_out, o_out, q_out, k_out, sco, w, ssem, rsem, local
):
    me, peer = place()
    t = lax.rem(me, TP)
    meet([peer(k) for k in range(1, TP)])
    sems = (ssem, rsem)
    share, cols = n // TP, o_out.shape[4]
    _, r, kh = q_out.shape
    half = kh // 2
    weights = pltpu.make_async_copy(qko.at[:, :, pl.ds(0, 2 * kh)], w, local.at[3])
    weights.start()
    gather = Gather(cot, cot_out, 0, cot.shape[0], sems, 0, local.at[0], peer)
    gather.start()
    copies, keeps = [], []

    def part(p, which):
        return qko.at[pl.ds(p * share, share), :, pl.ds(2 * kh + which * cols, cols)]

    for which in (0, 1):
        for k in range(1, TP):
            dev = peer(k)
            copy = remote(
                part(lax.rem(dev, TP), which), o_out.at[t, :, which], sems,
                GATHER_SEMS + which * TP + k, dev,
            )
            copy.start()
            copies.append(copy)
        keep = pltpu.make_async_copy(part(t, which), o_out.at[t, :, which], local.at[1 + which])
        keep.start()
        keeps.append(keep)
    weights.wait()

    def products(pairs):
        @pl.loop(*pairs)
        def _(j):
            rows = nrm[pl.ds(2 * j, 2)].reshape(2 * r, nrm.shape[2])
            for at, out in ((0, q_out), (kh, k_out)):
                y = jnp.dot(
                    rows, w[:, :, at : at + kh].reshape(nrm.shape[2], kh),
                    preferred_element_type=f32,
                )
                for i in (0, 1):
                    u, v = y[i * r : (i + 1) * r, :half], y[i * r : (i + 1) * r, half:]
                    cos, sin = cosine[2 * j + i], sine[2 * j + i]
                    out[2 * j + i, :, :half] = (u * cos - v * sin).astype(bf)
                    out[2 * j + i, :, half:] = (v * cos + u * sin).astype(bf)
            for i in (0, 1):
                plain = lax.dot_general(
                    q_out[2 * j + i], k_out[2 * j + i], (((1,), (1,)), ((), ())),
                    preferred_element_type=f32,
                )
                sco[2 * j + i] = (plain * mask[2 * j + i]).astype(bf)

    products((0, TP // 2))
    gather.forward()
    gather.finish()
    for copy in copies:
        copy.wait()
    for keep in keeps:
        keep.wait()


def fourth_exchange(n, cot, qko, nrm, cosine, sine, mask, cid):
    _, shard, width = qko.shape
    cols = (width - 2 * KH) // 2
    r = cot.shape[0]
    outs = (
        SDS((TP,) + cot.shape, bf),
        SDS((TP, n // TP, 2, shard, cols), bf),
        SDS((TP, r, KH), bf),
        SDS((TP, r, KH), bf),
        SDS(mask.shape, bf),
        SDS((n, shard, 2 * KH), bf),
    )
    kernel = functools.partial(fourth_kernel, n)
    return exchange_call(
        kernel, outs, (cot, qko, nrm, cosine, sine, mask),
        GATHER_SEMS + 2 * TP, 4, cid,
        specs=[VMEM, ANY, VMEM, VMEM, VMEM, VMEM],
        out_specs=(ANY, ANY, VMEM, VMEM, VMEM, VMEM), vmem=40 << 20,
    )


REDUCE_SEMS = 16
WIDE = 1024


class Reduce:
    def __init__(self, product, bufs, sems, base, peer, prepare=None, enter=None):
        self.product, self.prepare, self.sems, self.base = product, prepare, sems, base
        self.enter = enter
        self.po, self.pe, self.rc, self.sb, self.ring = bufs
        self.pc = peer(1)
        px, py = peer(2), peer(4)
        self.slots = ((0, 0, px), (1, 0, py), (0, 1, px), (1, 1, py), (1, 2, py), (0, 2, px))
        self.q = self.pe.shape[1] // 4
        self.waiting = True

    def core(self, i):
        return remote(self.po.at[i], self.rc.at[i], self.sems, self.base + i, self.pc)

    def link(self, c, slot):
        axis, at, dev = self.slots[slot]
        return remote(
            self.sb.at[c, slot], self.ring.at[axis, c, at], self.sems,
            self.base + 4 + 6 * c + slot, dev,
        )

    def add(self, halves, i, lower, out, more=None):
        step = 16
        steps = self.q // step
        first, count = halves

        @pl.loop(first * steps, (first + count) * steps)
        def _(j):
            c = lax.div(j, steps)
            there = pl.ds(pl.multiple_of(lax.rem(j, steps) * step, step), step)
            here = pl.ds(
                pl.multiple_of(lax.rem(j, steps) * step + (2 * c + lower) * self.q, step), step
            )
            total = self.pe[i, here, :].astype(f32) + self.rc[i, here, :].astype(f32)
            if more is not None:
                total = total + self.ring[more, c, 0, there, :].astype(f32)
            self.sb[c, out, there, :] = total.astype(bf)

    def both(self, slot, i, lower):
        self.add((0, 2), i, lower, slot)
        for c in (0, 1):
            self.link(c, slot).start()

    def six(self):
        self.core(3).wait_recv()
        self.both(0, 3, 0)
        self.both(1, 3, 1)

    def two(self):
        self.core(1).wait_recv()
        self.both(2, 1, 0)

    def four(self):
        self.core(2).wait_recv()
        self.both(3, 2, 1)

    def onward(self, c):
        self.link(c, 0).wait_recv()
        self.add((c, 1), 2, 0, 4, 0)
        self.link(c, 4).start()
        self.link(c, 1).wait_recv()
        self.add((c, 1), 1, 1, 5, 1)
        self.link(c, 5).start()

    def pair(self, it, i):
        self.product(it, i, self.po.at[i], self.pe.at[i])
        self.core(i).start()

    def run(self):
        if self.enter is not None:
            self.enter()

        @pl.loop(0, 4)
        def _(it):
            i = pair_at(it)
            if self.prepare is not None:
                self.prepare(it, i)
            else:
                self.pair(it, i)
            for k, stage in ((1, self.six), (2, self.two), (3, self.four)):
                pl.when(it == k)(stage)
            if self.prepare is not None:
                self.pair(it, i)

        for c in (0, 1):
            self.onward(c)

    def rows(self, c, step, body, unroll=2):
        if c == 0:
            self.core(0).wait_recv()
        for slot in (2, 3, 4, 5):
            self.link(c, slot).wait_recv()
        steps = self.q // step

        def some(j, _):
            lower = lax.div(j, steps)
            there = pl.ds(pl.multiple_of(lax.rem(j, steps) * step, step), step)
            here = pl.ds(pl.multiple_of(j * step + 2 * c * self.q, step), step)
            body(
                here,
                self.pe[0, here, :].astype(f32)
                + self.rc[0, here, :].astype(f32)
                + self.ring[lower, c, 1, there, :].astype(f32)
                + self.ring[1 - lower, c, 2, there, :].astype(f32),
            )
            return 0

        lax.fori_loop(0, 2 * steps, some, 0, unroll=unroll)

    def core_sent(self):
        for i in range(4):
            self.core(i).wait_send()
        self.waiting = False

    def finish(self):
        if self.waiting:
            self.core_sent()
        for c in (0, 1):
            for slot in range(6):
                self.link(c, slot).wait_send()


def pair_at(it):
    return it + 3 * (1 - lax.div(it + 2, 3)) - 3 * lax.div(it, 3)


class Load:
    def __init__(self, sems):
        self.sems, self.count = sems, 0

    def whole(self, src, dst):
        copy = pltpu.make_async_copy(src, dst, self.sems.at[self.count])
        self.count += 1
        copy.start()
        return copy.wait

    def paired(self, src, dst):
        base = self.count
        self.count += 4

        def piece(i):
            two = pl.ds(2 * i, 2)
            return pltpu.make_async_copy(src.at[two], dst.at[two], self.sems.at[base + i])

        return piece


def reduce_scratch(r, c, even=f32):
    q = r // 4
    return [
        pltpu.VMEM((4, r, c), bf),
        pltpu.VMEM((4, r, c), even),
        pltpu.VMEM((4, r, c), bf),
        pltpu.VMEM((2, 6, q, c), bf),
        pltpu.VMEM((2, 2, 3, q, c), bf),
    ]


def rows_of_pair(a, i):
    two, r, k = 2, a.shape[1], a.shape[2]
    return a[pl.ds(2 * i, two)].reshape(two * r, k)


def times(a, w, nt, arrive):
    def product(it, i, odd, even):
        r = a.shape[1]
        arrive(it, i)

        @pl.loop(0, even.shape[1] // WIDE)
        def _(j):
            at = pl.ds(pl.multiple_of(j * WIDE, WIDE), WIDE)
            x = rows_of_pair(a, i)
            if nt:
                y = lax.dot_general(
                    x, w[at, :], (((1,), (1,)), ((), ())), preferred_element_type=f32
                )
            else:
                y = jnp.dot(x, w[:, at], preferred_element_type=f32)
            even[:, at] = y[:r].astype(even.dtype)
            odd[:, at] = y[r:].astype(odd.dtype)

    return product


def exchange_and_gather(reduce, gathers, step, body, arrivals):
    reduce.run()
    for arrive in arrivals:
        arrive()
    for c in (0, 1):
        reduce.rows(c, step, body)
        gathers[c].start()
    for c in (0, 1):
        gathers[c].forward()
    for c in (0, 1):
        gathers[c].finish()
    reduce.finish()


def both_gathers(own, out, sems, local, peer):
    half = own.shape[0] // 2
    return [
        Gather(own, out, c * half, half, sems, REDUCE_SEMS + c * GATHER_SEMS, local.at[c], peer)
        for c in (0, 1)
    ]


EXCHANGE_SEMS = REDUCE_SEMS + 2 * GATHER_SEMS


def forward_kernel(
    nrm_in, wvs_in, sco, w_in, tok_in, vec, v_out, mix_out, ret_out, swi_out, mid, out,
    nrm, wvs, w, tok, v_buf, mix_buf, ret_buf, swi_buf, po, pe, rc, sb, ring, own,
    ssem, rsem, local, load,
):
    _, peer = place()
    enter = greet([peer(1), peer(2), peer(4)])
    sems = (ssem, rsem)
    r, width = v_buf.shape[1:]
    loads = Load(load)
    nrm_piece = loads.paired(nrm_in, nrm)
    nrm_piece(3).start()
    wvs_here = loads.whole(wvs_in, wvs)
    w_here = loads.whole(w_in, w)
    for i in (1, 2, 0):
        nrm_piece(i).start()
    tok_here = loads.whole(tok_in, tok)
    kept = ((v_buf, v_out), (mix_buf, mix_out), (ret_buf, ret_out), (swi_buf, swi_out))

    def keep(i):
        two = pl.ds(2 * i, 2)
        return [
            pltpu.make_async_copy(src.at[two], dst.at[two], local.at[2 + 4 * i + j])
            for j, (src, dst) in enumerate(kept)
        ]

    def prepare(it, i):
        first = 2 * i
        two = pl.ds(first, 2)
        pl.when(it == 0)(wvs_here)
        nrm_piece(i).wait()
        x = nrm[two].reshape(2 * r, nrm.shape[2])
        v = jnp.dot(x, wvs[:, :width], preferred_element_type=f32).astype(bf)
        v_buf[two] = v.reshape(2, r, width)
        for k in (0, 1):
            ret_buf[first + k] = jnp.dot(
                sco[first + k], v[k * r : (k + 1) * r], preferred_element_type=f32
            )
        s = jnp.dot(x, wvs[:, width:], preferred_element_type=f32)
        swi_buf[two] = s.reshape(2, r, width)

        def gated(j, _):
            k = first + lax.div(j, r // 32)
            at = pl.ds(pl.multiple_of(lax.rem(j, r // 32) * 32, 32), 32)
            value = ret_buf[k, at, :]
            centred = value - jnp.mean(value, axis=-1, keepdims=True)
            spread = jnp.mean(centred * centred, axis=-1, keepdims=True)
            gate = swi_buf[k, at, :]
            gate = gate / (1.0 + jnp.exp(-gate))
            mix_buf[k, at, :] = (
                gate * (centred * lax.rsqrt(jnp.maximum(spread, 0.25)))
            ).astype(bf)
            return 0

        lax.fori_loop(0, 2 * r // 32, gated, 0, unroll=4)
        for copy in keep(i):
            copy.start()

    def product(it, i, odd, even):
        step = w.shape[2]
        pl.when(it == 0)(w_here)

        def columns(j, _):
            at = pl.ds(pl.multiple_of(j * step, step), step)
            y = jnp.dot(rows_of_pair(mix_buf, i), w[j], preferred_element_type=f32)
            even[:, at] = y[:r].astype(even.dtype)
            odd[:, at] = y[r:].astype(odd.dtype)
            return 0

        lax.fori_loop(0, w.shape[0], columns, 0, unroll=2)

    def body(at, value):
        value = value + tok[at, :].astype(f32)
        mid[at, :] = value
        center = jnp.mean(value, axis=-1, keepdims=True)
        centred = value - center
        spread = jnp.mean(centred * centred, axis=-1, keepdims=True)
        own[at, :] = (
            centred * lax.rsqrt(spread + 1e-05) * vec[0:1, :] + vec[1:2, :]
        ).astype(bf)

    reduce = Reduce(product, (po, pe, rc, sb, ring), sems, 0, peer, prepare, enter)
    exchange_and_gather(reduce, both_gathers(own, out, sems, local, peer), 16, body, (tok_here,))
    for i in range(4):
        for copy in keep(i):
            copy.wait()


def forward_exchange(nrm, wvs, sco, w, tok, vec, cid):
    _, r, d = nrm.shape
    width = w.shape[1]
    count = EXCHANGE_SEMS
    blocks = [((TP, r, width), t) for t in (bf, bf, f32, f32)]
    return pl.pallas_call(
        forward_kernel,
        out_shape=tuple(SDS(*b) for b in blocks) + (SDS((r, d), f32), SDS((TP, r, d), bf)),
        in_specs=[ANY, ANY, VMEM, ANY, ANY, VMEM],
        out_specs=(ANY,) * 4 + (VMEM, ANY),
        scratch_shapes=[pltpu.VMEM(x.shape, x.dtype) for x in (nrm, wvs, w, tok)]
        + [pltpu.VMEM(*b) for b in blocks]
        + reduce_scratch(r, d)
        + [
            pltpu.VMEM((r, d), bf),
            pltpu.SemaphoreType.DMA((count,)),
            pltpu.SemaphoreType.DMA((count,)),
            pltpu.SemaphoreType.DMA((18,)),
            pltpu.SemaphoreType.DMA((7,)),
        ],
        compiler_params=pltpu.CompilerParams(
            collective_id=cid, has_side_effects=True, vmem_limit_bytes=60 << 20
        ),
        name="forward_exchange",
    )(nrm, wvs, sco, w, tok, vec)


def product_kernel(a, b, out):
    a, b = a[...].reshape(-1, a.shape[-1]), b[...].reshape(-1, b.shape[-1])
    out[...] = lax.dot_general(
        a, b, (((0,), (0,)), ((), ())), preferred_element_type=f32
    ).astype(bf)


def row_product(a, b):
    _, r, m = a.shape
    width = b.shape[2]
    tile, part = 512 if m >= 2048 else 256, min(width, 1024)
    return pl.pallas_call(
        product_kernel,
        grid=(width // part, m // tile),
        out_shape=SDS((m, width), bf),
        in_specs=[
            pl.BlockSpec((TP, r, tile), lambda j, i: (0, 0, i)),
            pl.BlockSpec((TP, r, part), lambda j, i: (0, 0, j)),
        ],
        out_specs=pl.BlockSpec((tile, part), lambda j, i: (i, j)),
        compiler_params=pltpu.CompilerParams(vmem_limit_bytes=56 << 20),
        cost_estimate=pl.CostEstimate(
            flops=2 * TP * r * m * width,
            bytes_accessed=2 * (a.size + b.size + m * width),
            transcendentals=0,
        ),
        name="row_product",
    )(a, b)


def hidden_kernel(x, gu, hid, act_out, slope_out):
    width = hid.shape[2]
    step = 256

    @pl.loop(0, width // step)
    def _(j):
        at = pl.ds(pl.multiple_of(j * step, step), step)
        behind = pl.ds(pl.multiple_of(j * step + width, step), step)
        rows = x[...].reshape(-1, x.shape[2])
        first = jnp.dot(rows, gu[:, at], preferred_element_type=f32)
        second = jnp.dot(rows, gu[:, behind], preferred_element_type=f32)
        share = 0.5 * (1.0 + lax.erf(first * math.sqrt(0.5)))
        act = first * share
        slope = share + first * (jnp.exp(-0.5 * first * first) * (1.0 / math.sqrt(2.0 * math.pi)))
        block = hid.shape[:2] + (step,)
        hid[:, :, at] = (act * second).astype(bf).reshape(block)
        act_out[:, :, at] = act.reshape(block)
        slope_out[:, :, at] = (slope * second).reshape(block)


def hidden_units(x, gu):
    _, r, d = x.shape
    width = gu.shape[1] // 2
    row = pl.BlockSpec((2, r, width), lambda k: (k, 0, 0))
    return pl.pallas_call(
        hidden_kernel,
        grid=(TP // 2,),
        out_shape=tuple(SDS((TP, r, width), t) for t in (bf, f32, f32)),
        in_specs=[
            pl.BlockSpec((2, r, d), lambda k: (k, 0, 0)),
            pl.BlockSpec(gu.shape, lambda k: (0, 0)),
        ],
        out_specs=(row, row, row),
        compiler_params=pltpu.CompilerParams(vmem_limit_bytes=56 << 20),
        cost_estimate=pl.CostEstimate(
            flops=4 * TP * r * d * width, bytes_accessed=24 << 20, transcendentals=2 * TP * r * width
        ),
        name="hidden_units",
    )(x, gu)


def hidden_back_kernel(cot, d0, d1, act, slope, out, down):
    width = act.shape[2]
    step = 512
    early, rows = d0.shape[1], d0.shape[1] + d1.shape[1]

    @pl.when(pl.program_id(0) == 0)
    def _():
        for g in range(d0.shape[0]):
            down[g * rows : g * rows + early] = d0[g]
            down[g * rows + early : (g + 1) * rows] = d1[g]

    @pl.loop(0, width // step)
    def _(j):
        at = pl.ds(pl.multiple_of(j * step, step), step)
        behind = pl.ds(pl.multiple_of(j * step + width, step), step)
        grad = lax.dot_general(
            cot[...].reshape(-1, cot.shape[2]), down[at, :], (((1,), (1,)), ((), ())),
            preferred_element_type=f32,
        ).reshape(act.shape[:2] + (step,))
        out[:, :, at] = (grad * slope[:, :, at]).astype(bf)
        out[:, :, behind] = (grad * act[:, :, at]).astype(bf)


def hidden_back(cot, d0, d1, act, slope):
    _, r, d = cot.shape
    width = act.shape[2]
    row = pl.BlockSpec((2, r, width), lambda k: (k, 0, 0))
    return pl.pallas_call(
        hidden_back_kernel,
        grid=(TP // 2,),
        out_shape=SDS((TP, r, 2 * width), bf),
        in_specs=[
            pl.BlockSpec((2, r, d), lambda k: (k, 0, 0)),
            pl.BlockSpec(d0.shape, lambda k: (0, 0, 0)),
            pl.BlockSpec(d1.shape, lambda k: (0, 0, 0)),
            row,
            row,
        ],
        scratch_shapes=[pltpu.VMEM((width, d), bf)],
        out_specs=pl.BlockSpec((2, r, 2 * width), lambda k: (k, 0, 0)),
        compiler_params=pltpu.CompilerParams(vmem_limit_bytes=56 << 20),
        cost_estimate=pl.CostEstimate(
            flops=2 * TP * r * d * width, bytes_accessed=24 << 20, transcendentals=0
        ),
        name="hidden_back",
    )(cot, d0, d1, act, slope)


def backward_kernel(
    a_in, w_in, mid_in, cot_in, vec, gmid, out, sums,
    a, w, mid, cot, po, pe, rc, sb, ring, own, acc, ssem, rsem, local, load,
):
    _, peer = place()
    enter = greet([peer(1), peer(2), peer(4)])
    sems = (ssem, rsem)
    loads = Load(load)
    piece = loads.paired(a_in, a)
    piece(3).start()
    w_here = loads.whole(w_in, w)
    for i in (1, 2, 0):
        piece(i).start()
    arrivals = (loads.whole(mid_in, mid), loads.whole(cot_in, cot))

    def arrive(it, i):
        pl.when(it == 0)(w_here)
        piece(i).wait()

    acc[...] = jnp.zeros_like(acc)

    def body(at, g):
        value = mid[at, :]
        center = jnp.mean(value, axis=-1, keepdims=True)
        centred = value - center
        inv = lax.rsqrt(jnp.mean(centred * centred, axis=-1, keepdims=True) + 1e-05)
        hat = centred * inv
        acc[0] += g * hat
        acc[1] += g
        scaled = g * vec[0:1, :]
        mean_g = jnp.mean(scaled, axis=-1, keepdims=True)
        mean_gh = jnp.mean(scaled * hat, axis=-1, keepdims=True)
        grad = cot[at, :].astype(f32) + inv * (scaled - mean_g - hat * mean_gh)
        gmid[at, :] = grad
        own[at, :] = grad.astype(bf)

    reduce = Reduce(
        times(a, w, True, arrive), (po, pe, rc, sb, ring), sems, 0, peer, enter=enter
    )
    exchange_and_gather(reduce, both_gathers(own, out, sems, local, peer), 16, body, arrivals)
    sums[0:1, :] = jnp.sum(acc[0], axis=0, keepdims=True)
    sums[1:2, :] = jnp.sum(acc[1], axis=0, keepdims=True)


def backward_exchange(a, w, mid, cot, vec, cid):
    _, r, _ = a.shape
    c = w.shape[0]
    count = EXCHANGE_SEMS
    return pl.pallas_call(
        backward_kernel,
        out_shape=(SDS((r, c), f32), SDS((TP, r, c), bf), SDS((2, c), f32)),
        in_specs=[ANY] * 4 + [VMEM],
        out_specs=(VMEM, ANY, VMEM),
        scratch_shapes=[pltpu.VMEM(x.shape, x.dtype) for x in (a, w, mid, cot)]
        + reduce_scratch(r, c)
        + [
            pltpu.VMEM((r, c), bf),
            pltpu.VMEM((2, 16, c), f32),
            pltpu.SemaphoreType.DMA((count,)),
            pltpu.SemaphoreType.DMA((count,)),
            pltpu.SemaphoreType.DMA((2,)),
            pltpu.SemaphoreType.DMA((7,)),
        ],
        compiler_params=pltpu.CompilerParams(
            collective_id=cid, has_side_effects=True, vmem_limit_bytes=52 << 20
        ),
        name="backward_exchange",
    )(a, w, mid, cot, vec)


def last_kernel(
    n, gqkv_in, gs_in, wqk_in, wvs_in, a2_in, d0, d1, tok_in, gain, sums2,
    gtok, ffn, vec_out, gqkv, gs, wqk, wvs, a2, w2, tok,
    po, pe, rc, sb, ring, pe2, rc2, sb2, ring2, acc, vecs, near, far, part, ssem, rsem, load,
):
    dp = n // TP
    me, peer = place()
    g = lax.div(me, TP)
    width = vec_out.shape[1]
    others = [lax.rem(me + TP * j, n) for j in range(1, dp)]
    enter = greet([peer(k) for k in range(1, TP)] + others)
    sems = (ssem, rsem)
    loads = Load(load)
    pieces = loads.paired(gqkv_in, gqkv), loads.paired(gs_in, gs)
    for piece in pieces:
        piece(3).start()
    weights = loads.whole(wqk_in, wqk), loads.whole(wvs_in, wvs)
    for i in (1, 2, 0):
        for piece in pieces:
            piece(i).start()
    second = [loads.whole(a2_in, a2)]
    early, rows = d0.shape[1], d0.shape[1] + d1.shape[1]
    for k in range(dp):
        second.append(loads.whole(d0.at[k], w2.at[pl.ds(k * rows, early)]))
        second.append(loads.whole(d1.at[k], w2.at[pl.ds(k * rows + early, rows - early)]))
    arrivals = (loads.whole(tok_in, tok),)

    def all_here(waits):
        def wait():
            for one in waits:
                one()

        return wait

    acc[...] = jnp.zeros_like(acc)
    nt = (((1,), (1,)), ((), ()))

    def product(it, i, odd, even):
        r, qk, v = gqkv.shape[1], wqk.shape[1], gs.shape[2]
        pl.when(it == 0)(all_here(weights))
        for piece in pieces:
            piece(i).wait()
        x, y = rows_of_pair(gqkv, i), rows_of_pair(gs, i)

        @pl.loop(0, even.shape[1] // WIDE)
        def _(j):
            at = pl.ds(pl.multiple_of(j * WIDE, WIDE), WIDE)
            z = lax.dot_general(x[:, :qk], wqk[at, :], nt, preferred_element_type=f32)
            z += lax.dot_general(x[:, qk:], wvs[at, :v], nt, preferred_element_type=f32)
            z += lax.dot_general(y, wvs[at, v:], nt, preferred_element_type=f32)
            even[:, at] = z[:r].astype(even.dtype)
            odd[:, at] = z[r:].astype(odd.dtype)

    one = Reduce(product, (po, pe, rc, sb, ring), sems, 0, peer, enter=enter)
    one.run()
    one.core_sent()

    def arrive(it, _):
        pl.when(it == 0)(all_here(second))

    two = Reduce(times(a2, w2, False, arrive), (po, pe2, rc2, sb2, ring2), sems, REDUCE_SEMS, peer)
    two.run()

    def body(at, grad):
        value = tok[at, :].astype(f32)
        center = jnp.mean(value, axis=-1, keepdims=True)
        centred = value - center
        inv = lax.rsqrt(jnp.mean(centred * centred, axis=-1, keepdims=True) + 1e-05)
        hat = centred * inv
        acc[0] += grad * hat
        acc[1] += grad
        scaled = grad * gain[...]
        mean_g = jnp.mean(scaled, axis=-1, keepdims=True)
        mean_gh = jnp.mean(scaled * hat, axis=-1, keepdims=True)
        gtok[at, :] = inv * (scaled - mean_g - hat * mean_gh)

    all_here(arrivals)()
    for c in (0, 1):
        one.rows(c, 16, body)
    vecs[...] = jnp.zeros_like(vecs)
    vecs[0:1, :] = jnp.sum(acc[0], axis=0, keepdims=True)
    vecs[1:2, :] = jnp.sum(acc[1], axis=0, keepdims=True)
    vecs[2:4, :] = sums2[...]
    base = 2 * REDUCE_SEMS
    copies = []
    for j, dev in enumerate(others):
        at = pl.multiple_of(lax.div(dev, TP) * width, 128)
        copy = remote(vecs.at[:, pl.ds(at, width)], far.at[j], sems, base + j, dev)
        copy.start()
        copies.append(copy)

    def keep(at, value):
        ffn[at, :] = value

    two.rows(0, 16, keep)
    total = vecs[:, pl.ds(pl.multiple_of(g * width, 128), width)]
    for j, copy in enumerate(copies):
        copy.wait()
        total = total + far[j]
    part[...] = total
    copies = []
    for k in range(1, TP):
        copy = remote(part, near.at[k - 1], sems, base + dp + k - 1, peer(k))
        copy.start()
        copies.append(copy)
    two.rows(1, 16, keep)
    for k, copy in enumerate(copies):
        copy.wait()
        total = total + near[k]
    vec_out[...] = total
    one.finish()
    two.finish()


def last_exchange(n, gqkv, gs, wqk, wvs, a2, d0, d1, tok, gain, sums2, cid):
    dp = n // TP
    _, r, _ = a2.shape
    c = d0.shape[2]
    width = c // dp
    count = 2 * REDUCE_SEMS + dp + TP
    return pl.pallas_call(
        functools.partial(last_kernel, n),
        out_shape=(SDS((r, c), f32), SDS((r, c), f32), SDS((8, width), f32)),
        in_specs=[ANY] * 8 + [VMEM] * 2,
        out_specs=(VMEM,) * 3,
        scratch_shapes=[
            pltpu.VMEM(x.shape, x.dtype)
            for x in (gqkv, gs, wqk, wvs, a2, SDS((a2.shape[2], c), bf), tok)
        ]
        + reduce_scratch(r, c)
        + reduce_scratch(r, c, bf)[1:]
        + [
            pltpu.VMEM((2, 16, c), f32),
            pltpu.VMEM((8, c), f32),
            pltpu.VMEM((TP - 1, 8, width), f32),
            pltpu.VMEM((dp, 8, width), f32),
            pltpu.VMEM((8, width), f32),
            pltpu.SemaphoreType.DMA((count,)),
            pltpu.SemaphoreType.DMA((count,)),
            pltpu.SemaphoreType.DMA((12 + 2 * dp,)),
        ],
        compiler_params=pltpu.CompilerParams(
            collective_id=cid, has_side_effects=True, vmem_limit_bytes=ALL_VMEM
        ),
        name="last_exchange",
    )(gqkv, gs, wqk, wvs, a2, d0, d1, tok, gain, sums2)


def gate_back_kernel(g_low, w, ret, swi, gret, gswi, whole):
    cols = w.shape[2]

    @pl.when(pl.program_id(0) == 0)
    def _():
        for j in range(w.shape[0]):
            whole[:, j * cols : (j + 1) * cols] = w[j]

    two, r, _ = gret.shape
    grads = lax.dot_general(
        g_low[...].reshape(two * r, g_low.shape[2]), whole[...], (((1,), (1,)), ((), ())),
        preferred_element_type=f32,
    )
    for i in range(two):
        grad, value, gate = grads[i * r : (i + 1) * r], ret[i], swi[i]
        centred = value - jnp.mean(value, axis=-1, keepdims=True)
        spread = jnp.mean(centred * centred, axis=-1, keepdims=True)
        inv = lax.rsqrt(jnp.maximum(spread, 0.25))
        share = 1.0 / (1.0 + jnp.exp(-gate))
        silu = gate * share
        gswi[i] = (grad * (centred * inv) * (share * (1.0 + gate * (1.0 - share)))).astype(bf)
        grad = grad * silu
        pull = jnp.mean(grad * centred, axis=-1, keepdims=True)
        pull = jnp.where(spread > 0.25, inv * inv * inv * pull, 0.0)
        grad = grad * inv - centred * pull
        gret[i] = (grad - jnp.mean(grad, axis=-1, keepdims=True)).astype(bf)


def gate_back(g_low, w, ret, swi):
    _, r, d = g_low.shape
    width = ret.shape[2]
    row = pl.BlockSpec((2, r, width), lambda k: (k, 0, 0))
    return pl.pallas_call(
        gate_back_kernel,
        grid=(TP // 2,),
        out_shape=(SDS(ret.shape, bf), SDS(ret.shape, bf)),
        in_specs=[
            pl.BlockSpec((2, r, d), lambda k: (k, 0, 0)),
            pl.BlockSpec(w.shape, lambda k: (0, 0, 0)),
            row,
            row,
        ],
        out_specs=(row, row),
        scratch_shapes=[pltpu.VMEM((width, d), bf)],
        compiler_params=pltpu.CompilerParams(vmem_limit_bytes=56 << 20),
        cost_estimate=pl.CostEstimate(
            flops=2 * TP * r * d * width, bytes_accessed=22 << 20, transcendentals=TP * r * width
        ),
        name="gate_back",
    )(g_low, w, ret, swi)


def scores_back_kernel(sco, mask, q, k, v, gret, cosine, sine, out):
    nt, tn = (((1,), (1,)), ((), ())), (((0,), (0,)), ((), ()))
    kh = q.shape[2]
    half = kh // 2
    out[0, :, 2 * kh :] = lax.dot_general(
        sco[0], gret[0], tn, preferred_element_type=f32
    ).astype(bf)
    grad = lax.dot_general(gret[0], v[0], nt, preferred_element_type=f32)
    grad = (grad * mask[0]).astype(bf)
    gq = jnp.dot(grad, k[0], preferred_element_type=f32)
    gk = lax.dot_general(grad, q[0], tn, preferred_element_type=f32)
    for i, g in enumerate((gq, gk)):
        u, w = g[:, :half], g[:, half:]
        at = i * kh
        out[0, :, at : at + half] = (u * cosine[0] + w * sine[0]).astype(bf)
        out[0, :, at + half : at + kh] = (w * cosine[0] - u * sine[0]).astype(bf)


def scores_back(sco, mask, q, k, v, gret, cosine, sine):
    _, r, kh = q.shape
    arrays = (sco, mask, q, k, v, gret, cosine, sine)
    width = 2 * kh + v.shape[2]
    spec = [pl.BlockSpec((1,) + x.shape[1:], lambda i: (i, 0, 0)) for x in arrays]
    return pl.pallas_call(
        scores_back_kernel,
        grid=(TP,),
        out_shape=SDS((TP, r, width), bf),
        in_specs=spec,
        out_specs=pl.BlockSpec((1, r, width), lambda i: (i, 0, 0)),
        compiler_params=pltpu.CompilerParams(vmem_limit_bytes=56 << 20),
        cost_estimate=pl.CostEstimate(
            flops=4 * TP * r * r * (kh + v.shape[2]), bytes_accessed=16 << 20, transcendentals=0
        ),
        name="scores_back",
    )(*arrays)


def spread_kernel(a_in, b_in, out, a, b, turned, made, ssem, rsem, local, load):
    me, peer = place()
    t = lax.rem(me, TP)
    place_of, low = lax.div(t, 2), lax.rem(t, 2)
    sems = (ssem, rsem)
    enter = greet([peer(k) for k in range(1, TP)])
    rows, tile = out.shape[1], 512
    tiles = out.shape[2] // tile

    def columns(j):
        return pl.ds(pl.multiple_of(j * tile, tile), tile)

    def piece(j):
        return pltpu.make_async_copy(
            b_in.at[:, :, columns(j)], b.at[:, :, columns(j)], load.at[1 + j]
        )

    def sends(j, act):
        for m in range(4):
            chunk = lax.rem(place_of + m, 4)
            dev = me - t + 4 * low + chunk
            src = made.at[pl.ds(pl.multiple_of(chunk * rows, rows), rows), columns(j)]
            dst = out.at[place_of, :, columns(j)]
            i = 4 * j + m
            away = remote(src, dst, sems, i, dev)
            here = pltpu.make_async_copy(src, dst, local.at[i])
            pl.when(dev != me)(getattr(away, act))
            pl.when(dev == me)(getattr(here, act))

    whole = pltpu.make_async_copy(a_in, a, load.at[0])
    whole.start()
    for j in range(tiles):
        piece(j).start()
    whole.wait()
    turned[...] = a[...].reshape(-1, a.shape[2]).T
    enter()

    @pl.loop(0, tiles)
    def _(j):
        piece(j).wait()
        made[:, columns(j)] = jnp.dot(
            turned[...], b[:, :, columns(j)].reshape(turned.shape[1], tile),
            preferred_element_type=f32,
        ).astype(bf)
        sends(j, "start")

    @pl.loop(0, tiles)
    def _(j):
        sends(j, "wait")


def spread_product(a, b, cid):
    _, r, m = a.shape
    width = b.shape[2]
    count = 4 * (width // 512)
    return pl.pallas_call(
        spread_kernel,
        out_shape=SDS((4, m // 4, width), bf),
        in_specs=[ANY, ANY],
        out_specs=ANY,
        scratch_shapes=[
            pltpu.VMEM(a.shape, bf),
            pltpu.VMEM(b.shape, bf),
            pltpu.VMEM((m, TP * r), bf),
            pltpu.VMEM((m, width), bf),
            pltpu.SemaphoreType.DMA((count,)),
            pltpu.SemaphoreType.DMA((count,)),
            pltpu.SemaphoreType.DMA((count,)),
            pltpu.SemaphoreType.DMA((1 + width // 512,)),
        ],
        compiler_params=pltpu.CompilerParams(
            collective_id=cid, has_side_effects=True, vmem_limit_bytes=ALL_VMEM
        ),
        name="spread_product",
    )(a, b)


def tp_groups(n):
    return [[g * TP + t for t in range(TP)] for g in range(n // TP)]


def dp_groups(n):
    return [[g * TP + t for g in range(n // TP)] for t in range(TP)]


def plane_a2a(x, n):
    return lax.all_to_all(x, AXIS, 0, 0, axis_index_groups=tp_groups(n), tiled=True)


def dp_gather(x, n):
    return lax.all_gather(x, AXIS, axis=0, tiled=True, axis_index_groups=dp_groups(n))


def dp_reduce(x, n):
    return lax.psum_scatter(
        x, AXIS, scatter_dimension=0, tiled=True, axis_index_groups=dp_groups(n)
    )


def seq_positions(lengths, rows):
    ends = jnp.cumsum(lengths, axis=1)
    starts = ends - lengths
    index = jnp.arange(rows, dtype=jnp.int32)
    segment = jnp.sum((index[None, :, None] >= ends[:, None, :]).astype(jnp.int32), axis=2)
    member = segment[:, :, None] == jnp.arange(lengths.shape[1], dtype=jnp.int32)
    offset = index[None, :] - jnp.sum(jnp.where(member, starts[:, None, :], 0), axis=2)
    return segment, offset


def rotary_tables(offset):
    half = KH // 2
    freq = jnp.exp(-math.log(10000.0) * jnp.arange(half, dtype=f32) / half)
    angle = offset.astype(f32)[..., None] * freq
    return jnp.cos(angle), jnp.sin(angle)


def decay_mask(segment, offset, head):
    diff = offset[:, :, None] - offset[:, None, :]
    valid = (segment[:, :, None] == segment[:, None, :]) & (diff >= 0)
    steps = jnp.where(valid, diff, 0).astype(f32)
    log = jnp.log(1.0 - jnp.exp2(-5.0 - head.astype(f32)))
    return jnp.where(valid, jnp.exp(log * steps), 0.0) / math.sqrt(KH)


def col_blocks(w):
    r, c = w.shape
    return w.reshape(r, TP, c // TP).transpose(1, 0, 2).reshape(TP * r, c // TP)


def join_kernel(widths, parts, x, *outs):
    at = 0
    for out, width, count in zip(outs, widths, parts):
        piece = width // count
        for t in range(TP):
            for p in range(count):
                to = (p * TP + t) * piece
                out[:, to : to + piece] = x[t, :, at + p * piece : at + (p + 1) * piece].astype(f32)
        at += width


def join(x, widths, parts):
    r = x.shape[1]
    if any(width // count % 128 for width, count in zip(widths, parts)):
        made, at = [], 0
        for width, count in zip(widths, parts):
            part = x[:, :, at : at + width].reshape(TP, r, count, width // count)
            made.append(part.transpose(1, 2, 0, 3).reshape(r, TP * width).astype(f32))
            at += width
        return made
    return pl.pallas_call(
        functools.partial(join_kernel, widths, parts),
        out_shape=tuple(SDS((r, TP * width), f32) for width in widths),
        in_specs=[VMEM],
        out_specs=tuple(VMEM for _ in widths),
        compiler_params=pltpu.CompilerParams(vmem_limit_bytes=10 << 20),
        cost_estimate=pl.CostEstimate(flops=0, bytes_accessed=6 * x.size, transcendentals=0),
        name="join",
    )(x)


def after(x, *deps):
    return lax.optimization_barrier((x,) + deps)[0]


def on_device(n, tokens, lengths, gain1, bias1, wq, wk, wv, ws, wo, gain2, bias2, wg, wu, wd, cot):
    rows, d = tokens.shape
    ff = wg.shape[1]
    dp = n // TP
    shard = d // n
    unit = ff // n
    me = lax.axis_index(AXIS)
    head = lax.rem(me, TP)

    def ff_blocks(w):
        return w.reshape(shard, dp, TP, unit).transpose(2, 0, 1, 3).reshape(TP, shard, dp * unit)

    lens = jnp.pad(lengths[0].astype(f32), (0, shard - lengths.shape[1]))
    vec = jnp.stack([v.astype(f32) for v in (gain1, bias1, gain2, bias2)] + [lens])
    vec = jnp.pad(vec, ((0, 3), (0, 128 - shard)))
    early = max(16, wd.shape[0] // 4)
    qko_blk, d0 = first_exchange(n, wq, wk, wo, wd, early, 1)
    qko = dp_gather(qko_blk.reshape(TP * shard, 4 * KH), n)
    tok_all, vec_all = second_exchange(n, after(tokens, qko_blk), vec, 2)
    gain1f, bias1f, gain2f, bias2f = (
        vec_all[:, :, i, :shard].reshape(1, d) for i in range(4)
    )
    vec2 = jnp.concatenate([gain2f, bias2f], axis=0)
    gu_in = jnp.concatenate([ff_blocks(wg), ff_blocks(wu)], axis=2)
    vs_blk, gu_blk, normed = third_exchange(wv, ws, gu_in, tok_all, gain1f, bias1f, 3)
    vs = dp_gather(vs_blk.reshape(TP * shard, 2 * VH), n)
    gu = dp_gather(gu_blk.reshape(TP * shard, 2 * dp * unit), n)
    down = d0, dp_gather(wd[early:], n).reshape(dp, wd.shape[0] - early, d)

    mine = lax.dynamic_slice_in_dim(vec_all, lax.div(me, TP), 1, 0)[0, :, 4, :3]
    order = jnp.arange(TP, dtype=jnp.int32)
    pick = (order[None, :] == (order[:, None] ^ head)).astype(f32)
    len_all = jnp.sum(pick[:, :, None] * mine[None], axis=1).astype(jnp.int32)
    segment, offset = seq_positions(len_all, rows)
    cosine, sine = rotary_tables(offset)
    mask = decay_mask(segment, offset, head)

    cot_all, out_blk, q_rot, k_rot, scores, qk = fourth_exchange(
        n, cot, qko.reshape(n, shard, 4 * KH), normed, cosine, sine, mask, 4
    )
    out_blk = out_blk.reshape(TP, VH, d // TP)
    qk = qk.reshape(d, 2 * KH)
    v_low, mixed, retained, swish_in, middle, normed2 = forward_exchange(
        normed, vs, scores, out_blk, tokens, vec2, 5
    )
    hidden, act, slope = hidden_units(normed2, gu)
    down_grad = row_product(hidden, cot_all)
    g_down = dp_reduce(down_grad, n)

    g_fs = hidden_back(cot_all, *down, act, slope)
    gu_grad = row_product(normed2, g_fs)
    g_gu = dp_reduce(gu_grad, n)
    g_middle, g_low, sums2 = backward_exchange(g_fs, gu, middle, cot, vec2, 6)

    g_retained, g_swish = gate_back(g_low, out_blk, retained, swish_in)
    swish_grad = row_product(normed, g_swish)
    g_swi = dp_reduce(swish_grad, n)
    spread = wo.shape[0] * HEADS == VH * 2
    if spread:
        out_grad = spread_product(mixed, g_low, 8).reshape(VH, d)
    else:
        out_grad = row_product(mixed, g_low)
        out_grad = plane_a2a(col_blocks(out_grad), n)
    g_qkv = scores_back(scores, mask, q_rot, k_rot, v_low, g_retained, cosine, sine)
    qkv_grad = row_product(normed, g_qkv)
    g_qkv_own = dp_reduce(qkv_grad, n)
    g_out = dp_reduce(out_grad, n)
    grad_part, ffn, g_vecs = last_exchange(
        n, g_qkv, g_swish, qk, vs, hidden, *down, tokens, gain1f, sums2, 7
    )
    grad_tokens = g_middle + grad_part
    layer_out = (middle + ffn).astype(bf)

    g_vecs = lax.dynamic_slice_in_dim(g_vecs, head * shard, shard, 1)
    grad_d = g_down.astype(f32)
    g_gs = plane_a2a(jnp.concatenate([g_gu, g_swi], axis=1), n)
    grad_g, grad_u, grad_s = join(
        g_gs.reshape(TP, shard, 2 * dp * unit + VH), (dp * unit, dp * unit, VH), (dp, dp, 1)
    )
    g_qkv_own = plane_a2a(g_qkv_own, n)
    grad_q, grad_k, grad_v = join(g_qkv_own.reshape(TP, shard, 2 * KH + VH), (KH, KH, VH), (1, 1, 1))
    if spread:
        grad_o = g_out.astype(f32)
    else:
        g_out = plane_a2a(g_out, n)
        (grad_o,) = join(g_out.reshape(TP, wo.shape[0], d // TP), (d // TP,), (1,))
    return (
        layer_out, grad_tokens, g_vecs[0], g_vecs[1], grad_q, grad_k, grad_v, grad_s, grad_o,
        g_vecs[2], g_vecs[3], grad_g, grad_u, grad_d,
    )


def solution(mesh):
    n = mesh.shape[AXIS]
    row, vec = P(AXIS, None), P(AXIS)
    ins = (row, row, vec, vec, row, row, row, row, row, vec, vec, row, row, row, row)
    outs = (row, row, vec, vec, row, row, row, row, row, vec, vec, row, row, row)

    def body(*args):
        return on_device(n, *args)

    return jax.shard_map(body, mesh=mesh, in_specs=ins, out_specs=outs, check_vma=False)
```
